32 devices in a mesh: lat: 16 (over z, y, x), batch: 2 (over core).
Axes of the slice: x: 2, y: 2, z: 4, core: 2. Of those that a mesh axis runs over, the one named last changes fastest.
Arguments:
- fields: bfloat16 [2, 192, 384, 384], P('batch', 'lat'), may hold values from -6 to 6
- cotangent: bfloat16 [2, 192, 384, 384], P('batch', 'lat'), may hold values from -6 to 6
- weights: bfloat16 [128, 2, 384, 384], P('lat'), may hold values from -0.21875 to 0.21875
- degree_of: int32 [128], replicated, may hold values from 0 to 127, each once
Outputs:
- grad_fields: bfloat16 [2, 192, 384, 384], P('batch', 'lat')
- grad_weights: bfloat16 [128, 2, 384, 384], P('lat')
The draws below stay inside these ranges and needn't reach their ends.
Inputs may be any that keep to these rules, and one draw needn't show every extreme that they name: `degree_of`: each degree 0 to 127 is held by exactly one slot.
All inputs are finite; a program needn't handle non-finite values.
Results may differ from the reference program's by a relative error of at most 0.018.
Values may be sent and summed in bfloat16 or wider, within the bound.
A program may use at most 64 MiB of HBM per device.

```python
import jax
import jax.numpy as jnp
from jax import lax

LATS = 192
LONS = 384
ORDERS = 128
DEGREES = 128
CHANNELS = 384
BATCH = 2


def shard_levels(key, extent, split, least, largest):
    loudness = 1.0
    for axis_at, blocks in split:
        draws = jax.random.uniform(jax.random.fold_in(jax.random.fold_in(key, 6), axis_at), (blocks,), jnp.float32, least / len(split), largest / len(split))
        loudness = loudness * jnp.repeat(jnp.exp(draws), extent[axis_at] // blocks).reshape((-1,) + (1,) * (len(extent) - 1 - axis_at))
    return loudness


def normal_values(own_key, dims, spread, limit, split=(), held_as=jnp.bfloat16):
    values = spread * jax.random.normal(own_key, dims, jnp.float32)
    if split:
        values = values * shard_levels(own_key, dims, split, -0.22, 0.18)
    return jnp.clip(values, -limit, limit).astype(held_as)


def setup_inputs(seed: int = 0) -> dict:
    keys = jax.random.split(jax.random.key(seed), 5)
    return {
        "fields": normal_values(keys[0], (BATCH, LATS, LONS, CHANNELS), 1.0, 6.0, ((0, 2), (1, 16))),
        "cotangent": normal_values(keys[1], (BATCH, LATS, LONS, CHANNELS), 1.0, 6.0, ((0, 2), (1, 16))),
        "weights": normal_values(keys[2], (DEGREES, 2, CHANNELS, CHANNELS), (2 * CHANNELS) ** -0.5, 0.21875, ((0, 16),)),
        "degree_of": jax.random.permutation(keys[3], DEGREES).astype(jnp.int32),
    }


def legendre_table(order_ids, lat_count, degree_count):
    colatitude = jnp.pi * (jnp.arange(lat_count, dtype=jnp.float32) + 0.5) / lat_count
    cosine = jnp.cos(colatitude)[None, :]
    log_sine = jnp.log(jnp.sin(colatitude))[None, :]
    order_col = order_ids.astype(jnp.int32)[:, None]
    order_real = order_col.astype(jnp.float32)
    steps_up = jnp.arange(1, degree_count + 1, dtype=jnp.float32)[None, :]
    factor = jnp.where(steps_up <= order_real, 0.5 * jnp.log((2.0 * steps_up + 1.0) / (2.0 * steps_up)), 0.0)
    log_start = 0.5 * jnp.log(1.0 / (4.0 * jnp.pi)) + lax.optimization_barrier(jnp.sum(factor, axis=1, keepdims=True))
    diagonal = jnp.exp(log_start + order_real * log_sine)
    squared = order_real * order_real

    def advance(carry, degree):
        previous, older = carry
        degree_real = degree.astype(jnp.float32)
        lead = jnp.sqrt(jnp.maximum(4.0 * degree_real * degree_real - 1.0, 0.0) / jnp.maximum(degree_real * degree_real - squared, 1.0))
        lower = degree_real - 1.0
        back = jnp.sqrt(jnp.maximum(lower * lower - squared, 0.0) / jnp.maximum(4.0 * lower * lower - 1.0, 1.0))
        general = lead * (cosine * previous - back * older)
        first = jnp.sqrt(2.0 * order_real + 3.0) * cosine * previous
        value = jnp.where(degree == order_col, diagonal, jnp.where(degree == order_col + 1, first, jnp.where(degree > order_col + 1, general, 0.0)))
        return ((value, previous), value)
    zeros = jnp.zeros((order_ids.shape[0], lat_count), jnp.float32)
    final_state, table = lax.scan(advance, (zeros, zeros), jnp.arange(degree_count, dtype=jnp.int32))
    return jnp.transpose(table, (1, 0, 2))

def spectral_tables(order_ids, degree_of, lat_count, degree_count):
    table = legendre_table(order_ids, lat_count, degree_count)
    chosen = jnp.take(table, degree_of.astype(jnp.int32), axis=1)
    colatitude = jnp.pi * (jnp.arange(lat_count, dtype=jnp.float32) + 0.5) / lat_count
    quadrature = 2.0 * jnp.pi * jnp.pi / lat_count * jnp.sin(colatitude)
    return ((chosen * quadrature[None, None, :]).astype(jnp.bfloat16), chosen.astype(jnp.bfloat16))

def fourier_tables(lon_count, order_count):
    lon_ids = jnp.arange(lon_count, dtype=jnp.int32)[:, None]
    order_ids = jnp.arange(order_count, dtype=jnp.int32)[None, :]
    phase = 2.0 * jnp.pi * (lon_ids * order_ids % lon_count).astype(jnp.float32) / lon_count
    forward = jnp.stack([jnp.cos(phase), -jnp.sin(phase)], axis=2).reshape(lon_count, 2 * order_count) / lon_count
    doubled = jnp.where(order_ids == 0, 1.0, 2.0)
    inverse = jnp.stack([doubled * jnp.cos(phase), -doubled * jnp.sin(phase)], axis=2).reshape(lon_count, 2 * order_count)
    return (forward.astype(jnp.bfloat16), jnp.transpose(inverse).astype(jnp.bfloat16))

def as_real(values):
    return values.astype(jnp.float32)

def sample_pass(field, cotangent, weights, forward, inverse, qslot, pslot):
    w_real = as_real(weights[:, 0])
    w_imag = as_real(weights[:, 1])
    spectra = jnp.einsum('ikc,kf->ifc', as_real(field), as_real(forward)).astype(jnp.bfloat16)
    spectra = spectra.reshape(LATS, ORDERS, 2, CHANNELS)
    coeffs = jnp.einsum('mji,imrc->jmrc', as_real(qslot), as_real(spectra)).astype(jnp.bfloat16)
    c_real = as_real(coeffs[:, :, 0])
    c_imag = as_real(coeffs[:, :, 1])
    f_real = jnp.einsum('jmc,jcd->jmd', c_real, w_real) - jnp.einsum('jmc,jcd->jmd', c_imag, w_imag)
    f_imag = jnp.einsum('jmc,jcd->jmd', c_real, w_imag) + jnp.einsum('jmc,jcd->jmd', c_imag, w_real)
    filtered = jnp.stack([f_real, f_imag], axis=2).astype(jnp.bfloat16)
    synth = jnp.einsum('mji,jmrc->imrc', as_real(pslot), as_real(filtered)).astype(jnp.bfloat16)
    response = jnp.einsum('ifc,fk->ikc', as_real(synth.reshape(LATS, 2 * ORDERS, CHANNELS)), as_real(inverse))
    activated, pullback = jax.vjp(jax.nn.gelu, response)
    upstream = pullback(as_real(cotangent))[0].astype(jnp.bfloat16)
    grad_synth = jnp.einsum('ikc,fk->ifc', as_real(upstream), as_real(inverse)).astype(jnp.bfloat16)
    grad_synth = grad_synth.reshape(LATS, ORDERS, 2, CHANNELS)
    grad_filtered = jnp.einsum('mji,imrc->jmrc', as_real(pslot), as_real(grad_synth)).astype(jnp.bfloat16)
    g_real = as_real(grad_filtered[:, :, 0])
    g_imag = as_real(grad_filtered[:, :, 1])
    dw_real = jnp.einsum('jmc,jmd->jcd', c_real, g_real) + jnp.einsum('jmc,jmd->jcd', c_imag, g_imag)
    dw_imag = jnp.einsum('jmc,jmd->jcd', c_real, g_imag) - jnp.einsum('jmc,jmd->jcd', c_imag, g_real)
    a_real = jnp.einsum('jmd,jcd->jmc', g_real, w_real) + jnp.einsum('jmd,jcd->jmc', g_imag, w_imag)
    a_imag = jnp.einsum('jmd,jcd->jmc', g_imag, w_real) - jnp.einsum('jmd,jcd->jmc', g_real, w_imag)
    grad_coeffs = jnp.stack([a_real, a_imag], axis=2).astype(jnp.bfloat16)
    grad_spectra = jnp.einsum('mji,jmrc->imrc', as_real(qslot), as_real(grad_coeffs)).astype(jnp.bfloat16)
    delta = jnp.einsum('ifc,kf->ikc', as_real(grad_spectra.reshape(LATS, 2 * ORDERS, CHANNELS)), as_real(forward))
    grad_field = (as_real(cotangent) + delta).astype(jnp.bfloat16)
    return (grad_field, jnp.stack([dw_real, dw_imag], axis=1))

def reference(fields, cotangent, weights, degree_of):
    forward, inverse = fourier_tables(LONS, ORDERS)
    qslot, pslot = spectral_tables(jnp.arange(ORDERS, dtype=jnp.int32), degree_of, LATS, DEGREES)

    def one_sample(total, pair):
        grad_field, weight_part = sample_pass(pair[0], pair[1], weights, forward, inverse, qslot, pslot)
        return (total + weight_part, grad_field)
    start = jnp.zeros((DEGREES, 2, CHANNELS, CHANNELS), jnp.float32)
    total, grad_fields = lax.scan(one_sample, start, (fields, cotangent))
    return (grad_fields, total.astype(jnp.bfloat16))
```

```python
import functools

import jax
import numpy as np
import jax.numpy as jnp
from jax import lax
from jax.experimental import pallas as pl
from jax.experimental.pallas import tpu as pltpu
from jax.sharding import PartitionSpec as P

LATS = 192
LONS = 384
ORDERS = 128
DEGREES = 128
CHANNELS = 384
LANES = 128
GROUP = 8


def table_kernel(deg_ref, diag_ref, cos_ref, quad_ref, order_ref, q_ref, p_ref, slot_ref, rows_ref):
    orders = diag_ref.shape[0]
    lats = q_ref.shape[2]
    degrees = deg_ref.shape[0]

    def invert(slot, carry):
        slot_ref[deg_ref[slot]] = slot
        return carry

    lax.fori_loop(0, degrees, invert, 0)
    order_real = order_ref[...]
    squared = order_real * order_real
    diagonal = diag_ref[...]
    cosine = cos_ref[...]
    first_lead = jnp.sqrt(2.0 * order_real + 3.0)
    halves = rows_ref.shape[0]

    def advance(degree, carry):
        previous, older = carry
        degree_real = degree.astype(jnp.float32)
        lead = jnp.sqrt(
            jnp.maximum(4.0 * degree_real * degree_real - 1.0, 0.0)
            / jnp.maximum(degree_real * degree_real - squared, 1.0)
        )
        lower = degree_real - 1.0
        back = jnp.sqrt(
            jnp.maximum(lower * lower - squared, 0.0) / jnp.maximum(4.0 * lower * lower - 1.0, 1.0)
        )
        general = lead * (cosine * previous - back * older)
        first = first_lead * cosine * previous
        value = jnp.where(
            degree_real == order_real,
            diagonal,
            jnp.where(
                degree_real == order_real + 1.0,
                first,
                jnp.where(degree_real > order_real + 1.0, general, 0.0),
            ),
        )
        slot = slot_ref[degree]
        for half in range(halves):
            rows_ref[half, pl.ds(slot, orders, stride=degrees), :] = value[
                :, half * LANES : (half + 1) * LANES
            ]
        return (value, previous)

    zeros = diagonal * 0.0
    lax.fori_loop(0, degrees, advance, (zeros, zeros), unroll=4)
    quadrature = quad_ref[...]
    for order in range(orders):
        for half in range(halves):
            low = half * LANES
            high = min(lats, low + LANES)
            chosen = rows_ref[half, order * degrees : (order + 1) * degrees, :][:, : high - low]
            p_ref[order, :, low:high] = chosen.astype(jnp.bfloat16)
            q_ref[order, :, low:high] = (chosen * quadrature[:, low:high]).astype(jnp.bfloat16)


def spectral_tables(start, ord_dev, degree_of):
    halves = -(-LATS // LANES)
    padded = halves * LANES
    order_col = (start + jnp.arange(ord_dev, dtype=jnp.int32)).astype(jnp.float32)[:, None]
    lat_ids = jnp.minimum(jnp.arange(padded, dtype=jnp.float32), LATS - 1.0)
    colatitude = jnp.pi * (lat_ids + 0.5) / LATS
    sine = jnp.sin(colatitude)[None, :]
    steps_up = jnp.arange(1, DEGREES + 1, dtype=jnp.float32)[None, :]
    factor = jnp.where(
        steps_up <= order_col, 0.5 * jnp.log((2.0 * steps_up + 1.0) / (2.0 * steps_up)), 0.0
    )
    log_start = 0.5 * jnp.log(1.0 / (4.0 * jnp.pi)) + jnp.sum(factor, axis=1, keepdims=True)
    diagonal = jnp.exp(log_start + order_col * jnp.log(sine))
    cosine = jnp.broadcast_to(jnp.cos(colatitude)[None, :], diagonal.shape)
    quadrature = 2.0 * jnp.pi * jnp.pi / LATS * sine
    orders = jnp.broadcast_to(order_col, diagonal.shape)
    vmem = pl.BlockSpec(memory_space=pltpu.VMEM)
    shape = jax.ShapeDtypeStruct((ord_dev, DEGREES, LATS), jnp.bfloat16)
    return pl.pallas_call(
        table_kernel,
        out_shape=(shape, shape),
        in_specs=[pl.BlockSpec(memory_space=pltpu.SMEM)] + [vmem] * 4,
        out_specs=(vmem, vmem),
        scratch_shapes=[
            pltpu.SMEM((DEGREES,), jnp.int32),
            pltpu.VMEM((halves, ord_dev * DEGREES, LANES), jnp.float32),
        ],
        name="legendre_tables",
    )(degree_of, diagonal, cosine, quadrature, orders)


def fourier_tables(lon_count, order_count):
    lon_ids = jnp.arange(lon_count, dtype=jnp.int32)[:, None]
    order_ids = jnp.arange(order_count, dtype=jnp.int32)[None, :]
    phase = 2.0 * jnp.pi * (lon_ids * order_ids % lon_count).astype(jnp.float32) / lon_count
    forward = (
        jnp.stack([jnp.cos(phase), -jnp.sin(phase)], axis=2).reshape(lon_count, 2 * order_count)
        / lon_count
    )
    doubled = jnp.where(order_ids == 0, 1.0, 2.0)
    inverse = jnp.stack([doubled * jnp.cos(phase), -doubled * jnp.sin(phase)], axis=2).reshape(
        lon_count, 2 * order_count
    )
    return (forward.astype(jnp.bfloat16), jnp.transpose(inverse).astype(jnp.bfloat16))


def to_orders(values):
    return lax.all_to_all(values, "lat", split_axis=1, concat_axis=0, tiled=True)


def to_degrees(values):
    return lax.all_to_all(values, "lat", split_axis=0, concat_axis=1, tiled=True)


def back_to_orders(values):
    return lax.all_to_all(values, "lat", split_axis=1, concat_axis=0, tiled=True)


def to_bands(values):
    return lax.all_to_all(values, "lat", split_axis=0, concat_axis=1, tiled=True)


def product(spec, left, right):
    return jnp.einsum(spec, left, right, preferred_element_type=jnp.float32)


def apply_filter(coeffs, weights):
    c_real = coeffs[:, :, 0]
    c_imag = coeffs[:, :, 1]
    w_real = weights[:, 0]
    w_imag = weights[:, 1]
    f_real = product("jmsc,jcd->jmsd", c_real, w_real) - product("jmsc,jcd->jmsd", c_imag, w_imag)
    f_imag = product("jmsc,jcd->jmsd", c_real, w_imag) + product("jmsc,jcd->jmsd", c_imag, w_real)
    return jnp.stack([f_real, f_imag], axis=2).astype(jnp.bfloat16)


def adjoint_filter(grads, weights):
    g_real = grads[:, :, 0]
    g_imag = grads[:, :, 1]
    w_real = weights[:, 0]
    w_imag = weights[:, 1]
    a_real = product("jmsd,jcd->jmsc", g_real, w_real) + product("jmsd,jcd->jmsc", g_imag, w_imag)
    a_imag = product("jmsd,jcd->jmsc", g_imag, w_real) - product("jmsd,jcd->jmsc", g_real, w_imag)
    return jnp.stack([a_real, a_imag], axis=2).astype(jnp.bfloat16)


def filter_grad(coeffs, grads):
    c_real = coeffs[:, :, 0]
    c_imag = coeffs[:, :, 1]
    g_real = grads[:, :, 0]
    g_imag = grads[:, :, 1]
    dw_real = product("jmsc,jmsd->jcd", c_real, g_real) + product("jmsc,jmsd->jcd", c_imag, g_imag)
    dw_imag = product("jmsc,jmsd->jcd", c_real, g_imag) - product("jmsc,jmsd->jcd", c_imag, g_real)
    return jnp.stack([dw_real, dw_imag], axis=1)


def constant_tables():
    sides = 2
    half = LATS // sides
    lat_ids = np.minimum(np.arange(LANES)[None, :], half - 1) + half * np.arange(sides)[:, None]
    colatitude = np.pi * (lat_ids + 0.5) / LATS
    sine = np.sin(colatitude)[:, None, :]
    ids = np.arange(ORDERS)
    steps_up = np.arange(1, ORDERS + 1)
    growth = np.cumsum(0.5 * np.log((2.0 * steps_up + 1.0) / (2.0 * steps_up)))
    log_start = 0.5 * np.log(1.0 / (4.0 * np.pi)) + np.concatenate([[0.0], growth[:-1]])
    diagonal = np.exp(log_start[None, :, None] + ids[None, :, None] * np.log(sine))
    cosine = np.broadcast_to(np.cos(colatitude)[:, None, :], (sides, GROUP, LANES))
    quadrature = np.broadcast_to(2.0 * np.pi * np.pi / LATS * sine, (sides, GROUP, LANES))
    phase = 2.0 * np.pi * (np.arange(LONS)[:, None] * ids[None, :] % LONS) / LONS
    forward = np.stack([np.cos(phase), -np.sin(phase)], axis=2).reshape(LONS, -1) / LONS
    doubled = np.where(ids == 0, 1.0, 2.0)[None, :]
    inverse = np.stack([doubled * np.cos(phase), -doubled * np.sin(phase)], axis=2)
    inverse = inverse.reshape(LONS, -1)
    floats = [jnp.asarray(t, jnp.float32) for t in (diagonal, cosine, quadrature)]
    waves = [forward.T, forward, inverse.T, inverse]
    halves = [jnp.asarray(np.float32(t).astype(jnp.bfloat16)) for t in waves]
    return floats, halves


def fill_tables(side, firsts, deg_ref, diag_ref, cos_ref, quad_ref, qtab, ptab, table, by_slot):
    kinds, orders, degrees, lats = qtab.shape
    every = kinds * orders
    cosine = cos_ref[side]
    diagonal, ids, squared, first_lead = [], [], [], []
    for first in firsts:
        diagonal.append(diag_ref[side, pl.ds(pl.multiple_of(first, orders), orders), :])
        ids.append(first + lax.broadcasted_iota(jnp.int32, cosine.shape, 0))
        real = ids[-1].astype(jnp.float32)
        squared.append(real * real)
        first_lead.append(jnp.sqrt(2.0 * real + 3.0))

    def advance(degree, carry):
        degree_real = degree.astype(jnp.float32)
        lower = degree_real - 1.0
        state = []
        for kind in range(kinds):
            previous, older = carry[kind]
            lead = jnp.sqrt(
                jnp.maximum(4.0 * degree_real * degree_real - 1.0, 0.0)
                / jnp.maximum(degree_real * degree_real - squared[kind], 1.0)
            )
            back = jnp.sqrt(
                jnp.maximum(lower * lower - squared[kind], 0.0)
                / jnp.maximum(4.0 * lower * lower - 1.0, 1.0)
            )
            general = lead * (cosine * previous - back * older)
            first = first_lead[kind] * cosine * previous
            value = jnp.where(
                ids[kind] == degree,
                diagonal[kind],
                jnp.where(
                    ids[kind] + 1 == degree,
                    first,
                    jnp.where(ids[kind] + 1 < degree, general, 0.0),
                ),
            )
            table[degree, kind * orders : (kind + 1) * orders, :] = value
            state.append((value, previous))
        return tuple(state)

    zeros = cosine * 0.0
    lax.fori_loop(0, degrees, advance, ((zeros, zeros),) * kinds)

    def place(slot, carry):
        by_slot[pl.ds(slot, every, stride=degrees), :] = table[deg_ref[slot]]
        return carry

    lax.fori_loop(0, degrees, place, 0)
    quadrature = quad_ref[side][:1, :lats]
    for kind in range(kinds):

        def keep(order, carry):
            start = pl.multiple_of((kind * orders + order) * degrees, degrees)
            chosen = by_slot[pl.ds(start, degrees), :][:, :lats]
            ptab[kind, order] = chosen.astype(jnp.bfloat16)
            qtab[kind, order] = (chosen * quadrature).astype(jnp.bfloat16)
            return carry

        lax.fori_loop(0, orders, keep, 0)


def pair_swap(values, even_sign):
    rows = values.shape[0]
    even = lax.broadcasted_iota(jnp.int32, values.shape, 0) % 2 == 0
    above = pltpu.roll(values, rows - 1, 0)
    below = pltpu.roll(values, 1, 0)
    return jnp.where(even, even_sign * above, -even_sign * below)


def gelu_slope(x):
    scale = 0.7978845608028654
    square = x * x
    t = jnp.tanh(scale * (x + 0.044715 * x * square))
    return 0.5 * (1.0 + t) + 0.5 * x * (1.0 - t * t) * (scale * (1.0 + 0.134145 * square))


def dot(left, right, dims=((1,), (0,))):
    return lax.dot_general(left, right, (dims, ((), ())), preferred_element_type=jnp.float32)


def block_kernel(
    n, nb, fields, cotangent, weights, deg_ref, diag_ref, cos_ref, quad_ref,
    fwd_fk, fwd_kf, inv_fk, inv_kf,
    grad_out, dw_out,
    fbuf, cbuf, wbuf, band_out, band_in, ord_in, ord_out, cross_out, cross_in, slot_out, slot_all,
    co, go, mixed, wide_a, wide_b, dw, dw_in, qtab, ptab, table,
    load_sem, send_sem, recv_sem, dw_send, dw_recv, out_sem,
):
    me = lax.axis_index("lat")
    me_b = lax.axis_index("batch")
    chunks, lat_dev = fbuf.shape[0], fbuf.shape[1]
    kinds, orders, degrees, side_lats = qtab.shape
    rows = 2 * orders
    slots = co.shape[1]
    quarter = n // kinds
    half = n // 2
    own = half * slots
    inner_kinds = ord_in.shape[0]
    pairs = kinds // 2
    jobs = kinds * chunks
    plane_rows = quarter * rows
    mesh_id = pl.DeviceIdType.MESH
    side = lax.div(me, half)
    place_in = lax.rem(me, half)
    column = lax.rem(me, quarter)
    inner = jnp.where(lax.div(me, quarter) == 1 + side, 1, 0)
    across = 1 - side

    def lanes(chunk):
        return pl.ds(chunk * LANES, LANES)

    def group(kind, at):
        return jnp.where(
            lax.rem(kind, 2) == 0, kind * quarter + at, (kind + 1) * quarter - 1 - at
        )

    def group_rows(kind, at):
        return pl.ds(pl.multiple_of(group(kind, at) * rows, rows), rows)

    def owner(kind, on_side, at):
        plane = jnp.where(kind < inner_kinds, 1 + on_side, (kinds - 1) * on_side)
        return plane * quarter + at

    def mine(kind):
        return jnp.where(kind < inner_kinds, 1, 0) == inner

    def job_of(job):
        per_pass = pairs * chunks
        inside = lax.rem(job, per_pass)
        kind = lax.div(job, per_pass) * pairs + lax.rem(inside, pairs)
        return kind, lax.div(inside, pairs), lax.rem(kind, inner_kinds)

    def job_at(kind, chunk):
        return (kind // pairs) * (pairs * chunks) + chunk * pairs + kind % pairs

    def load(chunk):
        return pltpu.make_async_copy(
            fields.at[0, :, :, lanes(chunk)], fbuf.at[chunk], load_sem.at[chunk]
        )

    def load_cot(chunk):
        return pltpu.make_async_copy(
            cotangent.at[0, :, :, lanes(chunk)], cbuf.at[chunk], load_sem.at[chunks + chunk]
        )

    load_w = pltpu.make_async_copy(weights, wbuf, load_sem.at[2 * chunks])
    for chunk in range(chunks):
        load(chunk).start()
    load_w.start()
    for chunk in range(chunks):
        load_cot(chunk).start()

    barrier = pltpu.get_barrier_semaphore()

    def greet(step, carry):
        peer = lax.rem(me + step, n)
        pl.semaphore_signal(barrier, inc=1, device_id={"lat": peer}, device_id_type=mesh_id)
        return carry

    lax.fori_loop(1, n, greet, 0)
    for step in range(1, nb):
        peer = lax.rem(me_b + step, nb)
        pl.semaphore_signal(barrier, inc=1, device_id={"batch": peer}, device_id_type=mesh_id)
    pl.semaphore_wait(barrier, n - 1 + nb - 1)

    def remote(stage, job, source, target, peer):
        pltpu.make_async_remote_copy(
            src_ref=source,
            dst_ref=target,
            send_sem=send_sem.at[stage, job],
            recv_sem=recv_sem.at[stage, job],
            device_id={"lat": peer},
            device_id_type=mesh_id,
        ).start()

    def await_bytes(view, sem):
        pltpu.make_async_copy(view, view, sem).wait()

    def to_owners(stage, kind, chunk, source, target, width):
        job = job_at(kind, chunk)
        for step in range(quarter):
            at = lax.rem(column + step, quarter)
            view = source.at[chunk, :, group_rows(kind, at), :]
            spot = target(kind % inner_kinds, chunk)
            peer = owner(kind, side, at)

            @pl.when(peer != me)
            def _():
                remote(stage, job, view, spot, peer)

            @pl.when(peer == me)
            def _():
                pltpu.make_async_copy(view, spot, recv_sem.at[stage, job]).start()

    def left_for_owners(stage, kind, chunk, source):
        job = job_at(kind, chunk)

        @pl.when(mine(kind))
        def _():
            await_bytes(source.at[chunk, :, 0 : plane_rows - rows, :], send_sem.at[stage, job])

        @pl.when(jnp.logical_not(mine(kind)))
        def _():
            await_bytes(source.at[chunk, :, 0:plane_rows, :], send_sem.at[stage, job])

    def from_owner(stage, job, kind, chunk, source, depth, target):
        place = lax.rem(kind, inner_kinds)
        spot = target.at[chunk, :, group_rows(kind, column), :]

        def send(step, carry):
            at = lax.rem(place_in + step, half)
            remote(
                stage, job, source.at[place, chunk, pl.ds(at * depth, depth)], spot,
                side * half + at,
            )
            return carry

        lax.fori_loop(1, half, send, 0)
        pltpu.make_async_copy(
            source.at[place, chunk, pl.ds(place_in * depth, depth)], spot, recv_sem.at[stage, job]
        ).start()

    def left_owner(stage, job, kind, chunk, source, depth):
        view = source.at[lax.rem(kind, inner_kinds), chunk, 0 : (half - 1) * depth]
        await_bytes(view, send_sem.at[stage, job])

    def reached_all(stage, kind, chunk, target):
        await_bytes(target.at[chunk, :, 0:plane_rows, :], recv_sem.at[stage, job_at(kind, chunk)])

    def lat_spot(place, chunk):
        return ord_in.at[place, chunk, pl.ds(place_in * lat_dev, lat_dev)]

    def slot_spot(place, chunk):
        return slot_all.at[place, chunk, pl.ds(me * slots, slots)]

    def wide_start(job):
        return pl.multiple_of(lax.rem(job, wide_b.shape[0] // wide_a.shape[0]) * wide_a.shape[0], 8)

    def widen(source, place, chunk, depth, count):
        def one(block, carry):
            piece = source[place, chunk, pl.ds(block * depth, depth)].astype(jnp.float32)
            wide_a[pl.ds(pl.multiple_of(block * depth * rows, depth * rows), depth * rows), :] = (
                piece.reshape(depth * rows, LANES)
            )
            return carry

        lax.fori_loop(0, count // depth, one, 0)

    def apply_table(tab, kind, start, depth_in, depth_out, dims):
        def one(order, carry):
            real = wide_a[pl.ds(2 * order, depth_in, stride=rows), :]
            imag = wide_a[pl.ds(2 * order + 1, depth_in, stride=rows), :]
            both = jnp.concatenate([real, imag], axis=1).astype(jnp.bfloat16)
            result = dot(tab[kind, order], both, dims)
            wide_b[pl.ds(start + 2 * order, depth_out, stride=rows), :] = result[:, :LANES]
            wide_b[pl.ds(start + 2 * order + 1, depth_out, stride=rows), :] = result[:, LANES:]
            return carry

        lax.fori_loop(0, orders, one, 0)

    def narrow(target, place, chunk, start, depth, count):
        def one(block, carry):
            low = pl.multiple_of(start + block * depth * rows, 8)
            piece = wide_b[pl.ds(low, depth * rows), :]
            target[place, chunk, pl.ds(block * depth, depth)] = piece.reshape(
                depth, rows, LANES
            ).astype(jnp.bfloat16)
            return carry

        lax.fori_loop(0, count // depth, one, 0)

    def analyse(base, tab, job):
        kind, chunk, place = job_of(job)

        @pl.when(mine(kind))
        def _():
            await_bytes(ord_in.at[place, chunk], recv_sem.at[base, job])
            widen(ord_in, place, chunk, lat_dev, side_lats)
            start = wide_start(job)
            apply_table(tab, kind, start, side_lats, degrees, ((1,), (0,)))
            if base:
                await_bytes(cross_out.at[place, chunk], send_sem.at[1, job])
            narrow(cross_out, place, chunk, start + across * own * rows, slots, own)
            remote(
                base + 1, job, cross_out.at[place, chunk], cross_in.at[place, chunk],
                owner(kind, across, column),
            )

    def settle(base, target, job):
        kind, chunk, place = job_of(job)

        @pl.when(mine(kind))
        def _():
            await_bytes(cross_in.at[place, chunk], recv_sem.at[base + 1, job])
            if base:
                left_owner(2, job, kind, chunk, slot_out, slots)
                await_bytes(slot_all.at[place, chunk, 0:own], send_sem.at[4, job])
            start = wide_start(job) + side * own * rows

            def one(block, carry):
                low = pl.multiple_of(start + block * slots * rows, 8)
                piece = wide_b[pl.ds(low, slots * rows), :].reshape(slots, rows, LANES)
                other = cross_in[place, chunk, pl.ds(block * slots, slots)].astype(jnp.float32)
                slot_out[place, chunk, pl.ds(block * slots, slots)] = (piece + other).astype(
                    jnp.bfloat16
                )
                return carry

            lax.fori_loop(0, half, one, 0)
            from_owner(base + 2, job, kind, chunk, slot_out, slots, target)

    def relay(base, job):
        kind, chunk, place = job_of(job)

        @pl.when(mine(kind))
        def _():
            await_bytes(slot_all.at[place, chunk, 0:own], recv_sem.at[base + 3, job])
            view = slot_all.at[place, chunk, pl.ds(side * own, own)]
            remote(base + 4, job, view, view, owner(kind, across, column))

    def synthesise(base, tab, job):
        kind, chunk, place = job_of(job)

        @pl.when(mine(kind))
        def _():
            await_bytes(slot_all.at[place, chunk, 0:own], recv_sem.at[base + 4, job])
            widen(slot_all, place, chunk, slots, degrees)
            start = wide_start(job)
            apply_table(tab, kind, start, degrees, side_lats, ((0,), (0,)))
            if base:
                left_owner(5, job, kind, chunk, ord_out, lat_dev)
            narrow(ord_out, place, chunk, start, lat_dev, side_lats)
            from_owner(base + 5, job, kind, chunk, ord_out, lat_dev, band_in)

    def loop(low, high, body):
        def one(job, carry):
            body(job)
            return carry

        lax.fori_loop(low, high, one, 0)

    def pair(source, chunk, row):
        return jnp.concatenate([source[chunk, 2 * row], source[chunk, 2 * row + 1]], axis=1)

    def put_pair(target, chunk, row, values):
        values = values.astype(jnp.bfloat16)
        target[chunk, 2 * row] = values[:, :LANES]
        target[chunk, 2 * row + 1] = values[:, LANES:]

    def joined(source, slot, span):
        return jnp.concatenate([source[chunk, slot, span] for chunk in range(chunks)], axis=1)

    def mix(part, chunk):
        low = part * pairs * plane_rows
        span = slice(low, low + pairs * plane_rows)
        columns = slice(chunk * LANES, (chunk + 1) * LANES)

        def one(slot, carry):
            both = dot(
                joined(co, slot, span),
                jnp.concatenate([wbuf[slot, 0, :, columns], wbuf[slot, 1, :, columns]], axis=1),
            )
            crossed = pair_swap(both[:, LANES:], -1.0)
            mixed[chunk, slot, span] = (both[:, :LANES] + crossed).astype(jnp.bfloat16)
            return carry

        return one

    def adjoint(part, chunk):
        low = part * pairs * plane_rows
        span = slice(low, low + pairs * plane_rows)
        columns = slice(chunk * LANES, (chunk + 1) * LANES)

        def one(slot, carry):
            both = dot(
                joined(go, slot, span),
                jnp.concatenate([wbuf[slot, 0, columns, :], wbuf[slot, 1, columns, :]], axis=0),
                ((1,), (1,)),
            )
            crossed = pair_swap(both[:, LANES:], 1.0)
            mixed[chunk, slot, span] = (both[:, :LANES] + crossed).astype(jnp.bfloat16)
            return carry

        return one

    def filter_part(base, part, source, make):
        part_kinds = range(part * pairs, (part + 1) * pairs)
        for chunk in range(chunks):
            for kind in part_kinds:
                reached_all(base + 2, kind, chunk, source)
        for chunk in range(chunks):
            if base:
                for kind in part_kinds:
                    left_for_owners(3, kind, chunk, mixed)
            lax.fori_loop(0, slots, make(part, chunk), 0)
            for kind in part_kinds:
                to_owners(base + 3, kind, chunk, mixed, slot_spot, slots)

    per_pass = pairs * chunks
    lag = 2

    def to_filter(base, tab, source, make):
        loop(0, lag, lambda job: analyse(base, tab, job))

        def step(job):
            analyse(base, tab, job)
            settle(base, source, job - lag)

        loop(lag, jobs, step)
        filter_part(base, 0, source, make)
        settle(base, source, jobs - lag)
        loop(0, per_pass, lambda job: relay(base, job))
        for job in range(jobs - lag + 1, jobs):
            settle(base, source, job)
        filter_part(base, 1, source, make)

    def from_filter(base, tab, finish):
        def step(job):
            synthesise(base, tab, job)
            relay(base, job + per_pass)

        loop(0, per_pass, step)
        for chunk in range(chunks):
            first = per_pass + chunk * pairs
            loop(first, first + pairs, lambda job: synthesise(base, tab, job))
            if chunk:
                finish(chunk - 1)
        finish(chunks - 1)

    def spread(stage, chunk, part):
        for kind in range(part * pairs, (part + 1) * pairs):
            to_owners(stage, kind, chunk, band_out, lat_spot, lat_dev)

    for chunk in range(chunks):
        load(chunk).wait()

        def fourier(row, carry):
            put_pair(band_out, chunk, row, dot(fwd_fk[...], pair(fbuf, chunk, row)))
            return carry

        lax.fori_loop(0, lat_dev // 2, fourier, 0)
        spread(0, chunk, 0)
    for chunk in range(chunks):
        spread(0, chunk, 1)
    fill_tables(
        side, [group(kind, column) * orders for kind in range(kinds)], deg_ref, diag_ref, cos_ref,
        quad_ref, qtab, ptab, table, wide_b,
    )
    load_w.wait()
    to_filter(0, qtab, co, mix)

    def between(chunk):
        load_cot(chunk).wait()
        for kind in range(kinds):
            reached_all(5, kind, chunk, band_in)
            left_for_owners(0, kind, chunk, band_out)

        def middle(row, carry):
            response = dot(inv_kf[...], pair(band_in, chunk, row))
            upstream = pair(cbuf, chunk, row).astype(jnp.float32) * gelu_slope(response)
            put_pair(band_out, chunk, row, dot(inv_fk[...], upstream.astype(jnp.bfloat16)))
            return carry

        lax.fori_loop(0, lat_dev // 2, middle, 0)
        spread(6, chunk, 0)

    from_filter(0, ptab, between)
    for chunk in range(chunks):
        spread(6, chunk, 1)
    to_filter(6, ptab, go, adjoint)

    def weight_grad(slot, carry):
        values = joined(co, slot, slice(None))
        grads = joined(go, slot, slice(None))
        turned = pair_swap(grads.astype(jnp.float32), 1.0).astype(jnp.bfloat16)
        span = ((0,), (0,))
        dw[slot, 0] = dot(values, grads, span).astype(jnp.bfloat16)
        dw[slot, 1] = dot(values, turned, span).astype(jnp.bfloat16)
        return carry

    lax.fori_loop(0, slots, weight_grad, 0)
    dw_copies = []
    for step in range(1, nb):
        peer = lax.rem(me_b + step, nb)
        copy = pltpu.make_async_remote_copy(
            src_ref=dw,
            dst_ref=dw_in.at[step - 1],
            send_sem=dw_send.at[step - 1],
            recv_sem=dw_recv.at[step - 1],
            device_id={"batch": peer},
            device_id_type=mesh_id,
        )
        copy.start()
        dw_copies.append(copy)

    def store(chunk):
        return pltpu.make_async_copy(
            cbuf.at[chunk], grad_out.at[0, :, :, lanes(chunk)], out_sem.at[chunk]
        )

    store_w = pltpu.make_async_copy(dw, dw_out, out_sem.at[chunks])

    def total(slot, carry):
        value = dw[slot].astype(jnp.float32)
        for step in range(nb - 1):
            value = value + dw_in[step, slot].astype(jnp.float32)
        dw[slot] = value.astype(jnp.bfloat16)
        return carry

    def last(chunk):
        if chunk == 0:
            for copy in dw_copies:
                copy.wait()
            lax.fori_loop(0, slots, total, 0)
            store_w.start()
        for kind in range(kinds):
            reached_all(11, kind, chunk, band_in)

        def finish(row, carry):
            delta = dot(fwd_kf[...], pair(band_in, chunk, row))
            put_pair(cbuf, chunk, row, pair(cbuf, chunk, row).astype(jnp.float32) + delta)
            return carry

        lax.fori_loop(0, lat_dev // 2, finish, 0)
        store(chunk).start()

    from_filter(6, qtab, last)
    for chunk in range(chunks):
        for kind in range(kinds):
            left_for_owners(6, kind, chunk, band_out)
            left_for_owners(9, kind, chunk, mixed)

    def drain(job):
        kind, chunk, place = job_of(job)

        @pl.when(mine(kind))
        def _():
            await_bytes(cross_out.at[place, chunk], send_sem.at[7, job])
            left_owner(8, job, kind, chunk, slot_out, slots)
            await_bytes(slot_all.at[place, chunk, 0:own], send_sem.at[10, job])
            left_owner(11, job, kind, chunk, ord_out, lat_dev)

    loop(0, jobs, drain)
    for chunk in range(chunks):
        store(chunk).wait()
    store_w.wait()


def local_kernel(fields, cotangent, weights, degree_of):
    n = lax.axis_size("lat")
    nb = lax.axis_size("batch")
    kinds = 4
    if fields.shape[0] != 1 or fields.shape[1] % 2 or n % kinds or ORDERS != n * GROUP:
        return local(fields, cotangent, weights, degree_of)
    lat_dev, lons, channels = fields.shape[1:]
    slots = weights.shape[0]
    rows = 2 * GROUP
    chunks = channels // LANES
    floats, waves = constant_tables()
    side_lats = LATS // 2
    held = kinds - 1
    vmem = pl.BlockSpec(memory_space=pltpu.VMEM)
    anywhere = pl.BlockSpec(memory_space=pl.ANY)

    def buffer(*dims):
        return pltpu.VMEM(dims, jnp.bfloat16)

    dma = pltpu.SemaphoreType.DMA
    others = max(nb - 1, 1)
    wide_rows = max(side_lats, DEGREES) * rows
    return pl.pallas_call(
        functools.partial(block_kernel, n, nb),
        out_shape=(
            jax.ShapeDtypeStruct(fields.shape, jnp.bfloat16),
            jax.ShapeDtypeStruct(weights.shape, jnp.bfloat16),
        ),
        in_specs=[anywhere] * 3 + [pl.BlockSpec(memory_space=pltpu.SMEM)] + [vmem] * 7,
        out_specs=(anywhere, anywhere),
        scratch_shapes=[
            buffer(chunks, lat_dev, lons, LANES),
            buffer(chunks, lat_dev, lons, LANES),
            buffer(*weights.shape),
            buffer(chunks, lat_dev, n * rows, LANES),
            buffer(chunks, lat_dev, n * rows, LANES),
            buffer(held, chunks, side_lats, rows, LANES),
            buffer(held, chunks, side_lats, rows, LANES),
            buffer(held, chunks, DEGREES // 2, rows, LANES),
            buffer(held, chunks, DEGREES // 2, rows, LANES),
            buffer(held, chunks, DEGREES // 2, rows, LANES),
            buffer(held, chunks, DEGREES, rows, LANES),
            buffer(chunks, slots, n * rows, LANES),
            buffer(chunks, slots, n * rows, LANES),
            buffer(chunks, slots, n * rows, LANES),
            pltpu.VMEM((wide_rows, LANES), jnp.float32),
            pltpu.VMEM((3 * wide_rows, LANES), jnp.float32),
            buffer(*weights.shape),
            buffer(others, *weights.shape),
            buffer(kinds, GROUP, DEGREES, side_lats),
            buffer(kinds, GROUP, DEGREES, side_lats),
            pltpu.VMEM((DEGREES, kinds * GROUP, LANES), jnp.float32),
            dma((2 * chunks + 1,)),
            dma((12, kinds * chunks)),
            dma((12, kinds * chunks)),
            dma((others,)),
            dma((others,)),
            dma((chunks + 1,)),
        ],
        compiler_params=pltpu.CompilerParams(
            collective_id=0, has_side_effects=True, vmem_limit_bytes=63 * 2**20
        ),
        name="filter_block",
    )(
        fields, cotangent, weights, degree_of, *floats, *waves,
    )


def local(fields, cotangent, weights, degree_of):
    samples = fields.shape[0]
    band_rows = fields.shape[1]
    ord_dev = ORDERS // lax.axis_size("lat")
    forward, inverse = fourier_tables(LONS, ORDERS)
    qslot, pslot = spectral_tables(lax.axis_index("lat") * ord_dev, ord_dev, degree_of)
    spectra = product("sikc,kf->ifsc", fields, forward).astype(jnp.bfloat16)
    spectra = spectra.reshape(band_rows, ORDERS, 2, samples, CHANNELS)
    gathered = to_orders(spectra)
    coeffs_local = product("mji,imrsc->jmrsc", qslot, gathered).astype(jnp.bfloat16)
    coeffs = to_degrees(coeffs_local)
    filtered = apply_filter(coeffs, weights)
    returned = back_to_orders(filtered)
    synth_local = product("mji,jmrsc->imrsc", pslot, returned).astype(jnp.bfloat16)
    synth = to_bands(synth_local)
    response = product(
        "ifsc,fk->sikc", synth.reshape(band_rows, 2 * ORDERS, samples, CHANNELS), inverse
    )
    activated, pullback = jax.vjp(jax.nn.gelu, response)
    upstream = pullback(cotangent.astype(jnp.float32))[0].astype(jnp.bfloat16)
    grad_synth = product("sikc,fk->ifsc", upstream, inverse).astype(jnp.bfloat16)
    grad_synth = grad_synth.reshape(band_rows, ORDERS, 2, samples, CHANNELS)
    grad_gathered = to_orders(grad_synth)
    grad_local = product("mji,imrsc->jmrsc", pslot, grad_gathered).astype(jnp.bfloat16)
    grad_filtered = to_degrees(grad_local)
    weight_total = lax.psum(filter_grad(coeffs, grad_filtered).astype(jnp.bfloat16), "batch")
    grad_coeffs = adjoint_filter(grad_filtered, weights)
    grad_back = back_to_orders(grad_coeffs)
    grad_local_spec = product("mji,jmrsc->imrsc", qslot, grad_back).astype(jnp.bfloat16)
    grad_bands = to_bands(grad_local_spec)
    delta = product(
        "ifsc,kf->sikc", grad_bands.reshape(band_rows, 2 * ORDERS, samples, CHANNELS), forward
    )
    grad_fields = (cotangent.astype(jnp.float32) + delta).astype(jnp.bfloat16)
    return (grad_fields, weight_total)


def solution(mesh):
    return jax.shard_map(
        local_kernel if CHANNELS % LANES == 0 else local,
        mesh=mesh,
        in_specs=(
            P("batch", "lat", None, None),
            P("batch", "lat", None, None),
            P("lat", None, None, None),
            P(),
        ),
        out_specs=(P("batch", "lat", None, None), P("lat", None, None, None)),
        check_vma=False,
    )
```

```python
import functools

import jax
import numpy as np
import jax.numpy as jnp
from jax import lax
from jax.experimental import pallas as pl
from jax.experimental.pallas import tpu as pltpu
from jax.sharding import PartitionSpec as P

LATS = 192
LONS = 384
ORDERS = 128
DEGREES = 128
CHANNELS = 384
LANES = 128
GROUP = 8


def table_kernel(deg_ref, diag_ref, cos_ref, quad_ref, order_ref, q_ref, p_ref, slot_ref, rows_ref):
    orders = diag_ref.shape[0]
    lats = q_ref.shape[2]
    degrees = deg_ref.shape[0]

    def invert(slot, carry):
        slot_ref[deg_ref[slot]] = slot
        return carry

    lax.fori_loop(0, degrees, invert, 0)
    order_real = order_ref[...]
    squared = order_real * order_real
    diagonal = diag_ref[...]
    cosine = cos_ref[...]
    first_lead = jnp.sqrt(2.0 * order_real + 3.0)
    halves = rows_ref.shape[0]

    def advance(degree, carry):
        previous, older = carry
        degree_real = degree.astype(jnp.float32)
        lead = jnp.sqrt(
            jnp.maximum(4.0 * degree_real * degree_real - 1.0, 0.0)
            / jnp.maximum(degree_real * degree_real - squared, 1.0)
        )
        lower = degree_real - 1.0
        back = jnp.sqrt(
            jnp.maximum(lower * lower - squared, 0.0) / jnp.maximum(4.0 * lower * lower - 1.0, 1.0)
        )
        general = lead * (cosine * previous - back * older)
        first = first_lead * cosine * previous
        value = jnp.where(
            degree_real == order_real,
            diagonal,
            jnp.where(
                degree_real == order_real + 1.0,
                first,
                jnp.where(degree_real > order_real + 1.0, general, 0.0),
            ),
        )
        slot = slot_ref[degree]
        for half in range(halves):
            rows_ref[half, pl.ds(slot, orders, stride=degrees), :] = value[
                :, half * LANES : (half + 1) * LANES
            ]
        return (value, previous)

    zeros = diagonal * 0.0
    lax.fori_loop(0, degrees, advance, (zeros, zeros), unroll=4)
    quadrature = quad_ref[...]
    for order in range(orders):
        for half in range(halves):
            low = half * LANES
            high = min(lats, low + LANES)
            chosen = rows_ref[half, order * degrees : (order + 1) * degrees, :][:, : high - low]
            p_ref[order, :, low:high] = chosen.astype(jnp.bfloat16)
            q_ref[order, :, low:high] = (chosen * quadrature[:, low:high]).astype(jnp.bfloat16)


def spectral_tables(start, ord_dev, degree_of):
    halves = -(-LATS // LANES)
    padded = halves * LANES
    order_col = (start + jnp.arange(ord_dev, dtype=jnp.int32)).astype(jnp.float32)[:, None]
    lat_ids = jnp.minimum(jnp.arange(padded, dtype=jnp.float32), LATS - 1.0)
    colatitude = jnp.pi * (lat_ids + 0.5) / LATS
    sine = jnp.sin(colatitude)[None, :]
    steps_up = jnp.arange(1, DEGREES + 1, dtype=jnp.float32)[None, :]
    factor = jnp.where(
        steps_up <= order_col, 0.5 * jnp.log((2.0 * steps_up + 1.0) / (2.0 * steps_up)), 0.0
    )
    log_start = 0.5 * jnp.log(1.0 / (4.0 * jnp.pi)) + jnp.sum(factor, axis=1, keepdims=True)
    diagonal = jnp.exp(log_start + order_col * jnp.log(sine))
    cosine = jnp.broadcast_to(jnp.cos(colatitude)[None, :], diagonal.shape)
    quadrature = 2.0 * jnp.pi * jnp.pi / LATS * sine
    orders = jnp.broadcast_to(order_col, diagonal.shape)
    vmem = pl.BlockSpec(memory_space=pltpu.VMEM)
    shape = jax.ShapeDtypeStruct((ord_dev, DEGREES, LATS), jnp.bfloat16)
    return pl.pallas_call(
        table_kernel,
        out_shape=(shape, shape),
        in_specs=[pl.BlockSpec(memory_space=pltpu.SMEM)] + [vmem] * 4,
        out_specs=(vmem, vmem),
        scratch_shapes=[
            pltpu.SMEM((DEGREES,), jnp.int32),
            pltpu.VMEM((halves, ord_dev * DEGREES, LANES), jnp.float32),
        ],
        name="legendre_tables",
    )(degree_of, diagonal, cosine, quadrature, orders)


def fourier_tables(lon_count, order_count):
    lon_ids = jnp.arange(lon_count, dtype=jnp.int32)[:, None]
    order_ids = jnp.arange(order_count, dtype=jnp.int32)[None, :]
    phase = 2.0 * jnp.pi * (lon_ids * order_ids % lon_count).astype(jnp.float32) / lon_count
    forward = (
        jnp.stack([jnp.cos(phase), -jnp.sin(phase)], axis=2).reshape(lon_count, 2 * order_count)
        / lon_count
    )
    doubled = jnp.where(order_ids == 0, 1.0, 2.0)
    inverse = jnp.stack([doubled * jnp.cos(phase), -doubled * jnp.sin(phase)], axis=2).reshape(
        lon_count, 2 * order_count
    )
    return (forward.astype(jnp.bfloat16), jnp.transpose(inverse).astype(jnp.bfloat16))


def to_orders(values):
    return lax.all_to_all(values, "lat", split_axis=1, concat_axis=0, tiled=True)


def to_degrees(values):
    return lax.all_to_all(values, "lat", split_axis=0, concat_axis=1, tiled=True)


def back_to_orders(values):
    return lax.all_to_all(values, "lat", split_axis=1, concat_axis=0, tiled=True)


def to_bands(values):
    return lax.all_to_all(values, "lat", split_axis=0, concat_axis=1, tiled=True)


def product(spec, left, right):
    return jnp.einsum(spec, left, right, preferred_element_type=jnp.float32)


def apply_filter(coeffs, weights):
    c_real = coeffs[:, :, 0]
    c_imag = coeffs[:, :, 1]
    w_real = weights[:, 0]
    w_imag = weights[:, 1]
    f_real = product("jmsc,jcd->jmsd", c_real, w_real) - product("jmsc,jcd->jmsd", c_imag, w_imag)
    f_imag = product("jmsc,jcd->jmsd", c_real, w_imag) + product("jmsc,jcd->jmsd", c_imag, w_real)
    return jnp.stack([f_real, f_imag], axis=2).astype(jnp.bfloat16)


def adjoint_filter(grads, weights):
    g_real = grads[:, :, 0]
    g_imag = grads[:, :, 1]
    w_real = weights[:, 0]
    w_imag = weights[:, 1]
    a_real = product("jmsd,jcd->jmsc", g_real, w_real) + product("jmsd,jcd->jmsc", g_imag, w_imag)
    a_imag = product("jmsd,jcd->jmsc", g_imag, w_real) - product("jmsd,jcd->jmsc", g_real, w_imag)
    return jnp.stack([a_real, a_imag], axis=2).astype(jnp.bfloat16)


def filter_grad(coeffs, grads):
    c_real = coeffs[:, :, 0]
    c_imag = coeffs[:, :, 1]
    g_real = grads[:, :, 0]
    g_imag = grads[:, :, 1]
    dw_real = product("jmsc,jmsd->jcd", c_real, g_real) + product("jmsc,jmsd->jcd", c_imag, g_imag)
    dw_imag = product("jmsc,jmsd->jcd", c_real, g_imag) - product("jmsc,jmsd->jcd", c_imag, g_real)
    return jnp.stack([dw_real, dw_imag], axis=1)


def constant_tables():
    sides = 2
    half = LATS // sides
    lat_ids = np.minimum(np.arange(LANES)[None, :], half - 1) + half * np.arange(sides)[:, None]
    colatitude = np.pi * (lat_ids + 0.5) / LATS
    sine = np.sin(colatitude)[:, None, :]
    ids = np.arange(ORDERS)
    steps_up = np.arange(1, ORDERS + 1)
    growth = np.cumsum(0.5 * np.log((2.0 * steps_up + 1.0) / (2.0 * steps_up)))
    log_start = 0.5 * np.log(1.0 / (4.0 * np.pi)) + np.concatenate([[0.0], growth[:-1]])
    diagonal = np.exp(log_start[None, :, None] + ids[None, :, None] * np.log(sine))
    cosine = np.broadcast_to(np.cos(colatitude)[:, None, :], (sides, GROUP, LANES))
    quadrature = np.broadcast_to(2.0 * np.pi * np.pi / LATS * sine, (sides, GROUP, LANES))
    phase = 2.0 * np.pi * (np.arange(LONS)[:, None] * ids[None, :] % LONS) / LONS
    forward = np.stack([np.cos(phase), -np.sin(phase)], axis=2).reshape(LONS, -1) / LONS
    doubled = np.where(ids == 0, 1.0, 2.0)[None, :]
    inverse = np.stack([doubled * np.cos(phase), -doubled * np.sin(phase)], axis=2)
    inverse = inverse.reshape(LONS, -1)
    floats = [jnp.asarray(t, jnp.float32) for t in (diagonal, cosine, quadrature)]
    waves = [forward.T, forward, inverse.T, inverse]
    halves = [jnp.asarray(np.float32(t).astype(jnp.bfloat16)) for t in waves]
    return floats, halves


def fill_tables(side, firsts, deg_ref, diag_ref, cos_ref, quad_ref, qtab, ptab, table, by_slot):
    kinds, orders, degrees, lats = qtab.shape
    every = kinds * orders
    cosine = cos_ref[side]
    diagonal, ids, squared, first_lead = [], [], [], []
    for first in firsts:
        diagonal.append(diag_ref[side, pl.ds(pl.multiple_of(first, orders), orders), :])
        ids.append(first + lax.broadcasted_iota(jnp.int32, cosine.shape, 0))
        real = ids[-1].astype(jnp.float32)
        squared.append(real * real)
        first_lead.append(jnp.sqrt(2.0 * real + 3.0))

    def advance(degree, carry):
        degree_real = degree.astype(jnp.float32)
        lower = degree_real - 1.0
        state = []
        for kind in range(kinds):
            previous, older = carry[kind]
            lead = jnp.sqrt(
                jnp.maximum(4.0 * degree_real * degree_real - 1.0, 0.0)
                / jnp.maximum(degree_real * degree_real - squared[kind], 1.0)
            )
            back = jnp.sqrt(
                jnp.maximum(lower * lower - squared[kind], 0.0)
                / jnp.maximum(4.0 * lower * lower - 1.0, 1.0)
            )
            general = lead * (cosine * previous - back * older)
            first = first_lead[kind] * cosine * previous
            value = jnp.where(
                ids[kind] == degree,
                diagonal[kind],
                jnp.where(
                    ids[kind] + 1 == degree,
                    first,
                    jnp.where(ids[kind] + 1 < degree, general, 0.0),
                ),
            )
            table[degree, kind * orders : (kind + 1) * orders, :] = value
            state.append((value, previous))
        return tuple(state)

    zeros = cosine * 0.0
    lax.fori_loop(0, degrees, advance, ((zeros, zeros),) * kinds)

    ahead = every // 2
    tail = degrees // 2

    def place(slot, carry):
        by_slot[pl.ds(slot, ahead, stride=degrees), :] = table[deg_ref[slot], :ahead]
        return carry

    lax.fori_loop(0, degrees, place, 0, unroll=4)

    def place_tail(row, carry):
        spots = pl.ds(ahead * degrees + row, ahead, stride=degrees)
        by_slot[spots, :] = table[tail + row, ahead:]
        return carry

    lax.fori_loop(0, tail, place_tail, 0, unroll=4)
    quadrature = quad_ref[side][:1, :lats]
    for kind in range(kinds):

        def keep(order, carry):
            start = pl.multiple_of((kind * orders + order) * degrees, degrees)
            depth = degrees if kind < kinds // 2 else tail
            chosen = by_slot[pl.ds(start, depth), :][:, :lats]
            ptab[kind, order, :depth] = chosen.astype(jnp.bfloat16)
            qtab[kind, order, :depth] = (chosen * quadrature).astype(jnp.bfloat16)
            return carry

        lax.fori_loop(0, orders, keep, 0)


def pair_swap(values, even_sign):
    rows = values.shape[0]
    even = lax.broadcasted_iota(jnp.int32, values.shape, 0) % 2 == 0
    above = pltpu.roll(values, rows - 1, 0)
    below = pltpu.roll(values, 1, 0)
    return jnp.where(even, even_sign * above, -even_sign * below)


def gelu_slope(x):
    scale = 0.7978845608028654
    square = x * x
    t = jnp.tanh(scale * (x + 0.044715 * x * square))
    return 0.5 * (1.0 + t) + 0.5 * x * (1.0 - t * t) * (scale * (1.0 + 0.134145 * square))


def dot(left, right, dims=((1,), (0,))):
    return lax.dot_general(left, right, (dims, ((), ())), preferred_element_type=jnp.float32)


def block_kernel(
    n, nb, fields, cotangent, weights, deg_ref, diag_ref, cos_ref, quad_ref,
    fwd_fk, fwd_kf, inv_fk, inv_kf,
    grad_out, dw_out,
    fbuf, cbuf, wbuf, band_out, band_in, ord_in, ord_out, cross_out, cross_in, slot_out, slot_all,
    tail_out, co, go, mixed, wide_a, wide_b, dw, dw_in, qtab, ptab, table, row_ref, slot_of, by_name,
    load_sem, send_sem, recv_sem, dw_send, dw_recv, out_sem,
):
    me = lax.axis_index("lat")
    me_b = lax.axis_index("batch")
    chunks, lat_dev = fbuf.shape[0], fbuf.shape[1]
    kinds, orders, degrees, side_lats = qtab.shape
    rows = 2 * orders
    slots = co.shape[1]
    quarter = n // kinds
    half = n // 2
    own = half * slots
    inner_kinds = ord_in.shape[0]
    pairs = kinds // 2
    jobs = kinds * chunks
    plane_rows = quarter * rows
    mesh_id = pl.DeviceIdType.MESH
    side = lax.div(me, half)
    place_in = lax.rem(me, half)
    column = lax.rem(me, quarter)
    inner = jnp.where(lax.div(me, quarter) == 1 + side, 1, 0)
    across = 1 - side

    def lanes(chunk):
        return pl.ds(chunk * LANES, LANES)

    def group(kind, at):
        return jnp.where(
            lax.rem(kind, 2) == 0, kind * quarter + at, (kind + 1) * quarter - 1 - at
        )

    def group_rows(kind, at):
        return pl.ds(pl.multiple_of(group(kind, at) * rows, rows), rows)

    def owner(kind, on_side, at):
        plane = jnp.where(kind < inner_kinds, 1 + on_side, (kinds - 1) * on_side)
        return plane * quarter + at

    def mine(kind):
        return jnp.where(kind < inner_kinds, 1, 0) == inner

    def job_of(job):
        per_pass = pairs * chunks
        inside = lax.rem(job, per_pass)
        kind = lax.div(job, per_pass) * pairs + lax.rem(inside, pairs)
        return kind, lax.div(inside, pairs), lax.rem(kind, inner_kinds)

    def first_block(kind):
        return group(kind, column) - own // orders

    def tail_blocks(kind, body):
        def one(block, carry):
            body(pl.multiple_of(block * orders, orders))
            return carry

        lax.fori_loop(first_block(kind), own // orders, one, 0)

    def await_tail(kind, view, sem):
        for first in range(own // orders):

            @pl.when(first_block(kind) == first)
            def _():
                await_bytes(view.at[pl.ds(0, own - first * orders)], sem)

    def job_at(kind, chunk):
        return (kind // pairs) * (pairs * chunks) + chunk * pairs + kind % pairs

    def load(chunk):
        return pltpu.make_async_copy(
            fields.at[0, :, :, lanes(chunk)], fbuf.at[chunk], load_sem.at[chunk]
        )

    def load_cot(chunk):
        return pltpu.make_async_copy(
            cotangent.at[0, :, :, lanes(chunk)], cbuf.at[chunk], load_sem.at[chunks + chunk]
        )

    load_w = pltpu.make_async_copy(weights, wbuf, load_sem.at[2 * chunks])
    for chunk in range(chunks):
        load(chunk).start()
    load_w.start()
    for chunk in range(chunks):
        load_cot(chunk).start()

    barrier = pltpu.get_barrier_semaphore()

    def greet(step, carry):
        peer = lax.rem(me + step, n)
        pl.semaphore_signal(barrier, inc=1, device_id={"lat": peer}, device_id_type=mesh_id)
        return carry

    lax.fori_loop(1, n, greet, 0)
    for step in range(1, nb):
        peer = lax.rem(me_b + step, nb)
        pl.semaphore_signal(barrier, inc=1, device_id={"batch": peer}, device_id_type=mesh_id)
    pl.semaphore_wait(barrier, n - 1 + nb - 1)

    def remote(stage, job, source, target, peer):
        pltpu.make_async_remote_copy(
            src_ref=source,
            dst_ref=target,
            send_sem=send_sem.at[stage, job],
            recv_sem=recv_sem.at[stage, job],
            device_id={"lat": peer},
            device_id_type=mesh_id,
        ).start()

    def await_bytes(view, sem):
        pltpu.make_async_copy(view, view, sem).wait()

    def to_owners(stage, kind, chunk, source, target, width):
        job = job_at(kind, chunk)
        for step in range(quarter):
            at = lax.rem(column + step, quarter)
            view = source.at[chunk, :, group_rows(kind, at), :]
            spot = target(kind % inner_kinds, chunk)
            peer = owner(kind, side, at)

            @pl.when(peer != me)
            def _():
                remote(stage, job, view, spot, peer)

            @pl.when(peer == me)
            def _():
                pltpu.make_async_copy(view, spot, recv_sem.at[stage, job]).start()

    def left_for_owners(stage, kind, chunk, source):
        job = job_at(kind, chunk)

        @pl.when(mine(kind))
        def _():
            await_bytes(source.at[chunk, :, 0 : plane_rows - rows, :], send_sem.at[stage, job])

        @pl.when(jnp.logical_not(mine(kind)))
        def _():
            await_bytes(source.at[chunk, :, 0:plane_rows, :], send_sem.at[stage, job])

    def from_owner(stage, job, kind, chunk, source, depth, target):
        place = lax.rem(kind, inner_kinds)
        spot = target.at[chunk, :, group_rows(kind, column), :]

        def send(step, carry):
            at = lax.rem(place_in + step, half)
            remote(
                stage, job, source.at[place, chunk, pl.ds(at * depth, depth)], spot,
                side * half + at,
            )
            return carry

        lax.fori_loop(1, half, send, 0)
        pltpu.make_async_copy(
            source.at[place, chunk, pl.ds(place_in * depth, depth)], spot, recv_sem.at[stage, job]
        ).start()

    def left_owner(stage, job, kind, chunk, source, depth):
        view = source.at[lax.rem(kind, inner_kinds), chunk, 0 : (half - 1) * depth]
        await_bytes(view, send_sem.at[stage, job])

    def reached_all(stage, kind, chunk, target):
        await_bytes(target.at[chunk, :, 0:plane_rows, :], recv_sem.at[stage, job_at(kind, chunk)])

    def lat_spot(place, chunk):
        return ord_in.at[place, chunk, pl.ds(place_in * lat_dev, lat_dev)]

    def slot_spot(place, chunk):
        return slot_all.at[place, chunk, pl.ds(me * slots, slots)]

    def wide_start(job):
        return pl.multiple_of(lax.rem(job, wide_b.shape[0] // wide_a.shape[0]) * wide_a.shape[0], 8)

    def widen(source, place, chunk, depth, count):
        def one(block, carry):
            piece = source[place, chunk, pl.ds(block * depth, depth)].astype(jnp.float32)
            wide_a[pl.ds(pl.multiple_of(block * depth * rows, depth * rows), depth * rows), :] = (
                piece.reshape(depth * rows, LANES)
            )
            return carry

        lax.fori_loop(0, count // depth, one, 0)

    def apply_table(tab, kind, kept, start, depth_in, depth_out, dims):
        def one(order, carry):
            real = wide_a[pl.ds(2 * order, depth_in, stride=rows), :]
            imag = wide_a[pl.ds(2 * order + 1, depth_in, stride=rows), :]
            both = jnp.concatenate([real, imag], axis=1).astype(jnp.bfloat16)
            result = dot(tab[kind, order, :kept], both, dims)
            wide_b[pl.ds(start + 2 * order, depth_out, stride=rows), :] = result[:, :LANES]
            wide_b[pl.ds(start + 2 * order + 1, depth_out, stride=rows), :] = result[:, LANES:]
            return carry

        lax.fori_loop(0, orders, one, 0)

    def narrow(target, place, chunk, start, depth, count):
        def one(block, carry):
            low = pl.multiple_of(start + block * depth * rows, 8)
            piece = wide_b[pl.ds(low, depth * rows), :]
            target[place, chunk, pl.ds(block * depth, depth)] = piece.reshape(
                depth, rows, LANES
            ).astype(jnp.bfloat16)
            return carry

        lax.fori_loop(0, count // depth, one, 0)

    def wide_rows(start, index, depth):
        return pl.ds(pl.multiple_of(start + index * rows, 8), depth * rows)

    def blank(first, count):
        def one(block, carry):
            by_name[pl.ds((first + block) * orders, orders)] = jnp.zeros(
                (orders, rows, LANES), jnp.bfloat16
            )
            return carry

        lax.fori_loop(0, count, one, 0)

    def analyse(base, tab, part, job):
        kind, chunk, place = job_of(job)

        @pl.when(mine(kind))
        def _():
            await_bytes(ord_in.at[place, chunk], recv_sem.at[base, job])
            widen(ord_in, place, chunk, lat_dev, side_lats)
            start = wide_start(job)
            peer = owner(kind, across, column)
            source = cross_out.at[place, chunk]
            target = cross_in.at[place, chunk]
            kept = own if part else degrees
            apply_table(tab, kind, kept, start, side_lats, kept, ((1,), (0,)))
            if not part:
                if base:
                    await_bytes(source, send_sem.at[1, job])
                narrow(cross_out, place, chunk, start + across * own * rows, slots, own)
                remote(base + 1, job, source, target, peer)
                return
            if base:
                await_tail(kind, source, send_sem.at[1, job])

            def send(low):
                span = pl.ds(low, orders)
                piece = wide_b[wide_rows(start, low, orders), :]
                cross_out[place, chunk, span] = piece.reshape(orders, rows, LANES).astype(
                    jnp.bfloat16
                )
                remote(base + 1, job, source.at[span], target.at[span], peer)

            tail_blocks(kind, send)

    def settle(base, target, part, job):
        kind, chunk, place = job_of(job)

        @pl.when(mine(kind))
        def _():
            start = wide_start(job)
            if part:
                await_tail(kind, cross_in.at[place, chunk], recv_sem.at[base + 1, job])
            else:
                await_bytes(cross_in.at[place, chunk], recv_sem.at[base + 1, job])
            if base:
                left_owner(2, job, kind, chunk, slot_out, slots)
                if part:
                    await_tail(kind, tail_out.at[chunk], send_sem.at[4, job])
                else:
                    await_bytes(slot_all.at[place, chunk, 0:own], send_sem.at[4, job])
            if part:

                blank(0, own // orders + first_block(kind))

                def add(low):
                    piece = wide_b[wide_rows(start, low, orders), :]
                    other = cross_in[place, chunk, pl.ds(low, orders)].astype(jnp.float32)
                    by_name[pl.ds(own + low, orders)] = (
                        piece.reshape(orders, rows, LANES) + other
                    ).astype(jnp.bfloat16)

                tail_blocks(kind, add)

                def pick(slot, carry):
                    slot_out[place, chunk, slot] = by_name[deg_ref[side * own + slot]]
                    return carry

                lax.fori_loop(0, own, pick, 0, unroll=4)
            else:

                def one(block, carry):
                    low = block * slots
                    piece = wide_b[wide_rows(start + side * own * rows, low, slots), :]
                    other = cross_in[place, chunk, pl.ds(low, slots)].astype(jnp.float32)
                    slot_out[place, chunk, pl.ds(low, slots)] = (
                        piece.reshape(slots, rows, LANES) + other
                    ).astype(jnp.bfloat16)
                    return carry

                lax.fori_loop(0, half, one, 0)
            from_owner(base + 2, job, kind, chunk, slot_out, slots, target)

    def relay(base, part, job):
        kind, chunk, place = job_of(job)

        @pl.when(mine(kind))
        def _():
            await_bytes(slot_all.at[place, chunk, 0:own], recv_sem.at[base + 3, job])
            peer = owner(kind, across, column)
            view = slot_all.at[place, chunk, pl.ds(side * own, own)]
            if not part:
                remote(base + 4, job, view, view, peer)
                return

            blank(across * (own // orders), own // orders)

            def copy(block, carry):
                span = pl.ds(side * own + block * slots, slots)
                by_name[span] = slot_all[place, chunk, span]
                return carry

            lax.fori_loop(0, half, copy, 0)

            def send(low):
                for step in range(orders):
                    tail_out[chunk, low + step] = by_name[slot_of[0, own + low + step]]
                span = pl.ds(low, orders)
                remote(base + 4, job, tail_out.at[chunk, span], view.at[span], peer)

            tail_blocks(kind, send)

    def synthesise(base, tab, part, job):
        kind, chunk, place = job_of(job)

        @pl.when(mine(kind))
        def _():
            start = wide_start(job)
            if part:
                await_tail(kind, tail_out.at[chunk], recv_sem.at[base + 4, job])

                def clear(block, carry):
                    wide_a[wide_rows(0, block * orders, orders), :] = jnp.zeros(
                        (orders * rows, LANES), jnp.float32
                    )
                    return carry

                lax.fori_loop(0, first_block(kind), clear, 0)

                def add(low):
                    near = tail_out[chunk, pl.ds(low, orders)].astype(jnp.float32)
                    far = slot_all[place, chunk, pl.ds(across * own + low, orders)]
                    wide_a[wide_rows(0, low, orders), :] = (
                        near + far.astype(jnp.float32)
                    ).reshape(orders * rows, LANES)

                tail_blocks(kind, add)
                apply_table(tab, kind, own, start, own, side_lats, ((0,), (0,)))
            else:
                await_bytes(slot_all.at[place, chunk, 0:own], recv_sem.at[base + 4, job])
                widen(slot_all, place, chunk, slots, degrees)
                apply_table(tab, kind, degrees, start, degrees, side_lats, ((0,), (0,)))
            if base:
                left_owner(5, job, kind, chunk, ord_out, lat_dev)
            narrow(ord_out, place, chunk, start, lat_dev, side_lats)
            from_owner(base + 5, job, kind, chunk, ord_out, lat_dev, band_in)

    def loop(low, high, body):
        def one(job, carry):
            body(job)
            return carry

        lax.fori_loop(low, high, one, 0)

    def pair(source, chunk, row):
        return jnp.concatenate([source[chunk, 2 * row], source[chunk, 2 * row + 1]], axis=1)

    def put_pair(target, chunk, row, values):
        values = values.astype(jnp.bfloat16)
        target[chunk, 2 * row] = values[:, :LANES]
        target[chunk, 2 * row + 1] = values[:, LANES:]

    def joined(source, slot, span):
        return jnp.concatenate([source[chunk, slot, span] for chunk in range(chunks)], axis=1)

    def mix(part, chunk):
        low = part * pairs * plane_rows
        span = slice(low, low + pairs * plane_rows)
        columns = slice(chunk * LANES, (chunk + 1) * LANES)

        def one(slot, carry):
            both = dot(
                joined(co, slot, span),
                jnp.concatenate([wbuf[slot, 0, :, columns], wbuf[slot, 1, :, columns]], axis=1),
            )
            crossed = pair_swap(both[:, LANES:], -1.0)
            mixed[chunk, slot, span] = (both[:, :LANES] + crossed).astype(jnp.bfloat16)
            return carry

        return one

    def adjoint(part, chunk):
        low = part * pairs * plane_rows
        span = slice(low, low + pairs * plane_rows)
        columns = slice(chunk * LANES, (chunk + 1) * LANES)

        def one(slot, carry):
            both = dot(
                joined(go, slot, span),
                jnp.concatenate([wbuf[slot, 0, columns, :], wbuf[slot, 1, columns, :]], axis=0),
                ((1,), (1,)),
            )
            crossed = pair_swap(both[:, LANES:], 1.0)
            mixed[chunk, slot, span] = (both[:, :LANES] + crossed).astype(jnp.bfloat16)
            return carry

        return one

    def filter_part(base, part, source, make):
        part_kinds = range(part * pairs, (part + 1) * pairs)
        for chunk in range(chunks):
            for kind in part_kinds:
                reached_all(base + 2, kind, chunk, source)
        for chunk in range(chunks):
            if base:
                for kind in part_kinds:
                    left_for_owners(3, kind, chunk, mixed)
            lax.fori_loop(0, slots, make(part, chunk), 0)
            for kind in part_kinds:
                to_owners(base + 3, kind, chunk, mixed, slot_spot, slots)

    per_pass = pairs * chunks
    lag = 2

    def to_filter(base, tab, source, make):
        for low, high, part, behind in (
            (0, lag, 0, None),
            (lag, per_pass, 0, 0),
            (per_pass, per_pass + lag, 1, 0),
            (per_pass + lag, jobs, 1, 1),
        ):

            def step(job):
                analyse(base, tab, part, job)
                if behind is not None:
                    settle(base, source, behind, job - lag)

            loop(low, high, step)
        filter_part(base, 0, source, make)
        settle(base, source, 1, jobs - lag)
        loop(0, per_pass, lambda job: relay(base, 0, job))
        for job in range(jobs - lag + 1, jobs):
            settle(base, source, 1, job)
        filter_part(base, 1, source, make)

    def from_filter(base, tab, finish):
        def step(job):
            synthesise(base, tab, 0, job)
            relay(base, 1, job + per_pass)

        loop(0, per_pass, step)
        for chunk in range(chunks):
            first = per_pass + chunk * pairs
            loop(first, first + pairs, lambda job: synthesise(base, tab, 1, job))
            if chunk:
                finish(chunk - 1)
        finish(chunks - 1)

    def spread(stage, chunk, part):
        for kind in range(part * pairs, (part + 1) * pairs):
            to_owners(stage, kind, chunk, band_out, lat_spot, lat_dev)

    for chunk in range(chunks):
        load(chunk).wait()

        def fourier(row, carry):
            put_pair(band_out, chunk, row, dot(fwd_fk[...], pair(fbuf, chunk, row)))
            return carry

        lax.fori_loop(0, lat_dev // 2, fourier, 0)
        spread(0, chunk, 0)
    for chunk in range(chunks):
        spread(0, chunk, 1)
    fill_tables(
        side, [group(kind, column) * orders for kind in range(kinds)], deg_ref, diag_ref, cos_ref,
        quad_ref, qtab, ptab, table, wide_b,
    )
    spots = lax.broadcasted_iota(jnp.int32, row_ref.shape, 1)

    def invert(slot, carry):
        return jnp.where(spots == deg_ref[slot], slot, carry)

    row_ref[...] = lax.fori_loop(0, degrees, invert, spots * 0, unroll=4)
    turn = pltpu.make_async_copy(row_ref, slot_of, load_sem.at[2 * chunks + 1])
    turn.start()
    turn.wait()
    load_w.wait()
    to_filter(0, qtab, co, mix)

    def between(chunk):
        load_cot(chunk).wait()
        for kind in range(kinds):
            reached_all(5, kind, chunk, band_in)
            left_for_owners(0, kind, chunk, band_out)

        def middle(row, carry):
            response = dot(inv_kf[...], pair(band_in, chunk, row))
            upstream = pair(cbuf, chunk, row).astype(jnp.float32) * gelu_slope(response)
            put_pair(band_out, chunk, row, dot(inv_fk[...], upstream.astype(jnp.bfloat16)))
            return carry

        lax.fori_loop(0, lat_dev // 2, middle, 0)
        spread(6, chunk, 0)

    from_filter(0, ptab, between)
    for chunk in range(chunks):
        spread(6, chunk, 1)
    to_filter(6, ptab, go, adjoint)

    def weight_grad(slot, carry):
        values = joined(co, slot, slice(None))
        grads = joined(go, slot, slice(None))
        turned = pair_swap(grads.astype(jnp.float32), 1.0).astype(jnp.bfloat16)
        span = ((0,), (0,))
        dw[slot, 0] = dot(values, grads, span).astype(jnp.bfloat16)
        dw[slot, 1] = dot(values, turned, span).astype(jnp.bfloat16)
        return carry

    lax.fori_loop(0, slots, weight_grad, 0)
    dw_copies = []
    for step in range(1, nb):
        peer = lax.rem(me_b + step, nb)
        copy = pltpu.make_async_remote_copy(
            src_ref=dw,
            dst_ref=dw_in.at[step - 1],
            send_sem=dw_send.at[step - 1],
            recv_sem=dw_recv.at[step - 1],
            device_id={"batch": peer},
            device_id_type=mesh_id,
        )
        copy.start()
        dw_copies.append(copy)

    def store(chunk):
        return pltpu.make_async_copy(
            cbuf.at[chunk], grad_out.at[0, :, :, lanes(chunk)], out_sem.at[chunk]
        )

    store_w = pltpu.make_async_copy(dw, dw_out, out_sem.at[chunks])

    def total(slot, carry):
        value = dw[slot].astype(jnp.float32)
        for step in range(nb - 1):
            value = value + dw_in[step, slot].astype(jnp.float32)
        dw[slot] = value.astype(jnp.bfloat16)
        return carry

    def last(chunk):
        if chunk == 0:
            for copy in dw_copies:
                copy.wait()
            lax.fori_loop(0, slots, total, 0)
            store_w.start()
        for kind in range(kinds):
            reached_all(11, kind, chunk, band_in)

        def finish(row, carry):
            delta = dot(fwd_kf[...], pair(band_in, chunk, row))
            put_pair(cbuf, chunk, row, pair(cbuf, chunk, row).astype(jnp.float32) + delta)
            return carry

        lax.fori_loop(0, lat_dev // 2, finish, 0)
        store(chunk).start()

    from_filter(6, qtab, last)
    for chunk in range(chunks):
        for kind in range(kinds):
            left_for_owners(6, kind, chunk, band_out)
            left_for_owners(9, kind, chunk, mixed)

    def drain(part, job):
        kind, chunk, place = job_of(job)

        @pl.when(mine(kind))
        def _():
            if part:
                await_tail(kind, cross_out.at[place, chunk], send_sem.at[7, job])
                await_tail(kind, tail_out.at[chunk], send_sem.at[10, job])
            else:
                await_bytes(cross_out.at[place, chunk], send_sem.at[7, job])
                await_bytes(slot_all.at[place, chunk, 0:own], send_sem.at[10, job])
            left_owner(8, job, kind, chunk, slot_out, slots)
            left_owner(11, job, kind, chunk, ord_out, lat_dev)

    loop(0, per_pass, lambda job: drain(0, job))
    loop(per_pass, jobs, lambda job: drain(1, job))
    for chunk in range(chunks):
        store(chunk).wait()
    store_w.wait()


def local_kernel(fields, cotangent, weights, degree_of):
    n = lax.axis_size("lat")
    nb = lax.axis_size("batch")
    kinds = 4
    if fields.shape[0] != 1 or fields.shape[1] % 2 or n % kinds or ORDERS != n * GROUP:
        return local(fields, cotangent, weights, degree_of)
    lat_dev, lons, channels = fields.shape[1:]
    slots = weights.shape[0]
    rows = 2 * GROUP
    chunks = channels // LANES
    floats, waves = constant_tables()
    side_lats = LATS // 2
    held = kinds - 1
    vmem = pl.BlockSpec(memory_space=pltpu.VMEM)
    anywhere = pl.BlockSpec(memory_space=pl.ANY)

    def buffer(*dims):
        return pltpu.VMEM(dims, jnp.bfloat16)

    dma = pltpu.SemaphoreType.DMA
    others = max(nb - 1, 1)
    wide_rows = max(side_lats, DEGREES) * rows
    return pl.pallas_call(
        functools.partial(block_kernel, n, nb),
        out_shape=(
            jax.ShapeDtypeStruct(fields.shape, jnp.bfloat16),
            jax.ShapeDtypeStruct(weights.shape, jnp.bfloat16),
        ),
        in_specs=[anywhere] * 3 + [pl.BlockSpec(memory_space=pltpu.SMEM)] + [vmem] * 7,
        out_specs=(anywhere, anywhere),
        scratch_shapes=[
            buffer(chunks, lat_dev, lons, LANES),
            buffer(chunks, lat_dev, lons, LANES),
            buffer(*weights.shape),
            buffer(chunks, lat_dev, n * rows, LANES),
            buffer(chunks, lat_dev, n * rows, LANES),
            buffer(held, chunks, side_lats, rows, LANES),
            buffer(held, chunks, side_lats, rows, LANES),
            buffer(held, chunks, DEGREES // 2, rows, LANES),
            buffer(held, chunks, DEGREES // 2, rows, LANES),
            buffer(held, chunks, DEGREES // 2, rows, LANES),
            buffer(held, chunks, DEGREES, rows, LANES),
            buffer(chunks, DEGREES // 2, rows, LANES),
            buffer(chunks, slots, n * rows, LANES),
            buffer(chunks, slots, n * rows, LANES),
            buffer(chunks, slots, n * rows, LANES),
            pltpu.VMEM((wide_rows, LANES), jnp.float32),
            pltpu.VMEM((3 * wide_rows, LANES), jnp.float32),
            buffer(*weights.shape),
            buffer(others, *weights.shape),
            buffer(kinds, GROUP, DEGREES, side_lats),
            buffer(kinds, GROUP, DEGREES, side_lats),
            pltpu.VMEM((DEGREES, kinds * GROUP, LANES), jnp.float32),
            pltpu.VMEM((GROUP, DEGREES), jnp.int32),
            pltpu.SMEM((GROUP, DEGREES), jnp.int32),
            buffer(DEGREES, rows, LANES),
            dma((2 * chunks + 2,)),
            dma((12, kinds * chunks)),
            dma((12, kinds * chunks)),
            dma((others,)),
            dma((others,)),
            dma((chunks + 1,)),
        ],
        compiler_params=pltpu.CompilerParams(
            collective_id=0, has_side_effects=True, vmem_limit_bytes=63 * 2**20
        ),
        name="filter_block",
    )(
        fields, cotangent, weights, degree_of, *floats, *waves,
    )


def local(fields, cotangent, weights, degree_of):
    samples = fields.shape[0]
    band_rows = fields.shape[1]
    ord_dev = ORDERS // lax.axis_size("lat")
    forward, inverse = fourier_tables(LONS, ORDERS)
    qslot, pslot = spectral_tables(lax.axis_index("lat") * ord_dev, ord_dev, degree_of)
    spectra = product("sikc,kf->ifsc", fields, forward).astype(jnp.bfloat16)
    spectra = spectra.reshape(band_rows, ORDERS, 2, samples, CHANNELS)
    gathered = to_orders(spectra)
    coeffs_local = product("mji,imrsc->jmrsc", qslot, gathered).astype(jnp.bfloat16)
    coeffs = to_degrees(coeffs_local)
    filtered = apply_filter(coeffs, weights)
    returned = back_to_orders(filtered)
    synth_local = product("mji,jmrsc->imrsc", pslot, returned).astype(jnp.bfloat16)
    synth = to_bands(synth_local)
    response = product(
        "ifsc,fk->sikc", synth.reshape(band_rows, 2 * ORDERS, samples, CHANNELS), inverse
    )
    activated, pullback = jax.vjp(jax.nn.gelu, response)
    upstream = pullback(cotangent.astype(jnp.float32))[0].astype(jnp.bfloat16)
    grad_synth = product("sikc,fk->ifsc", upstream, inverse).astype(jnp.bfloat16)
    grad_synth = grad_synth.reshape(band_rows, ORDERS, 2, samples, CHANNELS)
    grad_gathered = to_orders(grad_synth)
    grad_local = product("mji,imrsc->jmrsc", pslot, grad_gathered).astype(jnp.bfloat16)
    grad_filtered = to_degrees(grad_local)
    weight_total = lax.psum(filter_grad(coeffs, grad_filtered).astype(jnp.bfloat16), "batch")
    grad_coeffs = adjoint_filter(grad_filtered, weights)
    grad_back = back_to_orders(grad_coeffs)
    grad_local_spec = product("mji,jmrsc->imrsc", qslot, grad_back).astype(jnp.bfloat16)
    grad_bands = to_bands(grad_local_spec)
    delta = product(
        "ifsc,kf->sikc", grad_bands.reshape(band_rows, 2 * ORDERS, samples, CHANNELS), forward
    )
    grad_fields = (cotangent.astype(jnp.float32) + delta).astype(jnp.bfloat16)
    return (grad_fields, weight_total)


def solution(mesh):
    return jax.shard_map(
        local_kernel if CHANNELS % LANES == 0 else local,
        mesh=mesh,
        in_specs=(
            P("batch", "lat", None, None),
            P("batch", "lat", None, None),
            P("lat", None, None, None),
            P(),
        ),
        out_specs=(P("batch", "lat", None, None), P("lat", None, None, None)),
        check_vma=False,
    )
```

```python
import functools

import jax
import numpy as np
import jax.numpy as jnp
from jax import lax
from jax.experimental import pallas as pl
from jax.experimental.pallas import tpu as pltpu
from jax.sharding import PartitionSpec as P

LATS = 192
LONS = 384
ORDERS = 128
DEGREES = 128
CHANNELS = 384
LANES = 128
GROUP = 8


def table_kernel(deg_ref, diag_ref, cos_ref, quad_ref, order_ref, q_ref, p_ref, slot_ref, rows_ref):
    orders = diag_ref.shape[0]
    lats = q_ref.shape[2]
    degrees = deg_ref.shape[0]

    def invert(slot, carry):
        slot_ref[deg_ref[slot]] = slot
        return carry

    lax.fori_loop(0, degrees, invert, 0)
    order_real = order_ref[...]
    squared = order_real * order_real
    diagonal = diag_ref[...]
    cosine = cos_ref[...]
    first_lead = jnp.sqrt(2.0 * order_real + 3.0)
    halves = rows_ref.shape[0]

    def advance(degree, carry):
        previous, older = carry
        degree_real = degree.astype(jnp.float32)
        lead = jnp.sqrt(
            jnp.maximum(4.0 * degree_real * degree_real - 1.0, 0.0)
            / jnp.maximum(degree_real * degree_real - squared, 1.0)
        )
        lower = degree_real - 1.0
        back = jnp.sqrt(
            jnp.maximum(lower * lower - squared, 0.0) / jnp.maximum(4.0 * lower * lower - 1.0, 1.0)
        )
        general = lead * (cosine * previous - back * older)
        first = first_lead * cosine * previous
        value = jnp.where(
            degree_real == order_real,
            diagonal,
            jnp.where(
                degree_real == order_real + 1.0,
                first,
                jnp.where(degree_real > order_real + 1.0, general, 0.0),
            ),
        )
        slot = slot_ref[degree]
        for half in range(halves):
            rows_ref[half, pl.ds(slot, orders, stride=degrees), :] = value[
                :, half * LANES : (half + 1) * LANES
            ]
        return (value, previous)

    zeros = diagonal * 0.0
    lax.fori_loop(0, degrees, advance, (zeros, zeros), unroll=4)
    quadrature = quad_ref[...]
    for order in range(orders):
        for half in range(halves):
            low = half * LANES
            high = min(lats, low + LANES)
            chosen = rows_ref[half, order * degrees : (order + 1) * degrees, :][:, : high - low]
            p_ref[order, :, low:high] = chosen.astype(jnp.bfloat16)
            q_ref[order, :, low:high] = (chosen * quadrature[:, low:high]).astype(jnp.bfloat16)


def spectral_tables(start, ord_dev, degree_of):
    halves = -(-LATS // LANES)
    padded = halves * LANES
    order_col = (start + jnp.arange(ord_dev, dtype=jnp.int32)).astype(jnp.float32)[:, None]
    lat_ids = jnp.minimum(jnp.arange(padded, dtype=jnp.float32), LATS - 1.0)
    colatitude = jnp.pi * (lat_ids + 0.5) / LATS
    sine = jnp.sin(colatitude)[None, :]
    steps_up = jnp.arange(1, DEGREES + 1, dtype=jnp.float32)[None, :]
    factor = jnp.where(
        steps_up <= order_col, 0.5 * jnp.log((2.0 * steps_up + 1.0) / (2.0 * steps_up)), 0.0
    )
    log_start = 0.5 * jnp.log(1.0 / (4.0 * jnp.pi)) + jnp.sum(factor, axis=1, keepdims=True)
    diagonal = jnp.exp(log_start + order_col * jnp.log(sine))
    cosine = jnp.broadcast_to(jnp.cos(colatitude)[None, :], diagonal.shape)
    quadrature = 2.0 * jnp.pi * jnp.pi / LATS * sine
    orders = jnp.broadcast_to(order_col, diagonal.shape)
    vmem = pl.BlockSpec(memory_space=pltpu.VMEM)
    shape = jax.ShapeDtypeStruct((ord_dev, DEGREES, LATS), jnp.bfloat16)
    return pl.pallas_call(
        table_kernel,
        out_shape=(shape, shape),
        in_specs=[pl.BlockSpec(memory_space=pltpu.SMEM)] + [vmem] * 4,
        out_specs=(vmem, vmem),
        scratch_shapes=[
            pltpu.SMEM((DEGREES,), jnp.int32),
            pltpu.VMEM((halves, ord_dev * DEGREES, LANES), jnp.float32),
        ],
        name="legendre_tables",
    )(degree_of, diagonal, cosine, quadrature, orders)


def fourier_tables(lon_count, order_count):
    lon_ids = jnp.arange(lon_count, dtype=jnp.int32)[:, None]
    order_ids = jnp.arange(order_count, dtype=jnp.int32)[None, :]
    phase = 2.0 * jnp.pi * (lon_ids * order_ids % lon_count).astype(jnp.float32) / lon_count
    forward = (
        jnp.stack([jnp.cos(phase), -jnp.sin(phase)], axis=2).reshape(lon_count, 2 * order_count)
        / lon_count
    )
    doubled = jnp.where(order_ids == 0, 1.0, 2.0)
    inverse = jnp.stack([doubled * jnp.cos(phase), -doubled * jnp.sin(phase)], axis=2).reshape(
        lon_count, 2 * order_count
    )
    return (forward.astype(jnp.bfloat16), jnp.transpose(inverse).astype(jnp.bfloat16))


def to_orders(values):
    return lax.all_to_all(values, "lat", split_axis=1, concat_axis=0, tiled=True)


def to_degrees(values):
    return lax.all_to_all(values, "lat", split_axis=0, concat_axis=1, tiled=True)


def back_to_orders(values):
    return lax.all_to_all(values, "lat", split_axis=1, concat_axis=0, tiled=True)


def to_bands(values):
    return lax.all_to_all(values, "lat", split_axis=0, concat_axis=1, tiled=True)


def product(spec, left, right):
    return jnp.einsum(spec, left, right, preferred_element_type=jnp.float32)


def apply_filter(coeffs, weights):
    c_real = coeffs[:, :, 0]
    c_imag = coeffs[:, :, 1]
    w_real = weights[:, 0]
    w_imag = weights[:, 1]
    f_real = product("jmsc,jcd->jmsd", c_real, w_real) - product("jmsc,jcd->jmsd", c_imag, w_imag)
    f_imag = product("jmsc,jcd->jmsd", c_real, w_imag) + product("jmsc,jcd->jmsd", c_imag, w_real)
    return jnp.stack([f_real, f_imag], axis=2).astype(jnp.bfloat16)


def adjoint_filter(grads, weights):
    g_real = grads[:, :, 0]
    g_imag = grads[:, :, 1]
    w_real = weights[:, 0]
    w_imag = weights[:, 1]
    a_real = product("jmsd,jcd->jmsc", g_real, w_real) + product("jmsd,jcd->jmsc", g_imag, w_imag)
    a_imag = product("jmsd,jcd->jmsc", g_imag, w_real) - product("jmsd,jcd->jmsc", g_real, w_imag)
    return jnp.stack([a_real, a_imag], axis=2).astype(jnp.bfloat16)


def filter_grad(coeffs, grads):
    c_real = coeffs[:, :, 0]
    c_imag = coeffs[:, :, 1]
    g_real = grads[:, :, 0]
    g_imag = grads[:, :, 1]
    dw_real = product("jmsc,jmsd->jcd", c_real, g_real) + product("jmsc,jmsd->jcd", c_imag, g_imag)
    dw_imag = product("jmsc,jmsd->jcd", c_real, g_imag) - product("jmsc,jmsd->jcd", c_imag, g_real)
    return jnp.stack([dw_real, dw_imag], axis=1)


def constant_tables():
    sides = 2
    half = LATS // sides
    lat_ids = np.minimum(np.arange(LANES)[None, :], half - 1) + half * np.arange(sides)[:, None]
    colatitude = np.pi * (lat_ids + 0.5) / LATS
    sine = np.sin(colatitude)[:, None, :]
    ids = np.arange(ORDERS)
    steps_up = np.arange(1, ORDERS + 1)
    growth = np.cumsum(0.5 * np.log((2.0 * steps_up + 1.0) / (2.0 * steps_up)))
    log_start = 0.5 * np.log(1.0 / (4.0 * np.pi)) + np.concatenate([[0.0], growth[:-1]])
    diagonal = np.exp(log_start[None, :, None] + ids[None, :, None] * np.log(sine))
    cosine = np.broadcast_to(np.cos(colatitude)[:, None, :], (sides, GROUP, LANES))
    quadrature = np.broadcast_to(2.0 * np.pi * np.pi / LATS * sine, (sides, GROUP, LANES))
    phase = 2.0 * np.pi * (np.arange(LONS)[:, None] * ids[None, :] % LONS) / LONS
    forward = np.stack([np.cos(phase), -np.sin(phase)], axis=2).reshape(LONS, -1) / LONS
    doubled = np.where(ids == 0, 1.0, 2.0)[None, :]
    inverse = np.stack([doubled * np.cos(phase), -doubled * np.sin(phase)], axis=2)
    inverse = inverse.reshape(LONS, -1)
    floats = [jnp.asarray(t, jnp.float32) for t in (diagonal, cosine, quadrature)]
    waves = [forward.T, forward, inverse.T, inverse]
    halves = [jnp.asarray(np.float32(t).astype(jnp.bfloat16)) for t in waves]
    return floats, halves


def fill_tables(side, firsts, deg_ref, diag_ref, cos_ref, quad_ref, qtab, ptab, table, by_slot):
    kinds, orders, degrees, lats = qtab.shape
    every = kinds * orders
    cosine = cos_ref[side]
    diagonal, ids, squared, first_lead = [], [], [], []
    for first in firsts:
        diagonal.append(diag_ref[side, pl.ds(pl.multiple_of(first, orders), orders), :])
        ids.append(first + lax.broadcasted_iota(jnp.int32, cosine.shape, 0))
        real = ids[-1].astype(jnp.float32)
        squared.append(real * real)
        first_lead.append(jnp.sqrt(2.0 * real + 3.0))

    def advance(degree, carry):
        degree_real = degree.astype(jnp.float32)
        lower = degree_real - 1.0
        state = []
        for kind in range(kinds):
            previous, older = carry[kind]
            lead = jnp.sqrt(
                jnp.maximum(4.0 * degree_real * degree_real - 1.0, 0.0)
                / jnp.maximum(degree_real * degree_real - squared[kind], 1.0)
            )
            back = jnp.sqrt(
                jnp.maximum(lower * lower - squared[kind], 0.0)
                / jnp.maximum(4.0 * lower * lower - 1.0, 1.0)
            )
            general = lead * (cosine * previous - back * older)
            first = first_lead[kind] * cosine * previous
            value = jnp.where(
                ids[kind] == degree,
                diagonal[kind],
                jnp.where(
                    ids[kind] + 1 == degree,
                    first,
                    jnp.where(ids[kind] + 1 < degree, general, 0.0),
                ),
            )
            table[degree, kind * orders : (kind + 1) * orders, :] = value
            state.append((value, previous))
        return tuple(state)

    zeros = cosine * 0.0
    lax.fori_loop(0, degrees, advance, ((zeros, zeros),) * kinds)

    ahead = every // 2
    tail = degrees // 2

    def place(slot, carry):
        by_slot[pl.ds(slot, ahead, stride=degrees), :] = table[deg_ref[slot], :ahead]
        return carry

    lax.fori_loop(0, degrees, place, 0, unroll=4)

    def place_tail(row, carry):
        spots = pl.ds(ahead * degrees + row, ahead, stride=degrees)
        by_slot[spots, :] = table[tail + row, ahead:]
        return carry

    lax.fori_loop(0, tail, place_tail, 0, unroll=4)
    quadrature = quad_ref[side][:1, :lats]
    for kind in range(kinds):

        def keep(order, carry):
            start = pl.multiple_of((kind * orders + order) * degrees, degrees)
            depth = degrees if kind < kinds // 2 else tail
            chosen = by_slot[pl.ds(start, depth), :][:, :lats]
            ptab[kind, order, :depth] = chosen.astype(jnp.bfloat16)
            qtab[kind, order, :depth] = (chosen * quadrature).astype(jnp.bfloat16)
            return carry

        lax.fori_loop(0, orders, keep, 0)


def pair_swap(values, even_sign):
    rows = values.shape[0]
    even = lax.broadcasted_iota(jnp.int32, values.shape, 0) % 2 == 0
    above = pltpu.roll(values, rows - 1, 0)
    below = pltpu.roll(values, 1, 0)
    return jnp.where(even, even_sign * above, -even_sign * below)


def gelu_slope(x):
    scale = 0.7978845608028654
    square = x * x
    t = jnp.tanh(scale * (x + 0.044715 * x * square))
    return 0.5 * (1.0 + t) + 0.5 * x * (1.0 - t * t) * (scale * (1.0 + 0.134145 * square))


def dot(left, right, dims=((1,), (0,))):
    return lax.dot_general(left, right, (dims, ((), ())), preferred_element_type=jnp.float32)


def block_kernel(
    n, nb, fields, cotangent, weights, deg_ref, diag_ref, cos_ref, quad_ref,
    fwd_fk, fwd_kf, inv_fk, inv_kf,
    grad_out, dw_out,
    fbuf, cbuf, wbuf, band_out, band_in, ord_in, ord_out, cross_out, cross_in, slot_out, slot_all,
    tail_out, co, go, mixed, wide_a, wide_b, wide_c, dw, dw_in, qtab, ptab, table, row_ref, slot_of, by_name,
    load_sem, send_sem, recv_sem, dw_send, dw_recv, out_sem,
):
    me = lax.axis_index("lat")
    me_b = lax.axis_index("batch")
    chunks, lat_dev = fbuf.shape[0], fbuf.shape[1]
    kinds, orders, degrees, side_lats = qtab.shape
    rows = 2 * orders
    slots = co.shape[1]
    quarter = n // kinds
    half = n // 2
    own = half * slots
    inner_kinds = ord_in.shape[0]
    pairs = kinds // 2
    jobs = kinds * chunks
    plane_rows = quarter * rows
    mesh_id = pl.DeviceIdType.MESH
    side = lax.div(me, half)
    place_in = lax.rem(me, half)
    column = lax.rem(me, quarter)
    inner = jnp.where(lax.div(me, quarter) == 1 + side, 1, 0)
    across = 1 - side

    def lanes(chunk):
        return pl.ds(chunk * LANES, LANES)

    def group(kind, at):
        return jnp.where(
            lax.rem(kind, 2) == 0, kind * quarter + at, (kind + 1) * quarter - 1 - at
        )

    def group_rows(kind, at):
        return pl.ds(pl.multiple_of(group(kind, at) * rows, rows), rows)

    def owner(kind, on_side, at):
        plane = jnp.where(kind < inner_kinds, 1 + on_side, (kinds - 1) * on_side)
        return plane * quarter + at

    def mine(kind):
        return jnp.where(kind < inner_kinds, 1, 0) == inner

    def job_of(job):
        per_pass = pairs * chunks
        inside = lax.rem(job, per_pass)
        kind = lax.div(job, per_pass) * pairs + lax.rem(inside, pairs)
        return kind, lax.div(inside, pairs), lax.rem(kind, inner_kinds)

    def first_block(kind):
        return group(kind, column) - own // orders

    def tail_blocks(kind, body):
        def one(block, carry):
            body(pl.multiple_of(block * orders, orders))
            return carry

        lax.fori_loop(first_block(kind), own // orders, one, 0)

    def await_tail(kind, view, sem):
        for first in range(own // orders):

            @pl.when(first_block(kind) == first)
            def _():
                await_bytes(view.at[pl.ds(0, own - first * orders)], sem)

    def job_at(kind, chunk):
        return (kind // pairs) * (pairs * chunks) + chunk * pairs + kind % pairs

    def load(chunk):
        return pltpu.make_async_copy(
            fields.at[0, :, :, lanes(chunk)], fbuf.at[chunk], load_sem.at[chunk]
        )

    def load_cot(chunk):
        return pltpu.make_async_copy(
            cotangent.at[0, :, :, lanes(chunk)], cbuf.at[chunk], load_sem.at[chunks + chunk]
        )

    load_w = pltpu.make_async_copy(weights, wbuf, load_sem.at[2 * chunks])
    for chunk in range(chunks):
        load(chunk).start()
    load_w.start()
    for chunk in range(chunks):
        load_cot(chunk).start()

    barrier = pltpu.get_barrier_semaphore()

    def greet(step, carry):
        peer = lax.rem(me + step, n)
        pl.semaphore_signal(barrier, inc=1, device_id={"lat": peer}, device_id_type=mesh_id)
        return carry

    lax.fori_loop(1, n, greet, 0)
    for step in range(1, nb):
        peer = lax.rem(me_b + step, nb)
        pl.semaphore_signal(barrier, inc=1, device_id={"batch": peer}, device_id_type=mesh_id)

    def remote(stage, job, source, target, peer):
        pltpu.make_async_remote_copy(
            src_ref=source,
            dst_ref=target,
            send_sem=send_sem.at[stage, job],
            recv_sem=recv_sem.at[stage, job],
            device_id={"lat": peer},
            device_id_type=mesh_id,
        ).start()

    def await_bytes(view, sem):
        pltpu.make_async_copy(view, view, sem).wait()

    def to_owners(stage, kind, chunk, source, target, width):
        job = job_at(kind, chunk)
        for step in range(quarter):
            at = lax.rem(column + step, quarter)
            view = source.at[chunk, :, group_rows(kind, at), :]
            spot = target(kind % inner_kinds, chunk)
            peer = owner(kind, side, at)

            @pl.when(peer != me)
            def _():
                remote(stage, job, view, spot, peer)

            @pl.when(peer == me)
            def _():
                pltpu.make_async_copy(view, spot, recv_sem.at[stage, job]).start()

    def left_for_owners(stage, kind, chunk, source):
        job = job_at(kind, chunk)

        @pl.when(mine(kind))
        def _():
            await_bytes(source.at[chunk, :, 0 : plane_rows - rows, :], send_sem.at[stage, job])

        @pl.when(jnp.logical_not(mine(kind)))
        def _():
            await_bytes(source.at[chunk, :, 0:plane_rows, :], send_sem.at[stage, job])

    def from_owner(stage, job, kind, chunk, source, depth, target):
        place = lax.rem(kind, inner_kinds)
        spot = target.at[chunk, :, group_rows(kind, column), :]

        def send(step, carry):
            at = lax.rem(place_in + step, half)
            remote(
                stage, job, source.at[place, chunk, pl.ds(at * depth, depth)], spot,
                side * half + at,
            )
            return carry

        lax.fori_loop(1, half, send, 0)
        pltpu.make_async_copy(
            source.at[place, chunk, pl.ds(place_in * depth, depth)], spot, recv_sem.at[stage, job]
        ).start()

    def left_owner(stage, job, kind, chunk, source, depth):
        view = source.at[lax.rem(kind, inner_kinds), chunk, 0 : (half - 1) * depth]
        await_bytes(view, send_sem.at[stage, job])

    def reached_all(stage, kind, chunk, target):
        await_bytes(target.at[chunk, :, 0:plane_rows, :], recv_sem.at[stage, job_at(kind, chunk)])

    def lat_spot(place, chunk):
        return ord_in.at[place, chunk, pl.ds(place_in * lat_dev, lat_dev)]

    def slot_spot(place, chunk):
        return slot_all.at[place, chunk, pl.ds(me * slots, slots)]

    def wide_start(part, job):
        if part:
            spot = lax.rem(lax.div(job - pairs * chunks, pairs) + pairs, chunks)
        else:
            spot = jnp.where(job < 2 * pairs, lax.rem(job, pairs), job - pairs)
        return pl.multiple_of(spot * wide_a.shape[0], 8)

    def widen(source, place, chunk, depth, count):
        def one(block, carry):
            piece = source[place, chunk, pl.ds(block * depth, depth)].astype(jnp.float32)
            wide_a[pl.ds(pl.multiple_of(block * depth * rows, depth * rows), depth * rows), :] = (
                piece.reshape(depth * rows, LANES)
            )
            return carry

        lax.fori_loop(0, count // depth, one, 0)

    def apply_table(tab, kind, kept, result_ref, start, depth_in, depth_out, dims):
        def one(order, carry):
            real = wide_a[pl.ds(2 * order, depth_in, stride=rows), :]
            imag = wide_a[pl.ds(2 * order + 1, depth_in, stride=rows), :]
            both = jnp.concatenate([real, imag], axis=1).astype(jnp.bfloat16)
            result = dot(tab[kind, order, :kept], both, dims)
            result_ref[pl.ds(start + 2 * order, depth_out, stride=rows), :] = result[:, :LANES]
            result_ref[pl.ds(start + 2 * order + 1, depth_out, stride=rows), :] = result[:, LANES:]
            return carry

        lax.fori_loop(0, orders, one, 0)

    def narrow(source, target, place, chunk, start, depth, count):
        def one(block, carry):
            low = pl.multiple_of(start + block * depth * rows, 8)
            piece = source[pl.ds(low, depth * rows), :]
            target[place, chunk, pl.ds(block * depth, depth)] = piece.reshape(
                depth, rows, LANES
            ).astype(jnp.bfloat16)
            return carry

        lax.fori_loop(0, count // depth, one, 0)

    def wide_rows(start, index, depth):
        return pl.ds(pl.multiple_of(start + index * rows, 8), depth * rows)

    def blank(first, count):
        def one(block, carry):
            by_name[pl.ds((first + block) * orders, orders)] = jnp.zeros(
                (orders, rows, LANES), jnp.bfloat16
            )
            return carry

        lax.fori_loop(0, count, one, 0)

    def analyse(base, tab, part, job):
        kind, chunk, place = job_of(job)

        @pl.when(mine(kind))
        def _():
            await_bytes(ord_in.at[place, chunk], recv_sem.at[base, job])
            widen(ord_in, place, chunk, lat_dev, side_lats)
            start = wide_start(part, job)
            peer = owner(kind, across, column)
            source = cross_out.at[place, chunk]
            target = cross_in.at[place, chunk]
            kept = own if part else degrees
            apply_table(tab, kind, kept, wide_b, start, side_lats, kept, ((1,), (0,)))
            if not part:
                if base:
                    await_bytes(source, send_sem.at[1, job])
                narrow(wide_b, cross_out, place, chunk, start + across * own * rows, slots, own)
                remote(base + 1, job, source, target, peer)
                return
            if base:
                await_tail(kind, source, send_sem.at[1, job])

            def send(low):
                span = pl.ds(low, orders)
                piece = wide_b[wide_rows(start, low, orders), :]
                cross_out[place, chunk, span] = piece.reshape(orders, rows, LANES).astype(
                    jnp.bfloat16
                )
                remote(base + 1, job, source.at[span], target.at[span], peer)

            tail_blocks(kind, send)

    def settle(base, target, part, job):
        kind, chunk, place = job_of(job)

        @pl.when(mine(kind))
        def _():
            start = wide_start(part, job)
            if part:
                await_tail(kind, cross_in.at[place, chunk], recv_sem.at[base + 1, job])
            else:
                await_bytes(cross_in.at[place, chunk], recv_sem.at[base + 1, job])
            if base:
                left_owner(2, job, kind, chunk, slot_out, slots)
                if part:
                    await_tail(kind, tail_out.at[chunk], send_sem.at[4, job])
                else:
                    await_bytes(slot_all.at[place, chunk, 0:own], send_sem.at[4, job])
            if part:

                blank(0, own // orders + first_block(kind))

                def add(low):
                    piece = wide_b[wide_rows(start, low, orders), :]
                    other = cross_in[place, chunk, pl.ds(low, orders)].astype(jnp.float32)
                    by_name[pl.ds(own + low, orders)] = (
                        piece.reshape(orders, rows, LANES) + other
                    ).astype(jnp.bfloat16)

                tail_blocks(kind, add)

                def pick(slot, carry):
                    slot_out[place, chunk, slot] = by_name[deg_ref[side * own + slot]]
                    return carry

                lax.fori_loop(0, own, pick, 0, unroll=4)
            else:

                def one(block, carry):
                    low = block * slots
                    piece = wide_b[wide_rows(start + side * own * rows, low, slots), :]
                    other = cross_in[place, chunk, pl.ds(low, slots)].astype(jnp.float32)
                    slot_out[place, chunk, pl.ds(low, slots)] = (
                        piece.reshape(slots, rows, LANES) + other
                    ).astype(jnp.bfloat16)
                    return carry

                lax.fori_loop(0, half, one, 0)
            from_owner(base + 2, job, kind, chunk, slot_out, slots, target)

    def relay(base, part, job):
        kind, chunk, place = job_of(job)

        @pl.when(mine(kind))
        def _():
            await_bytes(slot_all.at[place, chunk, 0:own], recv_sem.at[base + 3, job])
            peer = owner(kind, across, column)
            view = slot_all.at[place, chunk, pl.ds(side * own, own)]
            if not part:
                remote(base + 4, job, view, view, peer)
                return

            blank(across * (own // orders), own // orders)

            def copy(block, carry):
                span = pl.ds(side * own + block * slots, slots)
                by_name[span] = slot_all[place, chunk, span]
                return carry

            lax.fori_loop(0, half, copy, 0)

            def send(low):
                for step in range(orders):
                    tail_out[chunk, low + step] = by_name[slot_of[0, own + low + step]]
                span = pl.ds(low, orders)
                remote(base + 4, job, tail_out.at[chunk, span], view.at[span], peer)

            tail_blocks(kind, send)

    def synthesise(base, tab, part, job):
        kind, chunk, place = job_of(job)

        @pl.when(mine(kind))
        def _():
            if part:
                await_tail(kind, tail_out.at[chunk], recv_sem.at[base + 4, job])

                def clear(block, carry):
                    wide_a[wide_rows(0, block * orders, orders), :] = jnp.zeros(
                        (orders * rows, LANES), jnp.float32
                    )
                    return carry

                lax.fori_loop(0, first_block(kind), clear, 0)

                def add(low):
                    near = tail_out[chunk, pl.ds(low, orders)].astype(jnp.float32)
                    far = slot_all[place, chunk, pl.ds(across * own + low, orders)]
                    wide_a[wide_rows(0, low, orders), :] = (
                        near + far.astype(jnp.float32)
                    ).reshape(orders * rows, LANES)

                tail_blocks(kind, add)
                apply_table(tab, kind, own, wide_c, 0, own, side_lats, ((0,), (0,)))
            else:
                await_bytes(slot_all.at[place, chunk, 0:own], recv_sem.at[base + 4, job])
                widen(slot_all, place, chunk, slots, degrees)
                apply_table(tab, kind, degrees, wide_c, 0, degrees, side_lats, ((0,), (0,)))
            if base:
                left_owner(5, job, kind, chunk, ord_out, lat_dev)
            narrow(wide_c, ord_out, place, chunk, 0, lat_dev, side_lats)
            from_owner(base + 5, job, kind, chunk, ord_out, lat_dev, band_in)

    def loop(low, high, body):
        def one(job, carry):
            body(job)
            return carry

        lax.fori_loop(low, high, one, 0)

    def pair(source, chunk, row):
        return jnp.concatenate([source[chunk, 2 * row], source[chunk, 2 * row + 1]], axis=1)

    def put_pair(target, chunk, row, values):
        values = values.astype(jnp.bfloat16)
        target[chunk, 2 * row] = values[:, :LANES]
        target[chunk, 2 * row + 1] = values[:, LANES:]

    def joined(source, slot, span):
        return jnp.concatenate([source[chunk, slot, span] for chunk in range(chunks)], axis=1)

    def mix(part, chunk):
        low = part * pairs * plane_rows
        span = slice(low, low + pairs * plane_rows)
        columns = slice(chunk * LANES, (chunk + 1) * LANES)

        def one(slot, carry):
            both = dot(
                joined(co, slot, span),
                jnp.concatenate([wbuf[slot, 0, :, columns], wbuf[slot, 1, :, columns]], axis=1),
            )
            crossed = pair_swap(both[:, LANES:], -1.0)
            mixed[chunk, slot, span] = (both[:, :LANES] + crossed).astype(jnp.bfloat16)
            return carry

        return one

    def adjoint(part, chunk):
        low = part * pairs * plane_rows
        span = slice(low, low + pairs * plane_rows)
        columns = slice(chunk * LANES, (chunk + 1) * LANES)

        def one(slot, carry):
            both = dot(
                joined(go, slot, span),
                jnp.concatenate([wbuf[slot, 0, columns, :], wbuf[slot, 1, columns, :]], axis=0),
                ((1,), (1,)),
            )
            crossed = pair_swap(both[:, LANES:], 1.0)
            mixed[chunk, slot, span] = (both[:, :LANES] + crossed).astype(jnp.bfloat16)
            return carry

        return one

    def filter_part(base, part, source, make):
        part_kinds = range(part * pairs, (part + 1) * pairs)
        for chunk in range(chunks):
            for kind in part_kinds:
                reached_all(base + 2, kind, chunk, source)
        for chunk in range(chunks):
            if base:
                for kind in part_kinds:
                    left_for_owners(3, kind, chunk, mixed)
            lax.fori_loop(0, slots, make(part, chunk), 0)
            for kind in part_kinds:
                to_owners(base + 3, kind, chunk, mixed, slot_spot, slots)

    per_pass = pairs * chunks
    def unit(part, chunk):
        first = part * per_pass + chunk * pairs
        return first, first + pairs

    def run(spans, body):
        loop(spans[0], spans[1], body)

    def to_filter_start(base, tab, source):
        run(unit(0, 0), lambda job: analyse(base, tab, 0, job))
        for low, high, part, behind in (
            (pairs, per_pass, 0, 0),
            (per_pass, per_pass + pairs, 1, 0),
            (per_pass + pairs, per_pass + 2 * pairs, 1, 1),
        ):

            def step(job):
                settle(base, source, behind, job - pairs)
                analyse(base, tab, part, job)

            loop(low, high, step)
        loop(per_pass + 2 * pairs, jobs, lambda job: analyse(base, tab, 1, job))

    def through_filter(base, tab, source, make):
        filter_part(base, 0, source, make)
        run(unit(1, 1), lambda job: settle(base, source, 1, job))
        run(unit(0, 0), lambda job: relay(base, 0, job))
        run(unit(1, 2), lambda job: settle(base, source, 1, job))
        run(unit(0, 1), lambda job: relay(base, 0, job))
        filter_part(base, 1, source, make)
        run(unit(0, 0), lambda job: synthesise(base, tab, 0, job))
        run(unit(1, 0), lambda job: relay(base, 1, job))
        run(unit(0, 2), lambda job: relay(base, 0, job))
        loop(per_pass + pairs, jobs, lambda job: relay(base, 1, job))

    def spread(stage, chunk, part):
        for kind in range(part * pairs, (part + 1) * pairs):
            to_owners(stage, kind, chunk, band_out, lat_spot, lat_dev)

    fill_tables(
        side, [group(kind, column) * orders for kind in range(kinds)], deg_ref, diag_ref, cos_ref,
        quad_ref, qtab, ptab, table, wide_b,
    )
    for chunk in range(chunks):
        load(chunk).wait()

        def fourier(row, carry):
            put_pair(band_out, chunk, row, dot(fwd_fk[...], pair(fbuf, chunk, row)))
            return carry

        lax.fori_loop(0, lat_dev // 2, fourier, 0)
        if chunk == 0:
            pl.semaphore_wait(barrier, n - 1 + nb - 1)
        spread(0, chunk, 0)
    for chunk in range(chunks):
        spread(0, chunk, 1)
    spots = lax.broadcasted_iota(jnp.int32, row_ref.shape, 1)

    def invert(slot, carry):
        return jnp.where(spots == deg_ref[slot], slot, carry)

    row_ref[...] = lax.fori_loop(0, degrees, invert, spots * 0, unroll=4)
    turn = pltpu.make_async_copy(row_ref, slot_of, load_sem.at[2 * chunks + 1])
    turn.start()
    turn.wait()
    load_w.wait()
    to_filter_start(0, qtab, co)
    through_filter(0, ptab, co, mix)

    def between(chunk):
        load_cot(chunk).wait()
        for kind in range(kinds):
            reached_all(5, kind, chunk, band_in)
            left_for_owners(0, kind, chunk, band_out)

        def middle(row, carry):
            response = dot(inv_kf[...], pair(band_in, chunk, row))
            upstream = pair(cbuf, chunk, row).astype(jnp.float32) * gelu_slope(response)
            put_pair(band_out, chunk, row, dot(inv_fk[...], upstream.astype(jnp.bfloat16)))
            return carry

        lax.fori_loop(0, lat_dev // 2, middle, 0)
        spread(6, chunk, 0)
        spread(6, chunk, 1)

    def forth(part, low, high):
        loop(low, high, lambda job: analyse(6, ptab, part, job))

    def back(part, low, high):
        loop(low, high, lambda job: settle(6, go, part, job))

    def synth(base, tab, part, low, high):
        loop(low, high, lambda job: synthesise(base, tab, part, job))

    far = per_pass
    synth(0, ptab, 0, 2, 4)
    synth(0, ptab, 1, far, far + 2)
    synth(0, ptab, 0, 4, 5)
    between(0)
    synth(0, ptab, 0, 5, 6)
    forth(0, 0, 2)
    synth(0, ptab, 1, far + 2, far + 4)
    forth(1, far, far + 2)
    synth(0, ptab, 1, far + 4, far + 6)
    between(1)
    back(0, 0, 1)
    between(2)
    back(0, 1, 2)
    forth(0, 2, 4)
    back(1, far, far + 2)
    forth(0, 4, 6)
    back(0, 2, 4)
    forth(1, far + 2, far + 6)
    back(0, 4, 6)
    through_filter(6, qtab, go, adjoint)

    def weight_grad(slot, carry):
        values = joined(co, slot, slice(None))
        grads = joined(go, slot, slice(None))
        turned = pair_swap(grads.astype(jnp.float32), 1.0).astype(jnp.bfloat16)
        span = ((0,), (0,))
        dw[slot, 0] = dot(values, grads, span).astype(jnp.bfloat16)
        dw[slot, 1] = dot(values, turned, span).astype(jnp.bfloat16)
        return carry

    lax.fori_loop(0, slots, weight_grad, 0)
    dw_copies = []
    for step in range(1, nb):
        peer = lax.rem(me_b + step, nb)
        copy = pltpu.make_async_remote_copy(
            src_ref=dw,
            dst_ref=dw_in.at[step - 1],
            send_sem=dw_send.at[step - 1],
            recv_sem=dw_recv.at[step - 1],
            device_id={"batch": peer},
            device_id_type=mesh_id,
        )
        copy.start()
        dw_copies.append(copy)

    def store(chunk):
        return pltpu.make_async_copy(
            cbuf.at[chunk], grad_out.at[0, :, :, lanes(chunk)], out_sem.at[chunk]
        )

    store_w = pltpu.make_async_copy(dw, dw_out, out_sem.at[chunks])

    def total(slot, carry):
        value = dw[slot].astype(jnp.float32)
        for step in range(nb - 1):
            value = value + dw_in[step, slot].astype(jnp.float32)
        dw[slot] = value.astype(jnp.bfloat16)
        return carry

    def last(chunk):
        if chunk == 0:
            for copy in dw_copies:
                copy.wait()
            lax.fori_loop(0, slots, total, 0)
            store_w.start()
        for kind in range(kinds):
            reached_all(11, kind, chunk, band_in)

        def finish(row, carry):
            delta = dot(fwd_kf[...], pair(band_in, chunk, row))
            put_pair(cbuf, chunk, row, pair(cbuf, chunk, row).astype(jnp.float32) + delta)
            return carry

        lax.fori_loop(0, lat_dev // 2, finish, 0)
        store(chunk).start()

    synth(6, qtab, 0, 2, 4)
    synth(6, qtab, 1, far, far + 2)
    synth(6, qtab, 0, 4, 5)
    last(0)
    synth(6, qtab, 0, 5, 6)
    synth(6, qtab, 1, far + 2, far + 4)
    synth(6, qtab, 1, far + 4, far + 6)
    last(1)
    last(2)
    for chunk in range(chunks):
        for kind in range(kinds):
            left_for_owners(6, kind, chunk, band_out)
            left_for_owners(9, kind, chunk, mixed)

    def drain(part, job):
        kind, chunk, place = job_of(job)

        @pl.when(mine(kind))
        def _():
            if part:
                await_tail(kind, cross_out.at[place, chunk], send_sem.at[7, job])
                await_tail(kind, tail_out.at[chunk], send_sem.at[10, job])
            else:
                await_bytes(cross_out.at[place, chunk], send_sem.at[7, job])
                await_bytes(slot_all.at[place, chunk, 0:own], send_sem.at[10, job])
            left_owner(8, job, kind, chunk, slot_out, slots)
            left_owner(11, job, kind, chunk, ord_out, lat_dev)

    loop(0, per_pass, lambda job: drain(0, job))
    loop(per_pass, jobs, lambda job: drain(1, job))
    for chunk in range(chunks):
        store(chunk).wait()
    store_w.wait()


def local_kernel(fields, cotangent, weights, degree_of):
    n = lax.axis_size("lat")
    nb = lax.axis_size("batch")
    kinds = 4
    if fields.shape[0] != 1 or fields.shape[1] % 2 or n % kinds or ORDERS != n * GROUP:
        return local(fields, cotangent, weights, degree_of)
    lat_dev, lons, channels = fields.shape[1:]
    slots = weights.shape[0]
    rows = 2 * GROUP
    chunks = channels // LANES
    floats, waves = constant_tables()
    side_lats = LATS // 2
    held = kinds - 1
    vmem = pl.BlockSpec(memory_space=pltpu.VMEM)
    anywhere = pl.BlockSpec(memory_space=pl.ANY)

    def buffer(*dims):
        return pltpu.VMEM(dims, jnp.bfloat16)

    dma = pltpu.SemaphoreType.DMA
    others = max(nb - 1, 1)
    wide_rows = max(side_lats, DEGREES) * rows
    return pl.pallas_call(
        functools.partial(block_kernel, n, nb),
        out_shape=(
            jax.ShapeDtypeStruct(fields.shape, jnp.bfloat16),
            jax.ShapeDtypeStruct(weights.shape, jnp.bfloat16),
        ),
        in_specs=[anywhere] * 3 + [pl.BlockSpec(memory_space=pltpu.SMEM)] + [vmem] * 7,
        out_specs=(anywhere, anywhere),
        scratch_shapes=[
            buffer(chunks, lat_dev, lons, LANES),
            buffer(chunks, lat_dev, lons, LANES),
            buffer(*weights.shape),
            buffer(chunks, lat_dev, n * rows, LANES),
            buffer(chunks, lat_dev, n * rows, LANES),
            buffer(held, chunks, side_lats, rows, LANES),
            buffer(held, chunks, side_lats, rows, LANES),
            buffer(held, chunks, DEGREES // 2, rows, LANES),
            buffer(held, chunks, DEGREES // 2, rows, LANES),
            buffer(held, chunks, DEGREES // 2, rows, LANES),
            buffer(held, chunks, DEGREES, rows, LANES),
            buffer(chunks, DEGREES // 2, rows, LANES),
            buffer(chunks, slots, n * rows, LANES),
            buffer(chunks, slots, n * rows, LANES),
            buffer(chunks, slots, n * rows, LANES),
            pltpu.VMEM((wide_rows, LANES), jnp.float32),
            pltpu.VMEM((4 * wide_rows, LANES), jnp.float32),
            pltpu.VMEM((side_lats * rows, LANES), jnp.float32),
            buffer(*weights.shape),
            buffer(others, *weights.shape),
            buffer(kinds, GROUP, DEGREES, side_lats),
            buffer(kinds, GROUP, DEGREES, side_lats),
            pltpu.VMEM((DEGREES, kinds * GROUP, LANES), jnp.float32),
            pltpu.VMEM((GROUP, DEGREES), jnp.int32),
            pltpu.SMEM((GROUP, DEGREES), jnp.int32),
            buffer(DEGREES, rows, LANES),
            dma((2 * chunks + 2,)),
            dma((12, kinds * chunks)),
            dma((12, kinds * chunks)),
            dma((others,)),
            dma((others,)),
            dma((chunks + 1,)),
        ],
        compiler_params=pltpu.CompilerParams(
            collective_id=0, has_side_effects=True, vmem_limit_bytes=63 * 2**20
        ),
        name="filter_block",
    )(
        fields, cotangent, weights, degree_of, *floats, *waves,
    )


def local(fields, cotangent, weights, degree_of):
    samples = fields.shape[0]
    band_rows = fields.shape[1]
    ord_dev = ORDERS // lax.axis_size("lat")
    forward, inverse = fourier_tables(LONS, ORDERS)
    qslot, pslot = spectral_tables(lax.axis_index("lat") * ord_dev, ord_dev, degree_of)
    spectra = product("sikc,kf->ifsc", fields, forward).astype(jnp.bfloat16)
    spectra = spectra.reshape(band_rows, ORDERS, 2, samples, CHANNELS)
    gathered = to_orders(spectra)
    coeffs_local = product("mji,imrsc->jmrsc", qslot, gathered).astype(jnp.bfloat16)
    coeffs = to_degrees(coeffs_local)
    filtered = apply_filter(coeffs, weights)
    returned = back_to_orders(filtered)
    synth_local = product("mji,jmrsc->imrsc", pslot, returned).astype(jnp.bfloat16)
    synth = to_bands(synth_local)
    response = product(
        "ifsc,fk->sikc", synth.reshape(band_rows, 2 * ORDERS, samples, CHANNELS), inverse
    )
    activated, pullback = jax.vjp(jax.nn.gelu, response)
    upstream = pullback(cotangent.astype(jnp.float32))[0].astype(jnp.bfloat16)
    grad_synth = product("sikc,fk->ifsc", upstream, inverse).astype(jnp.bfloat16)
    grad_synth = grad_synth.reshape(band_rows, ORDERS, 2, samples, CHANNELS)
    grad_gathered = to_orders(grad_synth)
    grad_local = product("mji,imrsc->jmrsc", pslot, grad_gathered).astype(jnp.bfloat16)
    grad_filtered = to_degrees(grad_local)
    weight_total = lax.psum(filter_grad(coeffs, grad_filtered).astype(jnp.bfloat16), "batch")
    grad_coeffs = adjoint_filter(grad_filtered, weights)
    grad_back = back_to_orders(grad_coeffs)
    grad_local_spec = product("mji,jmrsc->imrsc", qslot, grad_back).astype(jnp.bfloat16)
    grad_bands = to_bands(grad_local_spec)
    delta = product(
        "ifsc,kf->sikc", grad_bands.reshape(band_rows, 2 * ORDERS, samples, CHANNELS), forward
    )
    grad_fields = (cotangent.astype(jnp.float32) + delta).astype(jnp.bfloat16)
    return (grad_fields, weight_total)


def solution(mesh):
    return jax.shard_map(
        local_kernel if CHANNELS % LANES == 0 else local,
        mesh=mesh,
        in_specs=(
            P("batch", "lat", None, None),
            P("batch", "lat", None, None),
            P("lat", None, None, None),
            P(),
        ),
        out_specs=(P("batch", "lat", None, None), P("lat", None, None, None)),
        check_vma=False,
    )
```

```python
import functools

import jax
import numpy as np
import jax.numpy as jnp
from jax import lax
from jax.experimental import pallas as pl
from jax.experimental.pallas import tpu as pltpu
from jax.sharding import PartitionSpec as P

LATS = 192
LONS = 384
ORDERS = 128
DEGREES = 128
CHANNELS = 384
LANES = 128
GROUP = 8


def table_kernel(deg_ref, diag_ref, cos_ref, quad_ref, order_ref, q_ref, p_ref, slot_ref, rows_ref):
    orders = diag_ref.shape[0]
    lats = q_ref.shape[2]
    degrees = deg_ref.shape[0]

    def invert(slot, carry):
        slot_ref[deg_ref[slot]] = slot
        return carry

    lax.fori_loop(0, degrees, invert, 0)
    order_real = order_ref[...]
    squared = order_real * order_real
    diagonal = diag_ref[...]
    cosine = cos_ref[...]
    first_lead = jnp.sqrt(2.0 * order_real + 3.0)
    halves = rows_ref.shape[0]

    def advance(degree, carry):
        previous, older = carry
        degree_real = degree.astype(jnp.float32)
        lead = jnp.sqrt(
            jnp.maximum(4.0 * degree_real * degree_real - 1.0, 0.0)
            / jnp.maximum(degree_real * degree_real - squared, 1.0)
        )
        lower = degree_real - 1.0
        back = jnp.sqrt(
            jnp.maximum(lower * lower - squared, 0.0) / jnp.maximum(4.0 * lower * lower - 1.0, 1.0)
        )
        general = lead * (cosine * previous - back * older)
        first = first_lead * cosine * previous
        value = jnp.where(
            degree_real == order_real,
            diagonal,
            jnp.where(
                degree_real == order_real + 1.0,
                first,
                jnp.where(degree_real > order_real + 1.0, general, 0.0),
            ),
        )
        slot = slot_ref[degree]
        for half in range(halves):
            rows_ref[half, pl.ds(slot, orders, stride=degrees), :] = value[
                :, half * LANES : (half + 1) * LANES
            ]
        return (value, previous)

    zeros = diagonal * 0.0
    lax.fori_loop(0, degrees, advance, (zeros, zeros), unroll=4)
    quadrature = quad_ref[...]
    for order in range(orders):
        for half in range(halves):
            low = half * LANES
            high = min(lats, low + LANES)
            chosen = rows_ref[half, order * degrees : (order + 1) * degrees, :][:, : high - low]
            p_ref[order, :, low:high] = chosen.astype(jnp.bfloat16)
            q_ref[order, :, low:high] = (chosen * quadrature[:, low:high]).astype(jnp.bfloat16)


def spectral_tables(start, ord_dev, degree_of):
    halves = -(-LATS // LANES)
    padded = halves * LANES
    order_col = (start + jnp.arange(ord_dev, dtype=jnp.int32)).astype(jnp.float32)[:, None]
    lat_ids = jnp.minimum(jnp.arange(padded, dtype=jnp.float32), LATS - 1.0)
    colatitude = jnp.pi * (lat_ids + 0.5) / LATS
    sine = jnp.sin(colatitude)[None, :]
    steps_up = jnp.arange(1, DEGREES + 1, dtype=jnp.float32)[None, :]
    factor = jnp.where(
        steps_up <= order_col, 0.5 * jnp.log((2.0 * steps_up + 1.0) / (2.0 * steps_up)), 0.0
    )
    log_start = 0.5 * jnp.log(1.0 / (4.0 * jnp.pi)) + jnp.sum(factor, axis=1, keepdims=True)
    diagonal = jnp.exp(log_start + order_col * jnp.log(sine))
    cosine = jnp.broadcast_to(jnp.cos(colatitude)[None, :], diagonal.shape)
    quadrature = 2.0 * jnp.pi * jnp.pi / LATS * sine
    orders = jnp.broadcast_to(order_col, diagonal.shape)
    vmem = pl.BlockSpec(memory_space=pltpu.VMEM)
    shape = jax.ShapeDtypeStruct((ord_dev, DEGREES, LATS), jnp.bfloat16)
    return pl.pallas_call(
        table_kernel,
        out_shape=(shape, shape),
        in_specs=[pl.BlockSpec(memory_space=pltpu.SMEM)] + [vmem] * 4,
        out_specs=(vmem, vmem),
        scratch_shapes=[
            pltpu.SMEM((DEGREES,), jnp.int32),
            pltpu.VMEM((halves, ord_dev * DEGREES, LANES), jnp.float32),
        ],
        name="legendre_tables",
    )(degree_of, diagonal, cosine, quadrature, orders)


def fourier_tables(lon_count, order_count):
    lon_ids = jnp.arange(lon_count, dtype=jnp.int32)[:, None]
    order_ids = jnp.arange(order_count, dtype=jnp.int32)[None, :]
    phase = 2.0 * jnp.pi * (lon_ids * order_ids % lon_count).astype(jnp.float32) / lon_count
    forward = (
        jnp.stack([jnp.cos(phase), -jnp.sin(phase)], axis=2).reshape(lon_count, 2 * order_count)
        / lon_count
    )
    doubled = jnp.where(order_ids == 0, 1.0, 2.0)
    inverse = jnp.stack([doubled * jnp.cos(phase), -doubled * jnp.sin(phase)], axis=2).reshape(
        lon_count, 2 * order_count
    )
    return (forward.astype(jnp.bfloat16), jnp.transpose(inverse).astype(jnp.bfloat16))


def to_orders(values):
    return lax.all_to_all(values, "lat", split_axis=1, concat_axis=0, tiled=True)


def to_degrees(values):
    return lax.all_to_all(values, "lat", split_axis=0, concat_axis=1, tiled=True)


def back_to_orders(values):
    return lax.all_to_all(values, "lat", split_axis=1, concat_axis=0, tiled=True)


def to_bands(values):
    return lax.all_to_all(values, "lat", split_axis=0, concat_axis=1, tiled=True)


def product(spec, left, right):
    return jnp.einsum(spec, left, right, preferred_element_type=jnp.float32)


def apply_filter(coeffs, weights):
    c_real = coeffs[:, :, 0]
    c_imag = coeffs[:, :, 1]
    w_real = weights[:, 0]
    w_imag = weights[:, 1]
    f_real = product("jmsc,jcd->jmsd", c_real, w_real) - product("jmsc,jcd->jmsd", c_imag, w_imag)
    f_imag = product("jmsc,jcd->jmsd", c_real, w_imag) + product("jmsc,jcd->jmsd", c_imag, w_real)
    return jnp.stack([f_real, f_imag], axis=2).astype(jnp.bfloat16)


def adjoint_filter(grads, weights):
    g_real = grads[:, :, 0]
    g_imag = grads[:, :, 1]
    w_real = weights[:, 0]
    w_imag = weights[:, 1]
    a_real = product("jmsd,jcd->jmsc", g_real, w_real) + product("jmsd,jcd->jmsc", g_imag, w_imag)
    a_imag = product("jmsd,jcd->jmsc", g_imag, w_real) - product("jmsd,jcd->jmsc", g_real, w_imag)
    return jnp.stack([a_real, a_imag], axis=2).astype(jnp.bfloat16)


def filter_grad(coeffs, grads):
    c_real = coeffs[:, :, 0]
    c_imag = coeffs[:, :, 1]
    g_real = grads[:, :, 0]
    g_imag = grads[:, :, 1]
    dw_real = product("jmsc,jmsd->jcd", c_real, g_real) + product("jmsc,jmsd->jcd", c_imag, g_imag)
    dw_imag = product("jmsc,jmsd->jcd", c_real, g_imag) - product("jmsc,jmsd->jcd", c_imag, g_real)
    return jnp.stack([dw_real, dw_imag], axis=1)


def constant_tables():
    sides = 2
    half = LATS // sides
    lat_ids = np.minimum(np.arange(LANES)[None, :], half - 1) + half * np.arange(sides)[:, None]
    colatitude = np.pi * (lat_ids + 0.5) / LATS
    sine = np.sin(colatitude)[:, None, :]
    ids = np.arange(ORDERS)
    steps_up = np.arange(1, ORDERS + 1)
    growth = np.cumsum(0.5 * np.log((2.0 * steps_up + 1.0) / (2.0 * steps_up)))
    log_start = 0.5 * np.log(1.0 / (4.0 * np.pi)) + np.concatenate([[0.0], growth[:-1]])
    diagonal = np.exp(log_start[None, :, None] + ids[None, :, None] * np.log(sine))
    cosine = np.broadcast_to(np.cos(colatitude)[:, None, :], (sides, GROUP, LANES))
    quadrature = np.broadcast_to(2.0 * np.pi * np.pi / LATS * sine, (sides, GROUP, LANES))
    phase = 2.0 * np.pi * (np.arange(LONS)[:, None] * ids[None, :] % LONS) / LONS
    forward = np.stack([np.cos(phase), -np.sin(phase)], axis=2).reshape(LONS, -1) / LONS
    doubled = np.where(ids == 0, 1.0, 2.0)[None, :]
    inverse = np.stack([doubled * np.cos(phase), -doubled * np.sin(phase)], axis=2)
    inverse = inverse.reshape(LONS, -1)
    floats = [jnp.asarray(t, jnp.float32) for t in (diagonal, cosine, quadrature)]
    waves = [forward.T, forward, inverse.T, inverse]
    halves = [jnp.asarray(np.float32(t).astype(jnp.bfloat16)) for t in waves]
    return floats, halves


def fill_tables(side, firsts, deg_ref, diag_ref, cos_ref, quad_ref, qtab, ptab, table, by_slot):
    kinds, orders, degrees, lats = qtab.shape
    every = kinds * orders
    cosine = cos_ref[side]
    diagonal, ids, squared, first_lead = [], [], [], []
    for first in firsts:
        diagonal.append(diag_ref[side, pl.ds(pl.multiple_of(first, orders), orders), :])
        ids.append(first + lax.broadcasted_iota(jnp.int32, cosine.shape, 0))
        real = ids[-1].astype(jnp.float32)
        squared.append(real * real)
        first_lead.append(jnp.sqrt(2.0 * real + 3.0))

    def advance(degree, carry):
        degree_real = degree.astype(jnp.float32)
        lower = degree_real - 1.0
        state = []
        for kind in range(kinds):
            previous, older = carry[kind]
            lead = jnp.sqrt(
                jnp.maximum(4.0 * degree_real * degree_real - 1.0, 0.0)
                / jnp.maximum(degree_real * degree_real - squared[kind], 1.0)
            )
            back = jnp.sqrt(
                jnp.maximum(lower * lower - squared[kind], 0.0)
                / jnp.maximum(4.0 * lower * lower - 1.0, 1.0)
            )
            general = lead * (cosine * previous - back * older)
            first = first_lead[kind] * cosine * previous
            value = jnp.where(
                ids[kind] == degree,
                diagonal[kind],
                jnp.where(
                    ids[kind] + 1 == degree,
                    first,
                    jnp.where(ids[kind] + 1 < degree, general, 0.0),
                ),
            )
            table[degree, kind * orders : (kind + 1) * orders, :] = value
            state.append((value, previous))
        return tuple(state)

    zeros = cosine * 0.0
    lax.fori_loop(0, degrees, advance, ((zeros, zeros),) * kinds, unroll=2)

    ahead = every // 2
    tail = degrees // 2

    def place(slot, carry):
        by_slot[pl.ds(slot, ahead, stride=degrees), :] = table[deg_ref[slot], :ahead]
        return carry

    lax.fori_loop(0, degrees, place, 0, unroll=4)

    def place_tail(row, carry):
        spots = pl.ds(ahead * degrees + row, ahead, stride=degrees)
        by_slot[spots, :] = table[tail + row, ahead:]
        return carry

    lax.fori_loop(0, tail, place_tail, 0, unroll=4)
    quadrature = quad_ref[side][:1, :lats]
    for kind in range(kinds):

        def keep(order, carry):
            start = pl.multiple_of((kind * orders + order) * degrees, degrees)
            depth = degrees if kind < kinds // 2 else tail
            chosen = by_slot[pl.ds(start, depth), :][:, :lats]
            ptab[kind, order, :depth] = chosen.astype(jnp.bfloat16)
            qtab[kind, order, :depth] = (chosen * quadrature).astype(jnp.bfloat16)
            return carry

        lax.fori_loop(0, orders, keep, 0)


def pair_swap(values, even_sign):
    rows = values.shape[0]
    even = lax.broadcasted_iota(jnp.int32, values.shape, 0) % 2 == 0
    above = pltpu.roll(values, rows - 1, 0)
    below = pltpu.roll(values, 1, 0)
    return jnp.where(even, even_sign * above, -even_sign * below)


def gelu_slope(x):
    scale = 0.7978845608028654
    square = x * x
    t = jnp.tanh(scale * (x + 0.044715 * x * square))
    return 0.5 * (1.0 + t) + 0.5 * x * (1.0 - t * t) * (scale * (1.0 + 0.134145 * square))


def dot(left, right, dims=((1,), (0,))):
    return lax.dot_general(left, right, (dims, ((), ())), preferred_element_type=jnp.float32)


def block_kernel(
    n, nb, fields, cotangent, weights, deg_ref, diag_ref, cos_ref, quad_ref,
    fwd_fk, fwd_kf, inv_fk, inv_kf,
    grad_out, dw_out,
    fbuf, cbuf, wbuf, band_out, band_in, ord_in, ord_out, cross_out, cross_in, slot_out, slot_all,
    tail_out, co, go, mixed, wide_a, wide_b, wide_c, dw, dw_in, qtab, ptab, table, row_ref, slot_of, by_name,
    load_sem, send_sem, recv_sem, dw_send, dw_recv, out_sem,
):
    me = lax.axis_index("lat")
    me_b = lax.axis_index("batch")
    chunks, lat_dev = fbuf.shape[0], fbuf.shape[1]
    kinds, orders, degrees, side_lats = qtab.shape
    rows = 2 * orders
    slots = co.shape[1]
    quarter = n // kinds
    half = n // 2
    own = half * slots
    inner_kinds = ord_in.shape[0]
    pairs = kinds // 2
    jobs = kinds * chunks
    plane_rows = quarter * rows
    mesh_id = pl.DeviceIdType.MESH
    side = lax.div(me, half)
    place_in = lax.rem(me, half)
    column = lax.rem(me, quarter)
    inner = jnp.where(lax.div(me, quarter) == 1 + side, 1, 0)
    across = 1 - side

    def lanes(chunk):
        return pl.ds(chunk * LANES, LANES)

    def group(kind, at):
        return jnp.where(
            lax.rem(kind, 2) == 0, kind * quarter + at, (kind + 1) * quarter - 1 - at
        )

    def group_rows(kind, at):
        return pl.ds(pl.multiple_of(group(kind, at) * rows, rows), rows)

    def owner(kind, on_side, at):
        plane = jnp.where(kind < inner_kinds, 1 + on_side, (kinds - 1) * on_side)
        return plane * quarter + at

    def mine(kind):
        return jnp.where(kind < inner_kinds, 1, 0) == inner

    def job_of(job):
        per_pass = pairs * chunks
        inside = lax.rem(job, per_pass)
        kind = lax.div(job, per_pass) * pairs + lax.rem(inside, pairs)
        return kind, lax.div(inside, pairs), lax.rem(kind, inner_kinds)

    def first_block(kind):
        return group(kind, column) - own // orders

    def tail_blocks(kind, body):
        def one(block, carry):
            body(pl.multiple_of(block * orders, orders))
            return carry

        lax.fori_loop(first_block(kind), own // orders, one, 0)

    def await_tail(kind, view, sem):
        for first in range(own // orders):

            @pl.when(first_block(kind) == first)
            def _():
                await_bytes(view.at[pl.ds(0, own - first * orders)], sem)

    def job_at(kind, chunk):
        return (kind // pairs) * (pairs * chunks) + chunk * pairs + kind % pairs

    def load(chunk):
        return pltpu.make_async_copy(
            fields.at[0, :, :, lanes(chunk)], fbuf.at[chunk], load_sem.at[chunk]
        )

    def load_cot(chunk):
        return pltpu.make_async_copy(
            cotangent.at[0, :, :, lanes(chunk)], cbuf.at[chunk], load_sem.at[chunks + chunk]
        )

    load_w = pltpu.make_async_copy(weights, wbuf, load_sem.at[2 * chunks])
    for chunk in range(chunks):
        load(chunk).start()
    load_w.start()
    for chunk in range(chunks):
        load_cot(chunk).start()

    barrier = pltpu.get_barrier_semaphore()

    def greet(step, carry):
        peer = lax.rem(me + step, n)
        pl.semaphore_signal(barrier, inc=1, device_id={"lat": peer}, device_id_type=mesh_id)
        return carry

    lax.fori_loop(1, n, greet, 0)
    for step in range(1, nb):
        peer = lax.rem(me_b + step, nb)
        pl.semaphore_signal(barrier, inc=1, device_id={"batch": peer}, device_id_type=mesh_id)

    def remote(stage, job, source, target, peer):
        pltpu.make_async_remote_copy(
            src_ref=source,
            dst_ref=target,
            send_sem=send_sem.at[stage, job],
            recv_sem=recv_sem.at[stage, job],
            device_id={"lat": peer},
            device_id_type=mesh_id,
        ).start()

    def await_bytes(view, sem):
        pltpu.make_async_copy(view, view, sem).wait()

    def to_owners(stage, kind, chunk, source, target, width):
        job = job_at(kind, chunk)
        for step in range(quarter):
            at = lax.rem(column + step, quarter)
            view = source.at[chunk, :, group_rows(kind, at), :]
            spot = target(kind % inner_kinds, chunk)
            peer = owner(kind, side, at)

            @pl.when(peer != me)
            def _():
                remote(stage, job, view, spot, peer)

            @pl.when(peer == me)
            def _():
                pltpu.make_async_copy(view, spot, recv_sem.at[stage, job]).start()

    def left_for_owners(stage, kind, chunk, source):
        job = job_at(kind, chunk)

        @pl.when(mine(kind))
        def _():
            await_bytes(source.at[chunk, :, 0 : plane_rows - rows, :], send_sem.at[stage, job])

        @pl.when(jnp.logical_not(mine(kind)))
        def _():
            await_bytes(source.at[chunk, :, 0:plane_rows, :], send_sem.at[stage, job])

    def from_owner(stage, job, kind, chunk, source, depth, target):
        place = lax.rem(kind, inner_kinds)
        spot = target.at[chunk, :, group_rows(kind, column), :]

        def send(step, carry):
            at = lax.rem(place_in + step, half)
            remote(
                stage, job, source.at[place, chunk, pl.ds(at * depth, depth)], spot,
                side * half + at,
            )
            return carry

        lax.fori_loop(1, half, send, 0)
        pltpu.make_async_copy(
            source.at[place, chunk, pl.ds(place_in * depth, depth)], spot, recv_sem.at[stage, job]
        ).start()

    def left_owner(stage, job, kind, chunk, source, depth):
        view = source.at[lax.rem(kind, inner_kinds), chunk, 0 : (half - 1) * depth]
        await_bytes(view, send_sem.at[stage, job])

    def reached_all(stage, kind, chunk, target):
        await_bytes(target.at[chunk, :, 0:plane_rows, :], recv_sem.at[stage, job_at(kind, chunk)])

    def lat_spot(place, chunk):
        return ord_in.at[place, chunk, pl.ds(place_in * lat_dev, lat_dev)]

    def slot_spot(place, chunk):
        return slot_all.at[place, chunk, pl.ds(me * slots, slots)]

    def wide_start(part, job):
        if part:
            spot = lax.rem(lax.div(job - pairs * chunks, pairs) + pairs, chunks)
        else:
            spot = jnp.where(job < 2 * pairs, lax.rem(job, pairs), job - pairs)
        return pl.multiple_of(spot * wide_a.shape[0], 8)

    def widen(source, place, chunk, depth, count):
        def one(block, carry):
            piece = source[place, chunk, pl.ds(block * depth, depth)].astype(jnp.float32)
            wide_a[pl.ds(pl.multiple_of(block * depth * rows, depth * rows), depth * rows), :] = (
                piece.reshape(depth * rows, LANES)
            )
            return carry

        lax.fori_loop(0, count // depth, one, 0)

    def apply_table(tab, kind, kept, result_ref, start, depth_in, depth_out, dims):
        def one(order, carry):
            real = wide_a[pl.ds(2 * order, depth_in, stride=rows), :]
            imag = wide_a[pl.ds(2 * order + 1, depth_in, stride=rows), :]
            both = jnp.concatenate([real, imag], axis=1).astype(jnp.bfloat16)
            result = dot(tab[kind, order, :kept], both, dims)
            result_ref[pl.ds(start + 2 * order, depth_out, stride=rows), :] = result[:, :LANES]
            result_ref[pl.ds(start + 2 * order + 1, depth_out, stride=rows), :] = result[:, LANES:]
            return carry

        lax.fori_loop(0, orders, one, 0, unroll=8)

    def narrow(source, target, place, chunk, start, depth, count):
        def one(block, carry):
            low = pl.multiple_of(start + block * depth * rows, 8)
            piece = source[pl.ds(low, depth * rows), :]
            target[place, chunk, pl.ds(block * depth, depth)] = piece.reshape(
                depth, rows, LANES
            ).astype(jnp.bfloat16)
            return carry

        lax.fori_loop(0, count // depth, one, 0)

    def wide_rows(start, index, depth):
        return pl.ds(pl.multiple_of(start + index * rows, 8), depth * rows)

    def blank(first, count):
        def one(block, carry):
            by_name[pl.ds((first + block) * orders, orders)] = jnp.zeros(
                (orders, rows, LANES), jnp.bfloat16
            )
            return carry

        lax.fori_loop(0, count, one, 0)

    def analyse(base, tab, part, job):
        kind, chunk, place = job_of(job)

        @pl.when(mine(kind))
        def _():
            await_bytes(ord_in.at[place, chunk], recv_sem.at[base, job])
            widen(ord_in, place, chunk, lat_dev, side_lats)
            start = wide_start(part, job)
            peer = owner(kind, across, column)
            source = cross_out.at[place, chunk]
            target = cross_in.at[place, chunk]
            kept = own if part else degrees
            apply_table(tab, kind, kept, wide_b, start, side_lats, kept, ((1,), (0,)))
            if not part:
                if base:
                    await_bytes(source, send_sem.at[1, job])
                narrow(wide_b, cross_out, place, chunk, start + across * own * rows, slots, own)
                remote(base + 1, job, source, target, peer)
                return
            if base:
                await_tail(kind, source, send_sem.at[1, job])

            def send(low):
                span = pl.ds(low, orders)
                piece = wide_b[wide_rows(start, low, orders), :]
                cross_out[place, chunk, span] = piece.reshape(orders, rows, LANES).astype(
                    jnp.bfloat16
                )
                remote(base + 1, job, source.at[span], target.at[span], peer)

            tail_blocks(kind, send)

    def settle(base, target, part, job):
        kind, chunk, place = job_of(job)

        @pl.when(mine(kind))
        def _():
            start = wide_start(part, job)
            if part:
                await_tail(kind, cross_in.at[place, chunk], recv_sem.at[base + 1, job])
            else:
                await_bytes(cross_in.at[place, chunk], recv_sem.at[base + 1, job])
            if base:
                left_owner(2, job, kind, chunk, slot_out, slots)
                if part:
                    await_tail(kind, tail_out.at[chunk], send_sem.at[4, job])
                else:
                    await_bytes(slot_all.at[place, chunk, 0:own], send_sem.at[4, job])
            if part:

                blank(0, own // orders + first_block(kind))

                def add(low):
                    piece = wide_b[wide_rows(start, low, orders), :]
                    other = cross_in[place, chunk, pl.ds(low, orders)].astype(jnp.float32)
                    by_name[pl.ds(own + low, orders)] = (
                        piece.reshape(orders, rows, LANES) + other
                    ).astype(jnp.bfloat16)

                tail_blocks(kind, add)

                def pick(slot, carry):
                    slot_out[place, chunk, slot] = by_name[deg_ref[side * own + slot]]
                    return carry

                lax.fori_loop(0, own, pick, 0, unroll=4)
            else:

                def one(block, carry):
                    low = block * slots
                    piece = wide_b[wide_rows(start + side * own * rows, low, slots), :]
                    other = cross_in[place, chunk, pl.ds(low, slots)].astype(jnp.float32)
                    slot_out[place, chunk, pl.ds(low, slots)] = (
                        piece.reshape(slots, rows, LANES) + other
                    ).astype(jnp.bfloat16)
                    return carry

                lax.fori_loop(0, half, one, 0)
            from_owner(base + 2, job, kind, chunk, slot_out, slots, target)

    def relay(base, part, job):
        kind, chunk, place = job_of(job)

        @pl.when(mine(kind))
        def _():
            await_bytes(slot_all.at[place, chunk, 0:own], recv_sem.at[base + 3, job])
            peer = owner(kind, across, column)
            view = slot_all.at[place, chunk, pl.ds(side * own, own)]
            if not part:
                remote(base + 4, job, view, view, peer)
                return

            blank(across * (own // orders), own // orders)

            def copy(block, carry):
                span = pl.ds(side * own + block * slots, slots)
                by_name[span] = slot_all[place, chunk, span]
                return carry

            lax.fori_loop(0, half, copy, 0)

            def send(low):
                for step in range(orders):
                    tail_out[chunk, low + step] = by_name[slot_of[0, own + low + step]]
                span = pl.ds(low, orders)
                remote(base + 4, job, tail_out.at[chunk, span], view.at[span], peer)

            tail_blocks(kind, send)

    def synthesise(base, tab, part, job):
        kind, chunk, place = job_of(job)

        @pl.when(mine(kind))
        def _():
            if part:
                await_tail(kind, tail_out.at[chunk], recv_sem.at[base + 4, job])

                def clear(block, carry):
                    wide_a[wide_rows(0, block * orders, orders), :] = jnp.zeros(
                        (orders * rows, LANES), jnp.float32
                    )
                    return carry

                lax.fori_loop(0, first_block(kind), clear, 0)

                def add(low):
                    near = tail_out[chunk, pl.ds(low, orders)].astype(jnp.float32)
                    far = slot_all[place, chunk, pl.ds(across * own + low, orders)]
                    wide_a[wide_rows(0, low, orders), :] = (
                        near + far.astype(jnp.float32)
                    ).reshape(orders * rows, LANES)

                tail_blocks(kind, add)
                apply_table(tab, kind, own, wide_c, 0, own, side_lats, ((0,), (0,)))
            else:
                await_bytes(slot_all.at[place, chunk, 0:own], recv_sem.at[base + 4, job])
                widen(slot_all, place, chunk, slots, degrees)
                apply_table(tab, kind, degrees, wide_c, 0, degrees, side_lats, ((0,), (0,)))
            if base:
                left_owner(5, job, kind, chunk, ord_out, lat_dev)
            narrow(wide_c, ord_out, place, chunk, 0, lat_dev, side_lats)
            from_owner(base + 5, job, kind, chunk, ord_out, lat_dev, band_in)

    def loop(low, high, body):
        def one(job, carry):
            body(job)
            return carry

        lax.fori_loop(low, high, one, 0)

    def pair(source, chunk, row):
        return jnp.concatenate([source[chunk, 2 * row], source[chunk, 2 * row + 1]], axis=1)

    def put_pair(target, chunk, row, values):
        values = values.astype(jnp.bfloat16)
        target[chunk, 2 * row] = values[:, :LANES]
        target[chunk, 2 * row + 1] = values[:, LANES:]

    def joined(source, slot, span):
        return jnp.concatenate([source[chunk, slot, span] for chunk in range(chunks)], axis=1)

    def mix(part, chunk):
        low = part * pairs * plane_rows
        span = slice(low, low + pairs * plane_rows)
        columns = slice(chunk * LANES, (chunk + 1) * LANES)

        def one(slot, carry):
            both = dot(
                joined(co, slot, span),
                jnp.concatenate([wbuf[slot, 0, :, columns], wbuf[slot, 1, :, columns]], axis=1),
            )
            crossed = pair_swap(both[:, LANES:], -1.0)
            mixed[chunk, slot, span] = (both[:, :LANES] + crossed).astype(jnp.bfloat16)
            return carry

        return one

    def adjoint(part, chunk):
        low = part * pairs * plane_rows
        span = slice(low, low + pairs * plane_rows)
        columns = slice(chunk * LANES, (chunk + 1) * LANES)

        def one(slot, carry):
            both = dot(
                joined(go, slot, span),
                jnp.concatenate([wbuf[slot, 0, columns, :], wbuf[slot, 1, columns, :]], axis=0),
                ((1,), (1,)),
            )
            crossed = pair_swap(both[:, LANES:], 1.0)
            mixed[chunk, slot, span] = (both[:, :LANES] + crossed).astype(jnp.bfloat16)
            return carry

        return one

    def filter_part(base, part, source, make):
        part_kinds = range(part * pairs, (part + 1) * pairs)
        for chunk in range(chunks):
            for kind in part_kinds:
                reached_all(base + 2, kind, chunk, source)
        for chunk in range(chunks):
            if base:
                for kind in part_kinds:
                    left_for_owners(3, kind, chunk, mixed)
            lax.fori_loop(0, slots, make(part, chunk), 0, unroll=4)
            for kind in part_kinds:
                to_owners(base + 3, kind, chunk, mixed, slot_spot, slots)

    per_pass = pairs * chunks
    def unit(part, chunk):
        first = part * per_pass + chunk * pairs
        return first, first + pairs

    def run(spans, body):
        loop(spans[0], spans[1], body)

    def to_filter_start(base, tab, source):
        run(unit(0, 0), lambda job: analyse(base, tab, 0, job))
        for low, high, part, behind in (
            (pairs, per_pass, 0, 0),
            (per_pass, per_pass + pairs, 1, 0),
            (per_pass + pairs, per_pass + 2 * pairs, 1, 1),
        ):

            def step(job):
                settle(base, source, behind, job - pairs)
                analyse(base, tab, part, job)

            loop(low, high, step)
        loop(per_pass + 2 * pairs, jobs, lambda job: analyse(base, tab, 1, job))

    def through_filter(base, tab, source, make):
        filter_part(base, 0, source, make)
        run(unit(1, 1), lambda job: settle(base, source, 1, job))
        run(unit(0, 0), lambda job: relay(base, 0, job))
        run(unit(1, 2), lambda job: settle(base, source, 1, job))
        run(unit(0, 1), lambda job: relay(base, 0, job))
        run(unit(0, 0), lambda job: synthesise(base, tab, 0, job))
        filter_part(base, 1, source, make)
        run(unit(1, 0), lambda job: relay(base, 1, job))
        run(unit(0, 2), lambda job: relay(base, 0, job))
        loop(per_pass + pairs, jobs, lambda job: relay(base, 1, job))

    def spread(stage, chunk, part):
        for kind in range(part * pairs, (part + 1) * pairs):
            to_owners(stage, kind, chunk, band_out, lat_spot, lat_dev)

    def transform(chunk):
        load(chunk).wait()

        def fourier(row, carry):
            put_pair(band_out, chunk, row, dot(fwd_fk[...], pair(fbuf, chunk, row)))
            return carry

        lax.fori_loop(0, lat_dev // 2, fourier, 0, unroll=3)

    transform(0)
    pl.semaphore_wait(barrier, n - 1 + nb - 1)
    spread(0, 0, 0)
    transform(1)
    spread(0, 1, 0)
    fill_tables(
        side, [group(kind, column) * orders for kind in range(kinds)], deg_ref, diag_ref, cos_ref,
        quad_ref, qtab, ptab, table, wide_b,
    )
    for chunk in range(2, chunks):
        transform(chunk)
        spread(0, chunk, 0)
    for chunk in range(chunks):
        spread(0, chunk, 1)
    spots = lax.broadcasted_iota(jnp.int32, row_ref.shape, 1)

    def invert(slot, carry):
        return jnp.where(spots == deg_ref[slot], slot, carry)

    row_ref[...] = lax.fori_loop(0, degrees, invert, spots * 0, unroll=4)
    turn = pltpu.make_async_copy(row_ref, slot_of, load_sem.at[2 * chunks + 1])
    turn.start()
    turn.wait()
    load_w.wait()
    to_filter_start(0, qtab, co)
    through_filter(0, ptab, co, mix)

    def between(chunk):
        load_cot(chunk).wait()
        for kind in range(kinds):
            reached_all(5, kind, chunk, band_in)
            left_for_owners(0, kind, chunk, band_out)

        def middle(row, carry):
            response = dot(inv_kf[...], pair(band_in, chunk, row))
            upstream = pair(cbuf, chunk, row).astype(jnp.float32) * gelu_slope(response)
            put_pair(band_out, chunk, row, dot(inv_fk[...], upstream.astype(jnp.bfloat16)))
            return carry

        lax.fori_loop(0, lat_dev // 2, middle, 0, unroll=3)
        spread(6, chunk, 0)
        spread(6, chunk, 1)

    def synth(base, tab, part, low, high):
        loop(low, high, lambda job: synthesise(base, tab, part, job))

    far = per_pass
    synth(0, ptab, 0, 2, 4)
    synth(0, ptab, 1, far, far + 2)
    synth(0, ptab, 0, 4, 5)
    between(0)
    synth(0, ptab, 0, 5, 6)
    synth(0, ptab, 1, far + 2, far + 6)
    between(1)
    between(2)
    to_filter_start(6, ptab, go)
    through_filter(6, qtab, go, adjoint)

    def weight_grad(slot, carry):
        values = joined(co, slot, slice(None))
        grads = joined(go, slot, slice(None))
        turned = pair_swap(grads.astype(jnp.float32), 1.0).astype(jnp.bfloat16)
        span = ((0,), (0,))
        dw[slot, 0] = dot(values, grads, span).astype(jnp.bfloat16)
        dw[slot, 1] = dot(values, turned, span).astype(jnp.bfloat16)
        return carry

    lax.fori_loop(0, slots, weight_grad, 0)
    dw_copies = []
    for step in range(1, nb):
        peer = lax.rem(me_b + step, nb)
        copy = pltpu.make_async_remote_copy(
            src_ref=dw,
            dst_ref=dw_in.at[step - 1],
            send_sem=dw_send.at[step - 1],
            recv_sem=dw_recv.at[step - 1],
            device_id={"batch": peer},
            device_id_type=mesh_id,
        )
        copy.start()
        dw_copies.append(copy)

    def store(chunk):
        return pltpu.make_async_copy(
            cbuf.at[chunk], grad_out.at[0, :, :, lanes(chunk)], out_sem.at[chunk]
        )

    store_w = pltpu.make_async_copy(dw, dw_out, out_sem.at[chunks])

    def total(slot, carry):
        value = dw[slot].astype(jnp.float32)
        for step in range(nb - 1):
            value = value + dw_in[step, slot].astype(jnp.float32)
        dw[slot] = value.astype(jnp.bfloat16)
        return carry

    def last(chunk):
        if chunk == 0:
            for copy in dw_copies:
                copy.wait()
            lax.fori_loop(0, slots, total, 0)
            store_w.start()
        for kind in range(kinds):
            reached_all(11, kind, chunk, band_in)

        def finish(row, carry):
            delta = dot(fwd_kf[...], pair(band_in, chunk, row))
            put_pair(cbuf, chunk, row, pair(cbuf, chunk, row).astype(jnp.float32) + delta)
            return carry

        lax.fori_loop(0, lat_dev // 2, finish, 0, unroll=3)
        store(chunk).start()

    synth(6, qtab, 0, 2, 4)
    synth(6, qtab, 1, far, far + 2)
    synth(6, qtab, 0, 4, 5)
    last(0)
    synth(6, qtab, 0, 5, 6)
    synth(6, qtab, 1, far + 2, far + 6)
    last(1)
    last(2)
    for chunk in range(chunks):
        for kind in range(kinds):
            left_for_owners(6, kind, chunk, band_out)
            left_for_owners(9, kind, chunk, mixed)

    def drain(part, job):
        kind, chunk, place = job_of(job)

        @pl.when(mine(kind))
        def _():
            if part:
                await_tail(kind, cross_out.at[place, chunk], send_sem.at[7, job])
                await_tail(kind, tail_out.at[chunk], send_sem.at[10, job])
            else:
                await_bytes(cross_out.at[place, chunk], send_sem.at[7, job])
                await_bytes(slot_all.at[place, chunk, 0:own], send_sem.at[10, job])
            left_owner(8, job, kind, chunk, slot_out, slots)
            left_owner(11, job, kind, chunk, ord_out, lat_dev)

    loop(0, per_pass, lambda job: drain(0, job))
    loop(per_pass, jobs, lambda job: drain(1, job))
    for chunk in range(chunks):
        store(chunk).wait()
    store_w.wait()


def local_kernel(fields, cotangent, weights, degree_of):
    n = lax.axis_size("lat")
    nb = lax.axis_size("batch")
    kinds = 4
    if fields.shape[0] != 1 or fields.shape[1] % 2 or n % kinds or ORDERS != n * GROUP:
        return local(fields, cotangent, weights, degree_of)
    lat_dev, lons, channels = fields.shape[1:]
    slots = weights.shape[0]
    rows = 2 * GROUP
    chunks = channels // LANES
    floats, waves = constant_tables()
    side_lats = LATS // 2
    held = kinds - 1
    vmem = pl.BlockSpec(memory_space=pltpu.VMEM)
    anywhere = pl.BlockSpec(memory_space=pl.ANY)

    def buffer(*dims):
        return pltpu.VMEM(dims, jnp.bfloat16)

    dma = pltpu.SemaphoreType.DMA
    others = max(nb - 1, 1)
    wide_rows = max(side_lats, DEGREES) * rows
    return pl.pallas_call(
        functools.partial(block_kernel, n, nb),
        out_shape=(
            jax.ShapeDtypeStruct(fields.shape, jnp.bfloat16),
            jax.ShapeDtypeStruct(weights.shape, jnp.bfloat16),
        ),
        in_specs=[anywhere] * 3 + [pl.BlockSpec(memory_space=pltpu.SMEM)] + [vmem] * 7,
        out_specs=(anywhere, anywhere),
        scratch_shapes=[
            buffer(chunks, lat_dev, lons, LANES),
            buffer(chunks, lat_dev, lons, LANES),
            buffer(*weights.shape),
            buffer(chunks, lat_dev, n * rows, LANES),
            buffer(chunks, lat_dev, n * rows, LANES),
            buffer(held, chunks, side_lats, rows, LANES),
            buffer(held, chunks, side_lats, rows, LANES),
            buffer(held, chunks, DEGREES // 2, rows, LANES),
            buffer(held, chunks, DEGREES // 2, rows, LANES),
            buffer(held, chunks, DEGREES // 2, rows, LANES),
            buffer(held, chunks, DEGREES, rows, LANES),
            buffer(chunks, DEGREES // 2, rows, LANES),
            buffer(chunks, slots, n * rows, LANES),
            buffer(chunks, slots, n * rows, LANES),
            buffer(chunks, slots, n * rows, LANES),
            pltpu.VMEM((wide_rows, LANES), jnp.float32),
            pltpu.VMEM((4 * wide_rows, LANES), jnp.float32),
            pltpu.VMEM((side_lats * rows, LANES), jnp.float32),
            buffer(*weights.shape),
            buffer(others, *weights.shape),
            buffer(kinds, GROUP, DEGREES, side_lats),
            buffer(kinds, GROUP, DEGREES, side_lats),
            pltpu.VMEM((DEGREES, kinds * GROUP, LANES), jnp.float32),
            pltpu.VMEM((GROUP, DEGREES), jnp.int32),
            pltpu.SMEM((GROUP, DEGREES), jnp.int32),
            buffer(DEGREES, rows, LANES),
            dma((2 * chunks + 2,)),
            dma((12, kinds * chunks)),
            dma((12, kinds * chunks)),
            dma((others,)),
            dma((others,)),
            dma((chunks + 1,)),
        ],
        compiler_params=pltpu.CompilerParams(
            collective_id=0, has_side_effects=True, vmem_limit_bytes=63 * 2**20
        ),
        name="filter_block",
    )(
        fields, cotangent, weights, degree_of, *floats, *waves,
    )


def local(fields, cotangent, weights, degree_of):
    samples = fields.shape[0]
    band_rows = fields.shape[1]
    ord_dev = ORDERS // lax.axis_size("lat")
    forward, inverse = fourier_tables(LONS, ORDERS)
    qslot, pslot = spectral_tables(lax.axis_index("lat") * ord_dev, ord_dev, degree_of)
    spectra = product("sikc,kf->ifsc", fields, forward).astype(jnp.bfloat16)
    spectra = spectra.reshape(band_rows, ORDERS, 2, samples, CHANNELS)
    gathered = to_orders(spectra)
    coeffs_local = product("mji,imrsc->jmrsc", qslot, gathered).astype(jnp.bfloat16)
    coeffs = to_degrees(coeffs_local)
    filtered = apply_filter(coeffs, weights)
    returned = back_to_orders(filtered)
    synth_local = product("mji,jmrsc->imrsc", pslot, returned).astype(jnp.bfloat16)
    synth = to_bands(synth_local)
    response = product(
        "ifsc,fk->sikc", synth.reshape(band_rows, 2 * ORDERS, samples, CHANNELS), inverse
    )
    activated, pullback = jax.vjp(jax.nn.gelu, response)
    upstream = pullback(cotangent.astype(jnp.float32))[0].astype(jnp.bfloat16)
    grad_synth = product("sikc,fk->ifsc", upstream, inverse).astype(jnp.bfloat16)
    grad_synth = grad_synth.reshape(band_rows, ORDERS, 2, samples, CHANNELS)
    grad_gathered = to_orders(grad_synth)
    grad_local = product("mji,imrsc->jmrsc", pslot, grad_gathered).astype(jnp.bfloat16)
    grad_filtered = to_degrees(grad_local)
    weight_total = lax.psum(filter_grad(coeffs, grad_filtered).astype(jnp.bfloat16), "batch")
    grad_coeffs = adjoint_filter(grad_filtered, weights)
    grad_back = back_to_orders(grad_coeffs)
    grad_local_spec = product("mji,jmrsc->imrsc", qslot, grad_back).astype(jnp.bfloat16)
    grad_bands = to_bands(grad_local_spec)
    delta = product(
        "ifsc,kf->sikc", grad_bands.reshape(band_rows, 2 * ORDERS, samples, CHANNELS), forward
    )
    grad_fields = (cotangent.astype(jnp.float32) + delta).astype(jnp.bfloat16)
    return (grad_fields, weight_total)


def solution(mesh):
    return jax.shard_map(
        local_kernel if CHANNELS % LANES == 0 else local,
        mesh=mesh,
        in_specs=(
            P("batch", "lat", None, None),
            P("batch", "lat", None, None),
            P("lat", None, None, None),
            P(),
        ),
        out_specs=(P("batch", "lat", None, None), P("lat", None, None, None)),
        check_vma=False,
    )
```

```python
import functools

import jax
import numpy as np
import jax.numpy as jnp
from jax import lax
from jax.experimental import pallas as pl
from jax.experimental.pallas import tpu as pltpu
from jax.sharding import PartitionSpec as P

LATS = 192
LONS = 384
ORDERS = 128
DEGREES = 128
CHANNELS = 384
LANES = 128
GROUP = 8


def table_kernel(deg_ref, diag_ref, cos_ref, quad_ref, order_ref, q_ref, p_ref, slot_ref, rows_ref):
    orders = diag_ref.shape[0]
    lats = q_ref.shape[2]
    degrees = deg_ref.shape[0]

    def invert(slot, carry):
        slot_ref[deg_ref[slot]] = slot
        return carry

    lax.fori_loop(0, degrees, invert, 0)
    order_real = order_ref[...]
    squared = order_real * order_real
    diagonal = diag_ref[...]
    cosine = cos_ref[...]
    first_lead = jnp.sqrt(2.0 * order_real + 3.0)
    halves = rows_ref.shape[0]

    def advance(degree, carry):
        previous, older = carry
        degree_real = degree.astype(jnp.float32)
        lead = jnp.sqrt(
            jnp.maximum(4.0 * degree_real * degree_real - 1.0, 0.0)
            / jnp.maximum(degree_real * degree_real - squared, 1.0)
        )
        lower = degree_real - 1.0
        back = jnp.sqrt(
            jnp.maximum(lower * lower - squared, 0.0) / jnp.maximum(4.0 * lower * lower - 1.0, 1.0)
        )
        general = lead * (cosine * previous - back * older)
        first = first_lead * cosine * previous
        value = jnp.where(
            degree_real == order_real,
            diagonal,
            jnp.where(
                degree_real == order_real + 1.0,
                first,
                jnp.where(degree_real > order_real + 1.0, general, 0.0),
            ),
        )
        slot = slot_ref[degree]
        for half in range(halves):
            rows_ref[half, pl.ds(slot, orders, stride=degrees), :] = value[
                :, half * LANES : (half + 1) * LANES
            ]
        return (value, previous)

    zeros = diagonal * 0.0
    lax.fori_loop(0, degrees, advance, (zeros, zeros), unroll=4)
    quadrature = quad_ref[...]
    for order in range(orders):
        for half in range(halves):
            low = half * LANES
            high = min(lats, low + LANES)
            chosen = rows_ref[half, order * degrees : (order + 1) * degrees, :][:, : high - low]
            p_ref[order, :, low:high] = chosen.astype(jnp.bfloat16)
            q_ref[order, :, low:high] = (chosen * quadrature[:, low:high]).astype(jnp.bfloat16)


def spectral_tables(start, ord_dev, degree_of):
    halves = -(-LATS // LANES)
    padded = halves * LANES
    order_col = (start + jnp.arange(ord_dev, dtype=jnp.int32)).astype(jnp.float32)[:, None]
    lat_ids = jnp.minimum(jnp.arange(padded, dtype=jnp.float32), LATS - 1.0)
    colatitude = jnp.pi * (lat_ids + 0.5) / LATS
    sine = jnp.sin(colatitude)[None, :]
    steps_up = jnp.arange(1, DEGREES + 1, dtype=jnp.float32)[None, :]
    factor = jnp.where(
        steps_up <= order_col, 0.5 * jnp.log((2.0 * steps_up + 1.0) / (2.0 * steps_up)), 0.0
    )
    log_start = 0.5 * jnp.log(1.0 / (4.0 * jnp.pi)) + jnp.sum(factor, axis=1, keepdims=True)
    diagonal = jnp.exp(log_start + order_col * jnp.log(sine))
    cosine = jnp.broadcast_to(jnp.cos(colatitude)[None, :], diagonal.shape)
    quadrature = 2.0 * jnp.pi * jnp.pi / LATS * sine
    orders = jnp.broadcast_to(order_col, diagonal.shape)
    vmem = pl.BlockSpec(memory_space=pltpu.VMEM)
    shape = jax.ShapeDtypeStruct((ord_dev, DEGREES, LATS), jnp.bfloat16)
    return pl.pallas_call(
        table_kernel,
        out_shape=(shape, shape),
        in_specs=[pl.BlockSpec(memory_space=pltpu.SMEM)] + [vmem] * 4,
        out_specs=(vmem, vmem),
        scratch_shapes=[
            pltpu.SMEM((DEGREES,), jnp.int32),
            pltpu.VMEM((halves, ord_dev * DEGREES, LANES), jnp.float32),
        ],
        name="legendre_tables",
    )(degree_of, diagonal, cosine, quadrature, orders)


def fourier_tables(lon_count, order_count):
    lon_ids = jnp.arange(lon_count, dtype=jnp.int32)[:, None]
    order_ids = jnp.arange(order_count, dtype=jnp.int32)[None, :]
    phase = 2.0 * jnp.pi * (lon_ids * order_ids % lon_count).astype(jnp.float32) / lon_count
    forward = (
        jnp.stack([jnp.cos(phase), -jnp.sin(phase)], axis=2).reshape(lon_count, 2 * order_count)
        / lon_count
    )
    doubled = jnp.where(order_ids == 0, 1.0, 2.0)
    inverse = jnp.stack([doubled * jnp.cos(phase), -doubled * jnp.sin(phase)], axis=2).reshape(
        lon_count, 2 * order_count
    )
    return (forward.astype(jnp.bfloat16), jnp.transpose(inverse).astype(jnp.bfloat16))


def to_orders(values):
    return lax.all_to_all(values, "lat", split_axis=1, concat_axis=0, tiled=True)


def to_degrees(values):
    return lax.all_to_all(values, "lat", split_axis=0, concat_axis=1, tiled=True)


def back_to_orders(values):
    return lax.all_to_all(values, "lat", split_axis=1, concat_axis=0, tiled=True)


def to_bands(values):
    return lax.all_to_all(values, "lat", split_axis=0, concat_axis=1, tiled=True)


def product(spec, left, right):
    return jnp.einsum(spec, left, right, preferred_element_type=jnp.float32)


def apply_filter(coeffs, weights):
    c_real = coeffs[:, :, 0]
    c_imag = coeffs[:, :, 1]
    w_real = weights[:, 0]
    w_imag = weights[:, 1]
    f_real = product("jmsc,jcd->jmsd", c_real, w_real) - product("jmsc,jcd->jmsd", c_imag, w_imag)
    f_imag = product("jmsc,jcd->jmsd", c_real, w_imag) + product("jmsc,jcd->jmsd", c_imag, w_real)
    return jnp.stack([f_real, f_imag], axis=2).astype(jnp.bfloat16)


def adjoint_filter(grads, weights):
    g_real = grads[:, :, 0]
    g_imag = grads[:, :, 1]
    w_real = weights[:, 0]
    w_imag = weights[:, 1]
    a_real = product("jmsd,jcd->jmsc", g_real, w_real) + product("jmsd,jcd->jmsc", g_imag, w_imag)
    a_imag = product("jmsd,jcd->jmsc", g_imag, w_real) - product("jmsd,jcd->jmsc", g_real, w_imag)
    return jnp.stack([a_real, a_imag], axis=2).astype(jnp.bfloat16)


def filter_grad(coeffs, grads):
    c_real = coeffs[:, :, 0]
    c_imag = coeffs[:, :, 1]
    g_real = grads[:, :, 0]
    g_imag = grads[:, :, 1]
    dw_real = product("jmsc,jmsd->jcd", c_real, g_real) + product("jmsc,jmsd->jcd", c_imag, g_imag)
    dw_imag = product("jmsc,jmsd->jcd", c_real, g_imag) - product("jmsc,jmsd->jcd", c_imag, g_real)
    return jnp.stack([dw_real, dw_imag], axis=1)


def constant_tables():
    sides = 2
    half = LATS // sides
    lat_ids = np.minimum(np.arange(LANES)[None, :], half - 1) + half * np.arange(sides)[:, None]
    colatitude = np.pi * (lat_ids + 0.5) / LATS
    sine = np.sin(colatitude)[:, None, :]
    ids = np.arange(ORDERS)
    steps_up = np.arange(1, ORDERS + 1)
    growth = np.cumsum(0.5 * np.log((2.0 * steps_up + 1.0) / (2.0 * steps_up)))
    log_start = 0.5 * np.log(1.0 / (4.0 * np.pi)) + np.concatenate([[0.0], growth[:-1]])
    diagonal = np.exp(log_start[None, :, None] + ids[None, :, None] * np.log(sine))
    cosine = np.broadcast_to(np.cos(colatitude)[:, None, :], (sides, GROUP, LANES))
    quadrature = np.broadcast_to(2.0 * np.pi * np.pi / LATS * sine, (sides, GROUP, LANES))
    phase = 2.0 * np.pi * (np.arange(LONS)[:, None] * ids[None, :] % LONS) / LONS
    forward = np.stack([np.cos(phase), -np.sin(phase)], axis=2).reshape(LONS, -1) / LONS
    doubled = np.where(ids == 0, 1.0, 2.0)[None, :]
    inverse = np.stack([doubled * np.cos(phase), -doubled * np.sin(phase)], axis=2)
    inverse = inverse.reshape(LONS, -1)
    floats = [jnp.asarray(t, jnp.float32) for t in (diagonal, cosine, quadrature)]
    waves = [forward.T, forward, inverse.T, inverse]
    halves = [jnp.asarray(np.float32(t).astype(jnp.bfloat16)) for t in waves]
    return floats, halves


def fill_tables(side, firsts, deg_ref, diag_ref, cos_ref, quad_ref, qtab, ptab, table, by_slot):
    kinds, orders, degrees, lats = qtab.shape
    every = kinds * orders
    cosine = cos_ref[side]
    diagonal, ids, squared, first_lead = [], [], [], []
    for first in firsts:
        diagonal.append(diag_ref[side, pl.ds(pl.multiple_of(first, orders), orders), :])
        ids.append(first + lax.broadcasted_iota(jnp.int32, cosine.shape, 0))
        real = ids[-1].astype(jnp.float32)
        squared.append(real * real)
        first_lead.append(jnp.sqrt(2.0 * real + 3.0))

    def advance(degree, carry):
        degree_real = degree.astype(jnp.float32)
        lower = degree_real - 1.0
        state = []
        for kind in range(kinds):
            previous, older = carry[kind]
            lead = jnp.sqrt(
                jnp.maximum(4.0 * degree_real * degree_real - 1.0, 0.0)
                / jnp.maximum(degree_real * degree_real - squared[kind], 1.0)
            )
            back = jnp.sqrt(
                jnp.maximum(lower * lower - squared[kind], 0.0)
                / jnp.maximum(4.0 * lower * lower - 1.0, 1.0)
            )
            general = lead * (cosine * previous - back * older)
            first = first_lead[kind] * cosine * previous
            value = jnp.where(
                ids[kind] == degree,
                diagonal[kind],
                jnp.where(
                    ids[kind] + 1 == degree,
                    first,
                    jnp.where(ids[kind] + 1 < degree, general, 0.0),
                ),
            )
            table[degree, kind * orders : (kind + 1) * orders, :] = value
            state.append((value, previous))
        return tuple(state)

    zeros = cosine * 0.0
    lax.fori_loop(0, degrees, advance, ((zeros, zeros),) * kinds, unroll=2)

    ahead = every // 2
    tail = degrees // 2

    def place(slot, carry):
        by_slot[pl.ds(slot, ahead, stride=degrees), :] = table[deg_ref[slot], :ahead]
        return carry

    lax.fori_loop(0, degrees, place, 0, unroll=4)

    def place_tail(row, carry):
        spots = pl.ds(ahead * degrees + row, ahead, stride=degrees)
        by_slot[spots, :] = table[tail + row, ahead:]
        return carry

    lax.fori_loop(0, tail, place_tail, 0, unroll=4)
    quadrature = quad_ref[side][:1, :lats]
    for kind in range(kinds):

        def keep(order, carry):
            start = pl.multiple_of((kind * orders + order) * degrees, degrees)
            depth = degrees if kind < kinds // 2 else tail
            chosen = by_slot[pl.ds(start, depth), :][:, :lats]
            ptab[kind, order, :depth] = chosen.astype(jnp.bfloat16)
            qtab[kind, order, :depth] = (chosen * quadrature).astype(jnp.bfloat16)
            return carry

        lax.fori_loop(0, orders, keep, 0)


def pair_swap(values, even_sign):
    rows = values.shape[0]
    even = lax.broadcasted_iota(jnp.int32, values.shape, 0) % 2 == 0
    above = pltpu.roll(values, rows - 1, 0)
    below = pltpu.roll(values, 1, 0)
    return jnp.where(even, even_sign * above, -even_sign * below)


def gelu_slope(x):
    scale = 0.7978845608028654
    square = x * x
    t = jnp.tanh(scale * (x + 0.044715 * x * square))
    return 0.5 * (1.0 + t) + 0.5 * x * (1.0 - t * t) * (scale * (1.0 + 0.134145 * square))


def dot(left, right, dims=((1,), (0,))):
    return lax.dot_general(left, right, (dims, ((), ())), preferred_element_type=jnp.float32)


def block_kernel(
    n, nb, fields, cotangent, weights, deg_ref, diag_ref, cos_ref, quad_ref,
    fwd_fk, fwd_kf, inv_fk, inv_kf,
    grad_out, dw_out,
    fbuf, cbuf, wbuf, band_out, band_in, ord_in, ord_out, cross_out, cross_in, slot_out, slot_all,
    tail_out, co, go, mixed, wide_a, wide_b, wide_c, dw, dw_in, qtab, ptab, table, row_ref, slot_of, by_name,
    load_sem, send_sem, recv_sem, dw_send, dw_recv, out_sem,
):
    me = lax.axis_index("lat")
    me_b = lax.axis_index("batch")
    chunks, lat_dev = fbuf.shape[0], fbuf.shape[1]
    kinds, orders, degrees, side_lats = qtab.shape
    rows = 2 * orders
    slots = co.shape[1]
    quarter = n // kinds
    half = n // 2
    own = half * slots
    inner_kinds = ord_in.shape[0]
    pairs = kinds // 2
    jobs = kinds * chunks
    plane_rows = quarter * rows
    mesh_id = pl.DeviceIdType.MESH
    side = lax.div(me, half)
    place_in = lax.rem(me, half)
    column = lax.rem(me, quarter)
    inner = jnp.where(lax.div(me, quarter) == 1 + side, 1, 0)
    across = 1 - side

    def lanes(chunk):
        return pl.ds(chunk * LANES, LANES)

    def group(kind, at):
        return jnp.where(
            lax.rem(kind, 2) == 0, kind * quarter + at, (kind + 1) * quarter - 1 - at
        )

    def group_rows(kind, at):
        return pl.ds(pl.multiple_of(group(kind, at) * rows, rows), rows)

    def owner(kind, on_side, at):
        plane = jnp.where(kind < inner_kinds, 1 + on_side, (kinds - 1) * on_side)
        return plane * quarter + at

    def mine(kind):
        return jnp.where(kind < inner_kinds, 1, 0) == inner

    def job_of(job):
        per_pass = pairs * chunks
        inside = lax.rem(job, per_pass)
        kind = lax.div(job, per_pass) * pairs + lax.rem(inside, pairs)
        return kind, lax.div(inside, pairs), lax.rem(kind, inner_kinds)

    def first_block(kind):
        return group(kind, column) - own // orders

    def tail_blocks(kind, body):
        def one(block, carry):
            body(pl.multiple_of(block * orders, orders))
            return carry

        lax.fori_loop(first_block(kind), own // orders, one, 0)

    def await_tail(kind, view, sem):
        for first in range(own // orders):

            @pl.when(first_block(kind) == first)
            def _():
                await_bytes(view.at[pl.ds(0, own - first * orders)], sem)

    def job_at(kind, chunk):
        return (kind // pairs) * (pairs * chunks) + chunk * pairs + kind % pairs

    def load(chunk):
        return pltpu.make_async_copy(
            fields.at[0, :, :, lanes(chunk)], fbuf.at[chunk], load_sem.at[chunk]
        )

    def load_cot(chunk):
        return pltpu.make_async_copy(
            cotangent.at[0, :, :, lanes(chunk)], cbuf.at[chunk], load_sem.at[chunks + chunk]
        )

    load_w = pltpu.make_async_copy(weights, wbuf, load_sem.at[2 * chunks])
    for chunk in range(chunks):
        load(chunk).start()
    load_w.start()
    for chunk in range(chunks):
        load_cot(chunk).start()

    barrier = pltpu.get_barrier_semaphore()

    def greet(step, carry):
        peer = lax.rem(me + step, n)
        pl.semaphore_signal(barrier, inc=1, device_id={"lat": peer}, device_id_type=mesh_id)
        return carry

    lax.fori_loop(1, n, greet, 0)
    for step in range(1, nb):
        peer = lax.rem(me_b + step, nb)
        pl.semaphore_signal(barrier, inc=1, device_id={"batch": peer}, device_id_type=mesh_id)

    def remote(stage, job, source, target, peer):
        pltpu.make_async_remote_copy(
            src_ref=source,
            dst_ref=target,
            send_sem=send_sem.at[stage, job],
            recv_sem=recv_sem.at[stage, job],
            device_id={"lat": peer},
            device_id_type=mesh_id,
        ).start()

    def await_bytes(view, sem):
        pltpu.make_async_copy(view, view, sem).wait()

    def to_owners(stage, kind, chunk, source, target, width):
        job = job_at(kind, chunk)
        for step in range(quarter):
            at = lax.rem(column + step, quarter)
            view = source.at[chunk, :, group_rows(kind, at), :]
            spot = target(kind % inner_kinds, chunk)
            peer = owner(kind, side, at)

            @pl.when(peer != me)
            def _():
                remote(stage, job, view, spot, peer)

            @pl.when(peer == me)
            def _():
                pltpu.make_async_copy(view, spot, recv_sem.at[stage, job]).start()

    def left_for_owners(stage, kind, chunk, source):
        job = job_at(kind, chunk)

        @pl.when(mine(kind))
        def _():
            await_bytes(source.at[chunk, :, 0 : plane_rows - rows, :], send_sem.at[stage, job])

        @pl.when(jnp.logical_not(mine(kind)))
        def _():
            await_bytes(source.at[chunk, :, 0:plane_rows, :], send_sem.at[stage, job])

    def from_owner(stage, job, kind, chunk, source, depth, target):
        place = lax.rem(kind, inner_kinds)
        spot = target.at[chunk, :, group_rows(kind, column), :]

        def send(step, carry):
            at = lax.rem(place_in + step, half)
            remote(
                stage, job, source.at[place, chunk, pl.ds(at * depth, depth)], spot,
                side * half + at,
            )
            return carry

        lax.fori_loop(1, half, send, 0)
        pltpu.make_async_copy(
            source.at[place, chunk, pl.ds(place_in * depth, depth)], spot, recv_sem.at[stage, job]
        ).start()

    def left_owner(stage, job, kind, chunk, source, depth):
        view = source.at[lax.rem(kind, inner_kinds), chunk, 0 : (half - 1) * depth]
        await_bytes(view, send_sem.at[stage, job])

    def reached_all(stage, kind, chunk, target):
        await_bytes(target.at[chunk, :, 0:plane_rows, :], recv_sem.at[stage, job_at(kind, chunk)])

    def lat_spot(place, chunk):
        return ord_in.at[place, chunk, pl.ds(place_in * lat_dev, lat_dev)]

    def slot_spot(place, chunk):
        return slot_all.at[place, chunk, pl.ds(me * slots, slots)]

    def wide_start(part, job):
        if part:
            spot = lax.rem(lax.div(job - pairs * chunks, pairs) + pairs, chunks)
        else:
            spot = jnp.where(job < 2 * pairs, lax.rem(job, pairs), job - pairs)
        return pl.multiple_of(spot * wide_a.shape[0], 8)

    def widen(source, place, chunk, depth, count):
        def one(block, carry):
            piece = source[place, chunk, pl.ds(block * depth, depth)].astype(jnp.float32)
            wide_a[pl.ds(pl.multiple_of(block * depth * rows, depth * rows), depth * rows), :] = (
                piece.reshape(depth * rows, LANES)
            )
            return carry

        lax.fori_loop(0, count // depth, one, 0)

    def apply_table(tab, kind, kept, result_ref, start, depth_in, depth_out, dims):
        def one(order, carry):
            real = wide_a[pl.ds(2 * order, depth_in, stride=rows), :]
            imag = wide_a[pl.ds(2 * order + 1, depth_in, stride=rows), :]
            both = jnp.concatenate([real, imag], axis=1).astype(jnp.bfloat16)
            result = dot(tab[kind, order, :kept], both, dims)
            result_ref[pl.ds(start + 2 * order, depth_out, stride=rows), :] = result[:, :LANES]
            result_ref[pl.ds(start + 2 * order + 1, depth_out, stride=rows), :] = result[:, LANES:]
            return carry

        lax.fori_loop(0, orders, one, 0, unroll=4)

    def narrow(source, target, place, chunk, start, depth, count):
        def one(block, carry):
            low = pl.multiple_of(start + block * depth * rows, 8)
            piece = source[pl.ds(low, depth * rows), :]
            target[place, chunk, pl.ds(block * depth, depth)] = piece.reshape(
                depth, rows, LANES
            ).astype(jnp.bfloat16)
            return carry

        lax.fori_loop(0, count // depth, one, 0)

    def wide_rows(start, index, depth):
        return pl.ds(pl.multiple_of(start + index * rows, 8), depth * rows)

    def blank(first, count):
        def one(block, carry):
            by_name[pl.ds((first + block) * orders, orders)] = jnp.zeros(
                (orders, rows, LANES), jnp.bfloat16
            )
            return carry

        lax.fori_loop(0, count, one, 0)

    def analyse(base, tab, part, job):
        kind, chunk, place = job_of(job)

        @pl.when(mine(kind))
        def _():
            await_bytes(ord_in.at[place, chunk], recv_sem.at[base, job])
            widen(ord_in, place, chunk, lat_dev, side_lats)
            start = wide_start(part, job)
            peer = owner(kind, across, column)
            source = cross_out.at[place, chunk]
            target = cross_in.at[place, chunk]
            kept = own if part else degrees
            apply_table(tab, kind, kept, wide_b, start, side_lats, kept, ((1,), (0,)))
            if not part:
                if base:
                    await_bytes(source, send_sem.at[1, job])
                narrow(wide_b, cross_out, place, chunk, start + across * own * rows, slots, own)
                remote(base + 1, job, source, target, peer)
                return
            if base:
                await_tail(kind, source, send_sem.at[1, job])

            def send(low):
                span = pl.ds(low, orders)
                piece = wide_b[wide_rows(start, low, orders), :]
                cross_out[place, chunk, span] = piece.reshape(orders, rows, LANES).astype(
                    jnp.bfloat16
                )
                remote(base + 1, job, source.at[span], target.at[span], peer)

            tail_blocks(kind, send)

    def settle(base, target, part, job):
        kind, chunk, place = job_of(job)

        @pl.when(mine(kind))
        def _():
            start = wide_start(part, job)
            if part:
                await_tail(kind, cross_in.at[place, chunk], recv_sem.at[base + 1, job])
            else:
                await_bytes(cross_in.at[place, chunk], recv_sem.at[base + 1, job])
            if base:
                left_owner(2, job, kind, chunk, slot_out, slots)
                if part:
                    await_tail(kind, tail_out.at[chunk], send_sem.at[4, job])
                else:
                    await_bytes(slot_all.at[place, chunk, 0:own], send_sem.at[4, job])
            if part:

                blank(0, own // orders + first_block(kind))

                def add(low):
                    piece = wide_b[wide_rows(start, low, orders), :]
                    other = cross_in[place, chunk, pl.ds(low, orders)].astype(jnp.float32)
                    by_name[pl.ds(own + low, orders)] = (
                        piece.reshape(orders, rows, LANES) + other
                    ).astype(jnp.bfloat16)

                tail_blocks(kind, add)

                def pick(slot, carry):
                    slot_out[place, chunk, slot] = by_name[deg_ref[side * own + slot]]
                    return carry

                lax.fori_loop(0, own, pick, 0, unroll=4)
            else:

                def one(block, carry):
                    low = block * slots
                    piece = wide_b[wide_rows(start + side * own * rows, low, slots), :]
                    other = cross_in[place, chunk, pl.ds(low, slots)].astype(jnp.float32)
                    slot_out[place, chunk, pl.ds(low, slots)] = (
                        piece.reshape(slots, rows, LANES) + other
                    ).astype(jnp.bfloat16)
                    return carry

                lax.fori_loop(0, half, one, 0)
            from_owner(base + 2, job, kind, chunk, slot_out, slots, target)

    def relay(base, part, job):
        kind, chunk, place = job_of(job)

        @pl.when(mine(kind))
        def _():
            await_bytes(slot_all.at[place, chunk, 0:own], recv_sem.at[base + 3, job])
            peer = owner(kind, across, column)
            view = slot_all.at[place, chunk, pl.ds(side * own, own)]
            if not part:
                remote(base + 4, job, view, view, peer)
                return

            blank(across * (own // orders), own // orders)

            def copy(block, carry):
                span = pl.ds(side * own + block * slots, slots)
                by_name[span] = slot_all[place, chunk, span]
                return carry

            lax.fori_loop(0, half, copy, 0)

            def send(low):
                for step in range(orders):
                    tail_out[chunk, low + step] = by_name[slot_of[0, own + low + step]]
                span = pl.ds(low, orders)
                remote(base + 4, job, tail_out.at[chunk, span], view.at[span], peer)

            tail_blocks(kind, send)

    def synthesise(base, tab, part, job):
        kind, chunk, place = job_of(job)

        @pl.when(mine(kind))
        def _():
            if part:
                await_tail(kind, tail_out.at[chunk], recv_sem.at[base + 4, job])

                def clear(block, carry):
                    wide_a[wide_rows(0, block * orders, orders), :] = jnp.zeros(
                        (orders * rows, LANES), jnp.float32
                    )
                    return carry

                lax.fori_loop(0, first_block(kind), clear, 0)

                def add(low):
                    near = tail_out[chunk, pl.ds(low, orders)].astype(jnp.float32)
                    far = slot_all[place, chunk, pl.ds(across * own + low, orders)]
                    wide_a[wide_rows(0, low, orders), :] = (
                        near + far.astype(jnp.float32)
                    ).reshape(orders * rows, LANES)

                tail_blocks(kind, add)
                apply_table(tab, kind, own, wide_c, 0, own, side_lats, ((0,), (0,)))
            else:
                await_bytes(slot_all.at[place, chunk, 0:own], recv_sem.at[base + 4, job])
                widen(slot_all, place, chunk, slots, degrees)
                apply_table(tab, kind, degrees, wide_c, 0, degrees, side_lats, ((0,), (0,)))
            if base:
                left_owner(5, job, kind, chunk, ord_out, lat_dev)
            narrow(wide_c, ord_out, place, chunk, 0, lat_dev, side_lats)
            from_owner(base + 5, job, kind, chunk, ord_out, lat_dev, band_in)

    def loop(low, high, body):
        def one(job, carry):
            body(job)
            return carry

        lax.fori_loop(low, high, one, 0)

    def pair(source, chunk, row):
        return jnp.concatenate([source[chunk, 2 * row], source[chunk, 2 * row + 1]], axis=1)

    def put_pair(target, chunk, row, values):
        values = values.astype(jnp.bfloat16)
        target[chunk, 2 * row] = values[:, :LANES]
        target[chunk, 2 * row + 1] = values[:, LANES:]

    def joined(source, slot, span):
        return jnp.concatenate([source[chunk, slot, span] for chunk in range(chunks)], axis=1)

    def mix(part, chunk):
        low = part * pairs * plane_rows
        span = slice(low, low + pairs * plane_rows)
        columns = slice(chunk * LANES, (chunk + 1) * LANES)

        def one(slot, carry):
            both = dot(
                joined(co, slot, span),
                jnp.concatenate([wbuf[slot, 0, :, columns], wbuf[slot, 1, :, columns]], axis=1),
            )
            crossed = pair_swap(both[:, LANES:], -1.0)
            mixed[chunk, slot, span] = (both[:, :LANES] + crossed).astype(jnp.bfloat16)
            return carry

        return one

    def adjoint(part, chunk):
        low = part * pairs * plane_rows
        span = slice(low, low + pairs * plane_rows)
        columns = slice(chunk * LANES, (chunk + 1) * LANES)

        def one(slot, carry):
            both = dot(
                joined(go, slot, span),
                jnp.concatenate([wbuf[slot, 0, columns, :], wbuf[slot, 1, columns, :]], axis=0),
                ((1,), (1,)),
            )
            crossed = pair_swap(both[:, LANES:], 1.0)
            mixed[chunk, slot, span] = (both[:, :LANES] + crossed).astype(jnp.bfloat16)
            return carry

        return one

    def filter_part(base, part, source, make):
        part_kinds = range(part * pairs, (part + 1) * pairs)
        for chunk in range(chunks):
            for kind in part_kinds:
                reached_all(base + 2, kind, chunk, source)
        for chunk in range(chunks):
            if base:
                for kind in part_kinds:
                    left_for_owners(3, kind, chunk, mixed)
            lax.fori_loop(0, slots, make(part, chunk), 0, unroll=4)
            for kind in part_kinds:
                to_owners(base + 3, kind, chunk, mixed, slot_spot, slots)

    per_pass = pairs * chunks
    def unit(part, chunk):
        first = part * per_pass + chunk * pairs
        return first, first + pairs

    def run(spans, body):
        loop(spans[0], spans[1], body)

    def to_filter_start(base, tab, source, between_first):
        loop(0, 1, lambda job: analyse(base, tab, 0, job))
        between_first()
        loop(1, pairs, lambda job: analyse(base, tab, 0, job))
        for low, high, part, behind in (
            (pairs, per_pass, 0, 0),
            (per_pass, per_pass + pairs, 1, 0),
            (per_pass + pairs, per_pass + 2 * pairs, 1, 1),
        ):

            def step(job):
                settle(base, source, behind, job - pairs)
                analyse(base, tab, part, job)

            loop(low, high, step)
        loop(per_pass + 2 * pairs, jobs, lambda job: analyse(base, tab, 1, job))

    def through_filter(base, tab, source, make):
        filter_part(base, 0, source, make)
        run(unit(1, 1), lambda job: settle(base, source, 1, job))
        run(unit(0, 0), lambda job: relay(base, 0, job))
        run(unit(1, 2), lambda job: settle(base, source, 1, job))
        run(unit(0, 1), lambda job: relay(base, 0, job))
        run(unit(0, 0), lambda job: synthesise(base, tab, 0, job))
        run(unit(0, 2), lambda job: relay(base, 0, job))
        loop(pairs, pairs + 1, lambda job: synthesise(base, tab, 0, job))
        filter_part(base, 1, source, make)
        loop(pairs + 1, 2 * pairs, lambda job: synthesise(base, tab, 0, job))
        loop(per_pass, jobs, lambda job: relay(base, 1, job))

    def spread(stage, chunk, part):
        for kind in range(part * pairs, (part + 1) * pairs):
            to_owners(stage, kind, chunk, band_out, lat_spot, lat_dev)

    def transform(chunk):
        load(chunk).wait()

        def fourier(row, carry):
            put_pair(band_out, chunk, row, dot(fwd_fk[...], pair(fbuf, chunk, row)))
            return carry

        lax.fori_loop(0, lat_dev // 2, fourier, 0, unroll=3)

    transform(0)
    pl.semaphore_wait(barrier, n - 1 + nb - 1)
    spread(0, 0, 0)
    transform(1)
    spread(0, 1, 0)
    fill_tables(
        side, [group(kind, column) * orders for kind in range(kinds)], deg_ref, diag_ref, cos_ref,
        quad_ref, qtab, ptab, table, wide_b,
    )
    for chunk in range(2, chunks):
        transform(chunk)
        spread(0, chunk, 0)
    for chunk in range(chunks):
        spread(0, chunk, 1)
    spots = lax.broadcasted_iota(jnp.int32, row_ref.shape, 1)

    def invert(slot, carry):
        return jnp.where(spots == deg_ref[slot], slot, carry)

    row_ref[...] = lax.fori_loop(0, degrees, invert, spots * 0, unroll=4)
    turn = pltpu.make_async_copy(row_ref, slot_of, load_sem.at[2 * chunks + 1])
    turn.start()
    turn.wait()
    load_w.wait()
    to_filter_start(0, qtab, co, lambda: None)
    through_filter(0, ptab, co, mix)

    def between(chunk):
        load_cot(chunk).wait()
        for kind in range(kinds):
            reached_all(5, kind, chunk, band_in)
            left_for_owners(0, kind, chunk, band_out)

        def middle(row, carry):
            response = dot(inv_kf[...], pair(band_in, chunk, row))
            upstream = pair(cbuf, chunk, row).astype(jnp.float32) * gelu_slope(response)
            put_pair(band_out, chunk, row, dot(inv_fk[...], upstream.astype(jnp.bfloat16)))
            return carry

        lax.fori_loop(0, lat_dev // 2, middle, 0, unroll=3)
        spread(6, chunk, 0)
        spread(6, chunk, 1)

    def finish_synthesis(base, tab, finish):
        def apart(chunk):
            loop(0, 1, lambda step: synthesise(base, tab, 1, per_pass + chunk * pairs + step))

        loop(
            0, chunks, lambda step: synthesise(base, tab, 1, per_pass + (step + 1) * pairs - 1)
        )
        loop(2 * pairs, per_pass, lambda job: synthesise(base, tab, 0, job))
        apart(0)
        for chunk in range(1, chunks):
            apart(chunk)
            finish(chunk - 1)

    finish_synthesis(0, ptab, between)
    to_filter_start(6, ptab, go, lambda: between(chunks - 1))
    through_filter(6, qtab, go, adjoint)

    def weight_grad(slot, carry):
        values = joined(co, slot, slice(None))
        grads = joined(go, slot, slice(None))
        turned = pair_swap(grads.astype(jnp.float32), 1.0).astype(jnp.bfloat16)
        span = ((0,), (0,))
        dw[slot, 0] = dot(values, grads, span).astype(jnp.bfloat16)
        dw[slot, 1] = dot(values, turned, span).astype(jnp.bfloat16)
        return carry

    lax.fori_loop(0, slots, weight_grad, 0)
    dw_copies = []
    for step in range(1, nb):
        peer = lax.rem(me_b + step, nb)
        copy = pltpu.make_async_remote_copy(
            src_ref=dw,
            dst_ref=dw_in.at[step - 1],
            send_sem=dw_send.at[step - 1],
            recv_sem=dw_recv.at[step - 1],
            device_id={"batch": peer},
            device_id_type=mesh_id,
        )
        copy.start()
        dw_copies.append(copy)

    def store(chunk):
        return pltpu.make_async_copy(
            cbuf.at[chunk], grad_out.at[0, :, :, lanes(chunk)], out_sem.at[chunk]
        )

    store_w = pltpu.make_async_copy(dw, dw_out, out_sem.at[chunks])

    def total(slot, carry):
        value = dw[slot].astype(jnp.float32)
        for step in range(nb - 1):
            value = value + dw_in[step, slot].astype(jnp.float32)
        dw[slot] = value.astype(jnp.bfloat16)
        return carry

    def last(chunk):
        if chunk == 0:
            for copy in dw_copies:
                copy.wait()
            lax.fori_loop(0, slots, total, 0)
            store_w.start()
        for kind in range(kinds):
            reached_all(11, kind, chunk, band_in)

        def finish(row, carry):
            delta = dot(fwd_kf[...], pair(band_in, chunk, row))
            put_pair(cbuf, chunk, row, pair(cbuf, chunk, row).astype(jnp.float32) + delta)
            return carry

        lax.fori_loop(0, lat_dev // 2, finish, 0, unroll=3)
        store(chunk).start()

    finish_synthesis(6, qtab, last)
    last(chunks - 1)
    for chunk in range(chunks):
        for kind in range(kinds):
            left_for_owners(6, kind, chunk, band_out)
            left_for_owners(9, kind, chunk, mixed)

    def drain(part, job):
        kind, chunk, place = job_of(job)

        @pl.when(mine(kind))
        def _():
            if part:
                await_tail(kind, cross_out.at[place, chunk], send_sem.at[7, job])
                await_tail(kind, tail_out.at[chunk], send_sem.at[10, job])
            else:
                await_bytes(cross_out.at[place, chunk], send_sem.at[7, job])
                await_bytes(slot_all.at[place, chunk, 0:own], send_sem.at[10, job])
            left_owner(8, job, kind, chunk, slot_out, slots)
            left_owner(11, job, kind, chunk, ord_out, lat_dev)

    loop(0, per_pass, lambda job: drain(0, job))
    loop(per_pass, jobs, lambda job: drain(1, job))
    for chunk in range(chunks):
        store(chunk).wait()
    store_w.wait()


def local_kernel(fields, cotangent, weights, degree_of):
    n = lax.axis_size("lat")
    nb = lax.axis_size("batch")
    kinds = 4
    if fields.shape[0] != 1 or fields.shape[1] % 2 or n % kinds or ORDERS != n * GROUP:
        return local(fields, cotangent, weights, degree_of)
    lat_dev, lons, channels = fields.shape[1:]
    slots = weights.shape[0]
    rows = 2 * GROUP
    chunks = channels // LANES
    floats, waves = constant_tables()
    side_lats = LATS // 2
    held = kinds - 1
    vmem = pl.BlockSpec(memory_space=pltpu.VMEM)
    anywhere = pl.BlockSpec(memory_space=pl.ANY)

    def buffer(*dims):
        return pltpu.VMEM(dims, jnp.bfloat16)

    dma = pltpu.SemaphoreType.DMA
    others = max(nb - 1, 1)
    wide_rows = max(side_lats, DEGREES) * rows
    return pl.pallas_call(
        functools.partial(block_kernel, n, nb),
        out_shape=(
            jax.ShapeDtypeStruct(fields.shape, jnp.bfloat16),
            jax.ShapeDtypeStruct(weights.shape, jnp.bfloat16),
        ),
        in_specs=[anywhere] * 3 + [pl.BlockSpec(memory_space=pltpu.SMEM)] + [vmem] * 7,
        out_specs=(anywhere, anywhere),
        scratch_shapes=[
            buffer(chunks, lat_dev, lons, LANES),
            buffer(chunks, lat_dev, lons, LANES),
            buffer(*weights.shape),
            buffer(chunks, lat_dev, n * rows, LANES),
            buffer(chunks, lat_dev, n * rows, LANES),
            buffer(held, chunks, side_lats, rows, LANES),
            buffer(held, chunks, side_lats, rows, LANES),
            buffer(held, chunks, DEGREES // 2, rows, LANES),
            buffer(held, chunks, DEGREES // 2, rows, LANES),
            buffer(held, chunks, DEGREES // 2, rows, LANES),
            buffer(held, chunks, DEGREES, rows, LANES),
            buffer(chunks, DEGREES // 2, rows, LANES),
            buffer(chunks, slots, n * rows, LANES),
            buffer(chunks, slots, n * rows, LANES),
            buffer(chunks, slots, n * rows, LANES),
            pltpu.VMEM((wide_rows, LANES), jnp.float32),
            pltpu.VMEM((4 * wide_rows, LANES), jnp.float32),
            pltpu.VMEM((side_lats * rows, LANES), jnp.float32),
            buffer(*weights.shape),
            buffer(others, *weights.shape),
            buffer(kinds, GROUP, DEGREES, side_lats),
            buffer(kinds, GROUP, DEGREES, side_lats),
            pltpu.VMEM((DEGREES, kinds * GROUP, LANES), jnp.float32),
            pltpu.VMEM((GROUP, DEGREES), jnp.int32),
            pltpu.SMEM((GROUP, DEGREES), jnp.int32),
            buffer(DEGREES, rows, LANES),
            dma((2 * chunks + 2,)),
            dma((12, kinds * chunks)),
            dma((12, kinds * chunks)),
            dma((others,)),
            dma((others,)),
            dma((chunks + 1,)),
        ],
        compiler_params=pltpu.CompilerParams(
            collective_id=0, has_side_effects=True, vmem_limit_bytes=63 * 2**20
        ),
        name="filter_block",
    )(
        fields, cotangent, weights, degree_of, *floats, *waves,
    )


def local(fields, cotangent, weights, degree_of):
    samples = fields.shape[0]
    band_rows = fields.shape[1]
    ord_dev = ORDERS // lax.axis_size("lat")
    forward, inverse = fourier_tables(LONS, ORDERS)
    qslot, pslot = spectral_tables(lax.axis_index("lat") * ord_dev, ord_dev, degree_of)
    spectra = product("sikc,kf->ifsc", fields, forward).astype(jnp.bfloat16)
    spectra = spectra.reshape(band_rows, ORDERS, 2, samples, CHANNELS)
    gathered = to_orders(spectra)
    coeffs_local = product("mji,imrsc->jmrsc", qslot, gathered).astype(jnp.bfloat16)
    coeffs = to_degrees(coeffs_local)
    filtered = apply_filter(coeffs, weights)
    returned = back_to_orders(filtered)
    synth_local = product("mji,jmrsc->imrsc", pslot, returned).astype(jnp.bfloat16)
    synth = to_bands(synth_local)
    response = product(
        "ifsc,fk->sikc", synth.reshape(band_rows, 2 * ORDERS, samples, CHANNELS), inverse
    )
    activated, pullback = jax.vjp(jax.nn.gelu, response)
    upstream = pullback(cotangent.astype(jnp.float32))[0].astype(jnp.bfloat16)
    grad_synth = product("sikc,fk->ifsc", upstream, inverse).astype(jnp.bfloat16)
    grad_synth = grad_synth.reshape(band_rows, ORDERS, 2, samples, CHANNELS)
    grad_gathered = to_orders(grad_synth)
    grad_local = product("mji,imrsc->jmrsc", pslot, grad_gathered).astype(jnp.bfloat16)
    grad_filtered = to_degrees(grad_local)
    weight_total = lax.psum(filter_grad(coeffs, grad_filtered).astype(jnp.bfloat16), "batch")
    grad_coeffs = adjoint_filter(grad_filtered, weights)
    grad_back = back_to_orders(grad_coeffs)
    grad_local_spec = product("mji,jmrsc->imrsc", qslot, grad_back).astype(jnp.bfloat16)
    grad_bands = to_bands(grad_local_spec)
    delta = product(
        "ifsc,kf->sikc", grad_bands.reshape(band_rows, 2 * ORDERS, samples, CHANNELS), forward
    )
    grad_fields = (cotangent.astype(jnp.float32) + delta).astype(jnp.bfloat16)
    return (grad_fields, weight_total)


def solution(mesh):
    return jax.shard_map(
        local_kernel if CHANNELS % LANES == 0 else local,
        mesh=mesh,
        in_specs=(
            P("batch", "lat", None, None),
            P("batch", "lat", None, None),
            P("lat", None, None, None),
            P(),
        ),
        out_specs=(P("batch", "lat", None, None), P("lat", None, None, None)),
        check_vma=False,
    )
```

```python
import functools

import jax
import numpy as np
import jax.numpy as jnp
from jax import lax
from jax.experimental import pallas as pl
from jax.experimental.pallas import tpu as pltpu
from jax.sharding import PartitionSpec as P

LATS = 192
LONS = 384
ORDERS = 128
DEGREES = 128
CHANNELS = 384
LANES = 128
GROUP = 8


def table_kernel(deg_ref, diag_ref, cos_ref, quad_ref, order_ref, q_ref, p_ref, slot_ref, rows_ref):
    orders = diag_ref.shape[0]
    lats = q_ref.shape[2]
    degrees = deg_ref.shape[0]

    def invert(slot, carry):
        slot_ref[deg_ref[slot]] = slot
        return carry

    lax.fori_loop(0, degrees, invert, 0)
    order_real = order_ref[...]
    squared = order_real * order_real
    diagonal = diag_ref[...]
    cosine = cos_ref[...]
    first_lead = jnp.sqrt(2.0 * order_real + 3.0)
    halves = rows_ref.shape[0]

    def advance(degree, carry):
        previous, older = carry
        degree_real = degree.astype(jnp.float32)
        lead = jnp.sqrt(
            jnp.maximum(4.0 * degree_real * degree_real - 1.0, 0.0)
            / jnp.maximum(degree_real * degree_real - squared, 1.0)
        )
        lower = degree_real - 1.0
        back = jnp.sqrt(
            jnp.maximum(lower * lower - squared, 0.0) / jnp.maximum(4.0 * lower * lower - 1.0, 1.0)
        )
        general = lead * (cosine * previous - back * older)
        first = first_lead * cosine * previous
        value = jnp.where(
            degree_real == order_real,
            diagonal,
            jnp.where(
                degree_real == order_real + 1.0,
                first,
                jnp.where(degree_real > order_real + 1.0, general, 0.0),
            ),
        )
        slot = slot_ref[degree]
        for half in range(halves):
            rows_ref[half, pl.ds(slot, orders, stride=degrees), :] = value[
                :, half * LANES : (half + 1) * LANES
            ]
        return (value, previous)

    zeros = diagonal * 0.0
    lax.fori_loop(0, degrees, advance, (zeros, zeros), unroll=4)
    quadrature = quad_ref[...]
    for order in range(orders):
        for half in range(halves):
            low = half * LANES
            high = min(lats, low + LANES)
            chosen = rows_ref[half, order * degrees : (order + 1) * degrees, :][:, : high - low]
            p_ref[order, :, low:high] = chosen.astype(jnp.bfloat16)
            q_ref[order, :, low:high] = (chosen * quadrature[:, low:high]).astype(jnp.bfloat16)


def spectral_tables(start, ord_dev, degree_of):
    halves = -(-LATS // LANES)
    padded = halves * LANES
    order_col = (start + jnp.arange(ord_dev, dtype=jnp.int32)).astype(jnp.float32)[:, None]
    lat_ids = jnp.minimum(jnp.arange(padded, dtype=jnp.float32), LATS - 1.0)
    colatitude = jnp.pi * (lat_ids + 0.5) / LATS
    sine = jnp.sin(colatitude)[None, :]
    steps_up = jnp.arange(1, DEGREES + 1, dtype=jnp.float32)[None, :]
    factor = jnp.where(
        steps_up <= order_col, 0.5 * jnp.log((2.0 * steps_up + 1.0) / (2.0 * steps_up)), 0.0
    )
    log_start = 0.5 * jnp.log(1.0 / (4.0 * jnp.pi)) + jnp.sum(factor, axis=1, keepdims=True)
    diagonal = jnp.exp(log_start + order_col * jnp.log(sine))
    cosine = jnp.broadcast_to(jnp.cos(colatitude)[None, :], diagonal.shape)
    quadrature = 2.0 * jnp.pi * jnp.pi / LATS * sine
    orders = jnp.broadcast_to(order_col, diagonal.shape)
    vmem = pl.BlockSpec(memory_space=pltpu.VMEM)
    shape = jax.ShapeDtypeStruct((ord_dev, DEGREES, LATS), jnp.bfloat16)
    return pl.pallas_call(
        table_kernel,
        out_shape=(shape, shape),
        in_specs=[pl.BlockSpec(memory_space=pltpu.SMEM)] + [vmem] * 4,
        out_specs=(vmem, vmem),
        scratch_shapes=[
            pltpu.SMEM((DEGREES,), jnp.int32),
            pltpu.VMEM((halves, ord_dev * DEGREES, LANES), jnp.float32),
        ],
        name="legendre_tables",
    )(degree_of, diagonal, cosine, quadrature, orders)


def fourier_tables(lon_count, order_count):
    lon_ids = jnp.arange(lon_count, dtype=jnp.int32)[:, None]
    order_ids = jnp.arange(order_count, dtype=jnp.int32)[None, :]
    phase = 2.0 * jnp.pi * (lon_ids * order_ids % lon_count).astype(jnp.float32) / lon_count
    forward = (
        jnp.stack([jnp.cos(phase), -jnp.sin(phase)], axis=2).reshape(lon_count, 2 * order_count)
        / lon_count
    )
    doubled = jnp.where(order_ids == 0, 1.0, 2.0)
    inverse = jnp.stack([doubled * jnp.cos(phase), -doubled * jnp.sin(phase)], axis=2).reshape(
        lon_count, 2 * order_count
    )
    return (forward.astype(jnp.bfloat16), jnp.transpose(inverse).astype(jnp.bfloat16))


def to_orders(values):
    return lax.all_to_all(values, "lat", split_axis=1, concat_axis=0, tiled=True)


def to_degrees(values):
    return lax.all_to_all(values, "lat", split_axis=0, concat_axis=1, tiled=True)


def back_to_orders(values):
    return lax.all_to_all(values, "lat", split_axis=1, concat_axis=0, tiled=True)


def to_bands(values):
    return lax.all_to_all(values, "lat", split_axis=0, concat_axis=1, tiled=True)


def product(spec, left, right):
    return jnp.einsum(spec, left, right, preferred_element_type=jnp.float32)


def apply_filter(coeffs, weights):
    c_real = coeffs[:, :, 0]
    c_imag = coeffs[:, :, 1]
    w_real = weights[:, 0]
    w_imag = weights[:, 1]
    f_real = product("jmsc,jcd->jmsd", c_real, w_real) - product("jmsc,jcd->jmsd", c_imag, w_imag)
    f_imag = product("jmsc,jcd->jmsd", c_real, w_imag) + product("jmsc,jcd->jmsd", c_imag, w_real)
    return jnp.stack([f_real, f_imag], axis=2).astype(jnp.bfloat16)


def adjoint_filter(grads, weights):
    g_real = grads[:, :, 0]
    g_imag = grads[:, :, 1]
    w_real = weights[:, 0]
    w_imag = weights[:, 1]
    a_real = product("jmsd,jcd->jmsc", g_real, w_real) + product("jmsd,jcd->jmsc", g_imag, w_imag)
    a_imag = product("jmsd,jcd->jmsc", g_imag, w_real) - product("jmsd,jcd->jmsc", g_real, w_imag)
    return jnp.stack([a_real, a_imag], axis=2).astype(jnp.bfloat16)


def filter_grad(coeffs, grads):
    c_real = coeffs[:, :, 0]
    c_imag = coeffs[:, :, 1]
    g_real = grads[:, :, 0]
    g_imag = grads[:, :, 1]
    dw_real = product("jmsc,jmsd->jcd", c_real, g_real) + product("jmsc,jmsd->jcd", c_imag, g_imag)
    dw_imag = product("jmsc,jmsd->jcd", c_real, g_imag) - product("jmsc,jmsd->jcd", c_imag, g_real)
    return jnp.stack([dw_real, dw_imag], axis=1)


def constant_tables():
    sides = 2
    half = LATS // sides
    lat_ids = np.minimum(np.arange(LANES)[None, :], half - 1) + half * np.arange(sides)[:, None]
    colatitude = np.pi * (lat_ids + 0.5) / LATS
    sine = np.sin(colatitude)[:, None, :]
    ids = np.arange(ORDERS)
    steps_up = np.arange(1, ORDERS + 1)
    growth = np.cumsum(0.5 * np.log((2.0 * steps_up + 1.0) / (2.0 * steps_up)))
    log_start = 0.5 * np.log(1.0 / (4.0 * np.pi)) + np.concatenate([[0.0], growth[:-1]])
    diagonal = np.exp(log_start[None, :, None] + ids[None, :, None] * np.log(sine))
    cosine = np.broadcast_to(np.cos(colatitude)[:, None, :], (sides, GROUP, LANES))
    quadrature = np.broadcast_to(2.0 * np.pi * np.pi / LATS * sine, (sides, GROUP, LANES))
    phase = 2.0 * np.pi * (np.arange(LONS)[:, None] * ids[None, :] % LONS) / LONS
    forward = np.stack([np.cos(phase), -np.sin(phase)], axis=2).reshape(LONS, -1) / LONS
    doubled = np.where(ids == 0, 1.0, 2.0)[None, :]
    inverse = np.stack([doubled * np.cos(phase), -doubled * np.sin(phase)], axis=2)
    inverse = inverse.reshape(LONS, -1)
    floats = [jnp.asarray(t, jnp.float32) for t in (diagonal, cosine, quadrature)]
    waves = [forward.T, forward, inverse.T, inverse]
    halves = [jnp.asarray(np.float32(t).astype(jnp.bfloat16)) for t in waves]
    return floats, halves


def fill_tables(side, firsts, deg_ref, diag_ref, cos_ref, quad_ref, qtab, ptab, table, by_slot):
    kinds, orders, degrees, lats = qtab.shape
    every = kinds * orders
    cosine = cos_ref[side]
    diagonal, ids, squared, first_lead = [], [], [], []
    for first in firsts:
        diagonal.append(diag_ref[side, pl.ds(pl.multiple_of(first, orders), orders), :])
        ids.append(first + lax.broadcasted_iota(jnp.int32, cosine.shape, 0))
        real = ids[-1].astype(jnp.float32)
        squared.append(real * real)
        first_lead.append(jnp.sqrt(2.0 * real + 3.0))

    def advance(degree, carry):
        degree_real = degree.astype(jnp.float32)
        lower = degree_real - 1.0
        state = []
        for kind in range(kinds):
            previous, older = carry[kind]
            lead = jnp.sqrt(
                jnp.maximum(4.0 * degree_real * degree_real - 1.0, 0.0)
                / jnp.maximum(degree_real * degree_real - squared[kind], 1.0)
            )
            back = jnp.sqrt(
                jnp.maximum(lower * lower - squared[kind], 0.0)
                / jnp.maximum(4.0 * lower * lower - 1.0, 1.0)
            )
            general = lead * (cosine * previous - back * older)
            first = first_lead[kind] * cosine * previous
            value = jnp.where(
                ids[kind] == degree,
                diagonal[kind],
                jnp.where(
                    ids[kind] + 1 == degree,
                    first,
                    jnp.where(ids[kind] + 1 < degree, general, 0.0),
                ),
            )
            table[degree, kind * orders : (kind + 1) * orders, :] = value
            state.append((value, previous))
        return tuple(state)

    zeros = cosine * 0.0
    lax.fori_loop(0, degrees, advance, ((zeros, zeros),) * kinds, unroll=2)

    ahead = every // 2
    tail = degrees // 2

    def place(slot, carry):
        by_slot[pl.ds(slot, ahead, stride=degrees), :] = table[deg_ref[slot], :ahead]
        return carry

    lax.fori_loop(0, degrees, place, 0, unroll=4)

    def place_tail(row, carry):
        spots = pl.ds(ahead * degrees + row, ahead, stride=degrees)
        by_slot[spots, :] = table[tail + row, ahead:]
        return carry

    lax.fori_loop(0, tail, place_tail, 0, unroll=4)
    quadrature = quad_ref[side][:1, :lats]
    for kind in range(kinds):

        def keep(order, carry):
            start = pl.multiple_of((kind * orders + order) * degrees, degrees)
            depth = degrees if kind < kinds // 2 else tail
            chosen = by_slot[pl.ds(start, depth), :][:, :lats]
            ptab[kind, order, :depth] = chosen.astype(jnp.bfloat16)
            qtab[kind, order, :depth] = (chosen * quadrature).astype(jnp.bfloat16)
            return carry

        lax.fori_loop(0, orders, keep, 0)


def pair_swap(values, even_sign):
    rows = values.shape[0]
    even = lax.broadcasted_iota(jnp.int32, values.shape, 0) % 2 == 0
    above = pltpu.roll(values, rows - 1, 0)
    below = pltpu.roll(values, 1, 0)
    return jnp.where(even, even_sign * above, -even_sign * below)


def gelu_slope(x):
    scale = 0.7978845608028654
    square = x * x
    t = jnp.tanh(scale * (x + 0.044715 * x * square))
    return 0.5 * (1.0 + t) + 0.5 * x * (1.0 - t * t) * (scale * (1.0 + 0.134145 * square))


def dot(left, right, dims=((1,), (0,))):
    return lax.dot_general(left, right, (dims, ((), ())), preferred_element_type=jnp.float32)


def block_kernel(
    n, nb, fields, cotangent, weights, deg_ref, diag_ref, cos_ref, quad_ref,
    fwd_fk, fwd_kf, inv_fk, inv_kf,
    grad_out, dw_out,
    fbuf, cbuf, wbuf, band_out, band_in, ord_in, ord_out, cross_out, cross_in, slot_out, slot_all,
    tail_out, co, go, mixed, wide_a, wide_b, wide_c, dw, dw_in, qtab, ptab, table, row_ref, slot_of, by_name,
    load_sem, send_sem, recv_sem, dw_send, dw_recv, out_sem,
):
    me = lax.axis_index("lat")
    me_b = lax.axis_index("batch")
    chunks, lat_dev = fbuf.shape[0], fbuf.shape[1]
    kinds, orders, degrees, side_lats = qtab.shape
    rows = 2 * orders
    slots = co.shape[1]
    quarter = n // kinds
    half = n // 2
    own = half * slots
    inner_kinds = ord_in.shape[0]
    pairs = kinds // 2
    jobs = kinds * chunks
    plane_rows = quarter * rows
    mesh_id = pl.DeviceIdType.MESH
    side = lax.div(me, half)
    place_in = lax.rem(me, half)
    column = lax.rem(me, quarter)
    inner = jnp.where(lax.div(me, quarter) == 1 + side, 1, 0)
    across = 1 - side

    def lanes(chunk):
        return pl.ds(chunk * LANES, LANES)

    def group(kind, at):
        return jnp.where(
            lax.rem(kind, 2) == 0, kind * quarter + at, (kind + 1) * quarter - 1 - at
        )

    def group_rows(kind, at):
        return pl.ds(pl.multiple_of(group(kind, at) * rows, rows), rows)

    def owner(kind, on_side, at):
        plane = jnp.where(kind < inner_kinds, 1 + on_side, (kinds - 1) * on_side)
        return plane * quarter + at

    def mine(kind):
        return jnp.where(kind < inner_kinds, 1, 0) == inner

    def job_of(job):
        per_pass = pairs * chunks
        inside = lax.rem(job, per_pass)
        kind = lax.div(job, per_pass) * pairs + lax.rem(inside, pairs)
        return kind, lax.div(inside, pairs), lax.rem(kind, inner_kinds)

    def first_block(kind):
        return group(kind, column) - own // orders

    def tail_blocks(kind, body):
        def one(block, carry):
            body(pl.multiple_of(block * orders, orders))
            return carry

        lax.fori_loop(first_block(kind), own // orders, one, 0)

    def await_tail(kind, view, sem):
        for first in range(own // orders):

            @pl.when(first_block(kind) == first)
            def _():
                await_bytes(view.at[pl.ds(0, own - first * orders)], sem)

    def job_at(kind, chunk):
        return (kind // pairs) * (pairs * chunks) + chunk * pairs + kind % pairs

    def load(chunk):
        return pltpu.make_async_copy(
            fields.at[0, :, :, lanes(chunk)], fbuf.at[chunk], load_sem.at[chunk]
        )

    def load_cot(chunk):
        return pltpu.make_async_copy(
            cotangent.at[0, :, :, lanes(chunk)], cbuf.at[chunk], load_sem.at[chunks + chunk]
        )

    load_w = pltpu.make_async_copy(weights, wbuf, load_sem.at[2 * chunks])
    for chunk in range(chunks):
        load(chunk).start()
    load_w.start()
    for chunk in range(chunks):
        load_cot(chunk).start()

    barrier = pltpu.get_barrier_semaphore()

    def greet(step, carry):
        peer = lax.rem(me + step, n)
        pl.semaphore_signal(barrier, inc=1, device_id={"lat": peer}, device_id_type=mesh_id)
        return carry

    lax.fori_loop(1, n, greet, 0)
    for step in range(1, nb):
        peer = lax.rem(me_b + step, nb)
        pl.semaphore_signal(barrier, inc=1, device_id={"batch": peer}, device_id_type=mesh_id)

    def remote(stage, job, source, target, peer):
        pltpu.make_async_remote_copy(
            src_ref=source,
            dst_ref=target,
            send_sem=send_sem.at[stage, job],
            recv_sem=recv_sem.at[stage, job],
            device_id={"lat": peer},
            device_id_type=mesh_id,
        ).start()

    def await_bytes(view, sem):
        pltpu.make_async_copy(view, view, sem).wait()

    def to_owners(stage, kind, chunk, source, target, width):
        job = job_at(kind, chunk)
        for step in range(quarter):
            at = lax.rem(column + step, quarter)
            view = source.at[chunk, :, group_rows(kind, at), :]
            spot = target(kind % inner_kinds, chunk)
            peer = owner(kind, side, at)

            @pl.when(peer != me)
            def _():
                remote(stage, job, view, spot, peer)

            @pl.when(peer == me)
            def _():
                pltpu.make_async_copy(view, spot, recv_sem.at[stage, job]).start()

    def left_for_owners(stage, kind, chunk, source):
        job = job_at(kind, chunk)

        @pl.when(mine(kind))
        def _():
            await_bytes(source.at[chunk, :, 0 : plane_rows - rows, :], send_sem.at[stage, job])

        @pl.when(jnp.logical_not(mine(kind)))
        def _():
            await_bytes(source.at[chunk, :, 0:plane_rows, :], send_sem.at[stage, job])

    def from_owner(stage, job, kind, chunk, source, depth, target):
        place = lax.rem(kind, inner_kinds)
        spot = target.at[chunk, :, group_rows(kind, column), :]

        def send(step, carry):
            at = lax.rem(place_in + step, half)
            remote(
                stage, job, source.at[place, chunk, pl.ds(at * depth, depth)], spot,
                side * half + at,
            )
            return carry

        lax.fori_loop(1, half, send, 0)
        pltpu.make_async_copy(
            source.at[place, chunk, pl.ds(place_in * depth, depth)], spot, recv_sem.at[stage, job]
        ).start()

    def left_owner(stage, job, kind, chunk, source, depth):
        view = source.at[lax.rem(kind, inner_kinds), chunk, 0 : (half - 1) * depth]
        await_bytes(view, send_sem.at[stage, job])

    def reached_all(stage, kind, chunk, target):
        await_bytes(target.at[chunk, :, 0:plane_rows, :], recv_sem.at[stage, job_at(kind, chunk)])

    def lat_spot(place, chunk):
        return ord_in.at[place, chunk, pl.ds(place_in * lat_dev, lat_dev)]

    def slot_spot(place, chunk):
        return slot_all.at[place, chunk, pl.ds(me * slots, slots)]

    def wide_start(part, job):
        if part:
            spot = lax.rem(lax.div(job - pairs * chunks, pairs) + pairs, chunks)
        else:
            spot = jnp.where(job < 2 * pairs, lax.rem(job, pairs), job - pairs)
        return pl.multiple_of(spot * wide_a.shape[0], 8)

    def widen(source, place, chunk, depth, count):
        def one(block, carry):
            piece = source[place, chunk, pl.ds(block * depth, depth)].astype(jnp.float32)
            wide_a[pl.ds(pl.multiple_of(block * depth * rows, depth * rows), depth * rows), :] = (
                piece.reshape(depth * rows, LANES)
            )
            return carry

        lax.fori_loop(0, count // depth, one, 0)

    def apply_table(tab, kind, kept, result_ref, start, depth_in, depth_out, dims):
        def one(order, carry):
            real = wide_a[pl.ds(2 * order, depth_in, stride=rows), :]
            imag = wide_a[pl.ds(2 * order + 1, depth_in, stride=rows), :]
            both = jnp.concatenate([real, imag], axis=1).astype(jnp.bfloat16)
            result = dot(tab[kind, order, :kept], both, dims)
            result_ref[pl.ds(start + 2 * order, depth_out, stride=rows), :] = result[:, :LANES]
            result_ref[pl.ds(start + 2 * order + 1, depth_out, stride=rows), :] = result[:, LANES:]
            return carry

        lax.fori_loop(0, orders, one, 0, unroll=4)

    def narrow(source, target, place, chunk, start, depth, count):
        def one(block, carry):
            low = pl.multiple_of(start + block * depth * rows, 8)
            piece = source[pl.ds(low, depth * rows), :]
            target[place, chunk, pl.ds(block * depth, depth)] = piece.reshape(
                depth, rows, LANES
            ).astype(jnp.bfloat16)
            return carry

        lax.fori_loop(0, count // depth, one, 0)

    def wide_rows(start, index, depth):
        return pl.ds(pl.multiple_of(start + index * rows, 8), depth * rows)

    def blank(first, count):
        def one(block, carry):
            by_name[pl.ds((first + block) * orders, orders)] = jnp.zeros(
                (orders, rows, LANES), jnp.bfloat16
            )
            return carry

        lax.fori_loop(0, count, one, 0)

    def analyse(base, tab, part, job):
        kind, chunk, place = job_of(job)

        @pl.when(mine(kind))
        def _():
            await_bytes(ord_in.at[place, chunk], recv_sem.at[base, job])
            widen(ord_in, place, chunk, lat_dev, side_lats)
            start = wide_start(part, job)
            peer = owner(kind, across, column)
            source = cross_out.at[place, chunk]
            target = cross_in.at[place, chunk]
            kept = own if part else degrees
            apply_table(tab, kind, kept, wide_b, start, side_lats, kept, ((1,), (0,)))
            if not part:
                if base:
                    await_bytes(source, send_sem.at[1, job])
                narrow(wide_b, cross_out, place, chunk, start + across * own * rows, slots, own)
                remote(base + 1, job, source, target, peer)
                return
            if base:
                await_tail(kind, source, send_sem.at[1, job])

            def send(low):
                span = pl.ds(low, orders)
                piece = wide_b[wide_rows(start, low, orders), :]
                cross_out[place, chunk, span] = piece.reshape(orders, rows, LANES).astype(
                    jnp.bfloat16
                )
                remote(base + 1, job, source.at[span], target.at[span], peer)

            tail_blocks(kind, send)

    def settle(base, target, part, job):
        kind, chunk, place = job_of(job)

        @pl.when(mine(kind))
        def _():
            start = wide_start(part, job)
            if part:
                await_tail(kind, cross_in.at[place, chunk], recv_sem.at[base + 1, job])
            else:
                await_bytes(cross_in.at[place, chunk], recv_sem.at[base + 1, job])
            if base:
                left_owner(2, job, kind, chunk, slot_out, slots)
                if part:
                    await_tail(kind, tail_out.at[chunk], send_sem.at[4, job])
                else:
                    await_bytes(slot_all.at[place, chunk, 0:own], send_sem.at[4, job])
            if part:

                blank(0, own // orders + first_block(kind))

                def add(low):
                    piece = wide_b[wide_rows(start, low, orders), :]
                    other = cross_in[place, chunk, pl.ds(low, orders)].astype(jnp.float32)
                    by_name[pl.ds(own + low, orders)] = (
                        piece.reshape(orders, rows, LANES) + other
                    ).astype(jnp.bfloat16)

                tail_blocks(kind, add)

                def pick(slot, carry):
                    slot_out[place, chunk, slot] = by_name[deg_ref[side * own + slot]]
                    return carry

                lax.fori_loop(0, own, pick, 0, unroll=4)
            else:

                def one(block, carry):
                    low = block * slots
                    piece = wide_b[wide_rows(start + side * own * rows, low, slots), :]
                    other = cross_in[place, chunk, pl.ds(low, slots)].astype(jnp.float32)
                    slot_out[place, chunk, pl.ds(low, slots)] = (
                        piece.reshape(slots, rows, LANES) + other
                    ).astype(jnp.bfloat16)
                    return carry

                lax.fori_loop(0, half, one, 0)
            from_owner(base + 2, job, kind, chunk, slot_out, slots, target)

    def relay(base, part, job):
        kind, chunk, place = job_of(job)

        @pl.when(mine(kind))
        def _():
            await_bytes(slot_all.at[place, chunk, 0:own], recv_sem.at[base + 3, job])
            peer = owner(kind, across, column)
            view = slot_all.at[place, chunk, pl.ds(side * own, own)]
            if not part:
                remote(base + 4, job, view, view, peer)
                return

            blank(across * (own // orders), own // orders)

            def copy(block, carry):
                span = pl.ds(side * own + block * slots, slots)
                by_name[span] = slot_all[place, chunk, span]
                return carry

            lax.fori_loop(0, half, copy, 0)

            def send(low):
                for step in range(orders):
                    tail_out[chunk, low + step] = by_name[slot_of[0, own + low + step]]
                span = pl.ds(low, orders)
                remote(base + 4, job, tail_out.at[chunk, span], view.at[span], peer)

            tail_blocks(kind, send)

    def synthesise(base, tab, part, job):
        kind, chunk, place = job_of(job)

        @pl.when(mine(kind))
        def _():
            if part:
                await_tail(kind, tail_out.at[chunk], recv_sem.at[base + 4, job])

                def clear(block, carry):
                    wide_a[wide_rows(0, block * orders, orders), :] = jnp.zeros(
                        (orders * rows, LANES), jnp.float32
                    )
                    return carry

                lax.fori_loop(0, first_block(kind), clear, 0)

                def add(low):
                    near = tail_out[chunk, pl.ds(low, orders)].astype(jnp.float32)
                    far = slot_all[place, chunk, pl.ds(across * own + low, orders)]
                    wide_a[wide_rows(0, low, orders), :] = (
                        near + far.astype(jnp.float32)
                    ).reshape(orders * rows, LANES)

                tail_blocks(kind, add)
                apply_table(tab, kind, own, wide_c, 0, own, side_lats, ((0,), (0,)))
            else:
                await_bytes(slot_all.at[place, chunk, 0:own], recv_sem.at[base + 4, job])
                widen(slot_all, place, chunk, slots, degrees)
                apply_table(tab, kind, degrees, wide_c, 0, degrees, side_lats, ((0,), (0,)))
            if base:
                left_owner(5, job, kind, chunk, ord_out, lat_dev)
            narrow(wide_c, ord_out, place, chunk, 0, lat_dev, side_lats)
            from_owner(base + 5, job, kind, chunk, ord_out, lat_dev, band_in)

    def loop(low, high, body):
        def one(job, carry):
            body(job)
            return carry

        lax.fori_loop(low, high, one, 0)

    def pair(source, chunk, row):
        return jnp.concatenate([source[chunk, 2 * row], source[chunk, 2 * row + 1]], axis=1)

    def put_pair(target, chunk, row, values):
        values = values.astype(jnp.bfloat16)
        target[chunk, 2 * row] = values[:, :LANES]
        target[chunk, 2 * row + 1] = values[:, LANES:]

    def joined(source, slot, span):
        return jnp.concatenate([source[chunk, slot, span] for chunk in range(chunks)], axis=1)

    def mix(part, chunk):
        low = part * pairs * plane_rows
        span = slice(low, low + pairs * plane_rows)
        columns = slice(chunk * LANES, (chunk + 1) * LANES)

        def one(slot, carry):
            both = dot(
                joined(co, slot, span),
                jnp.concatenate([wbuf[slot, 0, :, columns], wbuf[slot, 1, :, columns]], axis=1),
            )
            crossed = pair_swap(both[:, LANES:], -1.0)
            mixed[chunk, slot, span] = (both[:, :LANES] + crossed).astype(jnp.bfloat16)
            return carry

        return one

    def adjoint(part, chunk):
        low = part * pairs * plane_rows
        span = slice(low, low + pairs * plane_rows)
        columns = slice(chunk * LANES, (chunk + 1) * LANES)

        def one(slot, carry):
            both = dot(
                joined(go, slot, span),
                jnp.concatenate([wbuf[slot, 0, columns, :], wbuf[slot, 1, columns, :]], axis=0),
                ((1,), (1,)),
            )
            crossed = pair_swap(both[:, LANES:], 1.0)
            mixed[chunk, slot, span] = (both[:, :LANES] + crossed).astype(jnp.bfloat16)
            return carry

        return one

    def filter_part(base, part, source, make):
        part_kinds = range(part * pairs, (part + 1) * pairs)
        for chunk in range(chunks):
            for kind in part_kinds:
                reached_all(base + 2, kind, chunk, source)
        for chunk in range(chunks):
            if base:
                for kind in part_kinds:
                    left_for_owners(3, kind, chunk, mixed)
            lax.fori_loop(0, slots, make(part, chunk), 0, unroll=4)
            for kind in part_kinds:
                to_owners(base + 3, kind, chunk, mixed, slot_spot, slots)

    per_pass = pairs * chunks
    def unit(part, chunk):
        first = part * per_pass + chunk * pairs
        return first, first + pairs

    def run(spans, body):
        loop(spans[0], spans[1], body)

    def to_filter_start(base, tab, source, between_first):
        run(unit(0, 0), lambda job: analyse(base, tab, 0, job))
        between_first()
        for low, high, part, behind in (
            (pairs, per_pass, 0, 0),
            (per_pass, per_pass + pairs, 1, 0),
            (per_pass + pairs, per_pass + 2 * pairs, 1, 1),
        ):

            def step(job):
                settle(base, source, behind, job - pairs)
                analyse(base, tab, part, job)

            loop(low, high, step)
        loop(per_pass + 2 * pairs, jobs, lambda job: analyse(base, tab, 1, job))

    def through_filter(base, tab, source, make):
        filter_part(base, 0, source, make)
        run(unit(1, 1), lambda job: settle(base, source, 1, job))
        run(unit(0, 0), lambda job: relay(base, 0, job))
        run(unit(1, 2), lambda job: settle(base, source, 1, job))
        run(unit(0, 1), lambda job: relay(base, 0, job))
        run(unit(0, 0), lambda job: synthesise(base, tab, 0, job))
        loop(pairs, pairs + 1, lambda job: synthesise(base, tab, 0, job))
        filter_part(base, 1, source, make)
        loop(pairs + 1, 2 * pairs, lambda job: synthesise(base, tab, 0, job))
        run(unit(1, 0), lambda job: relay(base, 1, job))
        run(unit(0, 2), lambda job: relay(base, 0, job))
        run(unit(1, 1), lambda job: relay(base, 1, job))

    def spread(stage, chunk, part):
        for kind in range(part * pairs, (part + 1) * pairs):
            to_owners(stage, kind, chunk, band_out, lat_spot, lat_dev)

    def transform(chunk):
        load(chunk).wait()

        def fourier(row, carry):
            put_pair(band_out, chunk, row, dot(fwd_fk[...], pair(fbuf, chunk, row)))
            return carry

        lax.fori_loop(0, lat_dev // 2, fourier, 0, unroll=3)

    transform(0)
    pl.semaphore_wait(barrier, n - 1 + nb - 1)
    spread(0, 0, 0)
    transform(1)
    spread(0, 1, 0)
    fill_tables(
        side, [group(kind, column) * orders for kind in range(kinds)], deg_ref, diag_ref, cos_ref,
        quad_ref, qtab, ptab, table, wide_b,
    )
    for chunk in range(2, chunks):
        transform(chunk)
        spread(0, chunk, 0)
    for chunk in range(chunks):
        spread(0, chunk, 1)
    spots = lax.broadcasted_iota(jnp.int32, row_ref.shape, 1)

    def invert(slot, carry):
        return jnp.where(spots == deg_ref[slot], slot, carry)

    row_ref[...] = lax.fori_loop(0, degrees, invert, spots * 0, unroll=4)
    turn = pltpu.make_async_copy(row_ref, slot_of, load_sem.at[2 * chunks + 1])
    turn.start()
    turn.wait()
    load_w.wait()
    to_filter_start(0, qtab, co, lambda: None)
    through_filter(0, ptab, co, mix)

    def between(chunk):
        load_cot(chunk).wait()
        for kind in range(kinds):
            reached_all(5, kind, chunk, band_in)
            left_for_owners(0, kind, chunk, band_out)

        def middle(row, carry):
            response = dot(inv_kf[...], pair(band_in, chunk, row))
            upstream = pair(cbuf, chunk, row).astype(jnp.float32) * gelu_slope(response)
            put_pair(band_out, chunk, row, dot(inv_fk[...], upstream.astype(jnp.bfloat16)))
            return carry

        lax.fori_loop(0, lat_dev // 2, middle, 0, unroll=3)
        spread(6, chunk, 0)
        spread(6, chunk, 1)

    def finish_synthesis(base, tab, finish):
        first, second = unit(0, 2)
        run(unit(1, 0), lambda job: synthesise(base, tab, 1, job))
        loop(first, first + 1, lambda job: synthesise(base, tab, 0, job))
        run(unit(1, 2), lambda job: relay(base, 1, job))
        finish(0)
        loop(first + 1, second, lambda job: synthesise(base, tab, 0, job))
        loop(per_pass + pairs, jobs, lambda job: synthesise(base, tab, 1, job))

    def rest(finish):
        for chunk in range(1, chunks):
            finish(chunk)

    finish_synthesis(0, ptab, between)
    to_filter_start(6, ptab, go, lambda: rest(between))
    through_filter(6, qtab, go, adjoint)

    def weight_grad(slot, carry):
        values = joined(co, slot, slice(None))
        grads = joined(go, slot, slice(None))
        turned = pair_swap(grads.astype(jnp.float32), 1.0).astype(jnp.bfloat16)
        span = ((0,), (0,))
        dw[slot, 0] = dot(values, grads, span).astype(jnp.bfloat16)
        dw[slot, 1] = dot(values, turned, span).astype(jnp.bfloat16)
        return carry

    lax.fori_loop(0, slots, weight_grad, 0)
    dw_copies = []
    for step in range(1, nb):
        peer = lax.rem(me_b + step, nb)
        copy = pltpu.make_async_remote_copy(
            src_ref=dw,
            dst_ref=dw_in.at[step - 1],
            send_sem=dw_send.at[step - 1],
            recv_sem=dw_recv.at[step - 1],
            device_id={"batch": peer},
            device_id_type=mesh_id,
        )
        copy.start()
        dw_copies.append(copy)

    def store(chunk):
        return pltpu.make_async_copy(
            cbuf.at[chunk], grad_out.at[0, :, :, lanes(chunk)], out_sem.at[chunk]
        )

    store_w = pltpu.make_async_copy(dw, dw_out, out_sem.at[chunks])

    def total(slot, carry):
        value = dw[slot].astype(jnp.float32)
        for step in range(nb - 1):
            value = value + dw_in[step, slot].astype(jnp.float32)
        dw[slot] = value.astype(jnp.bfloat16)
        return carry

    def last(chunk):
        if chunk == 0:
            for copy in dw_copies:
                copy.wait()
            lax.fori_loop(0, slots, total, 0)
            store_w.start()
        for kind in range(kinds):
            reached_all(11, kind, chunk, band_in)

        def finish(row, carry):
            delta = dot(fwd_kf[...], pair(band_in, chunk, row))
            put_pair(cbuf, chunk, row, pair(cbuf, chunk, row).astype(jnp.float32) + delta)
            return carry

        lax.fori_loop(0, lat_dev // 2, finish, 0, unroll=3)
        store(chunk).start()

    finish_synthesis(6, qtab, last)
    rest(last)
    for chunk in range(chunks):
        for kind in range(kinds):
            left_for_owners(6, kind, chunk, band_out)
            left_for_owners(9, kind, chunk, mixed)

    def drain(part, job):
        kind, chunk, place = job_of(job)

        @pl.when(mine(kind))
        def _():
            if part:
                await_tail(kind, cross_out.at[place, chunk], send_sem.at[7, job])
                await_tail(kind, tail_out.at[chunk], send_sem.at[10, job])
            else:
                await_bytes(cross_out.at[place, chunk], send_sem.at[7, job])
                await_bytes(slot_all.at[place, chunk, 0:own], send_sem.at[10, job])
            left_owner(8, job, kind, chunk, slot_out, slots)
            left_owner(11, job, kind, chunk, ord_out, lat_dev)

    loop(0, per_pass, lambda job: drain(0, job))
    loop(per_pass, jobs, lambda job: drain(1, job))
    for chunk in range(chunks):
        store(chunk).wait()
    store_w.wait()


def local_kernel(fields, cotangent, weights, degree_of):
    n = lax.axis_size("lat")
    nb = lax.axis_size("batch")
    kinds = 4
    if fields.shape[0] != 1 or fields.shape[1] % 2 or n % kinds or ORDERS != n * GROUP:
        return local(fields, cotangent, weights, degree_of)
    lat_dev, lons, channels = fields.shape[1:]
    slots = weights.shape[0]
    rows = 2 * GROUP
    chunks = channels // LANES
    floats, waves = constant_tables()
    side_lats = LATS // 2
    held = kinds - 1
    vmem = pl.BlockSpec(memory_space=pltpu.VMEM)
    anywhere = pl.BlockSpec(memory_space=pl.ANY)

    def buffer(*dims):
        return pltpu.VMEM(dims, jnp.bfloat16)

    dma = pltpu.SemaphoreType.DMA
    others = max(nb - 1, 1)
    wide_rows = max(side_lats, DEGREES) * rows
    return pl.pallas_call(
        functools.partial(block_kernel, n, nb),
        out_shape=(
            jax.ShapeDtypeStruct(fields.shape, jnp.bfloat16),
            jax.ShapeDtypeStruct(weights.shape, jnp.bfloat16),
        ),
        in_specs=[anywhere] * 3 + [pl.BlockSpec(memory_space=pltpu.SMEM)] + [vmem] * 7,
        out_specs=(anywhere, anywhere),
        scratch_shapes=[
            buffer(chunks, lat_dev, lons, LANES),
            buffer(chunks, lat_dev, lons, LANES),
            buffer(*weights.shape),
            buffer(chunks, lat_dev, n * rows, LANES),
            buffer(chunks, lat_dev, n * rows, LANES),
            buffer(held, chunks, side_lats, rows, LANES),
            buffer(held, chunks, side_lats, rows, LANES),
            buffer(held, chunks, DEGREES // 2, rows, LANES),
            buffer(held, chunks, DEGREES // 2, rows, LANES),
            buffer(held, chunks, DEGREES // 2, rows, LANES),
            buffer(held, chunks, DEGREES, rows, LANES),
            buffer(chunks, DEGREES // 2, rows, LANES),
            buffer(chunks, slots, n * rows, LANES),
            buffer(chunks, slots, n * rows, LANES),
            buffer(chunks, slots, n * rows, LANES),
            pltpu.VMEM((wide_rows, LANES), jnp.float32),
            pltpu.VMEM((4 * wide_rows, LANES), jnp.float32),
            pltpu.VMEM((side_lats * rows, LANES), jnp.float32),
            buffer(*weights.shape),
            buffer(others, *weights.shape),
            buffer(kinds, GROUP, DEGREES, side_lats),
            buffer(kinds, GROUP, DEGREES, side_lats),
            pltpu.VMEM((DEGREES, kinds * GROUP, LANES), jnp.float32),
            pltpu.VMEM((GROUP, DEGREES), jnp.int32),
            pltpu.SMEM((GROUP, DEGREES), jnp.int32),
            buffer(DEGREES, rows, LANES),
            dma((2 * chunks + 2,)),
            dma((12, kinds * chunks)),
            dma((12, kinds * chunks)),
            dma((others,)),
            dma((others,)),
            dma((chunks + 1,)),
        ],
        compiler_params=pltpu.CompilerParams(
            collective_id=0, has_side_effects=True, vmem_limit_bytes=63 * 2**20
        ),
        name="filter_block",
    )(
        fields, cotangent, weights, degree_of, *floats, *waves,
    )


def local(fields, cotangent, weights, degree_of):
    samples = fields.shape[0]
    band_rows = fields.shape[1]
    ord_dev = ORDERS // lax.axis_size("lat")
    forward, inverse = fourier_tables(LONS, ORDERS)
    qslot, pslot = spectral_tables(lax.axis_index("lat") * ord_dev, ord_dev, degree_of)
    spectra = product("sikc,kf->ifsc", fields, forward).astype(jnp.bfloat16)
    spectra = spectra.reshape(band_rows, ORDERS, 2, samples, CHANNELS)
    gathered = to_orders(spectra)
    coeffs_local = product("mji,imrsc->jmrsc", qslot, gathered).astype(jnp.bfloat16)
    coeffs = to_degrees(coeffs_local)
    filtered = apply_filter(coeffs, weights)
    returned = back_to_orders(filtered)
    synth_local = product("mji,jmrsc->imrsc", pslot, returned).astype(jnp.bfloat16)
    synth = to_bands(synth_local)
    response = product(
        "ifsc,fk->sikc", synth.reshape(band_rows, 2 * ORDERS, samples, CHANNELS), inverse
    )
    activated, pullback = jax.vjp(jax.nn.gelu, response)
    upstream = pullback(cotangent.astype(jnp.float32))[0].astype(jnp.bfloat16)
    grad_synth = product("sikc,fk->ifsc", upstream, inverse).astype(jnp.bfloat16)
    grad_synth = grad_synth.reshape(band_rows, ORDERS, 2, samples, CHANNELS)
    grad_gathered = to_orders(grad_synth)
    grad_local = product("mji,imrsc->jmrsc", pslot, grad_gathered).astype(jnp.bfloat16)
    grad_filtered = to_degrees(grad_local)
    weight_total = lax.psum(filter_grad(coeffs, grad_filtered).astype(jnp.bfloat16), "batch")
    grad_coeffs = adjoint_filter(grad_filtered, weights)
    grad_back = back_to_orders(grad_coeffs)
    grad_local_spec = product("mji,jmrsc->imrsc", qslot, grad_back).astype(jnp.bfloat16)
    grad_bands = to_bands(grad_local_spec)
    delta = product(
        "ifsc,kf->sikc", grad_bands.reshape(band_rows, 2 * ORDERS, samples, CHANNELS), forward
    )
    grad_fields = (cotangent.astype(jnp.float32) + delta).astype(jnp.bfloat16)
    return (grad_fields, weight_total)


def solution(mesh):
    return jax.shard_map(
        local_kernel if CHANNELS % LANES == 0 else local,
        mesh=mesh,
        in_specs=(
            P("batch", "lat", None, None),
            P("batch", "lat", None, None),
            P("lat", None, None, None),
            P(),
        ),
        out_specs=(P("batch", "lat", None, None), P("lat", None, None, None)),
        check_vma=False,
    )
```

```python
import functools

import jax
import numpy as np
import jax.numpy as jnp
from jax import lax
from jax.experimental import pallas as pl
from jax.experimental.pallas import tpu as pltpu
from jax.sharding import PartitionSpec as P

LATS = 192
LONS = 384
ORDERS = 128
DEGREES = 128
CHANNELS = 384
LANES = 128
GROUP = 8


def table_kernel(deg_ref, diag_ref, cos_ref, quad_ref, order_ref, q_ref, p_ref, slot_ref, rows_ref):
    orders = diag_ref.shape[0]
    lats = q_ref.shape[2]
    degrees = deg_ref.shape[0]

    def invert(slot, carry):
        slot_ref[deg_ref[slot]] = slot
        return carry

    lax.fori_loop(0, degrees, invert, 0)
    order_real = order_ref[...]
    squared = order_real * order_real
    diagonal = diag_ref[...]
    cosine = cos_ref[...]
    first_lead = jnp.sqrt(2.0 * order_real + 3.0)
    halves = rows_ref.shape[0]

    def advance(degree, carry):
        previous, older = carry
        degree_real = degree.astype(jnp.float32)
        lead = jnp.sqrt(
            jnp.maximum(4.0 * degree_real * degree_real - 1.0, 0.0)
            / jnp.maximum(degree_real * degree_real - squared, 1.0)
        )
        lower = degree_real - 1.0
        back = jnp.sqrt(
            jnp.maximum(lower * lower - squared, 0.0) / jnp.maximum(4.0 * lower * lower - 1.0, 1.0)
        )
        general = lead * (cosine * previous - back * older)
        first = first_lead * cosine * previous
        value = jnp.where(
            degree_real == order_real,
            diagonal,
            jnp.where(
                degree_real == order_real + 1.0,
                first,
                jnp.where(degree_real > order_real + 1.0, general, 0.0),
            ),
        )
        slot = slot_ref[degree]
        for half in range(halves):
            rows_ref[half, pl.ds(slot, orders, stride=degrees), :] = value[
                :, half * LANES : (half + 1) * LANES
            ]
        return (value, previous)

    zeros = diagonal * 0.0
    lax.fori_loop(0, degrees, advance, (zeros, zeros), unroll=4)
    quadrature = quad_ref[...]
    for order in range(orders):
        for half in range(halves):
            low = half * LANES
            high = min(lats, low + LANES)
            chosen = rows_ref[half, order * degrees : (order + 1) * degrees, :][:, : high - low]
            p_ref[order, :, low:high] = chosen.astype(jnp.bfloat16)
            q_ref[order, :, low:high] = (chosen * quadrature[:, low:high]).astype(jnp.bfloat16)


def spectral_tables(start, ord_dev, degree_of):
    halves = -(-LATS // LANES)
    padded = halves * LANES
    order_col = (start + jnp.arange(ord_dev, dtype=jnp.int32)).astype(jnp.float32)[:, None]
    lat_ids = jnp.minimum(jnp.arange(padded, dtype=jnp.float32), LATS - 1.0)
    colatitude = jnp.pi * (lat_ids + 0.5) / LATS
    sine = jnp.sin(colatitude)[None, :]
    steps_up = jnp.arange(1, DEGREES + 1, dtype=jnp.float32)[None, :]
    factor = jnp.where(
        steps_up <= order_col, 0.5 * jnp.log((2.0 * steps_up + 1.0) / (2.0 * steps_up)), 0.0
    )
    log_start = 0.5 * jnp.log(1.0 / (4.0 * jnp.pi)) + jnp.sum(factor, axis=1, keepdims=True)
    diagonal = jnp.exp(log_start + order_col * jnp.log(sine))
    cosine = jnp.broadcast_to(jnp.cos(colatitude)[None, :], diagonal.shape)
    quadrature = 2.0 * jnp.pi * jnp.pi / LATS * sine
    orders = jnp.broadcast_to(order_col, diagonal.shape)
    vmem = pl.BlockSpec(memory_space=pltpu.VMEM)
    shape = jax.ShapeDtypeStruct((ord_dev, DEGREES, LATS), jnp.bfloat16)
    return pl.pallas_call(
        table_kernel,
        out_shape=(shape, shape),
        in_specs=[pl.BlockSpec(memory_space=pltpu.SMEM)] + [vmem] * 4,
        out_specs=(vmem, vmem),
        scratch_shapes=[
            pltpu.SMEM((DEGREES,), jnp.int32),
            pltpu.VMEM((halves, ord_dev * DEGREES, LANES), jnp.float32),
        ],
        name="legendre_tables",
    )(degree_of, diagonal, cosine, quadrature, orders)


def fourier_tables(lon_count, order_count):
    lon_ids = jnp.arange(lon_count, dtype=jnp.int32)[:, None]
    order_ids = jnp.arange(order_count, dtype=jnp.int32)[None, :]
    phase = 2.0 * jnp.pi * (lon_ids * order_ids % lon_count).astype(jnp.float32) / lon_count
    forward = (
        jnp.stack([jnp.cos(phase), -jnp.sin(phase)], axis=2).reshape(lon_count, 2 * order_count)
        / lon_count
    )
    doubled = jnp.where(order_ids == 0, 1.0, 2.0)
    inverse = jnp.stack([doubled * jnp.cos(phase), -doubled * jnp.sin(phase)], axis=2).reshape(
        lon_count, 2 * order_count
    )
    return (forward.astype(jnp.bfloat16), jnp.transpose(inverse).astype(jnp.bfloat16))


def to_orders(values):
    return lax.all_to_all(values, "lat", split_axis=1, concat_axis=0, tiled=True)


def to_degrees(values):
    return lax.all_to_all(values, "lat", split_axis=0, concat_axis=1, tiled=True)


def back_to_orders(values):
    return lax.all_to_all(values, "lat", split_axis=1, concat_axis=0, tiled=True)


def to_bands(values):
    return lax.all_to_all(values, "lat", split_axis=0, concat_axis=1, tiled=True)


def product(spec, left, right):
    return jnp.einsum(spec, left, right, preferred_element_type=jnp.float32)


def apply_filter(coeffs, weights):
    c_real = coeffs[:, :, 0]
    c_imag = coeffs[:, :, 1]
    w_real = weights[:, 0]
    w_imag = weights[:, 1]
    f_real = product("jmsc,jcd->jmsd", c_real, w_real) - product("jmsc,jcd->jmsd", c_imag, w_imag)
    f_imag = product("jmsc,jcd->jmsd", c_real, w_imag) + product("jmsc,jcd->jmsd", c_imag, w_real)
    return jnp.stack([f_real, f_imag], axis=2).astype(jnp.bfloat16)


def adjoint_filter(grads, weights):
    g_real = grads[:, :, 0]
    g_imag = grads[:, :, 1]
    w_real = weights[:, 0]
    w_imag = weights[:, 1]
    a_real = product("jmsd,jcd->jmsc", g_real, w_real) + product("jmsd,jcd->jmsc", g_imag, w_imag)
    a_imag = product("jmsd,jcd->jmsc", g_imag, w_real) - product("jmsd,jcd->jmsc", g_real, w_imag)
    return jnp.stack([a_real, a_imag], axis=2).astype(jnp.bfloat16)


def filter_grad(coeffs, grads):
    c_real = coeffs[:, :, 0]
    c_imag = coeffs[:, :, 1]
    g_real = grads[:, :, 0]
    g_imag = grads[:, :, 1]
    dw_real = product("jmsc,jmsd->jcd", c_real, g_real) + product("jmsc,jmsd->jcd", c_imag, g_imag)
    dw_imag = product("jmsc,jmsd->jcd", c_real, g_imag) - product("jmsc,jmsd->jcd", c_imag, g_real)
    return jnp.stack([dw_real, dw_imag], axis=1)


def constant_tables():
    sides = 2
    half = LATS // sides
    lat_ids = np.minimum(np.arange(LANES)[None, :], half - 1) + half * np.arange(sides)[:, None]
    colatitude = np.pi * (lat_ids + 0.5) / LATS
    sine = np.sin(colatitude)[:, None, :]
    ids = np.arange(ORDERS)
    steps_up = np.arange(1, ORDERS + 1)
    growth = np.cumsum(0.5 * np.log((2.0 * steps_up + 1.0) / (2.0 * steps_up)))
    log_start = 0.5 * np.log(1.0 / (4.0 * np.pi)) + np.concatenate([[0.0], growth[:-1]])
    diagonal = np.exp(log_start[None, :, None] + ids[None, :, None] * np.log(sine))
    cosine = np.broadcast_to(np.cos(colatitude)[:, None, :], (sides, GROUP, LANES))
    quadrature = np.broadcast_to(2.0 * np.pi * np.pi / LATS * sine, (sides, GROUP, LANES))
    phase = 2.0 * np.pi * (np.arange(LONS)[:, None] * ids[None, :] % LONS) / LONS
    forward = np.stack([np.cos(phase), -np.sin(phase)], axis=2).reshape(LONS, -1) / LONS
    doubled = np.where(ids == 0, 1.0, 2.0)[None, :]
    inverse = np.stack([doubled * np.cos(phase), -doubled * np.sin(phase)], axis=2)
    inverse = inverse.reshape(LONS, -1)
    floats = [jnp.asarray(t, jnp.float32) for t in (diagonal, cosine, quadrature)]
    waves = [forward.T, forward, inverse.T, inverse]
    halves = [jnp.asarray(np.float32(t).astype(jnp.bfloat16)) for t in waves]
    return floats, halves


def fill_tables(side, firsts, deg_ref, diag_ref, cos_ref, quad_ref, qtab, ptab, table, by_slot):
    kinds, orders, degrees, lats = qtab.shape
    every = kinds * orders
    cosine = cos_ref[side]
    diagonal, ids, squared, first_lead = [], [], [], []
    for first in firsts:
        diagonal.append(diag_ref[side, pl.ds(pl.multiple_of(first, orders), orders), :])
        ids.append(first + lax.broadcasted_iota(jnp.int32, cosine.shape, 0))
        real = ids[-1].astype(jnp.float32)
        squared.append(real * real)
        first_lead.append(jnp.sqrt(2.0 * real + 3.0))

    def advance(degree, carry):
        degree_real = degree.astype(jnp.float32)
        lower = degree_real - 1.0
        state = []
        for kind in range(kinds):
            previous, older = carry[kind]
            lead = jnp.sqrt(
                jnp.maximum(4.0 * degree_real * degree_real - 1.0, 0.0)
                / jnp.maximum(degree_real * degree_real - squared[kind], 1.0)
            )
            back = jnp.sqrt(
                jnp.maximum(lower * lower - squared[kind], 0.0)
                / jnp.maximum(4.0 * lower * lower - 1.0, 1.0)
            )
            general = lead * (cosine * previous - back * older)
            first = first_lead[kind] * cosine * previous
            value = jnp.where(
                ids[kind] == degree,
                diagonal[kind],
                jnp.where(
                    ids[kind] + 1 == degree,
                    first,
                    jnp.where(ids[kind] + 1 < degree, general, 0.0),
                ),
            )
            table[degree, kind * orders : (kind + 1) * orders, :] = value
            state.append((value, previous))
        return tuple(state)

    zeros = cosine * 0.0
    lax.fori_loop(0, degrees, advance, ((zeros, zeros),) * kinds, unroll=2)

    ahead = every // 2
    tail = degrees // 2

    def place(slot, carry):
        by_slot[pl.ds(slot, ahead, stride=degrees), :] = table[deg_ref[slot], :ahead]
        return carry

    lax.fori_loop(0, degrees, place, 0, unroll=4)

    def place_tail(row, carry):
        spots = pl.ds(ahead * degrees + row, ahead, stride=degrees)
        by_slot[spots, :] = table[tail + row, ahead:]
        return carry

    lax.fori_loop(0, tail, place_tail, 0, unroll=4)
    quadrature = quad_ref[side][:1, :lats]
    for kind in range(kinds):

        def keep(order, carry):
            start = pl.multiple_of((kind * orders + order) * degrees, degrees)
            depth = degrees if kind < kinds // 2 else tail
            chosen = by_slot[pl.ds(start, depth), :][:, :lats]
            ptab[kind, order, :depth] = chosen.astype(jnp.bfloat16)
            qtab[kind, order, :depth] = (chosen * quadrature).astype(jnp.bfloat16)
            return carry

        lax.fori_loop(0, orders, keep, 0)


def pair_swap(values, even_sign):
    rows = values.shape[0]
    even = lax.broadcasted_iota(jnp.int32, values.shape, 0) % 2 == 0
    above = pltpu.roll(values, rows - 1, 0)
    below = pltpu.roll(values, 1, 0)
    return jnp.where(even, even_sign * above, -even_sign * below)


def gelu_slope(x):
    scale = 0.7978845608028654
    square = x * x
    t = jnp.tanh(scale * (x + 0.044715 * x * square))
    return 0.5 * (1.0 + t) + 0.5 * x * (1.0 - t * t) * (scale * (1.0 + 0.134145 * square))


def dot(left, right, dims=((1,), (0,))):
    return lax.dot_general(left, right, (dims, ((), ())), preferred_element_type=jnp.float32)


def block_kernel(
    n, nb, fields, cotangent, weights, deg_ref, diag_ref, cos_ref, quad_ref,
    fwd_fk, fwd_kf, inv_fk, inv_kf,
    grad_out, dw_out,
    fbuf, cbuf, wbuf, band_out, band_in, ord_in, ord_out, cross_out, cross_in, slot_out, slot_all,
    tail_out, co, go, mixed, wide_a, wide_b, wide_c, dw, dw_in, qtab, ptab, table, row_ref, slot_of, by_name,
    load_sem, send_sem, recv_sem, dw_send, dw_recv, out_sem,
):
    me = lax.axis_index("lat")
    me_b = lax.axis_index("batch")
    chunks, lat_dev = fbuf.shape[0], fbuf.shape[1]
    kinds, orders, degrees, side_lats = qtab.shape
    rows = 2 * orders
    slots = co.shape[1]
    quarter = n // kinds
    half = n // 2
    own = half * slots
    inner_kinds = ord_in.shape[0]
    pairs = kinds // 2
    jobs = kinds * chunks
    plane_rows = quarter * rows
    mesh_id = pl.DeviceIdType.MESH
    side = lax.div(me, half)
    place_in = lax.rem(me, half)
    column = lax.rem(me, quarter)
    inner = jnp.where(lax.div(me, quarter) == 1 + side, 1, 0)
    across = 1 - side

    def lanes(chunk):
        return pl.ds(chunk * LANES, LANES)

    def group(kind, at):
        return jnp.where(
            lax.rem(kind, 2) == 0, kind * quarter + at, (kind + 1) * quarter - 1 - at
        )

    def group_rows(kind, at):
        return pl.ds(pl.multiple_of(group(kind, at) * rows, rows), rows)

    def owner(kind, on_side, at):
        plane = jnp.where(kind < inner_kinds, 1 + on_side, (kinds - 1) * on_side)
        return plane * quarter + at

    def mine(kind):
        return jnp.where(kind < inner_kinds, 1, 0) == inner

    def job_of(job):
        per_pass = pairs * chunks
        inside = lax.rem(job, per_pass)
        kind = lax.div(job, per_pass) * pairs + lax.rem(inside, pairs)
        return kind, lax.div(inside, pairs), lax.rem(kind, inner_kinds)

    def first_block(kind):
        return group(kind, column) - own // orders

    def tail_blocks(kind, body):
        def one(block, carry):
            body(pl.multiple_of(block * orders, orders))
            return carry

        lax.fori_loop(first_block(kind), own // orders, one, 0)

    def await_tail(kind, view, sem):
        for first in range(own // orders):

            @pl.when(first_block(kind) == first)
            def _():
                await_bytes(view.at[pl.ds(0, own - first * orders)], sem)

    def job_at(kind, chunk):
        return (kind // pairs) * (pairs * chunks) + chunk * pairs + kind % pairs

    def load(chunk):
        return pltpu.make_async_copy(
            fields.at[0, :, :, lanes(chunk)], fbuf.at[chunk], load_sem.at[chunk]
        )

    def load_cot(chunk):
        return pltpu.make_async_copy(
            cotangent.at[0, :, :, lanes(chunk)], cbuf.at[chunk], load_sem.at[chunks + chunk]
        )

    load_w = pltpu.make_async_copy(weights, wbuf, load_sem.at[2 * chunks])
    for chunk in range(chunks):
        load(chunk).start()
    load_w.start()
    for chunk in range(chunks):
        load_cot(chunk).start()

    barrier = pltpu.get_barrier_semaphore()

    def greet(step, carry):
        peer = lax.rem(me + step, n)
        pl.semaphore_signal(barrier, inc=1, device_id={"lat": peer}, device_id_type=mesh_id)
        return carry

    lax.fori_loop(1, n, greet, 0)
    for step in range(1, nb):
        peer = lax.rem(me_b + step, nb)
        pl.semaphore_signal(barrier, inc=1, device_id={"batch": peer}, device_id_type=mesh_id)

    def remote(stage, job, source, target, peer):
        pltpu.make_async_remote_copy(
            src_ref=source,
            dst_ref=target,
            send_sem=send_sem.at[stage, job],
            recv_sem=recv_sem.at[stage, job],
            device_id={"lat": peer},
            device_id_type=mesh_id,
        ).start()

    def await_bytes(view, sem):
        pltpu.make_async_copy(view, view, sem).wait()

    def to_owners(stage, kind, chunk, source, target, width):
        job = job_at(kind, chunk)
        for step in range(quarter):
            at = lax.rem(column + step, quarter)
            view = source.at[chunk, :, group_rows(kind, at), :]
            spot = target(kind % inner_kinds, chunk)
            peer = owner(kind, side, at)

            @pl.when(peer != me)
            def _():
                remote(stage, job, view, spot, peer)

            @pl.when(peer == me)
            def _():
                pltpu.make_async_copy(view, spot, recv_sem.at[stage, job]).start()

    def left_for_owners(stage, kind, chunk, source):
        job = job_at(kind, chunk)

        @pl.when(mine(kind))
        def _():
            await_bytes(source.at[chunk, :, 0 : plane_rows - rows, :], send_sem.at[stage, job])

        @pl.when(jnp.logical_not(mine(kind)))
        def _():
            await_bytes(source.at[chunk, :, 0:plane_rows, :], send_sem.at[stage, job])

    def from_owner(stage, job, kind, chunk, source, depth, target):
        place = lax.rem(kind, inner_kinds)
        spot = target.at[chunk, :, group_rows(kind, column), :]

        def send(step, carry):
            at = lax.rem(place_in + step, half)
            remote(
                stage, job, source.at[place, chunk, pl.ds(at * depth, depth)], spot,
                side * half + at,
            )
            return carry

        lax.fori_loop(1, half, send, 0)
        pltpu.make_async_copy(
            source.at[place, chunk, pl.ds(place_in * depth, depth)], spot, recv_sem.at[stage, job]
        ).start()

    def left_owner(stage, job, kind, chunk, source, depth):
        view = source.at[lax.rem(kind, inner_kinds), chunk, 0 : (half - 1) * depth]
        await_bytes(view, send_sem.at[stage, job])

    def reached_all(stage, kind, chunk, target):
        await_bytes(target.at[chunk, :, 0:plane_rows, :], recv_sem.at[stage, job_at(kind, chunk)])

    def lat_spot(place, chunk):
        return ord_in.at[place, chunk, pl.ds(place_in * lat_dev, lat_dev)]

    def slot_spot(place, chunk):
        return slot_all.at[place, chunk, pl.ds(me * slots, slots)]

    def wide_start(part, job):
        if part:
            spot = lax.rem(lax.div(job - pairs * chunks, pairs) + pairs, chunks)
        else:
            spot = jnp.where(job < 2 * pairs, lax.rem(job, pairs), job - pairs)
        return pl.multiple_of(spot * wide_a.shape[0], 8)

    def widen(source, place, chunk, depth, count):
        def one(block, carry):
            piece = source[place, chunk, pl.ds(block * depth, depth)].astype(jnp.float32)
            wide_a[pl.ds(pl.multiple_of(block * depth * rows, depth * rows), depth * rows), :] = (
                piece.reshape(depth * rows, LANES)
            )
            return carry

        lax.fori_loop(0, count // depth, one, 0)

    def apply_table(tab, kind, kept, result_ref, start, depth_in, depth_out, dims):
        def one(order, carry):
            real = wide_a[pl.ds(2 * order, depth_in, stride=rows), :]
            imag = wide_a[pl.ds(2 * order + 1, depth_in, stride=rows), :]
            both = jnp.concatenate([real, imag], axis=1).astype(jnp.bfloat16)
            result = dot(tab[kind, order, :kept], both, dims)
            result_ref[pl.ds(start + 2 * order, depth_out, stride=rows), :] = result[:, :LANES]
            result_ref[pl.ds(start + 2 * order + 1, depth_out, stride=rows), :] = result[:, LANES:]
            return carry

        lax.fori_loop(0, orders, one, 0, unroll=4)

    def narrow(source, target, place, chunk, start, depth, count):
        def one(block, carry):
            low = pl.multiple_of(start + block * depth * rows, 8)
            piece = source[pl.ds(low, depth * rows), :]
            target[place, chunk, pl.ds(block * depth, depth)] = piece.reshape(
                depth, rows, LANES
            ).astype(jnp.bfloat16)
            return carry

        lax.fori_loop(0, count // depth, one, 0)

    def wide_rows(start, index, depth):
        return pl.ds(pl.multiple_of(start + index * rows, 8), depth * rows)

    def blank(first, count):
        def one(block, carry):
            by_name[pl.ds((first + block) * orders, orders)] = jnp.zeros(
                (orders, rows, LANES), jnp.bfloat16
            )
            return carry

        lax.fori_loop(0, count, one, 0)

    def analyse(base, tab, part, job):
        kind, chunk, place = job_of(job)

        @pl.when(mine(kind))
        def _():
            await_bytes(ord_in.at[place, chunk], recv_sem.at[base, job])
            widen(ord_in, place, chunk, lat_dev, side_lats)
            start = wide_start(part, job)
            peer = owner(kind, across, column)
            source = cross_out.at[place, chunk]
            target = cross_in.at[place, chunk]
            kept = own if part else degrees
            apply_table(tab, kind, kept, wide_b, start, side_lats, kept, ((1,), (0,)))
            if not part:
                if base:
                    await_bytes(source, send_sem.at[1, job])
                narrow(wide_b, cross_out, place, chunk, start + across * own * rows, slots, own)
                remote(base + 1, job, source, target, peer)
                return
            if base:
                await_tail(kind, source, send_sem.at[1, job])

            def send(low):
                span = pl.ds(low, orders)
                piece = wide_b[wide_rows(start, low, orders), :]
                cross_out[place, chunk, span] = piece.reshape(orders, rows, LANES).astype(
                    jnp.bfloat16
                )
                remote(base + 1, job, source.at[span], target.at[span], peer)

            tail_blocks(kind, send)

    def settle(base, target, part, job):
        kind, chunk, place = job_of(job)

        @pl.when(mine(kind))
        def _():
            start = wide_start(part, job)
            if part:
                await_tail(kind, cross_in.at[place, chunk], recv_sem.at[base + 1, job])
            else:
                await_bytes(cross_in.at[place, chunk], recv_sem.at[base + 1, job])
            if base:
                left_owner(2, job, kind, chunk, slot_out, slots)
                if part:
                    await_tail(kind, tail_out.at[chunk], send_sem.at[4, job])
                else:
                    await_bytes(slot_all.at[place, chunk, 0:own], send_sem.at[4, job])
            if part:

                blank(0, own // orders + first_block(kind))

                def add(low):
                    piece = wide_b[wide_rows(start, low, orders), :]
                    other = cross_in[place, chunk, pl.ds(low, orders)].astype(jnp.float32)
                    by_name[pl.ds(own + low, orders)] = (
                        piece.reshape(orders, rows, LANES) + other
                    ).astype(jnp.bfloat16)

                tail_blocks(kind, add)

                def pick(slot, carry):
                    slot_out[place, chunk, slot] = by_name[deg_ref[side * own + slot]]
                    return carry

                lax.fori_loop(0, own, pick, 0, unroll=4)
            else:

                def one(block, carry):
                    low = block * slots
                    piece = wide_b[wide_rows(start + side * own * rows, low, slots), :]
                    other = cross_in[place, chunk, pl.ds(low, slots)].astype(jnp.float32)
                    slot_out[place, chunk, pl.ds(low, slots)] = (
                        piece.reshape(slots, rows, LANES) + other
                    ).astype(jnp.bfloat16)
                    return carry

                lax.fori_loop(0, half, one, 0)
            from_owner(base + 2, job, kind, chunk, slot_out, slots, target)

    def relay(base, part, job):
        kind, chunk, place = job_of(job)

        @pl.when(mine(kind))
        def _():
            await_bytes(slot_all.at[place, chunk, 0:own], recv_sem.at[base + 3, job])
            peer = owner(kind, across, column)
            view = slot_all.at[place, chunk, pl.ds(side * own, own)]
            if not part:
                remote(base + 4, job, view, view, peer)
                return

            blank(across * (own // orders), own // orders)

            def copy(block, carry):
                span = pl.ds(side * own + block * slots, slots)
                by_name[span] = slot_all[place, chunk, span]
                return carry

            lax.fori_loop(0, half, copy, 0)

            def send(low):
                for step in range(orders):
                    tail_out[chunk, low + step] = by_name[slot_of[0, own + low + step]]
                span = pl.ds(low, orders)
                remote(base + 4, job, tail_out.at[chunk, span], view.at[span], peer)

            tail_blocks(kind, send)

    def synthesise(base, tab, part, job):
        kind, chunk, place = job_of(job)

        @pl.when(mine(kind))
        def _():
            if part:
                await_tail(kind, tail_out.at[chunk], recv_sem.at[base + 4, job])

                def clear(block, carry):
                    wide_a[wide_rows(0, block * orders, orders), :] = jnp.zeros(
                        (orders * rows, LANES), jnp.float32
                    )
                    return carry

                lax.fori_loop(0, first_block(kind), clear, 0)

                def add(low):
                    near = tail_out[chunk, pl.ds(low, orders)].astype(jnp.float32)
                    far = slot_all[place, chunk, pl.ds(across * own + low, orders)]
                    wide_a[wide_rows(0, low, orders), :] = (
                        near + far.astype(jnp.float32)
                    ).reshape(orders * rows, LANES)

                tail_blocks(kind, add)
                apply_table(tab, kind, own, wide_c, 0, own, side_lats, ((0,), (0,)))
            else:
                await_bytes(slot_all.at[place, chunk, 0:own], recv_sem.at[base + 4, job])
                widen(slot_all, place, chunk, slots, degrees)
                apply_table(tab, kind, degrees, wide_c, 0, degrees, side_lats, ((0,), (0,)))
            if base:
                left_owner(5, job, kind, chunk, ord_out, lat_dev)
            narrow(wide_c, ord_out, place, chunk, 0, lat_dev, side_lats)
            from_owner(base + 5, job, kind, chunk, ord_out, lat_dev, band_in)

    def loop(low, high, body):
        def one(job, carry):
            body(job)
            return carry

        lax.fori_loop(low, high, one, 0)

    def pair(source, chunk, row):
        return jnp.concatenate([source[chunk, 2 * row], source[chunk, 2 * row + 1]], axis=1)

    def put_pair(target, chunk, row, values):
        values = values.astype(jnp.bfloat16)
        target[chunk, 2 * row] = values[:, :LANES]
        target[chunk, 2 * row + 1] = values[:, LANES:]

    def joined(source, slot, span):
        return jnp.concatenate([source[chunk, slot, span] for chunk in range(chunks)], axis=1)

    def mix(part, chunk):
        low = part * pairs * plane_rows
        span = slice(low, low + pairs * plane_rows)
        columns = slice(chunk * LANES, (chunk + 1) * LANES)

        def one(slot, carry):
            both = dot(
                joined(co, slot, span),
                jnp.concatenate([wbuf[slot, 0, :, columns], wbuf[slot, 1, :, columns]], axis=1),
            )
            crossed = pair_swap(both[:, LANES:], -1.0)
            mixed[chunk, slot, span] = (both[:, :LANES] + crossed).astype(jnp.bfloat16)
            return carry

        return one

    def adjoint(part, chunk):
        low = part * pairs * plane_rows
        span = slice(low, low + pairs * plane_rows)
        columns = slice(chunk * LANES, (chunk + 1) * LANES)

        def one(slot, carry):
            both = dot(
                joined(go, slot, span),
                jnp.concatenate([wbuf[slot, 0, columns, :], wbuf[slot, 1, columns, :]], axis=0),
                ((1,), (1,)),
            )
            crossed = pair_swap(both[:, LANES:], 1.0)
            mixed[chunk, slot, span] = (both[:, :LANES] + crossed).astype(jnp.bfloat16)
            return carry

        return one

    def filter_part(base, part, source, make):
        part_kinds = range(part * pairs, (part + 1) * pairs)
        for chunk in range(chunks):
            for kind in part_kinds:
                reached_all(base + 2, kind, chunk, source)
        for chunk in range(chunks):
            if base:
                for kind in part_kinds:
                    left_for_owners(3, kind, chunk, mixed)
            lax.fori_loop(0, slots, make(part, chunk), 0, unroll=4)
            for kind in part_kinds:
                to_owners(base + 3, kind, chunk, mixed, slot_spot, slots)

    per_pass = pairs * chunks
    def unit(part, chunk):
        first = part * per_pass + chunk * pairs
        return first, first + pairs

    def run(spans, body):
        loop(spans[0], spans[1], body)

    def to_filter_start(base, tab, source):
        run(unit(0, 0), lambda job: analyse(base, tab, 0, job))
        for low, high, part, behind in (
            (pairs, per_pass, 0, 0),
            (per_pass, per_pass + pairs, 1, 0),
            (per_pass + pairs, per_pass + 2 * pairs, 1, 1),
        ):

            def step(job):
                settle(base, source, behind, job - pairs)
                analyse(base, tab, part, job)

            loop(low, high, step)
        loop(per_pass + 2 * pairs, jobs, lambda job: analyse(base, tab, 1, job))

    def to_filter_by_chunk(base, tab, source, rest):
        run(unit(0, 0), lambda job: analyse(base, tab, 0, job))
        run(unit(1, 0), lambda job: analyse(base, tab, 1, job))
        rest()

        def second(job):
            settle(base, source, 0, job - pairs)
            analyse(base, tab, 0, job)

        run(unit(0, 1), second)
        run(unit(1, 0), lambda job: settle(base, source, 1, job))
        run(unit(0, 2), lambda job: analyse(base, tab, 0, job))

        for job in range(pairs, 2 * pairs):
            settle(base, source, 0, job)
            run(unit(1, job - pairs + 1), lambda spot: analyse(base, tab, 1, spot))
        run(unit(0, 2), lambda job: settle(base, source, 0, job))

    def through_filter(base, tab, source, make):
        filter_part(base, 0, source, make)
        run(unit(1, 1), lambda job: settle(base, source, 1, job))
        run(unit(0, 0), lambda job: relay(base, 0, job))
        run(unit(1, 2), lambda job: settle(base, source, 1, job))
        run(unit(0, 1), lambda job: relay(base, 0, job))
        run(unit(0, 0), lambda job: synthesise(base, tab, 0, job))
        loop(pairs, pairs + 1, lambda job: synthesise(base, tab, 0, job))
        filter_part(base, 1, source, make)
        loop(pairs + 1, 2 * pairs, lambda job: synthesise(base, tab, 0, job))
        run(unit(1, 0), lambda job: relay(base, 1, job))
        run(unit(0, 2), lambda job: relay(base, 0, job))
        run(unit(1, 1), lambda job: relay(base, 1, job))

    def spread(stage, chunk, part):
        for kind in range(part * pairs, (part + 1) * pairs):
            to_owners(stage, kind, chunk, band_out, lat_spot, lat_dev)

    def transform(chunk):
        load(chunk).wait()

        def fourier(row, carry):
            put_pair(band_out, chunk, row, dot(fwd_fk[...], pair(fbuf, chunk, row)))
            return carry

        lax.fori_loop(0, lat_dev // 2, fourier, 0, unroll=3)

    transform(0)
    pl.semaphore_wait(barrier, n - 1 + nb - 1)
    spread(0, 0, 0)
    transform(1)
    spread(0, 1, 0)
    fill_tables(
        side, [group(kind, column) * orders for kind in range(kinds)], deg_ref, diag_ref, cos_ref,
        quad_ref, qtab, ptab, table, wide_b,
    )
    for chunk in range(2, chunks):
        transform(chunk)
        spread(0, chunk, 0)
    for chunk in range(chunks):
        spread(0, chunk, 1)
    spots = lax.broadcasted_iota(jnp.int32, row_ref.shape, 1)

    def invert(slot, carry):
        return jnp.where(spots == deg_ref[slot], slot, carry)

    row_ref[...] = lax.fori_loop(0, degrees, invert, spots * 0, unroll=4)
    turn = pltpu.make_async_copy(row_ref, slot_of, load_sem.at[2 * chunks + 1])
    turn.start()
    turn.wait()
    load_w.wait()
    to_filter_start(0, qtab, co)
    through_filter(0, ptab, co, mix)

    def between(chunk):
        load_cot(chunk).wait()
        for kind in range(kinds):
            reached_all(5, kind, chunk, band_in)
            left_for_owners(0, kind, chunk, band_out)

        def middle(row, carry):
            response = dot(inv_kf[...], pair(band_in, chunk, row))
            upstream = pair(cbuf, chunk, row).astype(jnp.float32) * gelu_slope(response)
            put_pair(band_out, chunk, row, dot(inv_fk[...], upstream.astype(jnp.bfloat16)))
            return carry

        lax.fori_loop(0, lat_dev // 2, middle, 0, unroll=3)
        spread(6, chunk, 0)
        spread(6, chunk, 1)

    def finish_synthesis(base, tab, finish):
        first, second = unit(0, 2)
        run(unit(1, 0), lambda job: synthesise(base, tab, 1, job))
        loop(first, first + 1, lambda job: synthesise(base, tab, 0, job))
        run(unit(1, 2), lambda job: relay(base, 1, job))
        if not base:
            finish(0)
        loop(first + 1, second, lambda job: synthesise(base, tab, 0, job))
        loop(per_pass + pairs, jobs, lambda job: synthesise(base, tab, 1, job))
        if base:
            finish(0)

    def rest(finish):
        for chunk in range(1, chunks):
            finish(chunk)

    finish_synthesis(0, ptab, between)
    to_filter_by_chunk(6, ptab, go, lambda: rest(between))
    through_filter(6, qtab, go, adjoint)

    def weight_grad(slot, carry):
        values = joined(co, slot, slice(None))
        grads = joined(go, slot, slice(None))
        turned = pair_swap(grads.astype(jnp.float32), 1.0).astype(jnp.bfloat16)
        span = ((0,), (0,))
        dw[slot, 0] = dot(values, grads, span).astype(jnp.bfloat16)
        dw[slot, 1] = dot(values, turned, span).astype(jnp.bfloat16)
        return carry

    lax.fori_loop(0, slots, weight_grad, 0)
    dw_copies = []
    for step in range(1, nb):
        peer = lax.rem(me_b + step, nb)
        copy = pltpu.make_async_remote_copy(
            src_ref=dw,
            dst_ref=dw_in.at[step - 1],
            send_sem=dw_send.at[step - 1],
            recv_sem=dw_recv.at[step - 1],
            device_id={"batch": peer},
            device_id_type=mesh_id,
        )
        copy.start()
        dw_copies.append(copy)

    def store(chunk):
        return pltpu.make_async_copy(
            cbuf.at[chunk], grad_out.at[0, :, :, lanes(chunk)], out_sem.at[chunk]
        )

    store_w = pltpu.make_async_copy(dw, dw_out, out_sem.at[chunks])

    def total(slot, carry):
        value = dw[slot].astype(jnp.float32)
        for step in range(nb - 1):
            value = value + dw_in[step, slot].astype(jnp.float32)
        dw[slot] = value.astype(jnp.bfloat16)
        return carry

    def last(chunk):
        if chunk == 0:
            for copy in dw_copies:
                copy.wait()
            lax.fori_loop(0, slots, total, 0)
            store_w.start()
        for kind in range(kinds):
            reached_all(11, kind, chunk, band_in)

        def finish(row, carry):
            delta = dot(fwd_kf[...], pair(band_in, chunk, row))
            put_pair(cbuf, chunk, row, pair(cbuf, chunk, row).astype(jnp.float32) + delta)
            return carry

        lax.fori_loop(0, lat_dev // 2, finish, 0, unroll=3)
        store(chunk).start()

    finish_synthesis(6, qtab, last)
    rest(last)
    for chunk in range(chunks):
        for kind in range(kinds):
            left_for_owners(6, kind, chunk, band_out)
            left_for_owners(9, kind, chunk, mixed)

    def drain(part, job):
        kind, chunk, place = job_of(job)

        @pl.when(mine(kind))
        def _():
            if part:
                await_tail(kind, cross_out.at[place, chunk], send_sem.at[7, job])
                await_tail(kind, tail_out.at[chunk], send_sem.at[10, job])
            else:
                await_bytes(cross_out.at[place, chunk], send_sem.at[7, job])
                await_bytes(slot_all.at[place, chunk, 0:own], send_sem.at[10, job])
            left_owner(8, job, kind, chunk, slot_out, slots)
            left_owner(11, job, kind, chunk, ord_out, lat_dev)

    loop(0, per_pass, lambda job: drain(0, job))
    loop(per_pass, jobs, lambda job: drain(1, job))
    for chunk in range(chunks):
        store(chunk).wait()
    store_w.wait()


def local_kernel(fields, cotangent, weights, degree_of):
    n = lax.axis_size("lat")
    nb = lax.axis_size("batch")
    kinds = 4
    if fields.shape[0] != 1 or fields.shape[1] % 2 or n % kinds or ORDERS != n * GROUP:
        return local(fields, cotangent, weights, degree_of)
    lat_dev, lons, channels = fields.shape[1:]
    slots = weights.shape[0]
    rows = 2 * GROUP
    chunks = channels // LANES
    floats, waves = constant_tables()
    side_lats = LATS // 2
    held = kinds - 1
    vmem = pl.BlockSpec(memory_space=pltpu.VMEM)
    anywhere = pl.BlockSpec(memory_space=pl.ANY)

    def buffer(*dims):
        return pltpu.VMEM(dims, jnp.bfloat16)

    dma = pltpu.SemaphoreType.DMA
    others = max(nb - 1, 1)
    wide_rows = max(side_lats, DEGREES) * rows
    return pl.pallas_call(
        functools.partial(block_kernel, n, nb),
        out_shape=(
            jax.ShapeDtypeStruct(fields.shape, jnp.bfloat16),
            jax.ShapeDtypeStruct(weights.shape, jnp.bfloat16),
        ),
        in_specs=[anywhere] * 3 + [pl.BlockSpec(memory_space=pltpu.SMEM)] + [vmem] * 7,
        out_specs=(anywhere, anywhere),
        scratch_shapes=[
            buffer(chunks, lat_dev, lons, LANES),
            buffer(chunks, lat_dev, lons, LANES),
            buffer(*weights.shape),
            buffer(chunks, lat_dev, n * rows, LANES),
            buffer(chunks, lat_dev, n * rows, LANES),
            buffer(held, chunks, side_lats, rows, LANES),
            buffer(held, chunks, side_lats, rows, LANES),
            buffer(held, chunks, DEGREES // 2, rows, LANES),
            buffer(held, chunks, DEGREES // 2, rows, LANES),
            buffer(held, chunks, DEGREES // 2, rows, LANES),
            buffer(held, chunks, DEGREES, rows, LANES),
            buffer(chunks, DEGREES // 2, rows, LANES),
            buffer(chunks, slots, n * rows, LANES),
            buffer(chunks, slots, n * rows, LANES),
            buffer(chunks, slots, n * rows, LANES),
            pltpu.VMEM((wide_rows, LANES), jnp.float32),
            pltpu.VMEM((4 * wide_rows, LANES), jnp.float32),
            pltpu.VMEM((side_lats * rows, LANES), jnp.float32),
            buffer(*weights.shape),
            buffer(others, *weights.shape),
            buffer(kinds, GROUP, DEGREES, side_lats),
            buffer(kinds, GROUP, DEGREES, side_lats),
            pltpu.VMEM((DEGREES, kinds * GROUP, LANES), jnp.float32),
            pltpu.VMEM((GROUP, DEGREES), jnp.int32),
            pltpu.SMEM((GROUP, DEGREES), jnp.int32),
            buffer(DEGREES, rows, LANES),
            dma((2 * chunks + 2,)),
            dma((12, kinds * chunks)),
            dma((12, kinds * chunks)),
            dma((others,)),
            dma((others,)),
            dma((chunks + 1,)),
        ],
        compiler_params=pltpu.CompilerParams(
            collective_id=0, has_side_effects=True, vmem_limit_bytes=63 * 2**20
        ),
        name="filter_block",
    )(
        fields, cotangent, weights, degree_of, *floats, *waves,
    )


def local(fields, cotangent, weights, degree_of):
    samples = fields.shape[0]
    band_rows = fields.shape[1]
    ord_dev = ORDERS // lax.axis_size("lat")
    forward, inverse = fourier_tables(LONS, ORDERS)
    qslot, pslot = spectral_tables(lax.axis_index("lat") * ord_dev, ord_dev, degree_of)
    spectra = product("sikc,kf->ifsc", fields, forward).astype(jnp.bfloat16)
    spectra = spectra.reshape(band_rows, ORDERS, 2, samples, CHANNELS)
    gathered = to_orders(spectra)
    coeffs_local = product("mji,imrsc->jmrsc", qslot, gathered).astype(jnp.bfloat16)
    coeffs = to_degrees(coeffs_local)
    filtered = apply_filter(coeffs, weights)
    returned = back_to_orders(filtered)
    synth_local = product("mji,jmrsc->imrsc", pslot, returned).astype(jnp.bfloat16)
    synth = to_bands(synth_local)
    response = product(
        "ifsc,fk->sikc", synth.reshape(band_rows, 2 * ORDERS, samples, CHANNELS), inverse
    )
    activated, pullback = jax.vjp(jax.nn.gelu, response)
    upstream = pullback(cotangent.astype(jnp.float32))[0].astype(jnp.bfloat16)
    grad_synth = product("sikc,fk->ifsc", upstream, inverse).astype(jnp.bfloat16)
    grad_synth = grad_synth.reshape(band_rows, ORDERS, 2, samples, CHANNELS)
    grad_gathered = to_orders(grad_synth)
    grad_local = product("mji,imrsc->jmrsc", pslot, grad_gathered).astype(jnp.bfloat16)
    grad_filtered = to_degrees(grad_local)
    weight_total = lax.psum(filter_grad(coeffs, grad_filtered).astype(jnp.bfloat16), "batch")
    grad_coeffs = adjoint_filter(grad_filtered, weights)
    grad_back = back_to_orders(grad_coeffs)
    grad_local_spec = product("mji,jmrsc->imrsc", qslot, grad_back).astype(jnp.bfloat16)
    grad_bands = to_bands(grad_local_spec)
    delta = product(
        "ifsc,kf->sikc", grad_bands.reshape(band_rows, 2 * ORDERS, samples, CHANNELS), forward
    )
    grad_fields = (cotangent.astype(jnp.float32) + delta).astype(jnp.bfloat16)
    return (grad_fields, weight_total)


def solution(mesh):
    return jax.shard_map(
        local_kernel if CHANNELS % LANES == 0 else local,
        mesh=mesh,
        in_specs=(
            P("batch", "lat", None, None),
            P("batch", "lat", None, None),
            P("lat", None, None, None),
            P(),
        ),
        out_specs=(P("batch", "lat", None, None), P("lat", None, None, None)),
        check_vma=False,
    )
```

```python
import functools

import jax
import numpy as np
import jax.numpy as jnp
from jax import lax
from jax.experimental import pallas as pl
from jax.experimental.pallas import tpu as pltpu
from jax.sharding import PartitionSpec as P

LATS = 192
LONS = 384
ORDERS = 128
DEGREES = 128
CHANNELS = 384
LANES = 128
GROUP = 8


def table_kernel(deg_ref, diag_ref, cos_ref, quad_ref, order_ref, q_ref, p_ref, slot_ref, rows_ref):
    orders = diag_ref.shape[0]
    lats = q_ref.shape[2]
    degrees = deg_ref.shape[0]

    def invert(slot, carry):
        slot_ref[deg_ref[slot]] = slot
        return carry

    lax.fori_loop(0, degrees, invert, 0)
    order_real = order_ref[...]
    squared = order_real * order_real
    diagonal = diag_ref[...]
    cosine = cos_ref[...]
    first_lead = jnp.sqrt(2.0 * order_real + 3.0)
    halves = rows_ref.shape[0]

    def advance(degree, carry):
        previous, older = carry
        degree_real = degree.astype(jnp.float32)
        lead = jnp.sqrt(
            jnp.maximum(4.0 * degree_real * degree_real - 1.0, 0.0)
            / jnp.maximum(degree_real * degree_real - squared, 1.0)
        )
        lower = degree_real - 1.0
        back = jnp.sqrt(
            jnp.maximum(lower * lower - squared, 0.0) / jnp.maximum(4.0 * lower * lower - 1.0, 1.0)
        )
        general = lead * (cosine * previous - back * older)
        first = first_lead * cosine * previous
        value = jnp.where(
            degree_real == order_real,
            diagonal,
            jnp.where(
                degree_real == order_real + 1.0,
                first,
                jnp.where(degree_real > order_real + 1.0, general, 0.0),
            ),
        )
        slot = slot_ref[degree]
        for half in range(halves):
            rows_ref[half, pl.ds(slot, orders, stride=degrees), :] = value[
                :, half * LANES : (half + 1) * LANES
            ]
        return (value, previous)

    zeros = diagonal * 0.0
    lax.fori_loop(0, degrees, advance, (zeros, zeros), unroll=4)
    quadrature = quad_ref[...]
    for order in range(orders):
        for half in range(halves):
            low = half * LANES
            high = min(lats, low + LANES)
            chosen = rows_ref[half, order * degrees : (order + 1) * degrees, :][:, : high - low]
            p_ref[order, :, low:high] = chosen.astype(jnp.bfloat16)
            q_ref[order, :, low:high] = (chosen * quadrature[:, low:high]).astype(jnp.bfloat16)


def spectral_tables(start, ord_dev, degree_of):
    halves = -(-LATS // LANES)
    padded = halves * LANES
    order_col = (start + jnp.arange(ord_dev, dtype=jnp.int32)).astype(jnp.float32)[:, None]
    lat_ids = jnp.minimum(jnp.arange(padded, dtype=jnp.float32), LATS - 1.0)
    colatitude = jnp.pi * (lat_ids + 0.5) / LATS
    sine = jnp.sin(colatitude)[None, :]
    steps_up = jnp.arange(1, DEGREES + 1, dtype=jnp.float32)[None, :]
    factor = jnp.where(
        steps_up <= order_col, 0.5 * jnp.log((2.0 * steps_up + 1.0) / (2.0 * steps_up)), 0.0
    )
    log_start = 0.5 * jnp.log(1.0 / (4.0 * jnp.pi)) + jnp.sum(factor, axis=1, keepdims=True)
    diagonal = jnp.exp(log_start + order_col * jnp.log(sine))
    cosine = jnp.broadcast_to(jnp.cos(colatitude)[None, :], diagonal.shape)
    quadrature = 2.0 * jnp.pi * jnp.pi / LATS * sine
    orders = jnp.broadcast_to(order_col, diagonal.shape)
    vmem = pl.BlockSpec(memory_space=pltpu.VMEM)
    shape = jax.ShapeDtypeStruct((ord_dev, DEGREES, LATS), jnp.bfloat16)
    return pl.pallas_call(
        table_kernel,
        out_shape=(shape, shape),
        in_specs=[pl.BlockSpec(memory_space=pltpu.SMEM)] + [vmem] * 4,
        out_specs=(vmem, vmem),
        scratch_shapes=[
            pltpu.SMEM((DEGREES,), jnp.int32),
            pltpu.VMEM((halves, ord_dev * DEGREES, LANES), jnp.float32),
        ],
        name="legendre_tables",
    )(degree_of, diagonal, cosine, quadrature, orders)


def fourier_tables(lon_count, order_count):
    lon_ids = jnp.arange(lon_count, dtype=jnp.int32)[:, None]
    order_ids = jnp.arange(order_count, dtype=jnp.int32)[None, :]
    phase = 2.0 * jnp.pi * (lon_ids * order_ids % lon_count).astype(jnp.float32) / lon_count
    forward = (
        jnp.stack([jnp.cos(phase), -jnp.sin(phase)], axis=2).reshape(lon_count, 2 * order_count)
        / lon_count
    )
    doubled = jnp.where(order_ids == 0, 1.0, 2.0)
    inverse = jnp.stack([doubled * jnp.cos(phase), -doubled * jnp.sin(phase)], axis=2).reshape(
        lon_count, 2 * order_count
    )
    return (forward.astype(jnp.bfloat16), jnp.transpose(inverse).astype(jnp.bfloat16))


def to_orders(values):
    return lax.all_to_all(values, "lat", split_axis=1, concat_axis=0, tiled=True)


def to_degrees(values):
    return lax.all_to_all(values, "lat", split_axis=0, concat_axis=1, tiled=True)


def back_to_orders(values):
    return lax.all_to_all(values, "lat", split_axis=1, concat_axis=0, tiled=True)


def to_bands(values):
    return lax.all_to_all(values, "lat", split_axis=0, concat_axis=1, tiled=True)


def product(spec, left, right):
    return jnp.einsum(spec, left, right, preferred_element_type=jnp.float32)


def apply_filter(coeffs, weights):
    c_real = coeffs[:, :, 0]
    c_imag = coeffs[:, :, 1]
    w_real = weights[:, 0]
    w_imag = weights[:, 1]
    f_real = product("jmsc,jcd->jmsd", c_real, w_real) - product("jmsc,jcd->jmsd", c_imag, w_imag)
    f_imag = product("jmsc,jcd->jmsd", c_real, w_imag) + product("jmsc,jcd->jmsd", c_imag, w_real)
    return jnp.stack([f_real, f_imag], axis=2).astype(jnp.bfloat16)


def adjoint_filter(grads, weights):
    g_real = grads[:, :, 0]
    g_imag = grads[:, :, 1]
    w_real = weights[:, 0]
    w_imag = weights[:, 1]
    a_real = product("jmsd,jcd->jmsc", g_real, w_real) + product("jmsd,jcd->jmsc", g_imag, w_imag)
    a_imag = product("jmsd,jcd->jmsc", g_imag, w_real) - product("jmsd,jcd->jmsc", g_real, w_imag)
    return jnp.stack([a_real, a_imag], axis=2).astype(jnp.bfloat16)


def filter_grad(coeffs, grads):
    c_real = coeffs[:, :, 0]
    c_imag = coeffs[:, :, 1]
    g_real = grads[:, :, 0]
    g_imag = grads[:, :, 1]
    dw_real = product("jmsc,jmsd->jcd", c_real, g_real) + product("jmsc,jmsd->jcd", c_imag, g_imag)
    dw_imag = product("jmsc,jmsd->jcd", c_real, g_imag) - product("jmsc,jmsd->jcd", c_imag, g_real)
    return jnp.stack([dw_real, dw_imag], axis=1)


def constant_tables():
    sides = 2
    half = LATS // sides
    lat_ids = np.minimum(np.arange(LANES)[None, :], half - 1) + half * np.arange(sides)[:, None]
    colatitude = np.pi * (lat_ids + 0.5) / LATS
    sine = np.sin(colatitude)[:, None, :]
    ids = np.arange(ORDERS)
    steps_up = np.arange(1, ORDERS + 1)
    growth = np.cumsum(0.5 * np.log((2.0 * steps_up + 1.0) / (2.0 * steps_up)))
    log_start = 0.5 * np.log(1.0 / (4.0 * np.pi)) + np.concatenate([[0.0], growth[:-1]])
    diagonal = np.exp(log_start[None, :, None] + ids[None, :, None] * np.log(sine))
    cosine = np.broadcast_to(np.cos(colatitude)[:, None, :], (sides, GROUP, LANES))
    quadrature = np.broadcast_to(2.0 * np.pi * np.pi / LATS * sine, (sides, GROUP, LANES))
    phase = 2.0 * np.pi * (np.arange(LONS)[:, None] * ids[None, :] % LONS) / LONS
    forward = np.stack([np.cos(phase), -np.sin(phase)], axis=2).reshape(LONS, -1) / LONS
    doubled = np.where(ids == 0, 1.0, 2.0)[None, :]
    inverse = np.stack([doubled * np.cos(phase), -doubled * np.sin(phase)], axis=2)
    inverse = inverse.reshape(LONS, -1)
    floats = [jnp.asarray(t, jnp.float32) for t in (diagonal, cosine, quadrature)]
    waves = [forward.T, forward, inverse.T, inverse]
    halves = [jnp.asarray(np.float32(t).astype(jnp.bfloat16)) for t in waves]
    return floats, halves


def fill_tables(side, firsts, deg_ref, diag_ref, cos_ref, quad_ref, qtab, ptab, table, by_slot):
    kinds, orders, degrees, lats = qtab.shape
    every = kinds * orders
    cosine = cos_ref[side]
    diagonal, ids, squared, first_lead = [], [], [], []
    for first in firsts:
        diagonal.append(diag_ref[side, pl.ds(pl.multiple_of(first, orders), orders), :])
        ids.append(first + lax.broadcasted_iota(jnp.int32, cosine.shape, 0))
        real = ids[-1].astype(jnp.float32)
        squared.append(real * real)
        first_lead.append(jnp.sqrt(2.0 * real + 3.0))

    def advance(degree, carry):
        degree_real = degree.astype(jnp.float32)
        lower = degree_real - 1.0
        state = []
        for kind in range(kinds):
            previous, older = carry[kind]
            lead = jnp.sqrt(
                jnp.maximum(4.0 * degree_real * degree_real - 1.0, 0.0)
                / jnp.maximum(degree_real * degree_real - squared[kind], 1.0)
            )
            back = jnp.sqrt(
                jnp.maximum(lower * lower - squared[kind], 0.0)
                / jnp.maximum(4.0 * lower * lower - 1.0, 1.0)
            )
            general = lead * (cosine * previous - back * older)
            first = first_lead[kind] * cosine * previous
            value = jnp.where(
                ids[kind] == degree,
                diagonal[kind],
                jnp.where(
                    ids[kind] + 1 == degree,
                    first,
                    jnp.where(ids[kind] + 1 < degree, general, 0.0),
                ),
            )
            table[degree, kind * orders : (kind + 1) * orders, :] = value
            state.append((value, previous))
        return tuple(state)

    zeros = cosine * 0.0
    lax.fori_loop(0, degrees, advance, ((zeros, zeros),) * kinds, unroll=2)

    ahead = every // 2
    tail = degrees // 2

    def place(slot, carry):
        by_slot[pl.ds(slot, ahead, stride=degrees), :] = table[deg_ref[slot], :ahead]
        return carry

    lax.fori_loop(0, degrees, place, 0, unroll=4)

    def place_tail(row, carry):
        spots = pl.ds(ahead * degrees + row, ahead, stride=degrees)
        by_slot[spots, :] = table[tail + row, ahead:]
        return carry

    lax.fori_loop(0, tail, place_tail, 0, unroll=4)
    quadrature = quad_ref[side][:1, :lats]
    for kind in range(kinds):

        def keep(order, carry):
            start = pl.multiple_of((kind * orders + order) * degrees, degrees)
            depth = degrees if kind < kinds // 2 else tail
            chosen = by_slot[pl.ds(start, depth), :][:, :lats]
            ptab[kind, order, :depth] = chosen.astype(jnp.bfloat16)
            qtab[kind, order, :depth] = (chosen * quadrature).astype(jnp.bfloat16)
            return carry

        lax.fori_loop(0, orders, keep, 0)


def pair_swap(values, even_sign):
    rows = values.shape[0]
    even = lax.broadcasted_iota(jnp.int32, values.shape, 0) % 2 == 0
    above = pltpu.roll(values, rows - 1, 0)
    below = pltpu.roll(values, 1, 0)
    return jnp.where(even, even_sign * above, -even_sign * below)


def gelu_slope(x):
    scale = 0.7978845608028654
    square = x * x
    t = jnp.tanh(scale * (x + 0.044715 * x * square))
    return 0.5 * (1.0 + t) + 0.5 * x * (1.0 - t * t) * (scale * (1.0 + 0.134145 * square))


def dot(left, right, dims=((1,), (0,))):
    return lax.dot_general(left, right, (dims, ((), ())), preferred_element_type=jnp.float32)


def block_kernel(
    n, nb, fields, cotangent, weights, deg_ref, diag_ref, cos_ref, quad_ref,
    fwd_fk, fwd_kf, inv_fk, inv_kf,
    grad_out, dw_out,
    fbuf, cbuf, wbuf, band_out, band_in, ord_in, ord_out, cross_out, cross_in, slot_out, slot_all,
    tail_out, co, go, mixed, wide_a, wide_b, wide_c, dw, dw_in, qtab, ptab, table, row_ref, slot_of, by_name,
    load_sem, send_sem, recv_sem, dw_send, dw_recv, out_sem,
):
    me = lax.axis_index("lat")
    me_b = lax.axis_index("batch")
    chunks, lat_dev = fbuf.shape[0], fbuf.shape[1]
    kinds, orders, degrees, side_lats = qtab.shape
    rows = 2 * orders
    slots = co.shape[1]
    quarter = n // kinds
    half = n // 2
    own = half * slots
    inner_kinds = ord_in.shape[0]
    pairs = kinds // 2
    jobs = kinds * chunks
    plane_rows = quarter * rows
    mesh_id = pl.DeviceIdType.MESH
    side = lax.div(me, half)
    place_in = lax.rem(me, half)
    column = lax.rem(me, quarter)
    inner = jnp.where(lax.div(me, quarter) == 1 + side, 1, 0)
    across = 1 - side

    def lanes(chunk):
        return pl.ds(chunk * LANES, LANES)

    def group(kind, at):
        return jnp.where(
            lax.rem(kind, 2) == 0, kind * quarter + at, (kind + 1) * quarter - 1 - at
        )

    def group_rows(kind, at):
        return pl.ds(pl.multiple_of(group(kind, at) * rows, rows), rows)

    def owner(kind, on_side, at):
        plane = jnp.where(kind < inner_kinds, 1 + on_side, (kinds - 1) * on_side)
        return plane * quarter + at

    def mine(kind):
        return jnp.where(kind < inner_kinds, 1, 0) == inner

    def job_of(job):
        per_pass = pairs * chunks
        inside = lax.rem(job, per_pass)
        kind = lax.div(job, per_pass) * pairs + lax.rem(inside, pairs)
        return kind, lax.div(inside, pairs), lax.rem(kind, inner_kinds)

    def first_block(kind):
        return group(kind, column) - own // orders

    def tail_blocks(kind, body):
        def one(block, carry):
            body(pl.multiple_of(block * orders, orders))
            return carry

        lax.fori_loop(first_block(kind), own // orders, one, 0)

    def await_tail(kind, view, sem):
        for first in range(own // orders):

            @pl.when(first_block(kind) == first)
            def _():
                await_bytes(view.at[pl.ds(0, own - first * orders)], sem)

    def job_at(kind, chunk):
        return (kind // pairs) * (pairs * chunks) + chunk * pairs + kind % pairs

    def load(chunk):
        return pltpu.make_async_copy(
            fields.at[0, :, :, lanes(chunk)], fbuf.at[chunk], load_sem.at[chunk]
        )

    def load_cot(chunk):
        return pltpu.make_async_copy(
            cotangent.at[0, :, :, lanes(chunk)], cbuf.at[chunk], load_sem.at[chunks + chunk]
        )

    load_w = pltpu.make_async_copy(weights, wbuf, load_sem.at[2 * chunks])
    for chunk in range(chunks):
        load(chunk).start()
    load_w.start()
    for chunk in range(chunks):
        load_cot(chunk).start()

    barrier = pltpu.get_barrier_semaphore()

    def greet(step, carry):
        peer = lax.rem(me + step, n)
        pl.semaphore_signal(barrier, inc=1, device_id={"lat": peer}, device_id_type=mesh_id)
        return carry

    lax.fori_loop(1, n, greet, 0)
    for step in range(1, nb):
        peer = lax.rem(me_b + step, nb)
        pl.semaphore_signal(barrier, inc=1, device_id={"batch": peer}, device_id_type=mesh_id)

    def remote(stage, job, source, target, peer):
        pltpu.make_async_remote_copy(
            src_ref=source,
            dst_ref=target,
            send_sem=send_sem.at[stage, job],
            recv_sem=recv_sem.at[stage, job],
            device_id={"lat": peer},
            device_id_type=mesh_id,
        ).start()

    def await_bytes(view, sem):
        pltpu.make_async_copy(view, view, sem).wait()

    def to_owners(stage, kind, chunk, source, target, width):
        job = job_at(kind, chunk)
        for step in range(quarter):
            at = lax.rem(column + step, quarter)
            view = source.at[chunk, :, group_rows(kind, at), :]
            spot = target(kind % inner_kinds, chunk)
            peer = owner(kind, side, at)

            @pl.when(peer != me)
            def _():
                remote(stage, job, view, spot, peer)

            @pl.when(peer == me)
            def _():
                pltpu.make_async_copy(view, spot, recv_sem.at[stage, job]).start()

    def left_for_owners(stage, kind, chunk, source):
        job = job_at(kind, chunk)

        @pl.when(mine(kind))
        def _():
            await_bytes(source.at[chunk, :, 0 : plane_rows - rows, :], send_sem.at[stage, job])

        @pl.when(jnp.logical_not(mine(kind)))
        def _():
            await_bytes(source.at[chunk, :, 0:plane_rows, :], send_sem.at[stage, job])

    def from_owner(stage, job, kind, chunk, source, depth, target):
        place = lax.rem(kind, inner_kinds)
        spot = target.at[chunk, :, group_rows(kind, column), :]

        def send(step, carry):
            at = lax.rem(place_in + step, half)
            remote(
                stage, job, source.at[place, chunk, pl.ds(at * depth, depth)], spot,
                side * half + at,
            )
            return carry

        lax.fori_loop(1, half, send, 0)
        pltpu.make_async_copy(
            source.at[place, chunk, pl.ds(place_in * depth, depth)], spot, recv_sem.at[stage, job]
        ).start()

    def left_owner(stage, job, kind, chunk, source, depth):
        view = source.at[lax.rem(kind, inner_kinds), chunk, 0 : (half - 1) * depth]
        await_bytes(view, send_sem.at[stage, job])

    def reached_all(stage, kind, chunk, target):
        await_bytes(target.at[chunk, :, 0:plane_rows, :], recv_sem.at[stage, job_at(kind, chunk)])

    def lat_spot(place, chunk):
        return ord_in.at[place, chunk, pl.ds(place_in * lat_dev, lat_dev)]

    def slot_spot(place, chunk):
        return slot_all.at[place, chunk, pl.ds(me * slots, slots)]

    def wide_start(part, job):
        if part:
            spot = lax.rem(lax.div(job - pairs * chunks, pairs) + pairs, chunks)
        else:
            spot = jnp.where(job < 2 * pairs, lax.rem(job, pairs), job - pairs)
        return pl.multiple_of(spot * wide_a.shape[0], 8)

    def widen(source, place, chunk, depth, count):
        def one(block, carry):
            piece = source[place, chunk, pl.ds(block * depth, depth)].astype(jnp.float32)
            wide_a[pl.ds(pl.multiple_of(block * depth * rows, depth * rows), depth * rows), :] = (
                piece.reshape(depth * rows, LANES)
            )
            return carry

        lax.fori_loop(0, count // depth, one, 0)

    def apply_table(tab, kind, kept, result_ref, start, depth_in, depth_out, dims):
        def one(order, carry):
            real = wide_a[pl.ds(2 * order, depth_in, stride=rows), :]
            imag = wide_a[pl.ds(2 * order + 1, depth_in, stride=rows), :]
            both = jnp.concatenate([real, imag], axis=1).astype(jnp.bfloat16)
            result = dot(tab[kind, order, :kept], both, dims)
            result_ref[pl.ds(start + 2 * order, depth_out, stride=rows), :] = result[:, :LANES]
            result_ref[pl.ds(start + 2 * order + 1, depth_out, stride=rows), :] = result[:, LANES:]
            return carry

        lax.fori_loop(0, orders, one, 0, unroll=4)

    def narrow(source, target, place, chunk, start, depth, count):
        def one(block, carry):
            low = pl.multiple_of(start + block * depth * rows, 8)
            piece = source[pl.ds(low, depth * rows), :]
            target[place, chunk, pl.ds(block * depth, depth)] = piece.reshape(
                depth, rows, LANES
            ).astype(jnp.bfloat16)
            return carry

        lax.fori_loop(0, count // depth, one, 0)

    def wide_rows(start, index, depth):
        return pl.ds(pl.multiple_of(start + index * rows, 8), depth * rows)

    def blank(first, count):
        def one(block, carry):
            by_name[pl.ds((first + block) * orders, orders)] = jnp.zeros(
                (orders, rows, LANES), jnp.bfloat16
            )
            return carry

        lax.fori_loop(0, count, one, 0)

    def analyse(base, tab, part, job):
        kind, chunk, place = job_of(job)

        @pl.when(mine(kind))
        def _():
            await_bytes(ord_in.at[place, chunk], recv_sem.at[base, job])
            widen(ord_in, place, chunk, lat_dev, side_lats)
            start = wide_start(part, job)
            peer = owner(kind, across, column)
            source = cross_out.at[place, chunk]
            target = cross_in.at[place, chunk]
            kept = own if part else degrees
            apply_table(tab, kind, kept, wide_b, start, side_lats, kept, ((1,), (0,)))
            if not part:
                if base:
                    await_bytes(source, send_sem.at[1, job])
                narrow(wide_b, cross_out, place, chunk, start + across * own * rows, slots, own)
                remote(base + 1, job, source, target, peer)
                return
            if base:
                await_tail(kind, source, send_sem.at[1, job])

            def send(low):
                span = pl.ds(low, orders)
                piece = wide_b[wide_rows(start, low, orders), :]
                cross_out[place, chunk, span] = piece.reshape(orders, rows, LANES).astype(
                    jnp.bfloat16
                )
                remote(base + 1, job, source.at[span], target.at[span], peer)

            tail_blocks(kind, send)

    def settle(base, target, part, job):
        kind, chunk, place = job_of(job)

        @pl.when(mine(kind))
        def _():
            start = wide_start(part, job)
            if part:
                await_tail(kind, cross_in.at[place, chunk], recv_sem.at[base + 1, job])
            else:
                await_bytes(cross_in.at[place, chunk], recv_sem.at[base + 1, job])
            if base:
                left_owner(2, job, kind, chunk, slot_out, slots)
                if part:
                    await_tail(kind, tail_out.at[chunk], send_sem.at[4, job])
                else:
                    await_bytes(slot_all.at[place, chunk, 0:own], send_sem.at[4, job])
            if part:

                blank(0, own // orders + first_block(kind))

                def add(low):
                    piece = wide_b[wide_rows(start, low, orders), :]
                    other = cross_in[place, chunk, pl.ds(low, orders)].astype(jnp.float32)
                    by_name[pl.ds(own + low, orders)] = (
                        piece.reshape(orders, rows, LANES) + other
                    ).astype(jnp.bfloat16)

                tail_blocks(kind, add)

                def pick(slot, carry):
                    slot_out[place, chunk, slot] = by_name[deg_ref[side * own + slot]]
                    return carry

                lax.fori_loop(0, own, pick, 0, unroll=4)
            else:

                def one(block, carry):
                    low = block * slots
                    piece = wide_b[wide_rows(start + side * own * rows, low, slots), :]
                    other = cross_in[place, chunk, pl.ds(low, slots)].astype(jnp.float32)
                    slot_out[place, chunk, pl.ds(low, slots)] = (
                        piece.reshape(slots, rows, LANES) + other
                    ).astype(jnp.bfloat16)
                    return carry

                lax.fori_loop(0, half, one, 0)
            from_owner(base + 2, job, kind, chunk, slot_out, slots, target)

    def relay(base, part, job):
        kind, chunk, place = job_of(job)

        @pl.when(mine(kind))
        def _():
            await_bytes(slot_all.at[place, chunk, 0:own], recv_sem.at[base + 3, job])
            peer = owner(kind, across, column)
            view = slot_all.at[place, chunk, pl.ds(side * own, own)]
            if not part:
                remote(base + 4, job, view, view, peer)
                return

            blank(across * (own // orders), own // orders)

            def copy(block, carry):
                span = pl.ds(side * own + block * slots, slots)
                by_name[span] = slot_all[place, chunk, span]
                return carry

            lax.fori_loop(0, half, copy, 0)

            def send(low):
                for step in range(orders):
                    tail_out[chunk, low + step] = by_name[slot_of[0, own + low + step]]
                span = pl.ds(low, orders)
                remote(base + 4, job, tail_out.at[chunk, span], view.at[span], peer)

            tail_blocks(kind, send)

    def synthesise(base, tab, part, job):
        kind, chunk, place = job_of(job)

        @pl.when(mine(kind))
        def _():
            if part:
                await_tail(kind, tail_out.at[chunk], recv_sem.at[base + 4, job])

                def clear(block, carry):
                    wide_a[wide_rows(0, block * orders, orders), :] = jnp.zeros(
                        (orders * rows, LANES), jnp.float32
                    )
                    return carry

                lax.fori_loop(0, first_block(kind), clear, 0)

                def add(low):
                    near = tail_out[chunk, pl.ds(low, orders)].astype(jnp.float32)
                    far = slot_all[place, chunk, pl.ds(across * own + low, orders)]
                    wide_a[wide_rows(0, low, orders), :] = (
                        near + far.astype(jnp.float32)
                    ).reshape(orders * rows, LANES)

                tail_blocks(kind, add)
                apply_table(tab, kind, own, wide_c, 0, own, side_lats, ((0,), (0,)))
            else:
                await_bytes(slot_all.at[place, chunk, 0:own], recv_sem.at[base + 4, job])
                widen(slot_all, place, chunk, slots, degrees)
                apply_table(tab, kind, degrees, wide_c, 0, degrees, side_lats, ((0,), (0,)))
            if base:
                left_owner(5, job, kind, chunk, ord_out, lat_dev)
            narrow(wide_c, ord_out, place, chunk, 0, lat_dev, side_lats)
            from_owner(base + 5, job, kind, chunk, ord_out, lat_dev, band_in)

    def loop(low, high, body):
        def one(job, carry):
            body(job)
            return carry

        lax.fori_loop(low, high, one, 0)

    def pair(source, chunk, row):
        return jnp.concatenate([source[chunk, 2 * row], source[chunk, 2 * row + 1]], axis=1)

    def put_pair(target, chunk, row, values):
        values = values.astype(jnp.bfloat16)
        target[chunk, 2 * row] = values[:, :LANES]
        target[chunk, 2 * row + 1] = values[:, LANES:]

    def joined(source, slot, span):
        return jnp.concatenate([source[chunk, slot, span] for chunk in range(chunks)], axis=1)

    def mix(part, chunk):
        low = part * pairs * plane_rows
        span = slice(low, low + pairs * plane_rows)
        columns = slice(chunk * LANES, (chunk + 1) * LANES)

        def one(slot, carry):
            both = dot(
                joined(co, slot, span),
                jnp.concatenate([wbuf[slot, 0, :, columns], wbuf[slot, 1, :, columns]], axis=1),
            )
            crossed = pair_swap(both[:, LANES:], -1.0)
            mixed[chunk, slot, span] = (both[:, :LANES] + crossed).astype(jnp.bfloat16)
            return carry

        return one

    def adjoint(part, chunk):
        low = part * pairs * plane_rows
        span = slice(low, low + pairs * plane_rows)
        columns = slice(chunk * LANES, (chunk + 1) * LANES)

        def one(slot, carry):
            both = dot(
                joined(go, slot, span),
                jnp.concatenate([wbuf[slot, 0, columns, :], wbuf[slot, 1, columns, :]], axis=0),
                ((1,), (1,)),
            )
            crossed = pair_swap(both[:, LANES:], 1.0)
            mixed[chunk, slot, span] = (both[:, :LANES] + crossed).astype(jnp.bfloat16)
            return carry

        return one

    def filter_part(base, part, source, make):
        part_kinds = range(part * pairs, (part + 1) * pairs)
        for chunk in range(chunks):
            for kind in part_kinds:
                reached_all(base + 2, kind, chunk, source)
        for chunk in range(chunks):
            if base:
                for kind in part_kinds:
                    left_for_owners(3, kind, chunk, mixed)
            lax.fori_loop(0, slots, make(part, chunk), 0, unroll=4)
            for kind in part_kinds:
                to_owners(base + 3, kind, chunk, mixed, slot_spot, slots)

    per_pass = pairs * chunks
    def unit(part, chunk):
        first = part * per_pass + chunk * pairs
        return first, first + pairs

    def run(spans, body):
        loop(spans[0], spans[1], body)

    def to_filter_start(base, tab, source):
        run(unit(0, 0), lambda job: analyse(base, tab, 0, job))
        for low, high, part, behind in (
            (pairs, per_pass, 0, 0),
            (per_pass, per_pass + pairs, 1, 0),
            (per_pass + pairs, per_pass + 2 * pairs, 1, 1),
        ):

            def step(job):
                settle(base, source, behind, job - pairs)
                analyse(base, tab, part, job)

            loop(low, high, step)
        loop(per_pass + 2 * pairs, jobs, lambda job: analyse(base, tab, 1, job))

    def to_filter_by_chunk(base, tab, source, rest):
        run(unit(0, 0), lambda job: analyse(base, tab, 0, job))
        run(unit(1, 0), lambda job: analyse(base, tab, 1, job))
        rest()

        def second(job):
            settle(base, source, 0, job - pairs)
            analyse(base, tab, 0, job)

        run(unit(0, 1), second)
        run(unit(1, 0), lambda job: settle(base, source, 1, job))
        run(unit(0, 2), lambda job: analyse(base, tab, 0, job))

        for job in range(pairs, 2 * pairs):
            settle(base, source, 0, job)
            run(unit(1, job - pairs + 1), lambda spot: analyse(base, tab, 1, spot))
        run(unit(0, 2), lambda job: settle(base, source, 0, job))

    def through_filter(base, tab, source, make):
        filter_part(base, 0, source, make)
        run(unit(1, 1), lambda job: settle(base, source, 1, job))
        run(unit(0, 0), lambda job: relay(base, 0, job))
        run(unit(1, 2), lambda job: settle(base, source, 1, job))
        run(unit(0, 1), lambda job: relay(base, 0, job))
        run(unit(0, 0), lambda job: synthesise(base, tab, 0, job))
        loop(pairs, pairs + 1, lambda job: synthesise(base, tab, 0, job))
        filter_part(base, 1, source, make)
        loop(pairs + 1, 2 * pairs, lambda job: synthesise(base, tab, 0, job))
        run(unit(1, 0), lambda job: relay(base, 1, job))
        run(unit(0, 2), lambda job: relay(base, 0, job))
        run(unit(1, 1), lambda job: relay(base, 1, job))

    def spread(stage, chunk, part):
        for kind in range(part * pairs, (part + 1) * pairs):
            to_owners(stage, kind, chunk, band_out, lat_spot, lat_dev)

    def transform(chunk):
        load(chunk).wait()

        def fourier(row, carry):
            put_pair(band_out, chunk, row, dot(fwd_fk[...], pair(fbuf, chunk, row)))
            return carry

        lax.fori_loop(0, lat_dev // 2, fourier, 0, unroll=3)

    transform(0)
    pl.semaphore_wait(barrier, n - 1 + nb - 1)
    spread(0, 0, 0)
    transform(1)
    spread(0, 1, 0)
    fill_tables(
        side, [group(kind, column) * orders for kind in range(kinds)], deg_ref, diag_ref, cos_ref,
        quad_ref, qtab, ptab, table, wide_b,
    )
    for chunk in range(2, chunks):
        transform(chunk)
        spread(0, chunk, 0)
    for chunk in range(chunks):
        spread(0, chunk, 1)
    spots = lax.broadcasted_iota(jnp.int32, row_ref.shape, 1)

    def invert(slot, carry):
        return jnp.where(spots == deg_ref[slot], slot, carry)

    row_ref[...] = lax.fori_loop(0, degrees, invert, spots * 0, unroll=4)
    turn = pltpu.make_async_copy(row_ref, slot_of, load_sem.at[2 * chunks + 1])
    turn.start()
    turn.wait()
    load_w.wait()
    to_filter_start(0, qtab, co)
    through_filter(0, ptab, co, mix)

    def between(chunk):
        load_cot(chunk).wait()
        for kind in range(kinds):
            reached_all(5, kind, chunk, band_in)
            left_for_owners(0, kind, chunk, band_out)

        def middle(row, carry):
            response = dot(inv_kf[...], pair(band_in, chunk, row))
            upstream = pair(cbuf, chunk, row).astype(jnp.float32) * gelu_slope(response)
            put_pair(band_out, chunk, row, dot(inv_fk[...], upstream.astype(jnp.bfloat16)))
            return carry

        lax.fori_loop(0, lat_dev // 2, middle, 0, unroll=3)
        spread(6, chunk, 0)
        if chunk == 0:
            spread(6, 0, 1)
        if chunk == chunks - 1:
            for earlier in range(1, chunks):
                spread(6, earlier, 1)

    def finish_synthesis(base, tab, finish):
        first, second = unit(0, 2)
        run(unit(1, 0), lambda job: synthesise(base, tab, 1, job))
        loop(first, first + 1, lambda job: synthesise(base, tab, 0, job))
        run(unit(1, 2), lambda job: relay(base, 1, job))
        if not base:
            finish(0)
        loop(first + 1, second, lambda job: synthesise(base, tab, 0, job))
        loop(per_pass + pairs, jobs, lambda job: synthesise(base, tab, 1, job))
        if base:
            finish(0)

    def rest(finish):
        for chunk in range(1, chunks):
            finish(chunk)

    finish_synthesis(0, ptab, between)
    to_filter_by_chunk(6, ptab, go, lambda: rest(between))
    through_filter(6, qtab, go, adjoint)

    def weight_grad(slot, carry):
        values = joined(co, slot, slice(None))
        grads = joined(go, slot, slice(None))
        turned = pair_swap(grads.astype(jnp.float32), 1.0).astype(jnp.bfloat16)
        span = ((0,), (0,))
        dw[slot, 0] = dot(values, grads, span).astype(jnp.bfloat16)
        dw[slot, 1] = dot(values, turned, span).astype(jnp.bfloat16)
        return carry

    lax.fori_loop(0, slots, weight_grad, 0)
    dw_copies = []
    for step in range(1, nb):
        peer = lax.rem(me_b + step, nb)
        copy = pltpu.make_async_remote_copy(
            src_ref=dw,
            dst_ref=dw_in.at[step - 1],
            send_sem=dw_send.at[step - 1],
            recv_sem=dw_recv.at[step - 1],
            device_id={"batch": peer},
            device_id_type=mesh_id,
        )
        copy.start()
        dw_copies.append(copy)

    def store(chunk):
        return pltpu.make_async_copy(
            cbuf.at[chunk], grad_out.at[0, :, :, lanes(chunk)], out_sem.at[chunk]
        )

    store_w = pltpu.make_async_copy(dw, dw_out, out_sem.at[chunks])

    def total(slot, carry):
        value = dw[slot].astype(jnp.float32)
        for step in range(nb - 1):
            value = value + dw_in[step, slot].astype(jnp.float32)
        dw[slot] = value.astype(jnp.bfloat16)
        return carry

    def last(chunk):
        if chunk == 0:
            for copy in dw_copies:
                copy.wait()
            lax.fori_loop(0, slots, total, 0)
            store_w.start()
        for kind in range(kinds):
            reached_all(11, kind, chunk, band_in)

        def finish(row, carry):
            delta = dot(fwd_kf[...], pair(band_in, chunk, row))
            put_pair(cbuf, chunk, row, pair(cbuf, chunk, row).astype(jnp.float32) + delta)
            return carry

        lax.fori_loop(0, lat_dev // 2, finish, 0, unroll=3)
        store(chunk).start()

    finish_synthesis(6, qtab, last)
    rest(last)
    for chunk in range(chunks):
        for kind in range(kinds):
            left_for_owners(6, kind, chunk, band_out)
            left_for_owners(9, kind, chunk, mixed)

    def drain(part, job):
        kind, chunk, place = job_of(job)

        @pl.when(mine(kind))
        def _():
            if part:
                await_tail(kind, cross_out.at[place, chunk], send_sem.at[7, job])
                await_tail(kind, tail_out.at[chunk], send_sem.at[10, job])
            else:
                await_bytes(cross_out.at[place, chunk], send_sem.at[7, job])
                await_bytes(slot_all.at[place, chunk, 0:own], send_sem.at[10, job])
            left_owner(8, job, kind, chunk, slot_out, slots)
            left_owner(11, job, kind, chunk, ord_out, lat_dev)

    loop(0, per_pass, lambda job: drain(0, job))
    loop(per_pass, jobs, lambda job: drain(1, job))
    for chunk in range(chunks):
        store(chunk).wait()
    store_w.wait()


def local_kernel(fields, cotangent, weights, degree_of):
    n = lax.axis_size("lat")
    nb = lax.axis_size("batch")
    kinds = 4
    if fields.shape[0] != 1 or fields.shape[1] % 2 or n % kinds or ORDERS != n * GROUP:
        return local(fields, cotangent, weights, degree_of)
    lat_dev, lons, channels = fields.shape[1:]
    slots = weights.shape[0]
    rows = 2 * GROUP
    chunks = channels // LANES
    floats, waves = constant_tables()
    side_lats = LATS // 2
    held = kinds - 1
    vmem = pl.BlockSpec(memory_space=pltpu.VMEM)
    anywhere = pl.BlockSpec(memory_space=pl.ANY)

    def buffer(*dims):
        return pltpu.VMEM(dims, jnp.bfloat16)

    dma = pltpu.SemaphoreType.DMA
    others = max(nb - 1, 1)
    wide_rows = max(side_lats, DEGREES) * rows
    return pl.pallas_call(
        functools.partial(block_kernel, n, nb),
        out_shape=(
            jax.ShapeDtypeStruct(fields.shape, jnp.bfloat16),
            jax.ShapeDtypeStruct(weights.shape, jnp.bfloat16),
        ),
        in_specs=[anywhere] * 3 + [pl.BlockSpec(memory_space=pltpu.SMEM)] + [vmem] * 7,
        out_specs=(anywhere, anywhere),
        scratch_shapes=[
            buffer(chunks, lat_dev, lons, LANES),
            buffer(chunks, lat_dev, lons, LANES),
            buffer(*weights.shape),
            buffer(chunks, lat_dev, n * rows, LANES),
            buffer(chunks, lat_dev, n * rows, LANES),
            buffer(held, chunks, side_lats, rows, LANES),
            buffer(held, chunks, side_lats, rows, LANES),
            buffer(held, chunks, DEGREES // 2, rows, LANES),
            buffer(held, chunks, DEGREES // 2, rows, LANES),
            buffer(held, chunks, DEGREES // 2, rows, LANES),
            buffer(held, chunks, DEGREES, rows, LANES),
            buffer(chunks, DEGREES // 2, rows, LANES),
            buffer(chunks, slots, n * rows, LANES),
            buffer(chunks, slots, n * rows, LANES),
            buffer(chunks, slots, n * rows, LANES),
            pltpu.VMEM((wide_rows, LANES), jnp.float32),
            pltpu.VMEM((4 * wide_rows, LANES), jnp.float32),
            pltpu.VMEM((side_lats * rows, LANES), jnp.float32),
            buffer(*weights.shape),
            buffer(others, *weights.shape),
            buffer(kinds, GROUP, DEGREES, side_lats),
            buffer(kinds, GROUP, DEGREES, side_lats),
            pltpu.VMEM((DEGREES, kinds * GROUP, LANES), jnp.float32),
            pltpu.VMEM((GROUP, DEGREES), jnp.int32),
            pltpu.SMEM((GROUP, DEGREES), jnp.int32),
            buffer(DEGREES, rows, LANES),
            dma((2 * chunks + 2,)),
            dma((12, kinds * chunks)),
            dma((12, kinds * chunks)),
            dma((others,)),
            dma((others,)),
            dma((chunks + 1,)),
        ],
        compiler_params=pltpu.CompilerParams(
            collective_id=0, has_side_effects=True, vmem_limit_bytes=63 * 2**20
        ),
        name="filter_block",
    )(
        fields, cotangent, weights, degree_of, *floats, *waves,
    )


def local(fields, cotangent, weights, degree_of):
    samples = fields.shape[0]
    band_rows = fields.shape[1]
    ord_dev = ORDERS // lax.axis_size("lat")
    forward, inverse = fourier_tables(LONS, ORDERS)
    qslot, pslot = spectral_tables(lax.axis_index("lat") * ord_dev, ord_dev, degree_of)
    spectra = product("sikc,kf->ifsc", fields, forward).astype(jnp.bfloat16)
    spectra = spectra.reshape(band_rows, ORDERS, 2, samples, CHANNELS)
    gathered = to_orders(spectra)
    coeffs_local = product("mji,imrsc->jmrsc", qslot, gathered).astype(jnp.bfloat16)
    coeffs = to_degrees(coeffs_local)
    filtered = apply_filter(coeffs, weights)
    returned = back_to_orders(filtered)
    synth_local = product("mji,jmrsc->imrsc", pslot, returned).astype(jnp.bfloat16)
    synth = to_bands(synth_local)
    response = product(
        "ifsc,fk->sikc", synth.reshape(band_rows, 2 * ORDERS, samples, CHANNELS), inverse
    )
    activated, pullback = jax.vjp(jax.nn.gelu, response)
    upstream = pullback(cotangent.astype(jnp.float32))[0].astype(jnp.bfloat16)
    grad_synth = product("sikc,fk->ifsc", upstream, inverse).astype(jnp.bfloat16)
    grad_synth = grad_synth.reshape(band_rows, ORDERS, 2, samples, CHANNELS)
    grad_gathered = to_orders(grad_synth)
    grad_local = product("mji,imrsc->jmrsc", pslot, grad_gathered).astype(jnp.bfloat16)
    grad_filtered = to_degrees(grad_local)
    weight_total = lax.psum(filter_grad(coeffs, grad_filtered).astype(jnp.bfloat16), "batch")
    grad_coeffs = adjoint_filter(grad_filtered, weights)
    grad_back = back_to_orders(grad_coeffs)
    grad_local_spec = product("mji,jmrsc->imrsc", qslot, grad_back).astype(jnp.bfloat16)
    grad_bands = to_bands(grad_local_spec)
    delta = product(
        "ifsc,kf->sikc", grad_bands.reshape(band_rows, 2 * ORDERS, samples, CHANNELS), forward
    )
    grad_fields = (cotangent.astype(jnp.float32) + delta).astype(jnp.bfloat16)
    return (grad_fields, weight_total)


def solution(mesh):
    return jax.shard_map(
        local_kernel if CHANNELS % LANES == 0 else local,
        mesh=mesh,
        in_specs=(
            P("batch", "lat", None, None),
            P("batch", "lat", None, None),
            P("lat", None, None, None),
            P(),
        ),
        out_specs=(P("batch", "lat", None, None), P("lat", None, None, None)),
        check_vma=False,
    )
```

```python
import functools

import jax
import numpy as np
import jax.numpy as jnp
from jax import lax
from jax.experimental import pallas as pl
from jax.experimental.pallas import tpu as pltpu
from jax.sharding import PartitionSpec as P

LATS = 192
LONS = 384
ORDERS = 128
DEGREES = 128
CHANNELS = 384
LANES = 128
GROUP = 8


def table_kernel(deg_ref, diag_ref, cos_ref, quad_ref, order_ref, q_ref, p_ref, slot_ref, rows_ref):
    orders = diag_ref.shape[0]
    lats = q_ref.shape[2]
    degrees = deg_ref.shape[0]

    def invert(slot, carry):
        slot_ref[deg_ref[slot]] = slot
        return carry

    lax.fori_loop(0, degrees, invert, 0)
    order_real = order_ref[...]
    squared = order_real * order_real
    diagonal = diag_ref[...]
    cosine = cos_ref[...]
    first_lead = jnp.sqrt(2.0 * order_real + 3.0)
    halves = rows_ref.shape[0]

    def advance(degree, carry):
        previous, older = carry
        degree_real = degree.astype(jnp.float32)
        lead = jnp.sqrt(
            jnp.maximum(4.0 * degree_real * degree_real - 1.0, 0.0)
            / jnp.maximum(degree_real * degree_real - squared, 1.0)
        )
        lower = degree_real - 1.0
        back = jnp.sqrt(
            jnp.maximum(lower * lower - squared, 0.0) / jnp.maximum(4.0 * lower * lower - 1.0, 1.0)
        )
        general = lead * (cosine * previous - back * older)
        first = first_lead * cosine * previous
        value = jnp.where(
            degree_real == order_real,
            diagonal,
            jnp.where(
                degree_real == order_real + 1.0,
                first,
                jnp.where(degree_real > order_real + 1.0, general, 0.0),
            ),
        )
        slot = slot_ref[degree]
        for half in range(halves):
            rows_ref[half, pl.ds(slot, orders, stride=degrees), :] = value[
                :, half * LANES : (half + 1) * LANES
            ]
        return (value, previous)

    zeros = diagonal * 0.0
    lax.fori_loop(0, degrees, advance, (zeros, zeros), unroll=4)
    quadrature = quad_ref[...]
    for order in range(orders):
        for half in range(halves):
            low = half * LANES
            high = min(lats, low + LANES)
            chosen = rows_ref[half, order * degrees : (order + 1) * degrees, :][:, : high - low]
            p_ref[order, :, low:high] = chosen.astype(jnp.bfloat16)
            q_ref[order, :, low:high] = (chosen * quadrature[:, low:high]).astype(jnp.bfloat16)


def spectral_tables(start, ord_dev, degree_of):
    halves = -(-LATS // LANES)
    padded = halves * LANES
    order_col = (start + jnp.arange(ord_dev, dtype=jnp.int32)).astype(jnp.float32)[:, None]
    lat_ids = jnp.minimum(jnp.arange(padded, dtype=jnp.float32), LATS - 1.0)
    colatitude = jnp.pi * (lat_ids + 0.5) / LATS
    sine = jnp.sin(colatitude)[None, :]
    steps_up = jnp.arange(1, DEGREES + 1, dtype=jnp.float32)[None, :]
    factor = jnp.where(
        steps_up <= order_col, 0.5 * jnp.log((2.0 * steps_up + 1.0) / (2.0 * steps_up)), 0.0
    )
    log_start = 0.5 * jnp.log(1.0 / (4.0 * jnp.pi)) + jnp.sum(factor, axis=1, keepdims=True)
    diagonal = jnp.exp(log_start + order_col * jnp.log(sine))
    cosine = jnp.broadcast_to(jnp.cos(colatitude)[None, :], diagonal.shape)
    quadrature = 2.0 * jnp.pi * jnp.pi / LATS * sine
    orders = jnp.broadcast_to(order_col, diagonal.shape)
    vmem = pl.BlockSpec(memory_space=pltpu.VMEM)
    shape = jax.ShapeDtypeStruct((ord_dev, DEGREES, LATS), jnp.bfloat16)
    return pl.pallas_call(
        table_kernel,
        out_shape=(shape, shape),
        in_specs=[pl.BlockSpec(memory_space=pltpu.SMEM)] + [vmem] * 4,
        out_specs=(vmem, vmem),
        scratch_shapes=[
            pltpu.SMEM((DEGREES,), jnp.int32),
            pltpu.VMEM((halves, ord_dev * DEGREES, LANES), jnp.float32),
        ],
        name="legendre_tables",
    )(degree_of, diagonal, cosine, quadrature, orders)


def fourier_tables(lon_count, order_count):
    lon_ids = jnp.arange(lon_count, dtype=jnp.int32)[:, None]
    order_ids = jnp.arange(order_count, dtype=jnp.int32)[None, :]
    phase = 2.0 * jnp.pi * (lon_ids * order_ids % lon_count).astype(jnp.float32) / lon_count
    forward = (
        jnp.stack([jnp.cos(phase), -jnp.sin(phase)], axis=2).reshape(lon_count, 2 * order_count)
        / lon_count
    )
    doubled = jnp.where(order_ids == 0, 1.0, 2.0)
    inverse = jnp.stack([doubled * jnp.cos(phase), -doubled * jnp.sin(phase)], axis=2).reshape(
        lon_count, 2 * order_count
    )
    return (forward.astype(jnp.bfloat16), jnp.transpose(inverse).astype(jnp.bfloat16))


def to_orders(values):
    return lax.all_to_all(values, "lat", split_axis=1, concat_axis=0, tiled=True)


def to_degrees(values):
    return lax.all_to_all(values, "lat", split_axis=0, concat_axis=1, tiled=True)


def back_to_orders(values):
    return lax.all_to_all(values, "lat", split_axis=1, concat_axis=0, tiled=True)


def to_bands(values):
    return lax.all_to_all(values, "lat", split_axis=0, concat_axis=1, tiled=True)


def product(spec, left, right):
    return jnp.einsum(spec, left, right, preferred_element_type=jnp.float32)


def apply_filter(coeffs, weights):
    c_real = coeffs[:, :, 0]
    c_imag = coeffs[:, :, 1]
    w_real = weights[:, 0]
    w_imag = weights[:, 1]
    f_real = product("jmsc,jcd->jmsd", c_real, w_real) - product("jmsc,jcd->jmsd", c_imag, w_imag)
    f_imag = product("jmsc,jcd->jmsd", c_real, w_imag) + product("jmsc,jcd->jmsd", c_imag, w_real)
    return jnp.stack([f_real, f_imag], axis=2).astype(jnp.bfloat16)


def adjoint_filter(grads, weights):
    g_real = grads[:, :, 0]
    g_imag = grads[:, :, 1]
    w_real = weights[:, 0]
    w_imag = weights[:, 1]
    a_real = product("jmsd,jcd->jmsc", g_real, w_real) + product("jmsd,jcd->jmsc", g_imag, w_imag)
    a_imag = product("jmsd,jcd->jmsc", g_imag, w_real) - product("jmsd,jcd->jmsc", g_real, w_imag)
    return jnp.stack([a_real, a_imag], axis=2).astype(jnp.bfloat16)


def filter_grad(coeffs, grads):
    c_real = coeffs[:, :, 0]
    c_imag = coeffs[:, :, 1]
    g_real = grads[:, :, 0]
    g_imag = grads[:, :, 1]
    dw_real = product("jmsc,jmsd->jcd", c_real, g_real) + product("jmsc,jmsd->jcd", c_imag, g_imag)
    dw_imag = product("jmsc,jmsd->jcd", c_real, g_imag) - product("jmsc,jmsd->jcd", c_imag, g_real)
    return jnp.stack([dw_real, dw_imag], axis=1)


def constant_tables():
    sides = 2
    half = LATS // sides
    lat_ids = np.minimum(np.arange(LANES)[None, :], half - 1) + half * np.arange(sides)[:, None]
    colatitude = np.pi * (lat_ids + 0.5) / LATS
    sine = np.sin(colatitude)[:, None, :]
    ids = np.arange(ORDERS)
    steps_up = np.arange(1, ORDERS + 1)
    growth = np.cumsum(0.5 * np.log((2.0 * steps_up + 1.0) / (2.0 * steps_up)))
    log_start = 0.5 * np.log(1.0 / (4.0 * np.pi)) + np.concatenate([[0.0], growth[:-1]])
    diagonal = np.exp(log_start[None, :, None] + ids[None, :, None] * np.log(sine))
    cosine = np.broadcast_to(np.cos(colatitude)[:, None, :], (sides, GROUP, LANES))
    quadrature = np.broadcast_to(2.0 * np.pi * np.pi / LATS * sine, (sides, GROUP, LANES))
    phase = 2.0 * np.pi * (np.arange(LONS)[:, None] * ids[None, :] % LONS) / LONS
    forward = np.stack([np.cos(phase), -np.sin(phase)], axis=2).reshape(LONS, -1) / LONS
    doubled = np.where(ids == 0, 1.0, 2.0)[None, :]
    inverse = np.stack([doubled * np.cos(phase), -doubled * np.sin(phase)], axis=2)
    inverse = inverse.reshape(LONS, -1)
    floats = [jnp.asarray(t, jnp.float32) for t in (diagonal, cosine, quadrature)]
    waves = [forward.T, forward, inverse.T, inverse]
    halves = [jnp.asarray(np.float32(t).astype(jnp.bfloat16)) for t in waves]
    return floats, halves


def fill_tables(side, firsts, deg_ref, diag_ref, cos_ref, quad_ref, qtab, ptab, table, by_slot):
    kinds, orders, degrees, lats = qtab.shape
    every = kinds * orders
    cosine = cos_ref[side]
    diagonal, ids, squared, first_lead = [], [], [], []
    for first in firsts:
        diagonal.append(diag_ref[side, pl.ds(pl.multiple_of(first, orders), orders), :])
        ids.append(first + lax.broadcasted_iota(jnp.int32, cosine.shape, 0))
        real = ids[-1].astype(jnp.float32)
        squared.append(real * real)
        first_lead.append(jnp.sqrt(2.0 * real + 3.0))

    def advance(degree, carry):
        degree_real = degree.astype(jnp.float32)
        lower = degree_real - 1.0
        state = []
        for kind in range(kinds):
            previous, older = carry[kind]
            lead = jnp.sqrt(
                jnp.maximum(4.0 * degree_real * degree_real - 1.0, 0.0)
                / jnp.maximum(degree_real * degree_real - squared[kind], 1.0)
            )
            back = jnp.sqrt(
                jnp.maximum(lower * lower - squared[kind], 0.0)
                / jnp.maximum(4.0 * lower * lower - 1.0, 1.0)
            )
            general = lead * (cosine * previous - back * older)
            first = first_lead[kind] * cosine * previous
            value = jnp.where(
                ids[kind] == degree,
                diagonal[kind],
                jnp.where(
                    ids[kind] + 1 == degree,
                    first,
                    jnp.where(ids[kind] + 1 < degree, general, 0.0),
                ),
            )
            table[degree, kind * orders : (kind + 1) * orders, :] = value
            state.append((value, previous))
        return tuple(state)

    zeros = cosine * 0.0
    lax.fori_loop(0, degrees, advance, ((zeros, zeros),) * kinds, unroll=2)

    ahead = every // 2
    tail = degrees // 2

    def place(slot, carry):
        by_slot[pl.ds(slot, ahead, stride=degrees), :] = table[deg_ref[slot], :ahead]
        return carry

    lax.fori_loop(0, degrees, place, 0, unroll=4)

    def place_tail(row, carry):
        spots = pl.ds(ahead * degrees + row, ahead, stride=degrees)
        by_slot[spots, :] = table[tail + row, ahead:]
        return carry

    lax.fori_loop(0, tail, place_tail, 0, unroll=4)
    quadrature = quad_ref[side][:1, :lats]
    for kind in range(kinds):

        def keep(order, carry):
            start = pl.multiple_of((kind * orders + order) * degrees, degrees)
            depth = degrees if kind < kinds // 2 else tail
            chosen = by_slot[pl.ds(start, depth), :][:, :lats]
            ptab[kind, order, :depth] = chosen.astype(jnp.bfloat16)
            qtab[kind, order, :depth] = (chosen * quadrature).astype(jnp.bfloat16)
            return carry

        lax.fori_loop(0, orders, keep, 0)


def pair_swap(values, even_sign):
    rows = values.shape[0]
    even = lax.broadcasted_iota(jnp.int32, values.shape, 0) % 2 == 0
    above = pltpu.roll(values, rows - 1, 0)
    below = pltpu.roll(values, 1, 0)
    return jnp.where(even, even_sign * above, -even_sign * below)


def gelu_slope(x):
    scale = 0.7978845608028654
    square = x * x
    t = jnp.tanh(scale * (x + 0.044715 * x * square))
    return 0.5 * (1.0 + t) + 0.5 * x * (1.0 - t * t) * (scale * (1.0 + 0.134145 * square))


def dot(left, right, dims=((1,), (0,))):
    return lax.dot_general(left, right, (dims, ((), ())), preferred_element_type=jnp.float32)


def block_kernel(
    n, nb, fields, cotangent, weights, deg_ref, diag_ref, cos_ref, quad_ref,
    fwd_fk, fwd_kf, inv_fk, inv_kf,
    grad_out, dw,
    fbuf, wbuf, band_out, band_in, ord_in, ord_out, cross_out, cross_in, slot_out, slot_all,
    tail_out, co, go, mixed, wide_a, wide_b, wide_c, dw_in, qtab, ptab, table, row_ref, slot_of, by_name,
    load_sem, send_sem, recv_sem, dw_send, dw_recv,
):
    me = lax.axis_index("lat")
    me_b = lax.axis_index("batch")
    chunks, lat_dev = fbuf.shape[0], fbuf.shape[1]
    kinds, orders, degrees, side_lats = qtab.shape
    rows = 2 * orders
    slots = co.shape[1]
    quarter = n // kinds
    half = n // 2
    own = half * slots
    inner_kinds = ord_in.shape[0]
    pairs = kinds // 2
    jobs = kinds * chunks
    plane_rows = quarter * rows
    mesh_id = pl.DeviceIdType.MESH
    side = lax.div(me, half)
    place_in = lax.rem(me, half)
    column = lax.rem(me, quarter)
    inner = jnp.where(lax.div(me, quarter) == 1 + side, 1, 0)
    across = 1 - side

    def lanes(chunk):
        return pl.ds(chunk * LANES, LANES)

    def group(kind, at):
        return jnp.where(
            lax.rem(kind, 2) == 0, kind * quarter + at, (kind + 1) * quarter - 1 - at
        )

    def group_rows(kind, at):
        return pl.ds(pl.multiple_of(group(kind, at) * rows, rows), rows)

    def owner(kind, on_side, at):
        plane = jnp.where(kind < inner_kinds, 1 + on_side, (kinds - 1) * on_side)
        return plane * quarter + at

    def mine(kind):
        return jnp.where(kind < inner_kinds, 1, 0) == inner

    def job_of(job):
        per_pass = pairs * chunks
        inside = lax.rem(job, per_pass)
        kind = lax.div(job, per_pass) * pairs + lax.rem(inside, pairs)
        return kind, lax.div(inside, pairs), lax.rem(kind, inner_kinds)

    def first_block(kind):
        return group(kind, column) - own // orders

    def tail_blocks(kind, body):
        def one(block, carry):
            body(pl.multiple_of(block * orders, orders))
            return carry

        lax.fori_loop(first_block(kind), own // orders, one, 0)

    def await_tail(kind, view, sem):
        for first in range(own // orders):

            @pl.when(first_block(kind) == first)
            def _():
                await_bytes(view.at[pl.ds(0, own - first * orders)], sem)

    def job_at(kind, chunk):
        return (kind // pairs) * (pairs * chunks) + chunk * pairs + kind % pairs

    def load(chunk):
        return pltpu.make_async_copy(
            fields.at[0, :, :, lanes(chunk)], fbuf.at[chunk], load_sem.at[chunk]
        )

    def load_cot(chunk):
        return pltpu.make_async_copy(
            cotangent.at[0, :, :, lanes(chunk)],
            grad_out.at[0, :, :, lanes(chunk)],
            load_sem.at[chunks + chunk],
        )

    load_w = pltpu.make_async_copy(weights, wbuf, load_sem.at[2 * chunks])
    for chunk in range(chunks):
        load(chunk).start()
    load_w.start()
    for chunk in range(chunks):
        load_cot(chunk).start()

    barrier = pltpu.get_barrier_semaphore()

    def greet(step, carry):
        peer = lax.rem(me + step, n)
        pl.semaphore_signal(barrier, inc=1, device_id={"lat": peer}, device_id_type=mesh_id)
        return carry

    lax.fori_loop(1, n, greet, 0)
    for step in range(1, nb):
        peer = lax.rem(me_b + step, nb)
        pl.semaphore_signal(barrier, inc=1, device_id={"batch": peer}, device_id_type=mesh_id)

    def remote(stage, job, source, target, peer):
        pltpu.make_async_remote_copy(
            src_ref=source,
            dst_ref=target,
            send_sem=send_sem.at[stage, job],
            recv_sem=recv_sem.at[stage, job],
            device_id={"lat": peer},
            device_id_type=mesh_id,
        ).start()

    def await_bytes(view, sem):
        pltpu.make_async_copy(view, view, sem).wait()

    def to_owners(stage, kind, chunk, source, target, width):
        job = job_at(kind, chunk)
        for step in range(quarter):
            at = lax.rem(column + step, quarter)
            view = source.at[chunk, :, group_rows(kind, at), :]
            spot = target(kind % inner_kinds, chunk)
            peer = owner(kind, side, at)

            @pl.when(peer != me)
            def _():
                remote(stage, job, view, spot, peer)

            @pl.when(peer == me)
            def _():
                pltpu.make_async_copy(view, spot, recv_sem.at[stage, job]).start()

    def left_for_owners(stage, kind, chunk, source):
        job = job_at(kind, chunk)

        @pl.when(mine(kind))
        def _():
            await_bytes(source.at[chunk, :, 0 : plane_rows - rows, :], send_sem.at[stage, job])

        @pl.when(jnp.logical_not(mine(kind)))
        def _():
            await_bytes(source.at[chunk, :, 0:plane_rows, :], send_sem.at[stage, job])

    def from_owner(stage, job, kind, chunk, source, depth, target):
        place = lax.rem(kind, inner_kinds)
        spot = target.at[chunk, :, group_rows(kind, column), :]

        def send(step, carry):
            at = lax.rem(place_in + step, half)
            remote(
                stage, job, source.at[place, chunk, pl.ds(at * depth, depth)], spot,
                side * half + at,
            )
            return carry

        lax.fori_loop(1, half, send, 0)
        pltpu.make_async_copy(
            source.at[place, chunk, pl.ds(place_in * depth, depth)], spot, recv_sem.at[stage, job]
        ).start()

    def left_owner(stage, job, kind, chunk, source, depth):
        view = source.at[lax.rem(kind, inner_kinds), chunk, 0 : (half - 1) * depth]
        await_bytes(view, send_sem.at[stage, job])

    def reached_all(stage, kind, chunk, target):
        await_bytes(target.at[chunk, :, 0:plane_rows, :], recv_sem.at[stage, job_at(kind, chunk)])

    def lat_spot(place, chunk):
        return ord_in.at[place, chunk, pl.ds(place_in * lat_dev, lat_dev)]

    def slot_spot(place, chunk):
        return slot_all.at[place, chunk, pl.ds(me * slots, slots)]

    def wide_start(part, job):
        if part:
            spot = lax.rem(lax.div(job - pairs * chunks, pairs) + pairs, chunks)
        else:
            spot = jnp.where(job < 2 * pairs, lax.rem(job, pairs), job - pairs)
        return pl.multiple_of(spot * wide_a.shape[0], 8)

    def widen(source, place, chunk, depth, count):
        def one(block, carry):
            piece = source[place, chunk, pl.ds(block * depth, depth)].astype(jnp.float32)
            wide_a[pl.ds(pl.multiple_of(block * depth * rows, depth * rows), depth * rows), :] = (
                piece.reshape(depth * rows, LANES)
            )
            return carry

        lax.fori_loop(0, count // depth, one, 0)

    def apply_table(tab, kind, kept, result_ref, start, depth_in, depth_out, dims):
        def one(order, carry):
            real = wide_a[pl.ds(2 * order, depth_in, stride=rows), :]
            imag = wide_a[pl.ds(2 * order + 1, depth_in, stride=rows), :]
            both = jnp.concatenate([real, imag], axis=1).astype(jnp.bfloat16)
            result = dot(tab[kind, order, :kept], both, dims)
            result_ref[pl.ds(start + 2 * order, depth_out, stride=rows), :] = result[:, :LANES]
            result_ref[pl.ds(start + 2 * order + 1, depth_out, stride=rows), :] = result[:, LANES:]
            return carry

        lax.fori_loop(0, orders, one, 0, unroll=4)

    def narrow(source, target, place, chunk, start, depth, count):
        def one(block, carry):
            low = pl.multiple_of(start + block * depth * rows, 8)
            piece = source[pl.ds(low, depth * rows), :]
            target[place, chunk, pl.ds(block * depth, depth)] = piece.reshape(
                depth, rows, LANES
            ).astype(jnp.bfloat16)
            return carry

        lax.fori_loop(0, count // depth, one, 0)

    def wide_rows(start, index, depth):
        return pl.ds(pl.multiple_of(start + index * rows, 8), depth * rows)

    def blank(first, count):
        def one(block, carry):
            by_name[pl.ds((first + block) * orders, orders)] = jnp.zeros(
                (orders, rows, LANES), jnp.bfloat16
            )
            return carry

        lax.fori_loop(0, count, one, 0)

    def analyse(base, tab, part, job):
        kind, chunk, place = job_of(job)

        @pl.when(mine(kind))
        def _():
            await_bytes(ord_in.at[place, chunk], recv_sem.at[base, job])
            widen(ord_in, place, chunk, lat_dev, side_lats)
            start = wide_start(part, job)
            peer = owner(kind, across, column)
            source = cross_out.at[place, chunk]
            target = cross_in.at[place, chunk]
            kept = own if part else degrees
            apply_table(tab, kind, kept, wide_b, start, side_lats, kept, ((1,), (0,)))
            if not part:
                if base:
                    await_bytes(source, send_sem.at[1, job])
                narrow(wide_b, cross_out, place, chunk, start + across * own * rows, slots, own)
                remote(base + 1, job, source, target, peer)
                return
            if base:
                await_tail(kind, source, send_sem.at[1, job])

            def send(low):
                span = pl.ds(low, orders)
                piece = wide_b[wide_rows(start, low, orders), :]
                cross_out[place, chunk, span] = piece.reshape(orders, rows, LANES).astype(
                    jnp.bfloat16
                )
                remote(base + 1, job, source.at[span], target.at[span], peer)

            tail_blocks(kind, send)

    def settle(base, target, part, job):
        kind, chunk, place = job_of(job)

        @pl.when(mine(kind))
        def _():
            start = wide_start(part, job)
            if part:
                await_tail(kind, cross_in.at[place, chunk], recv_sem.at[base + 1, job])
            else:
                await_bytes(cross_in.at[place, chunk], recv_sem.at[base + 1, job])
            if base:
                left_owner(2, job, kind, chunk, slot_out, slots)
                if part:
                    await_tail(kind, tail_out.at[chunk], send_sem.at[4, job])
                else:
                    await_bytes(slot_all.at[place, chunk, 0:own], send_sem.at[4, job])
            if part:

                blank(0, own // orders + first_block(kind))

                def add(low):
                    piece = wide_b[wide_rows(start, low, orders), :]
                    other = cross_in[place, chunk, pl.ds(low, orders)].astype(jnp.float32)
                    by_name[pl.ds(own + low, orders)] = (
                        piece.reshape(orders, rows, LANES) + other
                    ).astype(jnp.bfloat16)

                tail_blocks(kind, add)

                def pick(slot, carry):
                    slot_out[place, chunk, slot] = by_name[deg_ref[side * own + slot]]
                    return carry

                lax.fori_loop(0, own, pick, 0, unroll=4)
            else:

                def one(block, carry):
                    low = block * slots
                    piece = wide_b[wide_rows(start + side * own * rows, low, slots), :]
                    other = cross_in[place, chunk, pl.ds(low, slots)].astype(jnp.float32)
                    slot_out[place, chunk, pl.ds(low, slots)] = (
                        piece.reshape(slots, rows, LANES) + other
                    ).astype(jnp.bfloat16)
                    return carry

                lax.fori_loop(0, half, one, 0)
            from_owner(base + 2, job, kind, chunk, slot_out, slots, target)

    def relay(base, part, job):
        kind, chunk, place = job_of(job)

        @pl.when(mine(kind))
        def _():
            await_bytes(slot_all.at[place, chunk, 0:own], recv_sem.at[base + 3, job])
            peer = owner(kind, across, column)
            view = slot_all.at[place, chunk, pl.ds(side * own, own)]
            if not part:
                remote(base + 4, job, view, view, peer)
                return

            blank(across * (own // orders), own // orders)

            def copy(block, carry):
                span = pl.ds(side * own + block * slots, slots)
                by_name[span] = slot_all[place, chunk, span]
                return carry

            lax.fori_loop(0, half, copy, 0)

            def send(low):
                for step in range(orders):
                    tail_out[chunk, low + step] = by_name[slot_of[0, own + low + step]]
                span = pl.ds(low, orders)
                remote(base + 4, job, tail_out.at[chunk, span], view.at[span], peer)

            tail_blocks(kind, send)

    def synthesise(base, tab, part, job):
        kind, chunk, place = job_of(job)

        @pl.when(mine(kind))
        def _():
            if part:
                await_tail(kind, tail_out.at[chunk], recv_sem.at[base + 4, job])

                def clear(block, carry):
                    wide_a[wide_rows(0, block * orders, orders), :] = jnp.zeros(
                        (orders * rows, LANES), jnp.float32
                    )
                    return carry

                lax.fori_loop(0, first_block(kind), clear, 0)

                def add(low):
                    near = tail_out[chunk, pl.ds(low, orders)].astype(jnp.float32)
                    far = slot_all[place, chunk, pl.ds(across * own + low, orders)]
                    wide_a[wide_rows(0, low, orders), :] = (
                        near + far.astype(jnp.float32)
                    ).reshape(orders * rows, LANES)

                tail_blocks(kind, add)
                apply_table(tab, kind, own, wide_c, 0, own, side_lats, ((0,), (0,)))
            else:
                await_bytes(slot_all.at[place, chunk, 0:own], recv_sem.at[base + 4, job])
                widen(slot_all, place, chunk, slots, degrees)
                apply_table(tab, kind, degrees, wide_c, 0, degrees, side_lats, ((0,), (0,)))
            if base:
                left_owner(5, job, kind, chunk, ord_out, lat_dev)
            narrow(wide_c, ord_out, place, chunk, 0, lat_dev, side_lats)
            from_owner(base + 5, job, kind, chunk, ord_out, lat_dev, band_in)

    def loop(low, high, body):
        def one(job, carry):
            body(job)
            return carry

        lax.fori_loop(low, high, one, 0)

    def pair(source, chunk, row):
        return jnp.concatenate([source[chunk, 2 * row], source[chunk, 2 * row + 1]], axis=1)

    def field_pair(chunk, row):
        span = slice(chunk * LANES, (chunk + 1) * LANES)
        return jnp.concatenate(
            [grad_out[0, 2 * row, :, span], grad_out[0, 2 * row + 1, :, span]], axis=1
        )

    def put_field_pair(chunk, row, values):
        span = slice(chunk * LANES, (chunk + 1) * LANES)
        values = values.astype(jnp.bfloat16)
        grad_out[0, 2 * row, :, span] = values[:, :LANES]
        grad_out[0, 2 * row + 1, :, span] = values[:, LANES:]

    def put_pair(target, chunk, row, values):
        values = values.astype(jnp.bfloat16)
        target[chunk, 2 * row] = values[:, :LANES]
        target[chunk, 2 * row + 1] = values[:, LANES:]

    def joined(source, slot, span):
        return jnp.concatenate([source[chunk, slot, span] for chunk in range(chunks)], axis=1)

    def mix(part, chunk):
        low = part * pairs * plane_rows
        span = slice(low, low + pairs * plane_rows)
        columns = slice(chunk * LANES, (chunk + 1) * LANES)

        def one(slot, carry):
            both = dot(
                joined(co, slot, span),
                jnp.concatenate([wbuf[slot, 0, :, columns], wbuf[slot, 1, :, columns]], axis=1),
            )
            crossed = pair_swap(both[:, LANES:], -1.0)
            mixed[chunk, slot, span] = (both[:, :LANES] + crossed).astype(jnp.bfloat16)
            return carry

        return one

    def adjoint(part, chunk):
        low = part * pairs * plane_rows
        span = slice(low, low + pairs * plane_rows)
        columns = slice(chunk * LANES, (chunk + 1) * LANES)

        def one(slot, carry):
            both = dot(
                joined(go, slot, span),
                jnp.concatenate([wbuf[slot, 0, columns, :], wbuf[slot, 1, columns, :]], axis=0),
                ((1,), (1,)),
            )
            crossed = pair_swap(both[:, LANES:], 1.0)
            mixed[chunk, slot, span] = (both[:, :LANES] + crossed).astype(jnp.bfloat16)
            return carry

        return one

    def filter_part(base, part, source, make):
        part_kinds = range(part * pairs, (part + 1) * pairs)
        for chunk in range(chunks):
            for kind in part_kinds:
                reached_all(base + 2, kind, chunk, source)
        for chunk in range(chunks):
            if base:
                for kind in part_kinds:
                    left_for_owners(3, kind, chunk, mixed)
            lax.fori_loop(0, slots, make(part, chunk), 0, unroll=4)
            for kind in part_kinds:
                to_owners(base + 3, kind, chunk, mixed, slot_spot, slots)

    per_pass = pairs * chunks
    def unit(part, chunk):
        first = part * per_pass + chunk * pairs
        return first, first + pairs

    def run(spans, body):
        loop(spans[0], spans[1], body)

    def to_filter_start(base, tab, source):
        run(unit(0, 0), lambda job: analyse(base, tab, 0, job))
        for low, high, part, behind in (
            (pairs, per_pass, 0, 0),
            (per_pass, per_pass + pairs, 1, 0),
            (per_pass + pairs, per_pass + 2 * pairs, 1, 1),
        ):

            def step(job):
                settle(base, source, behind, job - pairs)
                analyse(base, tab, part, job)

            loop(low, high, step)
        loop(per_pass + 2 * pairs, jobs, lambda job: analyse(base, tab, 1, job))

    def to_filter_by_chunk(base, tab, source, rest):
        run(unit(0, 0), lambda job: analyse(base, tab, 0, job))
        run(unit(1, 0), lambda job: analyse(base, tab, 1, job))
        rest()

        def second(job):
            settle(base, source, 0, job - pairs)
            analyse(base, tab, 0, job)

        run(unit(0, 1), second)
        run(unit(1, 0), lambda job: settle(base, source, 1, job))
        run(unit(0, 2), lambda job: analyse(base, tab, 0, job))

        for job in range(pairs, 2 * pairs):
            settle(base, source, 0, job)
            run(unit(1, job - pairs + 1), lambda spot: analyse(base, tab, 1, spot))
        run(unit(0, 2), lambda job: settle(base, source, 0, job))

    def through_filter(base, tab, source, make):
        filter_part(base, 0, source, make)
        run(unit(1, 1), lambda job: settle(base, source, 1, job))
        run(unit(0, 0), lambda job: relay(base, 0, job))
        run(unit(1, 2), lambda job: settle(base, source, 1, job))
        run(unit(0, 1), lambda job: relay(base, 0, job))
        run(unit(0, 0), lambda job: synthesise(base, tab, 0, job))
        loop(pairs, pairs + 1, lambda job: synthesise(base, tab, 0, job))
        filter_part(base, 1, source, make)
        loop(pairs + 1, 2 * pairs, lambda job: synthesise(base, tab, 0, job))
        run(unit(1, 0), lambda job: relay(base, 1, job))
        run(unit(0, 2), lambda job: relay(base, 0, job))
        run(unit(1, 1), lambda job: relay(base, 1, job))

    def spread(stage, chunk, part):
        for kind in range(part * pairs, (part + 1) * pairs):
            to_owners(stage, kind, chunk, band_out, lat_spot, lat_dev)

    def transform(chunk):
        load(chunk).wait()

        def fourier(row, carry):
            put_pair(band_out, chunk, row, dot(fwd_fk[...], pair(fbuf, chunk, row)))
            return carry

        lax.fori_loop(0, lat_dev // 2, fourier, 0, unroll=3)

    transform(0)
    pl.semaphore_wait(barrier, n - 1 + nb - 1)
    spread(0, 0, 0)
    transform(1)
    spread(0, 1, 0)
    fill_tables(
        side, [group(kind, column) * orders for kind in range(kinds)], deg_ref, diag_ref, cos_ref,
        quad_ref, qtab, ptab, table, wide_b,
    )
    for chunk in range(2, chunks):
        transform(chunk)
        spread(0, chunk, 0)
    for chunk in range(chunks):
        spread(0, chunk, 1)
    spots = lax.broadcasted_iota(jnp.int32, row_ref.shape, 1)

    def invert(slot, carry):
        return jnp.where(spots == deg_ref[slot], slot, carry)

    row_ref[...] = lax.fori_loop(0, degrees, invert, spots * 0, unroll=4)
    turn = pltpu.make_async_copy(row_ref, slot_of, load_sem.at[2 * chunks + 1])
    turn.start()
    turn.wait()
    load_w.wait()
    to_filter_start(0, qtab, co)
    through_filter(0, ptab, co, mix)

    def between(chunk):
        load_cot(chunk).wait()
        for kind in range(kinds):
            reached_all(5, kind, chunk, band_in)
            left_for_owners(0, kind, chunk, band_out)

        def middle(row, carry):
            response = dot(inv_kf[...], pair(band_in, chunk, row))
            upstream = field_pair(chunk, row).astype(jnp.float32) * gelu_slope(response)
            put_pair(band_out, chunk, row, dot(inv_fk[...], upstream.astype(jnp.bfloat16)))
            return carry

        lax.fori_loop(0, lat_dev // 2, middle, 0, unroll=3)
        spread(6, chunk, 0)
        if chunk == 0:
            spread(6, 0, 1)
        if chunk == chunks - 1:
            for earlier in range(1, chunks):
                spread(6, earlier, 1)

    def finish_synthesis(base, tab, finish):
        first, second = unit(0, 2)
        run(unit(1, 0), lambda job: synthesise(base, tab, 1, job))
        loop(first, first + 1, lambda job: synthesise(base, tab, 0, job))
        run(unit(1, 2), lambda job: relay(base, 1, job))
        if not base:
            finish(0)
        loop(first + 1, second, lambda job: synthesise(base, tab, 0, job))
        loop(per_pass + pairs, jobs, lambda job: synthesise(base, tab, 1, job))
        if base:
            finish(0)

    def rest(finish):
        for chunk in range(1, chunks):
            finish(chunk)

    finish_synthesis(0, ptab, between)
    to_filter_by_chunk(6, ptab, go, lambda: rest(between))
    through_filter(6, qtab, go, adjoint)

    def weight_grad(slot, carry):
        values = joined(co, slot, slice(None))
        grads = joined(go, slot, slice(None))
        turned = pair_swap(grads.astype(jnp.float32), 1.0).astype(jnp.bfloat16)
        span = ((0,), (0,))
        dw[slot, 0] = dot(values, grads, span).astype(jnp.bfloat16)
        dw[slot, 1] = dot(values, turned, span).astype(jnp.bfloat16)
        return carry

    lax.fori_loop(0, slots, weight_grad, 0)
    dw_copies = []
    for step in range(1, nb):
        peer = lax.rem(me_b + step, nb)
        copy = pltpu.make_async_remote_copy(
            src_ref=dw,
            dst_ref=dw_in.at[step - 1],
            send_sem=dw_send.at[step - 1],
            recv_sem=dw_recv.at[step - 1],
            device_id={"batch": peer},
            device_id_type=mesh_id,
        )
        copy.start()
        dw_copies.append(copy)

    def total(slot, carry):
        value = dw[slot].astype(jnp.float32)
        for step in range(nb - 1):
            value = value + dw_in[step, slot].astype(jnp.float32)
        dw[slot] = value.astype(jnp.bfloat16)
        return carry

    def last(chunk):
        if chunk == 0:
            for copy in dw_copies:
                copy.wait()
            lax.fori_loop(0, slots, total, 0)
        for kind in range(kinds):
            reached_all(11, kind, chunk, band_in)

        def finish(row, carry):
            delta = dot(fwd_kf[...], pair(band_in, chunk, row))
            put_field_pair(chunk, row, field_pair(chunk, row).astype(jnp.float32) + delta)
            return carry

        lax.fori_loop(0, lat_dev // 2, finish, 0, unroll=3)

    finish_synthesis(6, qtab, last)
    rest(last)
    for chunk in range(chunks):
        for kind in range(kinds):
            left_for_owners(6, kind, chunk, band_out)
            left_for_owners(9, kind, chunk, mixed)

    def drain(part, job):
        kind, chunk, place = job_of(job)

        @pl.when(mine(kind))
        def _():
            if part:
                await_tail(kind, cross_out.at[place, chunk], send_sem.at[7, job])
                await_tail(kind, tail_out.at[chunk], send_sem.at[10, job])
            else:
                await_bytes(cross_out.at[place, chunk], send_sem.at[7, job])
                await_bytes(slot_all.at[place, chunk, 0:own], send_sem.at[10, job])
            left_owner(8, job, kind, chunk, slot_out, slots)
            left_owner(11, job, kind, chunk, ord_out, lat_dev)

    loop(0, per_pass, lambda job: drain(0, job))
    loop(per_pass, jobs, lambda job: drain(1, job))


def local_kernel(fields, cotangent, weights, degree_of):
    n = lax.axis_size("lat")
    nb = lax.axis_size("batch")
    kinds = 4
    if fields.shape[0] != 1 or fields.shape[1] % 2 or n % kinds or ORDERS != n * GROUP:
        return local(fields, cotangent, weights, degree_of)
    lat_dev, lons, channels = fields.shape[1:]
    slots = weights.shape[0]
    rows = 2 * GROUP
    chunks = channels // LANES
    floats, waves = constant_tables()
    side_lats = LATS // 2
    held = kinds - 1
    vmem = pl.BlockSpec(memory_space=pltpu.VMEM)
    anywhere = pl.BlockSpec(memory_space=pl.ANY)

    def buffer(*dims):
        return pltpu.VMEM(dims, jnp.bfloat16)

    dma = pltpu.SemaphoreType.DMA
    others = max(nb - 1, 1)
    wide_rows = max(side_lats, DEGREES) * rows
    return pl.pallas_call(
        functools.partial(block_kernel, n, nb),
        out_shape=(
            pltpu.VMEM(fields.shape, jnp.bfloat16),
            pltpu.VMEM(weights.shape, jnp.bfloat16),
        ),
        in_specs=[anywhere] * 3 + [pl.BlockSpec(memory_space=pltpu.SMEM)] + [vmem] * 7,
        out_specs=(vmem, vmem),
        scratch_shapes=[
            buffer(chunks, lat_dev, lons, LANES),
            buffer(*weights.shape),
            buffer(chunks, lat_dev, n * rows, LANES),
            buffer(chunks, lat_dev, n * rows, LANES),
            buffer(held, chunks, side_lats, rows, LANES),
            buffer(held, chunks, side_lats, rows, LANES),
            buffer(held, chunks, DEGREES // 2, rows, LANES),
            buffer(held, chunks, DEGREES // 2, rows, LANES),
            buffer(held, chunks, DEGREES // 2, rows, LANES),
            buffer(held, chunks, DEGREES, rows, LANES),
            buffer(chunks, DEGREES // 2, rows, LANES),
            buffer(chunks, slots, n * rows, LANES),
            buffer(chunks, slots, n * rows, LANES),
            buffer(chunks, slots, n * rows, LANES),
            pltpu.VMEM((wide_rows, LANES), jnp.float32),
            pltpu.VMEM((4 * wide_rows, LANES), jnp.float32),
            pltpu.VMEM((side_lats * rows, LANES), jnp.float32),
            buffer(others, *weights.shape),
            buffer(kinds, GROUP, DEGREES, side_lats),
            buffer(kinds, GROUP, DEGREES, side_lats),
            pltpu.VMEM((DEGREES, kinds * GROUP, LANES), jnp.float32),
            pltpu.VMEM((GROUP, DEGREES), jnp.int32),
            pltpu.SMEM((GROUP, DEGREES), jnp.int32),
            buffer(DEGREES, rows, LANES),
            dma((2 * chunks + 2,)),
            dma((12, kinds * chunks)),
            dma((12, kinds * chunks)),
            dma((others,)),
            dma((others,)),
        ],
        compiler_params=pltpu.CompilerParams(
            collective_id=0, has_side_effects=True, vmem_limit_bytes=54 * 2**20
        ),
        name="filter_block",
    )(
        fields, cotangent, weights, degree_of, *floats, *waves,
    )


def local(fields, cotangent, weights, degree_of):
    samples = fields.shape[0]
    band_rows = fields.shape[1]
    ord_dev = ORDERS // lax.axis_size("lat")
    forward, inverse = fourier_tables(LONS, ORDERS)
    qslot, pslot = spectral_tables(lax.axis_index("lat") * ord_dev, ord_dev, degree_of)
    spectra = product("sikc,kf->ifsc", fields, forward).astype(jnp.bfloat16)
    spectra = spectra.reshape(band_rows, ORDERS, 2, samples, CHANNELS)
    gathered = to_orders(spectra)
    coeffs_local = product("mji,imrsc->jmrsc", qslot, gathered).astype(jnp.bfloat16)
    coeffs = to_degrees(coeffs_local)
    filtered = apply_filter(coeffs, weights)
    returned = back_to_orders(filtered)
    synth_local = product("mji,jmrsc->imrsc", pslot, returned).astype(jnp.bfloat16)
    synth = to_bands(synth_local)
    response = product(
        "ifsc,fk->sikc", synth.reshape(band_rows, 2 * ORDERS, samples, CHANNELS), inverse
    )
    activated, pullback = jax.vjp(jax.nn.gelu, response)
    upstream = pullback(cotangent.astype(jnp.float32))[0].astype(jnp.bfloat16)
    grad_synth = product("sikc,fk->ifsc", upstream, inverse).astype(jnp.bfloat16)
    grad_synth = grad_synth.reshape(band_rows, ORDERS, 2, samples, CHANNELS)
    grad_gathered = to_orders(grad_synth)
    grad_local = product("mji,imrsc->jmrsc", pslot, grad_gathered).astype(jnp.bfloat16)
    grad_filtered = to_degrees(grad_local)
    weight_total = lax.psum(filter_grad(coeffs, grad_filtered).astype(jnp.bfloat16), "batch")
    grad_coeffs = adjoint_filter(grad_filtered, weights)
    grad_back = back_to_orders(grad_coeffs)
    grad_local_spec = product("mji,jmrsc->imrsc", qslot, grad_back).astype(jnp.bfloat16)
    grad_bands = to_bands(grad_local_spec)
    delta = product(
        "ifsc,kf->sikc", grad_bands.reshape(band_rows, 2 * ORDERS, samples, CHANNELS), forward
    )
    grad_fields = (cotangent.astype(jnp.float32) + delta).astype(jnp.bfloat16)
    return (grad_fields, weight_total)


def solution(mesh):
    return jax.shard_map(
        local_kernel if CHANNELS % LANES == 0 else local,
        mesh=mesh,
        in_specs=(
            P("batch", "lat", None, None),
            P("batch", "lat", None, None),
            P("lat", None, None, None),
            P(),
        ),
        out_specs=(P("batch", "lat", None, None), P("lat", None, None, None)),
        check_vma=False,
    )
```

```python
import functools

import jax
import numpy as np
import jax.numpy as jnp
from jax import lax
from jax.experimental import pallas as pl
from jax.experimental.pallas import tpu as pltpu
from jax.sharding import PartitionSpec as P

LATS = 192
LONS = 384
ORDERS = 128
DEGREES = 128
CHANNELS = 384
LANES = 128
GROUP = 8


def table_kernel(deg_ref, diag_ref, cos_ref, quad_ref, order_ref, q_ref, p_ref, slot_ref, rows_ref):
    orders = diag_ref.shape[0]
    lats = q_ref.shape[2]
    degrees = deg_ref.shape[0]

    def invert(slot, carry):
        slot_ref[deg_ref[slot]] = slot
        return carry

    lax.fori_loop(0, degrees, invert, 0)
    order_real = order_ref[...]
    squared = order_real * order_real
    diagonal = diag_ref[...]
    cosine = cos_ref[...]
    first_lead = jnp.sqrt(2.0 * order_real + 3.0)
    halves = rows_ref.shape[0]

    def advance(degree, carry):
        previous, older = carry
        degree_real = degree.astype(jnp.float32)
        lead = jnp.sqrt(
            jnp.maximum(4.0 * degree_real * degree_real - 1.0, 0.0)
            / jnp.maximum(degree_real * degree_real - squared, 1.0)
        )
        lower = degree_real - 1.0
        back = jnp.sqrt(
            jnp.maximum(lower * lower - squared, 0.0) / jnp.maximum(4.0 * lower * lower - 1.0, 1.0)
        )
        general = lead * (cosine * previous - back * older)
        first = first_lead * cosine * previous
        value = jnp.where(
            degree_real == order_real,
            diagonal,
            jnp.where(
                degree_real == order_real + 1.0,
                first,
                jnp.where(degree_real > order_real + 1.0, general, 0.0),
            ),
        )
        slot = slot_ref[degree]
        for half in range(halves):
            rows_ref[half, pl.ds(slot, orders, stride=degrees), :] = value[
                :, half * LANES : (half + 1) * LANES
            ]
        return (value, previous)

    zeros = diagonal * 0.0
    lax.fori_loop(0, degrees, advance, (zeros, zeros), unroll=4)
    quadrature = quad_ref[...]
    for order in range(orders):
        for half in range(halves):
            low = half * LANES
            high = min(lats, low + LANES)
            chosen = rows_ref[half, order * degrees : (order + 1) * degrees, :][:, : high - low]
            p_ref[order, :, low:high] = chosen.astype(jnp.bfloat16)
            q_ref[order, :, low:high] = (chosen * quadrature[:, low:high]).astype(jnp.bfloat16)


def spectral_tables(start, ord_dev, degree_of):
    halves = -(-LATS // LANES)
    padded = halves * LANES
    order_col = (start + jnp.arange(ord_dev, dtype=jnp.int32)).astype(jnp.float32)[:, None]
    lat_ids = jnp.minimum(jnp.arange(padded, dtype=jnp.float32), LATS - 1.0)
    colatitude = jnp.pi * (lat_ids + 0.5) / LATS
    sine = jnp.sin(colatitude)[None, :]
    steps_up = jnp.arange(1, DEGREES + 1, dtype=jnp.float32)[None, :]
    factor = jnp.where(
        steps_up <= order_col, 0.5 * jnp.log((2.0 * steps_up + 1.0) / (2.0 * steps_up)), 0.0
    )
    log_start = 0.5 * jnp.log(1.0 / (4.0 * jnp.pi)) + jnp.sum(factor, axis=1, keepdims=True)
    diagonal = jnp.exp(log_start + order_col * jnp.log(sine))
    cosine = jnp.broadcast_to(jnp.cos(colatitude)[None, :], diagonal.shape)
    quadrature = 2.0 * jnp.pi * jnp.pi / LATS * sine
    orders = jnp.broadcast_to(order_col, diagonal.shape)
    vmem = pl.BlockSpec(memory_space=pltpu.VMEM)
    shape = jax.ShapeDtypeStruct((ord_dev, DEGREES, LATS), jnp.bfloat16)
    return pl.pallas_call(
        table_kernel,
        out_shape=(shape, shape),
        in_specs=[pl.BlockSpec(memory_space=pltpu.SMEM)] + [vmem] * 4,
        out_specs=(vmem, vmem),
        scratch_shapes=[
            pltpu.SMEM((DEGREES,), jnp.int32),
            pltpu.VMEM((halves, ord_dev * DEGREES, LANES), jnp.float32),
        ],
        name="legendre_tables",
    )(degree_of, diagonal, cosine, quadrature, orders)


def fourier_tables(lon_count, order_count):
    lon_ids = jnp.arange(lon_count, dtype=jnp.int32)[:, None]
    order_ids = jnp.arange(order_count, dtype=jnp.int32)[None, :]
    phase = 2.0 * jnp.pi * (lon_ids * order_ids % lon_count).astype(jnp.float32) / lon_count
    forward = (
        jnp.stack([jnp.cos(phase), -jnp.sin(phase)], axis=2).reshape(lon_count, 2 * order_count)
        / lon_count
    )
    doubled = jnp.where(order_ids == 0, 1.0, 2.0)
    inverse = jnp.stack([doubled * jnp.cos(phase), -doubled * jnp.sin(phase)], axis=2).reshape(
        lon_count, 2 * order_count
    )
    return (forward.astype(jnp.bfloat16), jnp.transpose(inverse).astype(jnp.bfloat16))


def to_orders(values):
    return lax.all_to_all(values, "lat", split_axis=1, concat_axis=0, tiled=True)


def to_degrees(values):
    return lax.all_to_all(values, "lat", split_axis=0, concat_axis=1, tiled=True)


def back_to_orders(values):
    return lax.all_to_all(values, "lat", split_axis=1, concat_axis=0, tiled=True)


def to_bands(values):
    return lax.all_to_all(values, "lat", split_axis=0, concat_axis=1, tiled=True)


def product(spec, left, right):
    return jnp.einsum(spec, left, right, preferred_element_type=jnp.float32)


def apply_filter(coeffs, weights):
    c_real = coeffs[:, :, 0]
    c_imag = coeffs[:, :, 1]
    w_real = weights[:, 0]
    w_imag = weights[:, 1]
    f_real = product("jmsc,jcd->jmsd", c_real, w_real) - product("jmsc,jcd->jmsd", c_imag, w_imag)
    f_imag = product("jmsc,jcd->jmsd", c_real, w_imag) + product("jmsc,jcd->jmsd", c_imag, w_real)
    return jnp.stack([f_real, f_imag], axis=2).astype(jnp.bfloat16)


def adjoint_filter(grads, weights):
    g_real = grads[:, :, 0]
    g_imag = grads[:, :, 1]
    w_real = weights[:, 0]
    w_imag = weights[:, 1]
    a_real = product("jmsd,jcd->jmsc", g_real, w_real) + product("jmsd,jcd->jmsc", g_imag, w_imag)
    a_imag = product("jmsd,jcd->jmsc", g_imag, w_real) - product("jmsd,jcd->jmsc", g_real, w_imag)
    return jnp.stack([a_real, a_imag], axis=2).astype(jnp.bfloat16)


def filter_grad(coeffs, grads):
    c_real = coeffs[:, :, 0]
    c_imag = coeffs[:, :, 1]
    g_real = grads[:, :, 0]
    g_imag = grads[:, :, 1]
    dw_real = product("jmsc,jmsd->jcd", c_real, g_real) + product("jmsc,jmsd->jcd", c_imag, g_imag)
    dw_imag = product("jmsc,jmsd->jcd", c_real, g_imag) - product("jmsc,jmsd->jcd", c_imag, g_real)
    return jnp.stack([dw_real, dw_imag], axis=1)


def constant_tables():
    sides = 2
    half = LATS // sides
    lat_ids = np.minimum(np.arange(LANES)[None, :], half - 1) + half * np.arange(sides)[:, None]
    colatitude = np.pi * (lat_ids + 0.5) / LATS
    sine = np.sin(colatitude)[:, None, :]
    ids = np.arange(ORDERS)
    steps_up = np.arange(1, ORDERS + 1)
    growth = np.cumsum(0.5 * np.log((2.0 * steps_up + 1.0) / (2.0 * steps_up)))
    log_start = 0.5 * np.log(1.0 / (4.0 * np.pi)) + np.concatenate([[0.0], growth[:-1]])
    diagonal = np.exp(log_start[None, :, None] + ids[None, :, None] * np.log(sine))
    cosine = np.broadcast_to(np.cos(colatitude)[:, None, :], (sides, GROUP, LANES))
    quadrature = np.broadcast_to(2.0 * np.pi * np.pi / LATS * sine, (sides, GROUP, LANES))
    phase = 2.0 * np.pi * (np.arange(LONS)[:, None] * ids[None, :] % LONS) / LONS
    forward = np.stack([np.cos(phase), -np.sin(phase)], axis=2).reshape(LONS, -1) / LONS
    doubled = np.where(ids == 0, 1.0, 2.0)[None, :]
    inverse = np.stack([doubled * np.cos(phase), -doubled * np.sin(phase)], axis=2)
    inverse = inverse.reshape(LONS, -1)
    floats = [jnp.asarray(t, jnp.float32) for t in (diagonal, cosine, quadrature)]
    waves = [forward.T, forward, inverse.T, inverse]
    halves = [jnp.asarray(np.float32(t).astype(jnp.bfloat16)) for t in waves]
    return floats, halves


def fill_tables(side, firsts, deg_ref, diag_ref, cos_ref, quad_ref, qtab, ptab, table, by_slot):
    kinds, orders, degrees, lats = qtab.shape
    every = kinds * orders
    cosine = cos_ref[side]
    diagonal, ids, squared, first_lead = [], [], [], []
    for first in firsts:
        diagonal.append(diag_ref[side, pl.ds(pl.multiple_of(first, orders), orders), :])
        ids.append(first + lax.broadcasted_iota(jnp.int32, cosine.shape, 0))
        real = ids[-1].astype(jnp.float32)
        squared.append(real * real)
        first_lead.append(jnp.sqrt(2.0 * real + 3.0))

    def advance(degree, carry):
        degree_real = degree.astype(jnp.float32)
        lower = degree_real - 1.0
        state = []
        for kind in range(kinds):
            previous, older = carry[kind]
            lead = jnp.sqrt(
                jnp.maximum(4.0 * degree_real * degree_real - 1.0, 0.0)
                / jnp.maximum(degree_real * degree_real - squared[kind], 1.0)
            )
            back = jnp.sqrt(
                jnp.maximum(lower * lower - squared[kind], 0.0)
                / jnp.maximum(4.0 * lower * lower - 1.0, 1.0)
            )
            general = lead * (cosine * previous - back * older)
            first = first_lead[kind] * cosine * previous
            value = jnp.where(
                ids[kind] == degree,
                diagonal[kind],
                jnp.where(
                    ids[kind] + 1 == degree,
                    first,
                    jnp.where(ids[kind] + 1 < degree, general, 0.0),
                ),
            )
            table[degree, kind * orders : (kind + 1) * orders, :] = value
            state.append((value, previous))
        return tuple(state)

    zeros = cosine * 0.0
    lax.fori_loop(0, degrees, advance, ((zeros, zeros),) * kinds, unroll=2)

    ahead = every // 2
    tail = degrees // 2

    def place(slot, carry):
        by_slot[pl.ds(slot, ahead, stride=degrees), :] = table[deg_ref[slot], :ahead]
        return carry

    lax.fori_loop(0, degrees, place, 0, unroll=4)

    def place_tail(row, carry):
        spots = pl.ds(ahead * degrees + row, ahead, stride=degrees)
        by_slot[spots, :] = table[tail + row, ahead:]
        return carry

    lax.fori_loop(0, tail, place_tail, 0, unroll=4)
    quadrature = quad_ref[side][:1, :lats]
    for kind in range(kinds):

        def keep(order, carry):
            start = pl.multiple_of((kind * orders + order) * degrees, degrees)
            depth = degrees if kind < kinds // 2 else tail
            chosen = by_slot[pl.ds(start, depth), :][:, :lats]
            ptab[kind, order, :depth] = chosen.astype(jnp.bfloat16)
            qtab[kind, order, :depth] = (chosen * quadrature).astype(jnp.bfloat16)
            return carry

        lax.fori_loop(0, orders, keep, 0)


def pair_swap(values, even_sign):
    rows = values.shape[0]
    even = lax.broadcasted_iota(jnp.int32, values.shape, 0) % 2 == 0
    above = pltpu.roll(values, rows - 1, 0)
    below = pltpu.roll(values, 1, 0)
    return jnp.where(even, even_sign * above, -even_sign * below)


def gelu_slope(x):
    scale = 0.7978845608028654
    square = x * x
    t = jnp.tanh(scale * (x + 0.044715 * x * square))
    return 0.5 * (1.0 + t) + 0.5 * x * (1.0 - t * t) * (scale * (1.0 + 0.134145 * square))


def dot(left, right, dims=((1,), (0,))):
    return lax.dot_general(left, right, (dims, ((), ())), preferred_element_type=jnp.float32)


def block_kernel(
    n, nb, fields, cotangent, weights, deg_ref, diag_ref, cos_ref, quad_ref,
    fwd_fk, fwd_kf, inv_fk, inv_kf,
    grad_out, dw,
    fbuf, wbuf, band_out, band_in, ord_in, ord_out, cross_out, cross_in, slot_out, slot_all,
    tail_out, co, go, mixed, wide_a, wide_b, wide_c, dw_in, qtab, ptab, table, row_ref, slot_of, by_name,
    load_sem, send_sem, recv_sem, dw_send, dw_recv,
):
    me = lax.axis_index("lat")
    me_b = lax.axis_index("batch")
    chunks, lat_dev = fbuf.shape[0], fbuf.shape[1]
    kinds, orders, degrees, side_lats = qtab.shape
    rows = 2 * orders
    slots = co.shape[1]
    quarter = n // kinds
    half = n // 2
    own = half * slots
    inner_kinds = ord_in.shape[0]
    pairs = kinds // 2
    jobs = kinds * chunks
    plane_rows = quarter * rows
    mesh_id = pl.DeviceIdType.MESH
    side = lax.div(me, half)
    place_in = lax.rem(me, half)
    column = lax.rem(me, quarter)
    inner = jnp.where(lax.div(me, quarter) == 1 + side, 1, 0)
    across = 1 - side

    def lanes(chunk):
        return pl.ds(chunk * LANES, LANES)

    def group(kind, at):
        return jnp.where(
            lax.rem(kind, 2) == 0, kind * quarter + at, (kind + 1) * quarter - 1 - at
        )

    def group_rows(kind, at):
        return pl.ds(pl.multiple_of(group(kind, at) * rows, rows), rows)

    def owner(kind, on_side, at):
        plane = jnp.where(kind < inner_kinds, 1 + on_side, (kinds - 1) * on_side)
        return plane * quarter + at

    def mine(kind):
        return jnp.where(kind < inner_kinds, 1, 0) == inner

    def job_of(job):
        per_pass = pairs * chunks
        inside = lax.rem(job, per_pass)
        kind = lax.div(job, per_pass) * pairs + lax.rem(inside, pairs)
        return kind, lax.div(inside, pairs), lax.rem(kind, inner_kinds)

    def first_block(kind):
        return group(kind, column) - own // orders

    def tail_blocks(kind, body):
        def one(block, carry):
            body(pl.multiple_of(block * orders, orders))
            return carry

        lax.fori_loop(first_block(kind), own // orders, one, 0)

    def await_tail(kind, view, sem):
        for first in range(own // orders):

            @pl.when(first_block(kind) == first)
            def _():
                await_bytes(view.at[pl.ds(0, own - first * orders)], sem)

    def job_at(kind, chunk):
        return (kind // pairs) * (pairs * chunks) + chunk * pairs + kind % pairs

    def load(chunk):
        return pltpu.make_async_copy(
            fields.at[0, :, :, lanes(chunk)], fbuf.at[chunk], load_sem.at[chunk]
        )

    def load_cot(chunk):
        return pltpu.make_async_copy(
            cotangent.at[0, :, :, lanes(chunk)],
            grad_out.at[0, :, :, lanes(chunk)],
            load_sem.at[chunks + chunk],
        )

    load_w = pltpu.make_async_copy(weights, wbuf, load_sem.at[2 * chunks])
    for chunk in range(chunks):
        load(chunk).start()
    load_w.start()
    for chunk in range(chunks):
        load_cot(chunk).start()

    barrier = pltpu.get_barrier_semaphore()

    def greet(step, carry):
        peer = lax.rem(me + step, n)
        pl.semaphore_signal(barrier, inc=1, device_id={"lat": peer}, device_id_type=mesh_id)
        return carry

    lax.fori_loop(1, n, greet, 0)
    for step in range(1, nb):
        peer = lax.rem(me_b + step, nb)
        pl.semaphore_signal(barrier, inc=1, device_id={"batch": peer}, device_id_type=mesh_id)

    def remote(stage, job, source, target, peer):
        pltpu.make_async_remote_copy(
            src_ref=source,
            dst_ref=target,
            send_sem=send_sem.at[stage, job],
            recv_sem=recv_sem.at[stage, job],
            device_id={"lat": peer},
            device_id_type=mesh_id,
        ).start()

    def await_bytes(view, sem):
        pltpu.make_async_copy(view, view, sem).wait()

    def to_owners(stage, kind, chunk, source, target, width):
        job = job_at(kind, chunk)
        for step in range(quarter):
            at = lax.rem(column + step, quarter)
            view = source.at[chunk, :, group_rows(kind, at), :]
            spot = target(kind % inner_kinds, chunk)
            peer = owner(kind, side, at)

            @pl.when(peer != me)
            def _():
                remote(stage, job, view, spot, peer)

            @pl.when(peer == me)
            def _():
                pltpu.make_async_copy(view, spot, recv_sem.at[stage, job]).start()

    def left_for_owners(stage, kind, chunk, source):
        job = job_at(kind, chunk)

        @pl.when(mine(kind))
        def _():
            await_bytes(source.at[chunk, :, 0 : plane_rows - rows, :], send_sem.at[stage, job])

        @pl.when(jnp.logical_not(mine(kind)))
        def _():
            await_bytes(source.at[chunk, :, 0:plane_rows, :], send_sem.at[stage, job])

    def from_owner(stage, job, kind, chunk, source, depth, target):
        place = lax.rem(kind, inner_kinds)
        spot = target.at[chunk, :, group_rows(kind, column), :]

        def send(step, carry):
            at = lax.rem(place_in + step, half)
            remote(
                stage, job, source.at[place, chunk, pl.ds(at * depth, depth)], spot,
                side * half + at,
            )
            return carry

        lax.fori_loop(1, half, send, 0)
        pltpu.make_async_copy(
            source.at[place, chunk, pl.ds(place_in * depth, depth)], spot, recv_sem.at[stage, job]
        ).start()

    def left_owner(stage, job, kind, chunk, source, depth):
        view = source.at[lax.rem(kind, inner_kinds), chunk, 0 : (half - 1) * depth]
        await_bytes(view, send_sem.at[stage, job])

    def reached_all(stage, kind, chunk, target):
        await_bytes(target.at[chunk, :, 0:plane_rows, :], recv_sem.at[stage, job_at(kind, chunk)])

    def lat_spot(place, chunk):
        return ord_in.at[place, chunk, pl.ds(place_in * lat_dev, lat_dev)]

    def slot_spot(place, chunk):
        return slot_all.at[place, chunk, pl.ds(me * slots, slots)]

    def wide_start(part, job):
        if part:
            spot = lax.rem(lax.div(job - pairs * chunks, pairs) + pairs, chunks)
        else:
            spot = jnp.where(job < 2 * pairs, lax.rem(job, pairs), job - pairs)
        return pl.multiple_of(spot * wide_a.shape[0], 8)

    def widen(source, place, chunk, depth, count):
        def one(block, carry):
            piece = source[place, chunk, pl.ds(block * depth, depth)].astype(jnp.float32)
            wide_a[pl.ds(pl.multiple_of(block * depth * rows, depth * rows), depth * rows), :] = (
                piece.reshape(depth * rows, LANES)
            )
            return carry

        lax.fori_loop(0, count // depth, one, 0)

    def apply_table(tab, kind, kept, result_ref, start, depth_in, depth_out, dims):
        def one(order, carry):
            real = wide_a[pl.ds(2 * order, depth_in, stride=rows), :]
            imag = wide_a[pl.ds(2 * order + 1, depth_in, stride=rows), :]
            both = jnp.concatenate([real, imag], axis=1).astype(jnp.bfloat16)
            result = dot(tab[kind, order, :kept], both, dims)
            result_ref[pl.ds(start + 2 * order, depth_out, stride=rows), :] = result[:, :LANES]
            result_ref[pl.ds(start + 2 * order + 1, depth_out, stride=rows), :] = result[:, LANES:]
            return carry

        lax.fori_loop(0, orders, one, 0, unroll=8)

    def narrow(source, target, place, chunk, start, depth, count):
        def one(block, carry):
            low = pl.multiple_of(start + block * depth * rows, 8)
            piece = source[pl.ds(low, depth * rows), :]
            target[place, chunk, pl.ds(block * depth, depth)] = piece.reshape(
                depth, rows, LANES
            ).astype(jnp.bfloat16)
            return carry

        lax.fori_loop(0, count // depth, one, 0)

    def wide_rows(start, index, depth):
        return pl.ds(pl.multiple_of(start + index * rows, 8), depth * rows)

    def blank(first, count):
        def one(block, carry):
            by_name[pl.ds((first + block) * orders, orders)] = jnp.zeros(
                (orders, rows, LANES), jnp.bfloat16
            )
            return carry

        lax.fori_loop(0, count, one, 0)

    def analyse(base, tab, part, job):
        kind, chunk, place = job_of(job)

        @pl.when(mine(kind))
        def _():
            await_bytes(ord_in.at[place, chunk], recv_sem.at[base, job])
            widen(ord_in, place, chunk, lat_dev, side_lats)
            start = wide_start(part, job)
            peer = owner(kind, across, column)
            source = cross_out.at[place, chunk]
            target = cross_in.at[place, chunk]
            kept = own if part else degrees
            apply_table(tab, kind, kept, wide_b, start, side_lats, kept, ((1,), (0,)))
            if not part:
                if base:
                    await_bytes(source, send_sem.at[1, job])
                narrow(wide_b, cross_out, place, chunk, start + across * own * rows, slots, own)
                remote(base + 1, job, source, target, peer)
                return
            if base:
                await_tail(kind, source, send_sem.at[1, job])

            def send(low):
                span = pl.ds(low, orders)
                piece = wide_b[wide_rows(start, low, orders), :]
                cross_out[place, chunk, span] = piece.reshape(orders, rows, LANES).astype(
                    jnp.bfloat16
                )
                remote(base + 1, job, source.at[span], target.at[span], peer)

            tail_blocks(kind, send)

    def settle(base, target, part, job):
        kind, chunk, place = job_of(job)

        @pl.when(mine(kind))
        def _():
            start = wide_start(part, job)
            if part:
                await_tail(kind, cross_in.at[place, chunk], recv_sem.at[base + 1, job])
            else:
                await_bytes(cross_in.at[place, chunk], recv_sem.at[base + 1, job])
            if base:
                left_owner(2, job, kind, chunk, slot_out, slots)
                if part:
                    await_tail(kind, tail_out.at[chunk], send_sem.at[4, job])
                else:
                    await_bytes(slot_all.at[place, chunk, 0:own], send_sem.at[4, job])
            if part:

                blank(0, own // orders + first_block(kind))

                def add(low):
                    piece = wide_b[wide_rows(start, low, orders), :]
                    other = cross_in[place, chunk, pl.ds(low, orders)].astype(jnp.float32)
                    by_name[pl.ds(own + low, orders)] = (
                        piece.reshape(orders, rows, LANES) + other
                    ).astype(jnp.bfloat16)

                tail_blocks(kind, add)

                def pick(slot, carry):
                    slot_out[place, chunk, slot] = by_name[deg_ref[side * own + slot]]
                    return carry

                lax.fori_loop(0, own, pick, 0, unroll=4)
            else:

                def one(block, carry):
                    low = block * slots
                    piece = wide_b[wide_rows(start + side * own * rows, low, slots), :]
                    other = cross_in[place, chunk, pl.ds(low, slots)].astype(jnp.float32)
                    slot_out[place, chunk, pl.ds(low, slots)] = (
                        piece.reshape(slots, rows, LANES) + other
                    ).astype(jnp.bfloat16)
                    return carry

                lax.fori_loop(0, half, one, 0)
            from_owner(base + 2, job, kind, chunk, slot_out, slots, target)

    def relay(base, part, job):
        kind, chunk, place = job_of(job)

        @pl.when(mine(kind))
        def _():
            await_bytes(slot_all.at[place, chunk, 0:own], recv_sem.at[base + 3, job])
            peer = owner(kind, across, column)
            view = slot_all.at[place, chunk, pl.ds(side * own, own)]
            if not part:
                remote(base + 4, job, view, view, peer)
                return

            blank(across * (own // orders), own // orders)

            def copy(block, carry):
                span = pl.ds(side * own + block * slots, slots)
                by_name[span] = slot_all[place, chunk, span]
                return carry

            lax.fori_loop(0, half, copy, 0)

            def send(low):
                for step in range(orders):
                    tail_out[chunk, low + step] = by_name[slot_of[0, own + low + step]]
                span = pl.ds(low, orders)
                remote(base + 4, job, tail_out.at[chunk, span], view.at[span], peer)

            tail_blocks(kind, send)

    def synthesise(base, tab, part, job):
        kind, chunk, place = job_of(job)

        @pl.when(mine(kind))
        def _():
            if part:
                await_tail(kind, tail_out.at[chunk], recv_sem.at[base + 4, job])

                def clear(block, carry):
                    wide_a[wide_rows(0, block * orders, orders), :] = jnp.zeros(
                        (orders * rows, LANES), jnp.float32
                    )
                    return carry

                lax.fori_loop(0, first_block(kind), clear, 0)

                def add(low):
                    near = tail_out[chunk, pl.ds(low, orders)].astype(jnp.float32)
                    far = slot_all[place, chunk, pl.ds(across * own + low, orders)]
                    wide_a[wide_rows(0, low, orders), :] = (
                        near + far.astype(jnp.float32)
                    ).reshape(orders * rows, LANES)

                tail_blocks(kind, add)
                apply_table(tab, kind, own, wide_c, 0, own, side_lats, ((0,), (0,)))
            else:
                await_bytes(slot_all.at[place, chunk, 0:own], recv_sem.at[base + 4, job])
                widen(slot_all, place, chunk, slots, degrees)
                apply_table(tab, kind, degrees, wide_c, 0, degrees, side_lats, ((0,), (0,)))
            if base:
                left_owner(5, job, kind, chunk, ord_out, lat_dev)
            narrow(wide_c, ord_out, place, chunk, 0, lat_dev, side_lats)
            from_owner(base + 5, job, kind, chunk, ord_out, lat_dev, band_in)

    def loop(low, high, body):
        def one(job, carry):
            body(job)
            return carry

        lax.fori_loop(low, high, one, 0)

    def pair(source, chunk, row):
        return jnp.concatenate([source[chunk, 2 * row], source[chunk, 2 * row + 1]], axis=1)

    def field_pair(chunk, row):
        span = slice(chunk * LANES, (chunk + 1) * LANES)
        return jnp.concatenate(
            [grad_out[0, 2 * row, :, span], grad_out[0, 2 * row + 1, :, span]], axis=1
        )

    def put_field_pair(chunk, row, values):
        span = slice(chunk * LANES, (chunk + 1) * LANES)
        values = values.astype(jnp.bfloat16)
        grad_out[0, 2 * row, :, span] = values[:, :LANES]
        grad_out[0, 2 * row + 1, :, span] = values[:, LANES:]

    def put_pair(target, chunk, row, values):
        values = values.astype(jnp.bfloat16)
        target[chunk, 2 * row] = values[:, :LANES]
        target[chunk, 2 * row + 1] = values[:, LANES:]

    def joined(source, slot, span):
        return jnp.concatenate([source[chunk, slot, span] for chunk in range(chunks)], axis=1)

    def mix(part, chunk):
        low = part * pairs * plane_rows
        span = slice(low, low + pairs * plane_rows)
        columns = slice(chunk * LANES, (chunk + 1) * LANES)

        def one(slot, carry):
            both = dot(
                joined(co, slot, span),
                jnp.concatenate([wbuf[slot, 0, :, columns], wbuf[slot, 1, :, columns]], axis=1),
            )
            crossed = pair_swap(both[:, LANES:], -1.0)
            mixed[chunk, slot, span] = (both[:, :LANES] + crossed).astype(jnp.bfloat16)
            return carry

        return one

    def adjoint(part, chunk):
        low = part * pairs * plane_rows
        span = slice(low, low + pairs * plane_rows)
        columns = slice(chunk * LANES, (chunk + 1) * LANES)

        def one(slot, carry):
            both = dot(
                joined(go, slot, span),
                jnp.concatenate([wbuf[slot, 0, columns, :], wbuf[slot, 1, columns, :]], axis=0),
                ((1,), (1,)),
            )
            crossed = pair_swap(both[:, LANES:], 1.0)
            mixed[chunk, slot, span] = (both[:, :LANES] + crossed).astype(jnp.bfloat16)
            return carry

        return one

    def filter_part(base, part, source, make):
        part_kinds = range(part * pairs, (part + 1) * pairs)
        for chunk in range(chunks):
            for kind in part_kinds:
                reached_all(base + 2, kind, chunk, source)
        for chunk in range(chunks):
            if base:
                for kind in part_kinds:
                    left_for_owners(3, kind, chunk, mixed)
            lax.fori_loop(0, slots, make(part, chunk), 0, unroll=4)
            for kind in part_kinds:
                to_owners(base + 3, kind, chunk, mixed, slot_spot, slots)

    per_pass = pairs * chunks
    def unit(part, chunk):
        first = part * per_pass + chunk * pairs
        return first, first + pairs

    def run(spans, body):
        loop(spans[0], spans[1], body)

    def to_filter_start(base, tab, source):
        run(unit(0, 0), lambda job: analyse(base, tab, 0, job))
        for low, high, part, behind in (
            (pairs, per_pass, 0, 0),
            (per_pass, per_pass + pairs, 1, 0),
            (per_pass + pairs, per_pass + 2 * pairs, 1, 1),
        ):

            def step(job):
                settle(base, source, behind, job - pairs)
                analyse(base, tab, part, job)

            loop(low, high, step)
        loop(per_pass + 2 * pairs, jobs, lambda job: analyse(base, tab, 1, job))

    def to_filter_by_chunk(base, tab, source, rest):
        run(unit(0, 0), lambda job: analyse(base, tab, 0, job))
        run(unit(1, 0), lambda job: analyse(base, tab, 1, job))
        rest()

        def second(job):
            settle(base, source, 0, job - pairs)
            analyse(base, tab, 0, job)

        run(unit(0, 1), second)
        run(unit(1, 0), lambda job: settle(base, source, 1, job))
        run(unit(0, 2), lambda job: analyse(base, tab, 0, job))

        for job in range(pairs, 2 * pairs):
            settle(base, source, 0, job)
            run(unit(1, job - pairs + 1), lambda spot: analyse(base, tab, 1, spot))
        run(unit(0, 2), lambda job: settle(base, source, 0, job))

    def through_filter(base, tab, source, make):
        filter_part(base, 0, source, make)
        run(unit(1, 1), lambda job: settle(base, source, 1, job))
        run(unit(0, 0), lambda job: relay(base, 0, job))
        run(unit(1, 2), lambda job: settle(base, source, 1, job))
        run(unit(0, 1), lambda job: relay(base, 0, job))
        run(unit(0, 0), lambda job: synthesise(base, tab, 0, job))
        loop(pairs, pairs + 1, lambda job: synthesise(base, tab, 0, job))
        filter_part(base, 1, source, make)
        loop(pairs + 1, 2 * pairs, lambda job: synthesise(base, tab, 0, job))
        run(unit(1, 0), lambda job: relay(base, 1, job))
        run(unit(0, 2), lambda job: relay(base, 0, job))
        run(unit(1, 1), lambda job: relay(base, 1, job))

    def spread(stage, chunk, part):
        for kind in range(part * pairs, (part + 1) * pairs):
            to_owners(stage, kind, chunk, band_out, lat_spot, lat_dev)

    def transform(chunk):
        load(chunk).wait()

        def fourier(row, carry):
            put_pair(band_out, chunk, row, dot(fwd_fk[...], pair(fbuf, chunk, row)))
            return carry

        lax.fori_loop(0, lat_dev // 2, fourier, 0, unroll=3)

    transform(0)
    pl.semaphore_wait(barrier, n - 1 + nb - 1)
    spread(0, 0, 0)
    transform(1)
    spread(0, 1, 0)
    fill_tables(
        side, [group(kind, column) * orders for kind in range(kinds)], deg_ref, diag_ref, cos_ref,
        quad_ref, qtab, ptab, table, wide_b,
    )
    for chunk in range(2, chunks):
        transform(chunk)
        spread(0, chunk, 0)
    for chunk in range(chunks):
        spread(0, chunk, 1)
    spots = lax.broadcasted_iota(jnp.int32, row_ref.shape, 1)

    def invert(slot, carry):
        return jnp.where(spots == deg_ref[slot], slot, carry)

    row_ref[...] = lax.fori_loop(0, degrees, invert, spots * 0, unroll=4)
    turn = pltpu.make_async_copy(row_ref, slot_of, load_sem.at[2 * chunks + 1])
    turn.start()
    turn.wait()
    load_w.wait()
    to_filter_start(0, qtab, co)
    through_filter(0, ptab, co, mix)

    def between(chunk):
        load_cot(chunk).wait()
        for kind in range(kinds):
            reached_all(5, kind, chunk, band_in)
            left_for_owners(0, kind, chunk, band_out)

        def middle(row, carry):
            response = dot(inv_kf[...], pair(band_in, chunk, row))
            upstream = field_pair(chunk, row).astype(jnp.float32) * gelu_slope(response)
            put_pair(band_out, chunk, row, dot(inv_fk[...], upstream.astype(jnp.bfloat16)))
            return carry

        lax.fori_loop(0, lat_dev // 2, middle, 0, unroll=3)
        spread(6, chunk, 0)
        if chunk == 0:
            spread(6, 0, 1)
        if chunk == chunks - 1:
            for earlier in range(1, chunks):
                spread(6, earlier, 1)

    def finish_synthesis(base, tab, finish):
        first, second = unit(0, 2)
        run(unit(1, 0), lambda job: synthesise(base, tab, 1, job))
        loop(first, first + 1, lambda job: synthesise(base, tab, 0, job))
        run(unit(1, 2), lambda job: relay(base, 1, job))
        if not base:
            finish(0)
        loop(first + 1, second, lambda job: synthesise(base, tab, 0, job))
        loop(per_pass + pairs, jobs, lambda job: synthesise(base, tab, 1, job))
        if base:
            finish(0)

    def rest(finish):
        for chunk in range(1, chunks):
            finish(chunk)

    finish_synthesis(0, ptab, between)
    to_filter_by_chunk(6, ptab, go, lambda: rest(between))
    through_filter(6, qtab, go, adjoint)

    def weight_grad(slot, carry):
        values = joined(co, slot, slice(None))
        grads = joined(go, slot, slice(None))
        turned = pair_swap(grads.astype(jnp.float32), 1.0).astype(jnp.bfloat16)
        span = ((0,), (0,))
        dw[slot, 0] = dot(values, grads, span).astype(jnp.bfloat16)
        dw[slot, 1] = dot(values, turned, span).astype(jnp.bfloat16)
        return carry

    lax.fori_loop(0, slots, weight_grad, 0)
    dw_copies = []
    for step in range(1, nb):
        peer = lax.rem(me_b + step, nb)
        copy = pltpu.make_async_remote_copy(
            src_ref=dw,
            dst_ref=dw_in.at[step - 1],
            send_sem=dw_send.at[step - 1],
            recv_sem=dw_recv.at[step - 1],
            device_id={"batch": peer},
            device_id_type=mesh_id,
        )
        copy.start()
        dw_copies.append(copy)

    def total(slot, carry):
        value = dw[slot].astype(jnp.float32)
        for step in range(nb - 1):
            value = value + dw_in[step, slot].astype(jnp.float32)
        dw[slot] = value.astype(jnp.bfloat16)
        return carry

    def last(chunk):
        if chunk == 0:
            for copy in dw_copies:
                copy.wait()
            lax.fori_loop(0, slots, total, 0)
        for kind in range(kinds):
            reached_all(11, kind, chunk, band_in)

        def finish(row, carry):
            delta = dot(fwd_kf[...], pair(band_in, chunk, row))
            put_field_pair(chunk, row, field_pair(chunk, row).astype(jnp.float32) + delta)
            return carry

        lax.fori_loop(0, lat_dev // 2, finish, 0, unroll=3)

    finish_synthesis(6, qtab, last)
    rest(last)
    for chunk in range(chunks):
        for kind in range(kinds):
            left_for_owners(6, kind, chunk, band_out)
            left_for_owners(9, kind, chunk, mixed)

    def drain(part, job):
        kind, chunk, place = job_of(job)

        @pl.when(mine(kind))
        def _():
            if part:
                await_tail(kind, cross_out.at[place, chunk], send_sem.at[7, job])
                await_tail(kind, tail_out.at[chunk], send_sem.at[10, job])
            else:
                await_bytes(cross_out.at[place, chunk], send_sem.at[7, job])
                await_bytes(slot_all.at[place, chunk, 0:own], send_sem.at[10, job])
            left_owner(8, job, kind, chunk, slot_out, slots)
            left_owner(11, job, kind, chunk, ord_out, lat_dev)

    loop(0, per_pass, lambda job: drain(0, job))
    loop(per_pass, jobs, lambda job: drain(1, job))


def local_kernel(fields, cotangent, weights, degree_of):
    n = lax.axis_size("lat")
    nb = lax.axis_size("batch")
    kinds = 4
    if fields.shape[0] != 1 or fields.shape[1] % 2 or n % kinds or ORDERS != n * GROUP:
        return local(fields, cotangent, weights, degree_of)
    lat_dev, lons, channels = fields.shape[1:]
    slots = weights.shape[0]
    rows = 2 * GROUP
    chunks = channels // LANES
    floats, waves = constant_tables()
    side_lats = LATS // 2
    held = kinds - 1
    vmem = pl.BlockSpec(memory_space=pltpu.VMEM)
    anywhere = pl.BlockSpec(memory_space=pl.ANY)

    def buffer(*dims):
        return pltpu.VMEM(dims, jnp.bfloat16)

    dma = pltpu.SemaphoreType.DMA
    others = max(nb - 1, 1)
    wide_rows = max(side_lats, DEGREES) * rows
    return pl.pallas_call(
        functools.partial(block_kernel, n, nb),
        out_shape=(
            pltpu.VMEM(fields.shape, jnp.bfloat16),
            pltpu.VMEM(weights.shape, jnp.bfloat16),
        ),
        in_specs=[anywhere] * 3 + [pl.BlockSpec(memory_space=pltpu.SMEM)] + [vmem] * 7,
        out_specs=(vmem, vmem),
        scratch_shapes=[
            buffer(chunks, lat_dev, lons, LANES),
            buffer(*weights.shape),
            buffer(chunks, lat_dev, n * rows, LANES),
            buffer(chunks, lat_dev, n * rows, LANES),
            buffer(held, chunks, side_lats, rows, LANES),
            buffer(held, chunks, side_lats, rows, LANES),
            buffer(held, chunks, DEGREES // 2, rows, LANES),
            buffer(held, chunks, DEGREES // 2, rows, LANES),
            buffer(held, chunks, DEGREES // 2, rows, LANES),
            buffer(held, chunks, DEGREES, rows, LANES),
            buffer(chunks, DEGREES // 2, rows, LANES),
            buffer(chunks, slots, n * rows, LANES),
            buffer(chunks, slots, n * rows, LANES),
            buffer(chunks, slots, n * rows, LANES),
            pltpu.VMEM((wide_rows, LANES), jnp.float32),
            pltpu.VMEM((4 * wide_rows, LANES), jnp.float32),
            pltpu.VMEM((side_lats * rows, LANES), jnp.float32),
            buffer(others, *weights.shape),
            buffer(kinds, GROUP, DEGREES, side_lats),
            buffer(kinds, GROUP, DEGREES, side_lats),
            pltpu.VMEM((DEGREES, kinds * GROUP, LANES), jnp.float32),
            pltpu.VMEM((GROUP, DEGREES), jnp.int32),
            pltpu.SMEM((GROUP, DEGREES), jnp.int32),
            buffer(DEGREES, rows, LANES),
            dma((2 * chunks + 2,)),
            dma((12, kinds * chunks)),
            dma((12, kinds * chunks)),
            dma((others,)),
            dma((others,)),
        ],
        compiler_params=pltpu.CompilerParams(
            collective_id=0, has_side_effects=True, vmem_limit_bytes=54 * 2**20
        ),
        name="filter_block",
    )(
        fields, cotangent, weights, degree_of, *floats, *waves,
    )


def local(fields, cotangent, weights, degree_of):
    samples = fields.shape[0]
    band_rows = fields.shape[1]
    ord_dev = ORDERS // lax.axis_size("lat")
    forward, inverse = fourier_tables(LONS, ORDERS)
    qslot, pslot = spectral_tables(lax.axis_index("lat") * ord_dev, ord_dev, degree_of)
    spectra = product("sikc,kf->ifsc", fields, forward).astype(jnp.bfloat16)
    spectra = spectra.reshape(band_rows, ORDERS, 2, samples, CHANNELS)
    gathered = to_orders(spectra)
    coeffs_local = product("mji,imrsc->jmrsc", qslot, gathered).astype(jnp.bfloat16)
    coeffs = to_degrees(coeffs_local)
    filtered = apply_filter(coeffs, weights)
    returned = back_to_orders(filtered)
    synth_local = product("mji,jmrsc->imrsc", pslot, returned).astype(jnp.bfloat16)
    synth = to_bands(synth_local)
    response = product(
        "ifsc,fk->sikc", synth.reshape(band_rows, 2 * ORDERS, samples, CHANNELS), inverse
    )
    activated, pullback = jax.vjp(jax.nn.gelu, response)
    upstream = pullback(cotangent.astype(jnp.float32))[0].astype(jnp.bfloat16)
    grad_synth = product("sikc,fk->ifsc", upstream, inverse).astype(jnp.bfloat16)
    grad_synth = grad_synth.reshape(band_rows, ORDERS, 2, samples, CHANNELS)
    grad_gathered = to_orders(grad_synth)
    grad_local = product("mji,imrsc->jmrsc", pslot, grad_gathered).astype(jnp.bfloat16)
    grad_filtered = to_degrees(grad_local)
    weight_total = lax.psum(filter_grad(coeffs, grad_filtered).astype(jnp.bfloat16), "batch")
    grad_coeffs = adjoint_filter(grad_filtered, weights)
    grad_back = back_to_orders(grad_coeffs)
    grad_local_spec = product("mji,jmrsc->imrsc", qslot, grad_back).astype(jnp.bfloat16)
    grad_bands = to_bands(grad_local_spec)
    delta = product(
        "ifsc,kf->sikc", grad_bands.reshape(band_rows, 2 * ORDERS, samples, CHANNELS), forward
    )
    grad_fields = (cotangent.astype(jnp.float32) + delta).astype(jnp.bfloat16)
    return (grad_fields, weight_total)


def solution(mesh):
    return jax.shard_map(
        local_kernel if CHANNELS % LANES == 0 else local,
        mesh=mesh,
        in_specs=(
            P("batch", "lat", None, None),
            P("batch", "lat", None, None),
            P("lat", None, None, None),
            P(),
        ),
        out_specs=(P("batch", "lat", None, None), P("lat", None, None, None)),
        check_vma=False,
    )
```

```python
import functools

import jax
import numpy as np
import jax.numpy as jnp
from jax import lax
from jax.experimental import pallas as pl
from jax.experimental.pallas import tpu as pltpu
from jax.sharding import PartitionSpec as P

LATS = 192
LONS = 384
ORDERS = 128
DEGREES = 128
CHANNELS = 384
LANES = 128
GROUP = 8


def table_kernel(deg_ref, diag_ref, cos_ref, quad_ref, order_ref, q_ref, p_ref, slot_ref, rows_ref):
    orders = diag_ref.shape[0]
    lats = q_ref.shape[2]
    degrees = deg_ref.shape[0]

    def invert(slot, carry):
        slot_ref[deg_ref[slot]] = slot
        return carry

    lax.fori_loop(0, degrees, invert, 0)
    order_real = order_ref[...]
    squared = order_real * order_real
    diagonal = diag_ref[...]
    cosine = cos_ref[...]
    first_lead = jnp.sqrt(2.0 * order_real + 3.0)
    halves = rows_ref.shape[0]

    def advance(degree, carry):
        previous, older = carry
        degree_real = degree.astype(jnp.float32)
        lead = jnp.sqrt(
            jnp.maximum(4.0 * degree_real * degree_real - 1.0, 0.0)
            / jnp.maximum(degree_real * degree_real - squared, 1.0)
        )
        lower = degree_real - 1.0
        back = jnp.sqrt(
            jnp.maximum(lower * lower - squared, 0.0) / jnp.maximum(4.0 * lower * lower - 1.0, 1.0)
        )
        general = lead * (cosine * previous - back * older)
        first = first_lead * cosine * previous
        value = jnp.where(
            degree_real == order_real,
            diagonal,
            jnp.where(
                degree_real == order_real + 1.0,
                first,
                jnp.where(degree_real > order_real + 1.0, general, 0.0),
            ),
        )
        slot = slot_ref[degree]
        for half in range(halves):
            rows_ref[half, pl.ds(slot, orders, stride=degrees), :] = value[
                :, half * LANES : (half + 1) * LANES
            ]
        return (value, previous)

    zeros = diagonal * 0.0
    lax.fori_loop(0, degrees, advance, (zeros, zeros), unroll=4)
    quadrature = quad_ref[...]
    for order in range(orders):
        for half in range(halves):
            low = half * LANES
            high = min(lats, low + LANES)
            chosen = rows_ref[half, order * degrees : (order + 1) * degrees, :][:, : high - low]
            p_ref[order, :, low:high] = chosen.astype(jnp.bfloat16)
            q_ref[order, :, low:high] = (chosen * quadrature[:, low:high]).astype(jnp.bfloat16)


def spectral_tables(start, ord_dev, degree_of):
    halves = -(-LATS // LANES)
    padded = halves * LANES
    order_col = (start + jnp.arange(ord_dev, dtype=jnp.int32)).astype(jnp.float32)[:, None]
    lat_ids = jnp.minimum(jnp.arange(padded, dtype=jnp.float32), LATS - 1.0)
    colatitude = jnp.pi * (lat_ids + 0.5) / LATS
    sine = jnp.sin(colatitude)[None, :]
    steps_up = jnp.arange(1, DEGREES + 1, dtype=jnp.float32)[None, :]
    factor = jnp.where(
        steps_up <= order_col, 0.5 * jnp.log((2.0 * steps_up + 1.0) / (2.0 * steps_up)), 0.0
    )
    log_start = 0.5 * jnp.log(1.0 / (4.0 * jnp.pi)) + jnp.sum(factor, axis=1, keepdims=True)
    diagonal = jnp.exp(log_start + order_col * jnp.log(sine))
    cosine = jnp.broadcast_to(jnp.cos(colatitude)[None, :], diagonal.shape)
    quadrature = 2.0 * jnp.pi * jnp.pi / LATS * sine
    orders = jnp.broadcast_to(order_col, diagonal.shape)
    vmem = pl.BlockSpec(memory_space=pltpu.VMEM)
    shape = jax.ShapeDtypeStruct((ord_dev, DEGREES, LATS), jnp.bfloat16)
    return pl.pallas_call(
        table_kernel,
        out_shape=(shape, shape),
        in_specs=[pl.BlockSpec(memory_space=pltpu.SMEM)] + [vmem] * 4,
        out_specs=(vmem, vmem),
        scratch_shapes=[
            pltpu.SMEM((DEGREES,), jnp.int32),
            pltpu.VMEM((halves, ord_dev * DEGREES, LANES), jnp.float32),
        ],
        name="legendre_tables",
    )(degree_of, diagonal, cosine, quadrature, orders)


def fourier_tables(lon_count, order_count):
    lon_ids = jnp.arange(lon_count, dtype=jnp.int32)[:, None]
    order_ids = jnp.arange(order_count, dtype=jnp.int32)[None, :]
    phase = 2.0 * jnp.pi * (lon_ids * order_ids % lon_count).astype(jnp.float32) / lon_count
    forward = (
        jnp.stack([jnp.cos(phase), -jnp.sin(phase)], axis=2).reshape(lon_count, 2 * order_count)
        / lon_count
    )
    doubled = jnp.where(order_ids == 0, 1.0, 2.0)
    inverse = jnp.stack([doubled * jnp.cos(phase), -doubled * jnp.sin(phase)], axis=2).reshape(
        lon_count, 2 * order_count
    )
    return (forward.astype(jnp.bfloat16), jnp.transpose(inverse).astype(jnp.bfloat16))


def to_orders(values):
    return lax.all_to_all(values, "lat", split_axis=1, concat_axis=0, tiled=True)


def to_degrees(values):
    return lax.all_to_all(values, "lat", split_axis=0, concat_axis=1, tiled=True)


def back_to_orders(values):
    return lax.all_to_all(values, "lat", split_axis=1, concat_axis=0, tiled=True)


def to_bands(values):
    return lax.all_to_all(values, "lat", split_axis=0, concat_axis=1, tiled=True)


def product(spec, left, right):
    return jnp.einsum(spec, left, right, preferred_element_type=jnp.float32)


def apply_filter(coeffs, weights):
    c_real = coeffs[:, :, 0]
    c_imag = coeffs[:, :, 1]
    w_real = weights[:, 0]
    w_imag = weights[:, 1]
    f_real = product("jmsc,jcd->jmsd", c_real, w_real) - product("jmsc,jcd->jmsd", c_imag, w_imag)
    f_imag = product("jmsc,jcd->jmsd", c_real, w_imag) + product("jmsc,jcd->jmsd", c_imag, w_real)
    return jnp.stack([f_real, f_imag], axis=2).astype(jnp.bfloat16)


def adjoint_filter(grads, weights):
    g_real = grads[:, :, 0]
    g_imag = grads[:, :, 1]
    w_real = weights[:, 0]
    w_imag = weights[:, 1]
    a_real = product("jmsd,jcd->jmsc", g_real, w_real) + product("jmsd,jcd->jmsc", g_imag, w_imag)
    a_imag = product("jmsd,jcd->jmsc", g_imag, w_real) - product("jmsd,jcd->jmsc", g_real, w_imag)
    return jnp.stack([a_real, a_imag], axis=2).astype(jnp.bfloat16)


def filter_grad(coeffs, grads):
    c_real = coeffs[:, :, 0]
    c_imag = coeffs[:, :, 1]
    g_real = grads[:, :, 0]
    g_imag = grads[:, :, 1]
    dw_real = product("jmsc,jmsd->jcd", c_real, g_real) + product("jmsc,jmsd->jcd", c_imag, g_imag)
    dw_imag = product("jmsc,jmsd->jcd", c_real, g_imag) - product("jmsc,jmsd->jcd", c_imag, g_real)
    return jnp.stack([dw_real, dw_imag], axis=1)


def constant_tables():
    sides = 2
    half = LATS // sides
    lat_ids = np.minimum(np.arange(LANES)[None, :], half - 1) + half * np.arange(sides)[:, None]
    colatitude = np.pi * (lat_ids + 0.5) / LATS
    sine = np.sin(colatitude)[:, None, :]
    ids = np.arange(ORDERS)
    steps_up = np.arange(1, ORDERS + 1)
    growth = np.cumsum(0.5 * np.log((2.0 * steps_up + 1.0) / (2.0 * steps_up)))
    log_start = 0.5 * np.log(1.0 / (4.0 * np.pi)) + np.concatenate([[0.0], growth[:-1]])
    diagonal = np.exp(log_start[None, :, None] + ids[None, :, None] * np.log(sine))
    cosine = np.broadcast_to(np.cos(colatitude)[:, None, :], (sides, GROUP, LANES))
    quadrature = np.broadcast_to(2.0 * np.pi * np.pi / LATS * sine, (sides, GROUP, LANES))
    phase = 2.0 * np.pi * (np.arange(LONS)[:, None] * ids[None, :] % LONS) / LONS
    forward = np.stack([np.cos(phase), -np.sin(phase)], axis=2).reshape(LONS, -1) / LONS
    doubled = np.where(ids == 0, 1.0, 2.0)[None, :]
    inverse = np.stack([doubled * np.cos(phase), -doubled * np.sin(phase)], axis=2)
    inverse = inverse.reshape(LONS, -1)
    floats = [jnp.asarray(t, jnp.float32) for t in (diagonal, cosine, quadrature)]
    waves = [forward.T, forward, inverse.T, inverse]
    halves = [jnp.asarray(np.float32(t).astype(jnp.bfloat16)) for t in waves]
    return floats, halves


def fill_tables(side, firsts, deg_ref, diag_ref, cos_ref, quad_ref, qtab, ptab, table, by_slot):
    kinds, orders, degrees, lats = qtab.shape
    every = kinds * orders
    cosine = cos_ref[side]
    diagonal, ids, squared, first_lead = [], [], [], []
    for first in firsts:
        diagonal.append(diag_ref[side, pl.ds(pl.multiple_of(first, orders), orders), :])
        ids.append(first + lax.broadcasted_iota(jnp.int32, cosine.shape, 0))
        real = ids[-1].astype(jnp.float32)
        squared.append(real * real)
        first_lead.append(jnp.sqrt(2.0 * real + 3.0))

    def advance(degree, carry):
        degree_real = degree.astype(jnp.float32)
        lower = degree_real - 1.0
        state = []
        for kind in range(kinds):
            previous, older = carry[kind]
            lead = jnp.sqrt(
                jnp.maximum(4.0 * degree_real * degree_real - 1.0, 0.0)
                / jnp.maximum(degree_real * degree_real - squared[kind], 1.0)
            )
            back = jnp.sqrt(
                jnp.maximum(lower * lower - squared[kind], 0.0)
                / jnp.maximum(4.0 * lower * lower - 1.0, 1.0)
            )
            general = lead * (cosine * previous - back * older)
            first = first_lead[kind] * cosine * previous
            value = jnp.where(
                ids[kind] == degree,
                diagonal[kind],
                jnp.where(
                    ids[kind] + 1 == degree,
                    first,
                    jnp.where(ids[kind] + 1 < degree, general, 0.0),
                ),
            )
            table[degree, kind * orders : (kind + 1) * orders, :] = value
            state.append((value, previous))
        return tuple(state)

    zeros = cosine * 0.0
    lax.fori_loop(0, degrees, advance, ((zeros, zeros),) * kinds, unroll=2)

    ahead = every // 2
    tail = degrees // 2

    def place(slot, carry):
        by_slot[pl.ds(slot, ahead, stride=degrees), :] = table[deg_ref[slot], :ahead]
        return carry

    lax.fori_loop(0, degrees, place, 0, unroll=4)

    def place_tail(row, carry):
        spots = pl.ds(ahead * degrees + row, ahead, stride=degrees)
        by_slot[spots, :] = table[tail + row, ahead:]
        return carry

    lax.fori_loop(0, tail, place_tail, 0, unroll=4)
    quadrature = quad_ref[side][:1, :lats]
    for kind in range(kinds):

        def keep(order, carry):
            start = pl.multiple_of((kind * orders + order) * degrees, degrees)
            depth = degrees if kind < kinds // 2 else tail
            chosen = by_slot[pl.ds(start, depth), :][:, :lats]
            ptab[kind, order, :depth] = chosen.astype(jnp.bfloat16)
            qtab[kind, order, :depth] = (chosen * quadrature).astype(jnp.bfloat16)
            return carry

        lax.fori_loop(0, orders, keep, 0)


def pair_swap(values, even_sign):
    rows = values.shape[0]
    even = lax.broadcasted_iota(jnp.int32, values.shape, 0) % 2 == 0
    above = pltpu.roll(values, rows - 1, 0)
    below = pltpu.roll(values, 1, 0)
    return jnp.where(even, even_sign * above, -even_sign * below)


def gelu_slope(x):
    scale = 0.7978845608028654
    square = x * x
    t = jnp.tanh(scale * (x + 0.044715 * x * square))
    return 0.5 * (1.0 + t) + 0.5 * x * (1.0 - t * t) * (scale * (1.0 + 0.134145 * square))


def dot(left, right, dims=((1,), (0,))):
    return lax.dot_general(left, right, (dims, ((), ())), preferred_element_type=jnp.float32)


def block_kernel(
    n, nb, fields, cotangent, weights, deg_ref, diag_ref, cos_ref, quad_ref,
    fwd_fk, fwd_kf, inv_fk, inv_kf,
    grad_out, dw,
    fbuf, wbuf, band_out, band_in, ord_in, ord_out, cross_out, cross_in, slot_out, slot_all,
    tail_out, co, go, mixed, wide_a, wide_b, wide_c, dw_in, qtab, ptab, table, row_ref, slot_of, by_name,
    load_sem, send_sem, recv_sem, dw_send, dw_recv,
):
    me = lax.axis_index("lat")
    me_b = lax.axis_index("batch")
    chunks, lat_dev = fbuf.shape[0], fbuf.shape[1]
    kinds, orders, degrees, side_lats = qtab.shape
    rows = 2 * orders
    slots = co.shape[1]
    quarter = n // kinds
    half = n // 2
    own = half * slots
    inner_kinds = ord_in.shape[0]
    pairs = kinds // 2
    jobs = kinds * chunks
    plane_rows = quarter * rows
    mesh_id = pl.DeviceIdType.MESH
    side = lax.div(me, half)
    place_in = lax.rem(me, half)
    column = lax.rem(me, quarter)
    inner = jnp.where(lax.div(me, quarter) == 1 + side, 1, 0)
    across = 1 - side

    def lanes(chunk):
        return pl.ds(chunk * LANES, LANES)

    def group(kind, at):
        return jnp.where(
            lax.rem(kind, 2) == 0, kind * quarter + at, (kind + 1) * quarter - 1 - at
        )

    def group_rows(kind, at):
        return pl.ds(pl.multiple_of(group(kind, at) * rows, rows), rows)

    def owner(kind, on_side, at):
        plane = jnp.where(kind < inner_kinds, 1 + on_side, (kinds - 1) * on_side)
        return plane * quarter + at

    def mine(kind):
        return jnp.where(kind < inner_kinds, 1, 0) == inner

    def job_of(job):
        per_pass = pairs * chunks
        inside = lax.rem(job, per_pass)
        kind = lax.div(job, per_pass) * pairs + lax.rem(inside, pairs)
        return kind, lax.div(inside, pairs), lax.rem(kind, inner_kinds)

    def first_block(kind):
        return group(kind, column) - own // orders

    def tail_blocks(kind, body):
        def one(block, carry):
            body(pl.multiple_of(block * orders, orders))
            return carry

        lax.fori_loop(first_block(kind), own // orders, one, 0)

    def await_tail(kind, view, sem):
        for first in range(own // orders):

            @pl.when(first_block(kind) == first)
            def _():
                await_bytes(view.at[pl.ds(0, own - first * orders)], sem)

    def job_at(kind, chunk):
        return (kind // pairs) * (pairs * chunks) + chunk * pairs + kind % pairs

    def load(chunk):
        return pltpu.make_async_copy(
            fields.at[0, :, :, lanes(chunk)], fbuf.at[chunk], load_sem.at[chunk]
        )

    def load_cot(chunk):
        return pltpu.make_async_copy(
            cotangent.at[0, :, :, lanes(chunk)],
            grad_out.at[0, :, :, lanes(chunk)],
            load_sem.at[chunks + chunk],
        )

    load_w = pltpu.make_async_copy(weights, wbuf, load_sem.at[2 * chunks])
    barrier = pltpu.get_barrier_semaphore()

    def greet(step, carry):
        peer = lax.rem(me + step, n)
        pl.semaphore_signal(barrier, inc=1, device_id={"lat": peer}, device_id_type=mesh_id)
        return carry

    lax.fori_loop(1, n, greet, 0)
    for step in range(1, nb):
        peer = lax.rem(me_b + step, nb)
        pl.semaphore_signal(barrier, inc=1, device_id={"batch": peer}, device_id_type=mesh_id)
    for chunk in range(chunks):
        load(chunk).start()
    load_w.start()
    for chunk in range(chunks):
        load_cot(chunk).start()

    def remote(stage, job, source, target, peer):
        pltpu.make_async_remote_copy(
            src_ref=source,
            dst_ref=target,
            send_sem=send_sem.at[stage, job],
            recv_sem=recv_sem.at[stage, job],
            device_id={"lat": peer},
            device_id_type=mesh_id,
        ).start()

    def await_bytes(view, sem):
        pltpu.make_async_copy(view, view, sem).wait()

    def to_owners(stage, kind, chunk, source, target, width):
        job = job_at(kind, chunk)
        for step in range(quarter):
            at = lax.rem(column + step, quarter)
            view = source.at[chunk, :, group_rows(kind, at), :]
            spot = target(kind % inner_kinds, chunk)
            peer = owner(kind, side, at)

            @pl.when(peer != me)
            def _():
                remote(stage, job, view, spot, peer)

            @pl.when(peer == me)
            def _():
                pltpu.make_async_copy(view, spot, recv_sem.at[stage, job]).start()

    def left_for_owners(stage, kind, chunk, source):
        job = job_at(kind, chunk)

        @pl.when(mine(kind))
        def _():
            await_bytes(source.at[chunk, :, 0 : plane_rows - rows, :], send_sem.at[stage, job])

        @pl.when(jnp.logical_not(mine(kind)))
        def _():
            await_bytes(source.at[chunk, :, 0:plane_rows, :], send_sem.at[stage, job])

    def from_owner(stage, job, kind, chunk, source, depth, target):
        place = lax.rem(kind, inner_kinds)
        spot = target.at[chunk, :, group_rows(kind, column), :]

        def send(step, carry):
            at = lax.rem(place_in + step, half)
            remote(
                stage, job, source.at[place, chunk, pl.ds(at * depth, depth)], spot,
                side * half + at,
            )
            return carry

        lax.fori_loop(1, half, send, 0)
        pltpu.make_async_copy(
            source.at[place, chunk, pl.ds(place_in * depth, depth)], spot, recv_sem.at[stage, job]
        ).start()

    def left_owner(stage, job, kind, chunk, source, depth):
        view = source.at[lax.rem(kind, inner_kinds), chunk, 0 : (half - 1) * depth]
        await_bytes(view, send_sem.at[stage, job])

    def reached_all(stage, kind, chunk, target):
        await_bytes(target.at[chunk, :, 0:plane_rows, :], recv_sem.at[stage, job_at(kind, chunk)])

    def lat_spot(place, chunk):
        return ord_in.at[place, chunk, pl.ds(place_in * lat_dev, lat_dev)]

    def slot_spot(place, chunk):
        return slot_all.at[place, chunk, pl.ds(me * slots, slots)]

    def wide_start(part, job):
        if part:
            spot = lax.rem(lax.div(job - pairs * chunks, pairs) + pairs, chunks)
        else:
            spot = jnp.where(job < 2 * pairs, lax.rem(job, pairs), job - pairs)
        return pl.multiple_of(spot * wide_a.shape[0], 8)

    def widen(source, place, chunk, depth, count):
        def one(block, carry):
            piece = source[place, chunk, pl.ds(block * depth, depth)].astype(jnp.float32)
            wide_a[pl.ds(pl.multiple_of(block * depth * rows, depth * rows), depth * rows), :] = (
                piece.reshape(depth * rows, LANES)
            )
            return carry

        lax.fori_loop(0, count // depth, one, 0)

    def apply_table(tab, kind, kept, result_ref, start, depth_in, depth_out, dims):
        def one(order, carry):
            real = wide_a[pl.ds(2 * order, depth_in, stride=rows), :]
            imag = wide_a[pl.ds(2 * order + 1, depth_in, stride=rows), :]
            both = jnp.concatenate([real, imag], axis=1).astype(jnp.bfloat16)
            result = dot(tab[kind, order, :kept], both, dims)
            result_ref[pl.ds(start + 2 * order, depth_out, stride=rows), :] = result[:, :LANES]
            result_ref[pl.ds(start + 2 * order + 1, depth_out, stride=rows), :] = result[:, LANES:]
            return carry

        lax.fori_loop(0, orders, one, 0, unroll=8)

    def narrow(source, target, place, chunk, start, depth, count):
        def one(block, carry):
            low = pl.multiple_of(start + block * depth * rows, 8)
            piece = source[pl.ds(low, depth * rows), :]
            target[place, chunk, pl.ds(block * depth, depth)] = piece.reshape(
                depth, rows, LANES
            ).astype(jnp.bfloat16)
            return carry

        lax.fori_loop(0, count // depth, one, 0)

    def wide_rows(start, index, depth):
        return pl.ds(pl.multiple_of(start + index * rows, 8), depth * rows)

    def blank(first, count):
        def one(block, carry):
            by_name[pl.ds((first + block) * orders, orders)] = jnp.zeros(
                (orders, rows, LANES), jnp.bfloat16
            )
            return carry

        lax.fori_loop(0, count, one, 0)

    def analyse(base, tab, part, job):
        kind, chunk, place = job_of(job)

        @pl.when(mine(kind))
        def _():
            await_bytes(ord_in.at[place, chunk], recv_sem.at[base, job])
            widen(ord_in, place, chunk, lat_dev, side_lats)
            start = wide_start(part, job)
            peer = owner(kind, across, column)
            source = cross_out.at[place, chunk]
            target = cross_in.at[place, chunk]
            kept = own if part else degrees
            apply_table(tab, kind, kept, wide_b, start, side_lats, kept, ((1,), (0,)))
            if not part:
                if base:
                    await_bytes(source, send_sem.at[1, job])
                narrow(wide_b, cross_out, place, chunk, start + across * own * rows, slots, own)
                remote(base + 1, job, source, target, peer)
                return
            if base:
                await_tail(kind, source, send_sem.at[1, job])

            def send(low):
                span = pl.ds(low, orders)
                piece = wide_b[wide_rows(start, low, orders), :]
                cross_out[place, chunk, span] = piece.reshape(orders, rows, LANES).astype(
                    jnp.bfloat16
                )
                remote(base + 1, job, source.at[span], target.at[span], peer)

            tail_blocks(kind, send)

    def settle(base, target, part, job):
        kind, chunk, place = job_of(job)

        @pl.when(mine(kind))
        def _():
            start = wide_start(part, job)
            if part:
                await_tail(kind, cross_in.at[place, chunk], recv_sem.at[base + 1, job])
            else:
                await_bytes(cross_in.at[place, chunk], recv_sem.at[base + 1, job])
            if base:
                left_owner(2, job, kind, chunk, slot_out, slots)
                if part:
                    await_tail(kind, tail_out.at[chunk], send_sem.at[4, job])
                else:
                    await_bytes(slot_all.at[place, chunk, 0:own], send_sem.at[4, job])
            if part:

                blank(0, own // orders + first_block(kind))

                def add(low):
                    piece = wide_b[wide_rows(start, low, orders), :]
                    other = cross_in[place, chunk, pl.ds(low, orders)].astype(jnp.float32)
                    by_name[pl.ds(own + low, orders)] = (
                        piece.reshape(orders, rows, LANES) + other
                    ).astype(jnp.bfloat16)

                tail_blocks(kind, add)

                def pick(slot, carry):
                    slot_out[place, chunk, slot] = by_name[deg_ref[side * own + slot]]
                    return carry

                lax.fori_loop(0, own, pick, 0, unroll=8)
            else:

                def one(block, carry):
                    low = block * slots
                    piece = wide_b[wide_rows(start + side * own * rows, low, slots), :]
                    other = cross_in[place, chunk, pl.ds(low, slots)].astype(jnp.float32)
                    slot_out[place, chunk, pl.ds(low, slots)] = (
                        piece.reshape(slots, rows, LANES) + other
                    ).astype(jnp.bfloat16)
                    return carry

                lax.fori_loop(0, half, one, 0)
            from_owner(base + 2, job, kind, chunk, slot_out, slots, target)

    def relay(base, part, job):
        kind, chunk, place = job_of(job)

        @pl.when(mine(kind))
        def _():
            await_bytes(slot_all.at[place, chunk, 0:own], recv_sem.at[base + 3, job])
            peer = owner(kind, across, column)
            view = slot_all.at[place, chunk, pl.ds(side * own, own)]
            if not part:
                remote(base + 4, job, view, view, peer)
                return

            blank(across * (own // orders), own // orders)

            def copy(block, carry):
                span = pl.ds(side * own + block * slots, slots)
                by_name[span] = slot_all[place, chunk, span]
                return carry

            lax.fori_loop(0, half, copy, 0)

            def send(low):
                for step in range(orders):
                    tail_out[chunk, low + step] = by_name[slot_of[0, own + low + step]]
                span = pl.ds(low, orders)
                remote(base + 4, job, tail_out.at[chunk, span], view.at[span], peer)

            tail_blocks(kind, send)

    def synthesise(base, tab, part, job):
        kind, chunk, place = job_of(job)

        @pl.when(mine(kind))
        def _():
            if part:
                await_tail(kind, tail_out.at[chunk], recv_sem.at[base + 4, job])

                def clear(block, carry):
                    wide_a[wide_rows(0, block * orders, orders), :] = jnp.zeros(
                        (orders * rows, LANES), jnp.float32
                    )
                    return carry

                lax.fori_loop(0, first_block(kind), clear, 0)

                def add(low):
                    near = tail_out[chunk, pl.ds(low, orders)].astype(jnp.float32)
                    far = slot_all[place, chunk, pl.ds(across * own + low, orders)]
                    wide_a[wide_rows(0, low, orders), :] = (
                        near + far.astype(jnp.float32)
                    ).reshape(orders * rows, LANES)

                tail_blocks(kind, add)
                apply_table(tab, kind, own, wide_c, 0, own, side_lats, ((0,), (0,)))
            else:
                await_bytes(slot_all.at[place, chunk, 0:own], recv_sem.at[base + 4, job])
                widen(slot_all, place, chunk, slots, degrees)
                apply_table(tab, kind, degrees, wide_c, 0, degrees, side_lats, ((0,), (0,)))
            if base:
                left_owner(5, job, kind, chunk, ord_out, lat_dev)
            narrow(wide_c, ord_out, place, chunk, 0, lat_dev, side_lats)
            from_owner(base + 5, job, kind, chunk, ord_out, lat_dev, band_in)

    def loop(low, high, body):
        def one(job, carry):
            body(job)
            return carry

        lax.fori_loop(low, high, one, 0)

    def pair(source, chunk, row):
        return jnp.concatenate([source[chunk, 2 * row], source[chunk, 2 * row + 1]], axis=1)

    def field_pair(chunk, row):
        span = slice(chunk * LANES, (chunk + 1) * LANES)
        return jnp.concatenate(
            [grad_out[0, 2 * row, :, span], grad_out[0, 2 * row + 1, :, span]], axis=1
        )

    def put_field_pair(chunk, row, values):
        span = slice(chunk * LANES, (chunk + 1) * LANES)
        values = values.astype(jnp.bfloat16)
        grad_out[0, 2 * row, :, span] = values[:, :LANES]
        grad_out[0, 2 * row + 1, :, span] = values[:, LANES:]

    def put_pair(target, chunk, row, values):
        values = values.astype(jnp.bfloat16)
        target[chunk, 2 * row] = values[:, :LANES]
        target[chunk, 2 * row + 1] = values[:, LANES:]

    def joined(source, slot, span):
        return jnp.concatenate([source[chunk, slot, span] for chunk in range(chunks)], axis=1)

    def mix(part, chunk):
        low = part * pairs * plane_rows
        span = slice(low, low + pairs * plane_rows)
        columns = slice(chunk * LANES, (chunk + 1) * LANES)

        def one(slot, carry):
            both = dot(
                joined(co, slot, span),
                jnp.concatenate([wbuf[slot, 0, :, columns], wbuf[slot, 1, :, columns]], axis=1),
            )
            crossed = pair_swap(both[:, LANES:], -1.0)
            mixed[chunk, slot, span] = (both[:, :LANES] + crossed).astype(jnp.bfloat16)
            return carry

        return one

    def adjoint(part, chunk):
        low = part * pairs * plane_rows
        span = slice(low, low + pairs * plane_rows)
        columns = slice(chunk * LANES, (chunk + 1) * LANES)

        def one(slot, carry):
            both = dot(
                joined(go, slot, span),
                jnp.concatenate([wbuf[slot, 0, columns, :], wbuf[slot, 1, columns, :]], axis=0),
                ((1,), (1,)),
            )
            crossed = pair_swap(both[:, LANES:], 1.0)
            mixed[chunk, slot, span] = (both[:, :LANES] + crossed).astype(jnp.bfloat16)
            return carry

        return one

    def filter_part(base, part, source, make):
        part_kinds = range(part * pairs, (part + 1) * pairs)
        for chunk in range(chunks):
            for kind in part_kinds:
                reached_all(base + 2, kind, chunk, source)
        for chunk in range(chunks):
            if base:
                for kind in part_kinds:
                    left_for_owners(3, kind, chunk, mixed)
            lax.fori_loop(0, slots, make(part, chunk), 0, unroll=4)
            for kind in part_kinds:
                to_owners(base + 3, kind, chunk, mixed, slot_spot, slots)

    per_pass = pairs * chunks
    def unit(part, chunk):
        first = part * per_pass + chunk * pairs
        return first, first + pairs

    def run(spans, body):
        loop(spans[0], spans[1], body)

    def to_filter_start(base, tab, source):
        run(unit(0, 0), lambda job: analyse(base, tab, 0, job))
        for low, high, part, behind in (
            (pairs, per_pass, 0, 0),
            (per_pass, per_pass + pairs, 1, 0),
            (per_pass + pairs, per_pass + 2 * pairs, 1, 1),
        ):

            def step(job):
                settle(base, source, behind, job - pairs)
                analyse(base, tab, part, job)

            loop(low, high, step)
        loop(per_pass + 2 * pairs, jobs, lambda job: analyse(base, tab, 1, job))

    def to_filter_by_chunk(base, tab, source, rest):
        run(unit(0, 0), lambda job: analyse(base, tab, 0, job))
        run(unit(1, 0), lambda job: analyse(base, tab, 1, job))
        rest()

        def second(job):
            settle(base, source, 0, job - pairs)
            analyse(base, tab, 0, job)

        run(unit(0, 1), second)
        run(unit(1, 0), lambda job: settle(base, source, 1, job))
        run(unit(0, 2), lambda job: analyse(base, tab, 0, job))

        for job in range(pairs, 2 * pairs):
            settle(base, source, 0, job)
            run(unit(1, job - pairs + 1), lambda spot: analyse(base, tab, 1, spot))
        run(unit(0, 2), lambda job: settle(base, source, 0, job))

    def through_filter(base, tab, source, make):
        filter_part(base, 0, source, make)
        run(unit(1, 1), lambda job: settle(base, source, 1, job))
        run(unit(0, 0), lambda job: relay(base, 0, job))
        run(unit(1, 2), lambda job: settle(base, source, 1, job))
        run(unit(0, 1), lambda job: relay(base, 0, job))
        run(unit(0, 0), lambda job: synthesise(base, tab, 0, job))
        loop(pairs, pairs + 1, lambda job: synthesise(base, tab, 0, job))
        filter_part(base, 1, source, make)
        loop(pairs + 1, 2 * pairs, lambda job: synthesise(base, tab, 0, job))
        run(unit(1, 0), lambda job: relay(base, 1, job))
        run(unit(0, 2), lambda job: relay(base, 0, job))
        run(unit(1, 1), lambda job: relay(base, 1, job))

    def spread(stage, chunk, part):
        for kind in range(part * pairs, (part + 1) * pairs):
            to_owners(stage, kind, chunk, band_out, lat_spot, lat_dev)

    def transform(chunk):
        load(chunk).wait()

        def fourier(row, carry):
            put_pair(band_out, chunk, row, dot(fwd_fk[...], pair(fbuf, chunk, row)))
            return carry

        lax.fori_loop(0, lat_dev // 2, fourier, 0, unroll=3)

    transform(0)
    pl.semaphore_wait(barrier, n - 1 + nb - 1)
    spread(0, 0, 0)
    transform(1)
    spread(0, 1, 0)
    fill_tables(
        side, [group(kind, column) * orders for kind in range(kinds)], deg_ref, diag_ref, cos_ref,
        quad_ref, qtab, ptab, table, wide_b,
    )
    for chunk in range(2, chunks):
        transform(chunk)
        spread(0, chunk, 0)
    for chunk in range(chunks):
        spread(0, chunk, 1)
    spots = lax.broadcasted_iota(jnp.int32, row_ref.shape, 1)

    def invert(slot, carry):
        return jnp.where(spots == deg_ref[slot], slot, carry)

    row_ref[...] = lax.fori_loop(0, degrees, invert, spots * 0, unroll=4)
    turn = pltpu.make_async_copy(row_ref, slot_of, load_sem.at[2 * chunks + 1])
    turn.start()
    turn.wait()
    load_w.wait()
    to_filter_start(0, qtab, co)
    through_filter(0, ptab, co, mix)

    def between(chunk):
        load_cot(chunk).wait()
        for kind in range(kinds):
            reached_all(5, kind, chunk, band_in)
            left_for_owners(0, kind, chunk, band_out)

        def middle(row, carry):
            response = dot(inv_kf[...], pair(band_in, chunk, row))
            upstream = field_pair(chunk, row).astype(jnp.float32) * gelu_slope(response)
            put_pair(band_out, chunk, row, dot(inv_fk[...], upstream.astype(jnp.bfloat16)))
            return carry

        lax.fori_loop(0, lat_dev // 2, middle, 0, unroll=3)
        spread(6, chunk, 0)
        if chunk == 0:
            spread(6, 0, 1)
        if chunk == chunks - 1:
            for earlier in range(1, chunks):
                spread(6, earlier, 1)

    def finish_synthesis(base, tab, finish):
        first, second = unit(0, 2)
        run(unit(1, 0), lambda job: synthesise(base, tab, 1, job))
        loop(first, first + 1, lambda job: synthesise(base, tab, 0, job))
        run(unit(1, 2), lambda job: relay(base, 1, job))
        if not base:
            finish(0)
        loop(first + 1, second, lambda job: synthesise(base, tab, 0, job))
        loop(per_pass + pairs, jobs, lambda job: synthesise(base, tab, 1, job))
        if base:
            finish(0)

    def rest(finish):
        for chunk in range(1, chunks):
            finish(chunk)

    finish_synthesis(0, ptab, between)
    to_filter_by_chunk(6, ptab, go, lambda: rest(between))
    through_filter(6, qtab, go, adjoint)

    def weight_grad(slot, carry):
        values = joined(co, slot, slice(None))
        grads = joined(go, slot, slice(None))
        turned = pair_swap(grads.astype(jnp.float32), 1.0).astype(jnp.bfloat16)
        span = ((0,), (0,))
        dw[slot, 0] = dot(values, grads, span).astype(jnp.bfloat16)
        dw[slot, 1] = dot(values, turned, span).astype(jnp.bfloat16)
        return carry

    lax.fori_loop(0, slots, weight_grad, 0)
    dw_copies = []
    for step in range(1, nb):
        peer = lax.rem(me_b + step, nb)
        copy = pltpu.make_async_remote_copy(
            src_ref=dw,
            dst_ref=dw_in.at[step - 1],
            send_sem=dw_send.at[step - 1],
            recv_sem=dw_recv.at[step - 1],
            device_id={"batch": peer},
            device_id_type=mesh_id,
        )
        copy.start()
        dw_copies.append(copy)

    def total(slot, carry):
        value = dw[slot].astype(jnp.float32)
        for step in range(nb - 1):
            value = value + dw_in[step, slot].astype(jnp.float32)
        dw[slot] = value.astype(jnp.bfloat16)
        return carry

    def last(chunk):
        if chunk == 0:
            for copy in dw_copies:
                copy.wait()
            lax.fori_loop(0, slots, total, 0)
        for kind in range(kinds):
            reached_all(11, kind, chunk, band_in)

        def finish(row, carry):
            delta = dot(fwd_kf[...], pair(band_in, chunk, row))
            put_field_pair(chunk, row, field_pair(chunk, row).astype(jnp.float32) + delta)
            return carry

        lax.fori_loop(0, lat_dev // 2, finish, 0, unroll=3)

    finish_synthesis(6, qtab, last)
    rest(last)
    for chunk in range(chunks):
        for kind in range(kinds):
            left_for_owners(6, kind, chunk, band_out)
            left_for_owners(9, kind, chunk, mixed)

    def drain(part, job):
        kind, chunk, place = job_of(job)

        @pl.when(mine(kind))
        def _():
            if part:
                await_tail(kind, cross_out.at[place, chunk], send_sem.at[7, job])
                await_tail(kind, tail_out.at[chunk], send_sem.at[10, job])
            else:
                await_bytes(cross_out.at[place, chunk], send_sem.at[7, job])
                await_bytes(slot_all.at[place, chunk, 0:own], send_sem.at[10, job])
            left_owner(8, job, kind, chunk, slot_out, slots)
            left_owner(11, job, kind, chunk, ord_out, lat_dev)

    loop(0, per_pass, lambda job: drain(0, job))
    loop(per_pass, jobs, lambda job: drain(1, job))


def local_kernel(fields, cotangent, weights, degree_of):
    n = lax.axis_size("lat")
    nb = lax.axis_size("batch")
    kinds = 4
    if fields.shape[0] != 1 or fields.shape[1] % 2 or n % kinds or ORDERS != n * GROUP:
        return local(fields, cotangent, weights, degree_of)
    lat_dev, lons, channels = fields.shape[1:]
    slots = weights.shape[0]
    rows = 2 * GROUP
    chunks = channels // LANES
    floats, waves = constant_tables()
    side_lats = LATS // 2
    held = kinds - 1
    vmem = pl.BlockSpec(memory_space=pltpu.VMEM)
    anywhere = pl.BlockSpec(memory_space=pl.ANY)

    def buffer(*dims):
        return pltpu.VMEM(dims, jnp.bfloat16)

    dma = pltpu.SemaphoreType.DMA
    others = max(nb - 1, 1)
    wide_rows = max(side_lats, DEGREES) * rows
    return pl.pallas_call(
        functools.partial(block_kernel, n, nb),
        out_shape=(
            pltpu.VMEM(fields.shape, jnp.bfloat16),
            pltpu.VMEM(weights.shape, jnp.bfloat16),
        ),
        in_specs=[anywhere] * 3 + [pl.BlockSpec(memory_space=pltpu.SMEM)] + [vmem] * 7,
        out_specs=(vmem, vmem),
        scratch_shapes=[
            buffer(chunks, lat_dev, lons, LANES),
            buffer(*weights.shape),
            buffer(chunks, lat_dev, n * rows, LANES),
            buffer(chunks, lat_dev, n * rows, LANES),
            buffer(held, chunks, side_lats, rows, LANES),
            buffer(held, chunks, side_lats, rows, LANES),
            buffer(held, chunks, DEGREES // 2, rows, LANES),
            buffer(held, chunks, DEGREES // 2, rows, LANES),
            buffer(held, chunks, DEGREES // 2, rows, LANES),
            buffer(held, chunks, DEGREES, rows, LANES),
            buffer(chunks, DEGREES // 2, rows, LANES),
            buffer(chunks, slots, n * rows, LANES),
            buffer(chunks, slots, n * rows, LANES),
            buffer(chunks, slots, n * rows, LANES),
            pltpu.VMEM((wide_rows, LANES), jnp.float32),
            pltpu.VMEM((4 * wide_rows, LANES), jnp.float32),
            pltpu.VMEM((side_lats * rows, LANES), jnp.float32),
            buffer(others, *weights.shape),
            buffer(kinds, GROUP, DEGREES, side_lats),
            buffer(kinds, GROUP, DEGREES, side_lats),
            pltpu.VMEM((DEGREES, kinds * GROUP, LANES), jnp.float32),
            pltpu.VMEM((GROUP, DEGREES), jnp.int32),
            pltpu.SMEM((GROUP, DEGREES), jnp.int32),
            buffer(DEGREES, rows, LANES),
            dma((2 * chunks + 2,)),
            dma((12, kinds * chunks)),
            dma((12, kinds * chunks)),
            dma((others,)),
            dma((others,)),
        ],
        compiler_params=pltpu.CompilerParams(
            collective_id=0, has_side_effects=True, vmem_limit_bytes=54 * 2**20
        ),
        name="filter_block",
    )(
        fields, cotangent, weights, degree_of, *floats, *waves,
    )


def local(fields, cotangent, weights, degree_of):
    samples = fields.shape[0]
    band_rows = fields.shape[1]
    ord_dev = ORDERS // lax.axis_size("lat")
    forward, inverse = fourier_tables(LONS, ORDERS)
    qslot, pslot = spectral_tables(lax.axis_index("lat") * ord_dev, ord_dev, degree_of)
    spectra = product("sikc,kf->ifsc", fields, forward).astype(jnp.bfloat16)
    spectra = spectra.reshape(band_rows, ORDERS, 2, samples, CHANNELS)
    gathered = to_orders(spectra)
    coeffs_local = product("mji,imrsc->jmrsc", qslot, gathered).astype(jnp.bfloat16)
    coeffs = to_degrees(coeffs_local)
    filtered = apply_filter(coeffs, weights)
    returned = back_to_orders(filtered)
    synth_local = product("mji,jmrsc->imrsc", pslot, returned).astype(jnp.bfloat16)
    synth = to_bands(synth_local)
    response = product(
        "ifsc,fk->sikc", synth.reshape(band_rows, 2 * ORDERS, samples, CHANNELS), inverse
    )
    activated, pullback = jax.vjp(jax.nn.gelu, response)
    upstream = pullback(cotangent.astype(jnp.float32))[0].astype(jnp.bfloat16)
    grad_synth = product("sikc,fk->ifsc", upstream, inverse).astype(jnp.bfloat16)
    grad_synth = grad_synth.reshape(band_rows, ORDERS, 2, samples, CHANNELS)
    grad_gathered = to_orders(grad_synth)
    grad_local = product("mji,imrsc->jmrsc", pslot, grad_gathered).astype(jnp.bfloat16)
    grad_filtered = to_degrees(grad_local)
    weight_total = lax.psum(filter_grad(coeffs, grad_filtered).astype(jnp.bfloat16), "batch")
    grad_coeffs = adjoint_filter(grad_filtered, weights)
    grad_back = back_to_orders(grad_coeffs)
    grad_local_spec = product("mji,jmrsc->imrsc", qslot, grad_back).astype(jnp.bfloat16)
    grad_bands = to_bands(grad_local_spec)
    delta = product(
        "ifsc,kf->sikc", grad_bands.reshape(band_rows, 2 * ORDERS, samples, CHANNELS), forward
    )
    grad_fields = (cotangent.astype(jnp.float32) + delta).astype(jnp.bfloat16)
    return (grad_fields, weight_total)


def solution(mesh):
    return jax.shard_map(
        local_kernel if CHANNELS % LANES == 0 else local,
        mesh=mesh,
        in_specs=(
            P("batch", "lat", None, None),
            P("batch", "lat", None, None),
            P("lat", None, None, None),
            P(),
        ),
        out_specs=(P("batch", "lat", None, None), P("lat", None, None, None)),
        check_vma=False,
    )
```
